32 devices in a mesh: seq: 16 (over z, y, x), head: 2 (over core).
Axes of the slice: x: 2, y: 2, z: 4, core: 2. Of those that a mesh axis runs over, the one named last changes fastest.
Arguments:
- hidden: bfloat16 [8192, 1536], P('seq'), may hold values from -6 to 6
- cotangent: bfloat16 [8192, 1536], P('seq'), may hold values from -6 to 6
- norm_gain: float32 [1536], replicated, may hold values from 0.5 to 1.5
- proj_inner: bfloat16 [1536, 2, 3072], P(None, None, 'head'), may hold values from -0.15625 to 0.15625
- proj_step: bfloat16 [1536, 48], P(None, 'head'), may hold values from -0.15625 to 0.15625
- proj_shared: bfloat16 [1536, 256], replicated, may hold values from -0.15625 to 0.15625
- conv_values: float32 [5, 3072], P(None, 'head'), may hold values from -0.8 to 0.8
- conv_shared: float32 [5, 256], replicated, may hold values from -0.8 to 0.8
- step_bias: float32 [48], P('head'), may hold values from -4 to -2
- decay_log: float32 [48], P('head'), may hold values from -12 to 0
- skip_gain: float32 [48], P('head'), may hold values from 0.1 to 1.9
- gate_gain: float32 [3072], P('head'), may hold values from 0.5 to 1.5
- proj_out: bfloat16 [1536, 3072], P(None, 'head'), may hold values from -0.109375 to 0.109375
Outputs:
- block_out: float32 [8192, 1536], P('seq')
- grad_hidden: float32 [8192, 1536], P('seq')
- grad_norm_gain: float32 [1536], replicated
- grad_proj_inner: float32 [1536, 2, 3072], P('seq', None, 'head')
- grad_proj_step: float32 [1536, 48], P('seq', 'head')
- grad_proj_shared: float32 [1536, 256], P('seq', 'head')
- grad_conv_values: float32 [5, 3072], P(None, 'head')
- grad_conv_shared: float32 [5, 256], P(None, 'head')
- grad_step_bias: float32 [48], P('head')
- grad_decay_log: float32 [48], P('head')
- grad_skip_gain: float32 [48], P('head')
- grad_gate_gain: float32 [3072], P('head')
- grad_proj_out: float32 [1536, 3072], P('seq', 'head')
The draws below stay inside these ranges and needn't reach their ends.
All inputs are finite; a program needn't handle non-finite values.
Results may differ from the reference program's by a relative error of at most 0.012.
The reference program's roundings to bfloat16 on the way (of `normed`, `values_in`, `shared_in`, `gated_w`, `grad_mixed` and `grad_inner`) count: a program that leaves them out, or rounds other values in their place, can miss the bound.
Values may be sent and summed in bfloat16 or wider, within the bound.
A program may use at most 192 MiB of HBM per device.

```python
import math
import jax
import jax.numpy as jnp
from jax import lax

DIM = 1536
HEADS = 48
HEAD_DIM = 64
STATE = 128
CONV = 4
GROUP = 256
INNER = 3072
TOKENS = 8192


def draw_decay_log(key, part):
    pick_key, amount_key = jax.random.split(jax.random.fold_in(key, 11))
    slow_heads = jax.random.uniform(pick_key, (HEADS,), jnp.float32) < 0.5
    spread = jax.random.uniform(amount_key, (HEADS,), jnp.float32, 0.0, 1.0)
    fast_rate = jnp.log(0.15) + spread * (jnp.log(0.6) - jnp.log(0.15))
    slow_rate = jnp.log(0.005) + spread * jnp.log(10.0)
    return jnp.where(slow_heads, slow_rate, fast_rate).astype(jnp.float32)


def strengthened(values, own_key, source, target, blocks, factor):
    owner, partner = [(jnp.arange(values.shape[position]) // (values.shape[position] // blocks)).reshape([-1 if axis == position else 1 for axis in range(values.ndim)]) for position in (source, target)]
    chosen = jax.random.permutation(own_key, blocks)[partner]
    strong = (owner == chosen) | (owner == (partner + blocks // 2) % blocks)
    return jnp.where(strong, factor * values, values)


def shard_levels(own_key, extent, pieces, least, high):
    gain, own = 1.0, jax.random.fold_in(own_key, 6)
    for dim, blocks in pieces:
        steps = jnp.exp(jax.random.uniform(jax.random.fold_in(own, dim), (blocks,), jnp.float32, least / len(pieces), high / len(pieces)))
        gain = gain * jnp.repeat(steps, extent[dim] // blocks).reshape([-1 if axis == dim else 1 for axis in range(len(extent))])
    return gain


def centred(key, dims, width, limit, shards=(), held_as=jnp.bfloat16):
    entries = width * jax.random.normal(key, dims, jnp.float32)
    if shards:
        entries = entries * shard_levels(key, dims, shards, -0.22, 0.18)
    return jnp.clip(entries, -limit, limit).astype(held_as)


def bell_draw_with(own_key, dims, width, most, pieces, heavy, kind=jnp.bfloat16):
    values = width * jax.random.normal(own_key, dims, jnp.float32)
    if pieces:
        values = values * shard_levels(own_key, dims, pieces, -0.22, 0.18)
    return jnp.clip(strengthened(values, jax.random.fold_in(own_key, 3), *heavy), -most, most).astype(kind)


def setup_inputs(seed: int = 0) -> dict:
    key_list = jax.random.split(jax.random.key(seed), 14)
    hidden = centred(key_list[0], (TOKENS, DIM), 1.0, 6.0, ((0, 16),))
    cotangent = bell_draw_with(key_list[1], (TOKENS, DIM), 1.0, 6.0, ((0, 16),), (0, 1, 16, 2.0))
    norm_gain = jnp.clip(1.0 + 0.1 * jax.random.normal(key_list[2], (DIM,), jnp.float32), 0.5, 1.5)
    proj_inner = centred(key_list[3], (DIM, 2, INNER), DIM ** -0.5, 0.15625, ((2, 2),))
    proj_step = centred(key_list[4], (DIM, HEADS), DIM ** -0.5, 0.15625, ((1, 2),))
    proj_shared = centred(key_list[5], (DIM, 2 * STATE), DIM ** -0.5, 0.15625)
    conv_values = jnp.clip(jax.random.uniform(key_list[6], (CONV + 1, INNER), jnp.float32, -0.8, 0.8) * shard_levels(key_list[6], (CONV + 1, INNER), ((1, 2),), -0.4, 0.0), -0.8, 0.8)
    conv_shared = jnp.clip(jax.random.uniform(key_list[7], (CONV + 1, 2 * STATE), jnp.float32, -0.8, 0.8), -0.8, 0.8)
    step_bias = jnp.clip(-4.0 + 2.0 * jax.random.uniform(key_list[8], (HEADS,), jnp.float32) ** shard_levels(key_list[8], (HEADS,), ((0, 2),), -0.2, 0.2), -4.0, -2.0)
    decay_log = draw_decay_log(jax.random.fold_in(key_list[13], 71), 0)
    skip_gain = jnp.clip(1.0 + 0.18 * jax.random.normal(key_list[10], (HEADS,), jnp.float32), 0.1, 1.9)
    gate_gain = jnp.clip(1.0 + 0.1 * jax.random.normal(key_list[11], (INNER,), jnp.float32), 0.5, 1.5)
    proj_out = centred(key_list[12], (DIM, INNER), INNER ** -0.5, 0.109375, ((1, 2),))
    return {"hidden": hidden, "cotangent": cotangent, "norm_gain": norm_gain, "proj_inner": proj_inner, "proj_step": proj_step, "proj_shared": proj_shared, "conv_values": conv_values, "conv_shared": conv_shared, "step_bias": step_bias, "decay_log": decay_log, "skip_gain": skip_gain, "gate_gain": gate_gain, "proj_out": proj_out}


norm_eps = 1e-05
highest = lax.Precision.HIGHEST

def silu_grad(values):
    sigmoid = jax.nn.sigmoid(values)
    return sigmoid * (1.0 + values * (1.0 - sigmoid))

def within_groups(rates):
    group_count = rates.shape[0] // GROUP
    lower_mask = (jnp.arange(GROUP)[:, None] >= jnp.arange(GROUP)[None, :]).astype(rates.dtype)
    return jnp.einsum('ij,cjh->cih', lower_mask, rates.reshape(group_count, GROUP, rates.shape[1]), precision=highest)

def ssd_parts(values_f, step_raw, input_map, output_map, step_bias, decay_log, skip_gain):
    token_count, head_count, head_width = values_f.shape
    group_count = token_count // GROUP
    step_size = jax.nn.softplus(step_raw + step_bias)
    rates = -step_size * jnp.exp(decay_log)
    running = within_groups(rates)
    values_c = values_f.reshape(group_count, GROUP, head_count, head_width)
    weighted = values_c * step_size.reshape(group_count, GROUP, head_count)[..., None]
    inputs_c = input_map.reshape(group_count, GROUP, -1)
    outputs_c = output_map.reshape(group_count, GROUP, -1)
    scores = jnp.einsum('cin,cjn->cij', outputs_c, inputs_c, precision=highest)
    lower_mask = jnp.arange(GROUP)[:, None] >= jnp.arange(GROUP)[None, :]
    causal_mask = lower_mask[None, :, :, None]
    log_gap = running[:, :, None, :] - running[:, None, :, :]
    decay_mat = jnp.where(causal_mask, jnp.exp(jnp.where(causal_mask, log_gap, 0.0)), 0.0)
    within_part = jnp.einsum('cijh,cjhp->cihp', scores[:, :, :, None] * decay_mat, weighted, precision=highest)
    group_total = running[:, -1, :]
    to_end = jnp.exp(group_total[:, None, :] - running)
    group_states = jnp.einsum('cjhp,cjn->chpn', weighted * to_end[..., None], inputs_c, precision=highest)

    def carry_step(carry_state, group_item):
        gain_log, group_state = group_item
        return (jnp.exp(gain_log)[:, None, None] * carry_state + group_state, carry_state)
    zero_state = jnp.zeros((head_count, head_width, input_map.shape[1]), jnp.float32)
    state_final, entering = lax.scan(carry_step, zero_state, (group_total, group_states))
    from_state = jnp.exp(running)[..., None] * jnp.einsum('cin,chpn->cihp', outputs_c, entering, precision=highest)
    local_part = (within_part + from_state).reshape(values_f.shape) + skip_gain[None, :, None] * values_f
    offsets = jnp.cumsum(group_total, axis=0) - group_total
    running_log = (running + offsets[:, None, :]).reshape(token_count, head_count)
    return (local_part, state_final, running_log, lax.optimization_barrier(jnp.sum(group_total, axis=0)))

def ssd_full(values_f, step_raw, input_map, output_map, step_bias, decay_log, skip_gain, state_in):
    local_part, state_final, running_log, decay_total = ssd_parts(values_f, step_raw, input_map, output_map, step_bias, decay_log, skip_gain)
    carried = jnp.exp(running_log)[:, :, None] * jnp.einsum('tn,hpn->thp', output_map, state_in, precision=highest)
    return (local_part + carried, jnp.exp(decay_total)[:, None, None] * state_in + state_final)

def causal_conv(padded, conv_taps):
    out_rows = padded.shape[0] - (CONV - 1)
    wide_ext = padded.astype(jnp.float32)
    result = conv_taps[CONV][None, :] + conv_taps[0][None, :] * wide_ext[0:out_rows]
    for offset in range(1, CONV):
        result = result + conv_taps[offset][None, :] * wide_ext[offset:offset + out_rows]
    return result

def conv_back(padded, conv_taps, conv_grad):
    out_rows = conv_grad.shape[0]
    wide_ext = padded.astype(jnp.float32)
    tap_rows = [lax.optimization_barrier(jnp.sum(wide_ext[offset:offset + out_rows] * conv_grad, axis=0)) for offset in range(CONV)]
    tap_rows.append(lax.optimization_barrier(jnp.sum(conv_grad, axis=0)))
    spread = jnp.pad(conv_taps[0][None, :] * conv_grad, ((0, CONV - 1), (0, 0)))
    for offset in range(1, CONV):
        spread = spread + jnp.pad(conv_taps[offset][None, :] * conv_grad, ((offset, CONV - 1 - offset), (0, 0)))
    return (spread, jnp.stack(tap_rows))

def front(hidden, norm_gain, proj_inner, proj_step, proj_shared):
    wide_hidden = hidden.astype(jnp.float32)
    norm_scale = lax.rsqrt(lax.optimization_barrier(jnp.mean(wide_hidden * wide_hidden, axis=1, keepdims=True)) + norm_eps)
    normed = (wide_hidden * norm_scale * norm_gain).astype(jnp.bfloat16)
    both_inner = jnp.dot(normed, proj_inner.reshape(proj_inner.shape[0], -1), preferred_element_type=jnp.float32)
    both_inner = both_inner.reshape(hidden.shape[0], 2, -1)
    gate_in = both_inner[:, 0]
    values_in = both_inner[:, 1].astype(jnp.bfloat16)
    step_raw = jnp.dot(normed, proj_step, preferred_element_type=jnp.float32)
    shared_in = jnp.dot(normed, proj_shared, preferred_element_type=jnp.float32).astype(jnp.bfloat16)
    return (wide_hidden, norm_scale, normed, gate_in, values_in, step_raw, shared_in)

def reference(hidden, cotangent, norm_gain, proj_inner, proj_step, proj_shared, conv_values, conv_shared, step_bias, decay_log, skip_gain, gate_gain, proj_out):
    block_rows = math.gcd(TOKENS, 4096)
    block_count = TOKENS // block_rows
    halo_rows = CONV - 1
    contract_cols = (((1,), (1,)), ((), ()))
    contract_rows = (((0,), (0,)), ((), ()))

    def forward_parts(hidden_rows, values_tail, shared_tail, state_in):
        wide_hidden, norm_scale, normed, gate_in, values_in, step_raw, shared_in = front(hidden_rows, norm_gain, proj_inner, proj_step, proj_shared)
        values_ext = jnp.concatenate([values_tail, values_in], axis=0)
        shared_ext = jnp.concatenate([shared_tail, shared_in], axis=0)
        values_conv = causal_conv(values_ext, conv_values)
        shared_conv = causal_conv(shared_ext, conv_shared)
        values_act = jax.nn.silu(values_conv).astype(jnp.bfloat16)
        shared_act = jax.nn.silu(shared_conv).astype(jnp.bfloat16)
        ssd_inputs = (values_act.astype(jnp.float32).reshape(block_rows, HEADS, HEAD_DIM), step_raw, shared_act[:, :STATE].astype(jnp.float32), shared_act[:, STATE:].astype(jnp.float32), step_bias, decay_log, skip_gain, state_in)
        output_y, state_out = ssd_full(*ssd_inputs)
        output_y = output_y.reshape(block_rows, INNER)
        gate_act = jax.nn.silu(gate_in)
        gated_out = output_y * gate_act
        inverse = lax.rsqrt(lax.optimization_barrier(jnp.mean(gated_out * gated_out, axis=1)) + norm_eps)
        gated_w = (gated_out * gate_gain).astype(jnp.bfloat16)
        mixed_sum = lax.dot_general(gated_w, proj_out, contract_cols, preferred_element_type=jnp.float32)
        block_out = wide_hidden + mixed_sum * inverse[:, None]
        return {'wide_hidden': wide_hidden, 'norm_scale': norm_scale, 'normed': normed, 'gate_in': gate_in, 'values_in': values_in, 'shared_in': shared_in, 'values_ext': values_ext, 'shared_ext': shared_ext, 'values_conv': values_conv, 'shared_conv': shared_conv, 'ssd_inputs': ssd_inputs, 'output_y': output_y, 'gate_act': gate_act, 'gated_out': gated_out, 'inverse': inverse, 'gated_w': gated_w, 'mixed_sum': mixed_sum, 'block_out': block_out, 'state_out': state_out}

    def forward_step(carry, hidden_rows):
        values_tail, shared_tail, state_in = carry
        parts = forward_parts(hidden_rows, values_tail, shared_tail, state_in)
        next_carry = (parts['values_in'][-halo_rows:], parts['shared_in'][-halo_rows:], parts['state_out'])
        return (next_carry, (parts['block_out'], values_tail, shared_tail, state_in))
    initial = (jnp.zeros((halo_rows, INNER), jnp.bfloat16), jnp.zeros((halo_rows, 2 * STATE), jnp.bfloat16), jnp.zeros((HEADS, HEAD_DIM, STATE), jnp.float32))
    hidden_blocks = hidden.reshape(block_count, block_rows, DIM)
    cot_blocks = cotangent.reshape(block_count, block_rows, DIM)
    _, (out_blocks, values_tails, shared_tails, states_in) = lax.scan(forward_step, initial, hidden_blocks)

    def backward_step(carry, item):
        grad_state, values_back, shared_back, sums = carry
        hidden_rows, cot_rows, values_tail, shared_tail, state_in = item
        parts = forward_parts(hidden_rows, values_tail, shared_tail, state_in)
        wide_cot = cot_rows.astype(jnp.float32)
        inverse = parts['inverse']
        gated_out = parts['gated_out']
        grad_mixed = (wide_cot * inverse[:, None]).astype(jnp.bfloat16)
        grad_inverse = lax.optimization_barrier(jnp.sum(wide_cot * parts['mixed_sum'], axis=1))
        grad_gated_w = jnp.dot(grad_mixed, proj_out, preferred_element_type=jnp.float32)
        term_out = lax.dot_general(grad_mixed, parts['gated_w'], contract_rows, preferred_element_type=jnp.float32)
        grad_gated = grad_gated_w * gate_gain - (grad_inverse * inverse ** 3 / INNER)[:, None] * gated_out
        term_gate = lax.optimization_barrier(jnp.sum(grad_gated_w * gated_out, axis=0))
        grad_y = grad_gated * parts['gate_act']
        grad_gate_in = grad_gated * parts['output_y'] * silu_grad(parts['gate_in'])
        _, pullback = jax.vjp(ssd_full, *parts['ssd_inputs'])
        grad_values_act, grad_step_raw, grad_bmat, grad_cmat, grad_step_bias, grad_decay, grad_skip, grad_state_in = pullback((grad_y.reshape(block_rows, HEADS, HEAD_DIM), grad_state))
        grad_values_conv = grad_values_act.reshape(block_rows, INNER) * silu_grad(parts['values_conv'])
        grad_shared_conv = jnp.concatenate([grad_bmat, grad_cmat], axis=1) * silu_grad(parts['shared_conv'])
        values_spread, term_conv_values = conv_back(parts['values_ext'], conv_values, grad_values_conv)
        shared_spread, term_conv_shared = conv_back(parts['shared_ext'], conv_shared, grad_shared_conv)
        grad_values_in = values_spread[halo_rows:] + jnp.pad(values_back, ((block_rows - halo_rows, 0), (0, 0)))
        grad_shared_in = shared_spread[halo_rows:] + jnp.pad(shared_back, ((block_rows - halo_rows, 0), (0, 0)))
        grad_inner = jnp.stack([grad_gate_in, grad_values_in], axis=1).astype(jnp.bfloat16).reshape(block_rows, 2 * INNER)
        grad_step_w = grad_step_raw.astype(jnp.bfloat16)
        grad_shared_w = grad_shared_in.astype(jnp.bfloat16)
        normed = parts['normed']
        grad_normed = lax.dot_general(grad_inner, proj_inner.reshape(DIM, -1), contract_cols, preferred_element_type=jnp.float32)
        grad_normed = grad_normed + lax.dot_general(grad_step_w, proj_step, contract_cols, preferred_element_type=jnp.float32)
        grad_normed = grad_normed + lax.dot_general(grad_shared_w, proj_shared, contract_cols, preferred_element_type=jnp.float32)
        term_inner = lax.dot_general(normed, grad_inner, contract_rows, preferred_element_type=jnp.float32).reshape(DIM, 2, INNER)
        term_step = lax.dot_general(normed, grad_step_w, contract_rows, preferred_element_type=jnp.float32)
        term_shared = lax.dot_general(normed, grad_shared_w, contract_rows, preferred_element_type=jnp.float32)
        normal_hat = parts['wide_hidden'] * parts['norm_scale']
        term_norm = lax.optimization_barrier(jnp.sum(grad_normed * normal_hat, axis=0))
        grad_hat = grad_normed * norm_gain
        grad_hidden = wide_cot + parts['norm_scale'] * (grad_hat - normal_hat * lax.optimization_barrier(jnp.mean(grad_hat * normal_hat, axis=1, keepdims=True)))
        terms = (term_norm, term_inner, term_step, term_shared, term_conv_values, term_conv_shared, grad_step_bias, grad_decay, grad_skip, term_gate, term_out)
        new_sums = jax.tree.map(jnp.add, sums, terms)
        return ((grad_state_in, values_spread[:halo_rows], shared_spread[:halo_rows], new_sums), grad_hidden)
    zero_sums = (jnp.zeros((DIM,), jnp.float32), jnp.zeros((DIM, 2, INNER), jnp.float32), jnp.zeros((DIM, HEADS), jnp.float32), jnp.zeros((DIM, 2 * STATE), jnp.float32), jnp.zeros((CONV + 1, INNER), jnp.float32), jnp.zeros((CONV + 1, 2 * STATE), jnp.float32), jnp.zeros((HEADS,), jnp.float32), jnp.zeros((HEADS,), jnp.float32), jnp.zeros((HEADS,), jnp.float32), jnp.zeros((INNER,), jnp.float32), jnp.zeros((DIM, INNER), jnp.float32))
    back_init = (jnp.zeros((HEADS, HEAD_DIM, STATE), jnp.float32), jnp.zeros((halo_rows, INNER), jnp.float32), jnp.zeros((halo_rows, 2 * STATE), jnp.float32), zero_sums)
    (_, _, _, sums), grad_blocks = lax.scan(backward_step, back_init, (hidden_blocks, cot_blocks, values_tails, shared_tails, states_in), reverse=True)
    return (out_blocks.reshape(TOKENS, DIM), grad_blocks.reshape(TOKENS, DIM), sums[0], sums[1], sums[2], sums[3], sums[4], sums[5], sums[6], sums[7], sums[8], sums[9], sums[10])
```

```python
import functools

import jax
import jax.numpy as jnp
from jax import lax
from jax.experimental import pallas as pl
from jax.experimental.pallas import tpu as pltpu
from jax.sharding import PartitionSpec as P

HEAD_DIM = 64
STATE = 128
CONV = 4
INNER = 3072
CHUNK = 128
LANES = 128
BLOCK = 256
HALO = 16
BLOCK_HEADS = BLOCK // HEAD_DIM

norm_eps = 1e-05
highest = lax.Precision.HIGHEST
f32 = jnp.float32
bf16 = jnp.bfloat16
NN = (((1,), (0,)), ((), ()))
NT = (((1,), (1,)), ((), ()))
TN = (((0,), (0,)), ((), ()))


def flip(shard, bit):
    size = lax.axis_size("seq")
    return lax.ppermute(shard, "seq", [(i, i ^ (1 << bit)) for i in range(size)])


def swap(shard):
    return lax.ppermute(shard, "head", [(0, 1), (1, 0)])


def from_behind(shard, by):
    size = lax.axis_size("seq")
    pairs = [(i, i + by) for i in range(size) if 0 <= i + by < size]
    return lax.ppermute(shard, "seq", pairs)


def silu_grad(values):
    sigmoid = 1.0 / (1.0 + jnp.exp(-values))
    return sigmoid * (1.0 + values * (1.0 - sigmoid))


def silu(values):
    return values / (1.0 + jnp.exp(-values))


def mm(a, b, dims=NN):
    return lax.dot_general(a, b, dims, preferred_element_type=f32)


def parts(a):
    high = a.astype(bf16)
    return high, (a - high.astype(f32)).astype(bf16)


def mm_left(a, b, dims=NN):
    high, low = parts(a)
    return mm(high, b, dims) + mm(low, b, dims)


def mm_right(a, b, dims=NN):
    high, low = parts(b)
    return mm(a, high, dims) + mm(a, low, dims)


def mm_both(a, b, dims=NN):
    a_high, a_low = parts(a)
    b_high, b_low = parts(b)
    return mm(a_high, b_high, dims) + mm(a_low, b_high, dims) + mm(a_high, b_low, dims)


def mm_exact(a, b, dims=NN):
    return lax.dot_general(a, b, dims, precision=highest, preferred_element_type=f32)


def widen(cols):
    rows = cols.shape[0]
    lane = lax.broadcasted_iota(jnp.int32, (rows, LANES), 1)
    pieces = []
    for pair in range(BLOCK // LANES):
        first = jnp.broadcast_to(cols[:, 2 * pair : 2 * pair + 1], (rows, LANES))
        second = jnp.broadcast_to(cols[:, 2 * pair + 1 : 2 * pair + 2], (rows, LANES))
        pieces.append(jnp.where(lane < HEAD_DIM, first, second))
    return jnp.concatenate(pieces, axis=1)


def rolled(full, step):
    shift = lax.rem(LANES - BLOCK_HEADS * step, LANES)
    return pltpu.roll(full, shift, 1)


def causal():
    rows = lax.broadcasted_iota(jnp.int32, (CHUNK, CHUNK), 0)
    cols = lax.broadcasted_iota(jnp.int32, (CHUNK, CHUNK), 1)
    return rows >= cols


def conv_rows(ext, taps, first, rows):
    out = taps[CONV : CONV + 1, :]
    for k in range(CONV):
        out = out + taps[k : k + 1, :] * ext[first + k : first + k + rows, :]
    return out


def stack_pair(block):
    lane = lax.broadcasted_iota(jnp.int32, block.shape, 1)
    low = jnp.where(lane < HEAD_DIM, block, jnp.zeros_like(block))
    return low, block - low


def front_kernel(
    hid_ref,
    halo_ref,
    gain_ref,
    wg_ref,
    wv_ref,
    wstep_ref,
    wshared_ref,
    cv_ref,
    cs_ref,
    bias_ref,
    decay_ref,
    skip_ref,
    normed_ref,
    scale_ref,
    gate_ref,
    vext_ref,
    yloc_ref,
    after_ref,
    step_ref,
    slope_ref,
    run_ref,
    runt_ref,
    stept_ref,
    sext_ref,
    bc_ref,
    nx,
    scores,
    bt,
    end_w,
    vwide,
):
    j = pl.program_id(0)
    tokens = hid_ref.shape[0]
    chunks = tokens // CHUNK

    @pl.when(j == 0)
    def _():
        def norm_rows(rows):
            wide = rows.astype(f32)
            scale = lax.rsqrt(jnp.mean(wide * wide, axis=1, keepdims=True) + norm_eps)
            return (wide * scale * gain_ref[...]).astype(bf16), scale

        nx[0:HALO, :] = norm_rows(halo_ref[...])[0]

        @pl.loop(0, tokens // 64)
        def _(i):
            start = pl.multiple_of(i * 64, 64)
            rows, scale = norm_rows(hid_ref[pl.ds(start, 64), :])
            nx[pl.ds(pl.multiple_of(HALO + start, HALO), 64), :] = rows
            normed_ref[pl.ds(start, 64), :] = rows
            scale_ref[pl.ds(start, 64), :] = jnp.broadcast_to(scale, (64, LANES))

        shared = mm(nx[...], wshared_ref[...]).astype(bf16)
        sext_ref[0] = shared[:, :STATE]
        sext_ref[1] = shared[:, STATE:]
        conv = conv_rows(shared.astype(f32), cs_ref[...], HALO - CONV + 1, tokens)
        act = silu(conv).astype(bf16)
        bc_ref[...] = act
        raw = mm(nx[HALO:, :], wstep_ref[...]) + bias_ref[...]
        small = jnp.exp(-jnp.abs(raw))
        step = jnp.maximum(raw, 0.0) + jnp.log1p(small)
        step_ref[...] = step
        slope_ref[...] = 1.0 / (1.0 + jnp.exp(-raw))
        rate = -step * jnp.exp(decay_ref[...])
        tri = causal().astype(f32)
        for c in range(chunks):
            rows = slice(c * CHUNK, (c + 1) * CHUNK)
            run = mm_exact(tri, rate[rows, :])
            run_ref[rows, :] = run
            run_t = run.T
            step_t = step[rows, :].T
            for b in range(runt_ref.shape[0]):
                heads = slice(BLOCK_HEADS * b, BLOCK_HEADS * (b + 1))
                runt_ref[b, 0:BLOCK_HEADS, rows] = run_t[heads, :]
                stept_ref[b, 0:BLOCK_HEADS, rows] = step_t[heads, :]
            end_w[rows, :] = step[rows, :] * jnp.exp(run[CHUNK - 1 :, :] - run)
            b_rows = act[rows, :STATE]
            c_rows = act[rows, STATE:]
            scores[c] = mm(c_rows, b_rows, NT)
            bt[:, rows] = b_rows.astype(f32).T.astype(bf16)

    gate_ref[...] = mm(nx[HALO:, :], wg_ref[0])
    values = mm(nx[...], wv_ref[0]).astype(bf16)
    vext_ref[...] = values
    vwide[...] = values.astype(f32)
    conv = conv_rows(vwide, cv_ref[...], HALO - CONV + 1, tokens)
    act = silu(conv).astype(bf16)
    run_cols = rolled(run_ref[...], j)
    end_cols = rolled(end_w[...], j)
    mask = causal()
    skip = widen(rolled(skip_ref[...], j)[:, :BLOCK_HEADS])
    state = jnp.zeros((STATE, BLOCK), f32)
    for c in range(chunks):
        rows = slice(c * CHUNK, (c + 1) * CHUNK)
        cols = run_cols[rows, :BLOCK_HEADS]
        x = act[rows, :]
        y_pairs = []
        for pair in range(BLOCK // LANES):
            mats = []
            for k in range(2):
                head = 2 * pair + k
                gap = cols[:, head : head + 1] - runt_ref[j, head : head + 1, rows]
                keep = jnp.exp(jnp.where(mask, gap, -1e30))
                mats.append(scores[c] * keep * stept_ref[j, head : head + 1, rows])
            low, high = stack_pair(x[:, pair * LANES : (pair + 1) * LANES])
            y_pairs.append(
                mm_left(jnp.concatenate(mats, axis=1), jnp.concatenate([low, high], axis=0))
            )
        wide_x = x.astype(f32)
        y = jnp.concatenate(y_pairs, axis=1) + skip * wide_x
        if c:
            y = y + widen(jnp.exp(cols)) * mm_right(bc_ref[rows, STATE:], state)
        yloc_ref[rows, :] = y
        weighted = wide_x * widen(end_cols[rows, :BLOCK_HEADS])
        last = widen(jnp.exp(cols[CHUNK - 1 :, :]))
        state = last * state + mm_right(bt[:, rows], weighted)
        after_ref[c] = state


def front_call(hid, halo, gain, both, wstep, wshared, conv_values, conv_shared, bias, decay, skip):
    tokens, width = hid.shape
    inner = both.shape[2]
    chunks = tokens // CHUNK
    full = lambda shape: pl.BlockSpec(shape, lambda j: (0,) * len(shape))
    block = lambda rows: pl.BlockSpec((rows, BLOCK), lambda j: (0, j))
    shapes = [
        ((tokens, width), bf16, full((tokens, width))),
        ((tokens, LANES), f32, full((tokens, LANES))),
        ((tokens, inner), f32, block(tokens)),
        ((HALO + tokens, inner), bf16, block(HALO + tokens)),
        ((tokens, inner), f32, block(tokens)),
        ((chunks, STATE, inner), f32, pl.BlockSpec((chunks, STATE, BLOCK), lambda j: (0, 0, j))),
        ((tokens, LANES), f32, full((tokens, LANES))),
        ((tokens, LANES), f32, full((tokens, LANES))),
        ((tokens, LANES), f32, full((tokens, LANES))),
        ((inner // BLOCK, 8, tokens), f32, full((inner // BLOCK, 8, tokens))),
        ((inner // BLOCK, 8, tokens), f32, full((inner // BLOCK, 8, tokens))),
        ((2, HALO + tokens, STATE), bf16, full((2, HALO + tokens, STATE))),
        ((tokens, 2 * STATE), bf16, full((tokens, 2 * STATE))),
    ]
    return pl.pallas_call(
        front_kernel,
        grid=(inner // BLOCK,),
        in_specs=[
            full((tokens, width)),
            full((HALO, width)),
            full((1, width)),
            pl.BlockSpec((1, width, BLOCK), lambda j: (0, 0, j)),
            pl.BlockSpec((1, width, BLOCK), lambda j: (1, 0, j)),
            full((width, LANES)),
            full((width, 2 * STATE)),
            block(CONV + 1),
            full((CONV + 1, 2 * STATE)),
            full((1, LANES)),
            full((1, LANES)),
            full((1, LANES)),
        ],
        out_shape=[jax.ShapeDtypeStruct(s, d) for s, d, _ in shapes],
        out_specs=[spec for _, _, spec in shapes],
        scratch_shapes=[
            pltpu.VMEM((HALO + tokens, width), bf16),
            pltpu.VMEM((chunks, CHUNK, CHUNK), f32),
            pltpu.VMEM((STATE, tokens), bf16),
            pltpu.VMEM((tokens, LANES), f32),
            pltpu.VMEM((HALO + tokens, BLOCK), f32),
        ],
        name="front",
    )(hid, halo, gain, both, both, wstep, wshared, conv_values, conv_shared, bias, decay, skip)


def offsets_of(run_ref, chunks):
    rows = [jnp.zeros((1, LANES), f32)]
    for c in range(chunks):
        rows.append(rows[-1] + run_ref[(c + 1) * CHUNK - 1 : (c + 1) * CHUNK, :])
    return rows


def mix_kernel(
    yloc_ref, gate_ref, in_ref, run_ref, bc_ref, gain_ref, wout_ref, y_ref, gw_ref, mix_ref, sq_ref
):
    j = pl.program_id(0)
    tokens = yloc_ref.shape[0]
    chunks = tokens // CHUNK
    offsets = offsets_of(run_ref, chunks)
    gated = []
    for c in range(chunks):
        rows = slice(c * CHUNK, (c + 1) * CHUNK)
        grow = rolled(jnp.exp(run_ref[rows, :] + offsets[c]), j)[:, :BLOCK_HEADS]
        y = yloc_ref[rows, :] + widen(grow) * mm_right(bc_ref[rows, STATE:], in_ref[...])
        y_ref[rows, :] = y
        out = y * silu(gate_ref[rows, :])
        gw_ref[rows, :] = (out * gain_ref[...]).astype(bf16)
        gated.append(jnp.broadcast_to(jnp.sum(out * out, axis=1, keepdims=True), (CHUNK, LANES)))
    part = mm(gw_ref[...], wout_ref[...], NT)
    squares = jnp.concatenate(gated, axis=0)

    @pl.when(j == 0)
    def _():
        mix_ref[...] = part
        sq_ref[...] = squares

    @pl.when(j > 0)
    def _():
        mix_ref[...] += part
        sq_ref[...] += squares


def mix_call(yloc, gate, state_in, run, bc, gain, wout):
    tokens, inner = yloc.shape
    width = wout.shape[0]
    full = lambda shape: pl.BlockSpec(shape, lambda j: (0,) * len(shape))
    block = lambda rows: pl.BlockSpec((rows, BLOCK), lambda j: (0, j))
    return pl.pallas_call(
        mix_kernel,
        grid=(inner // BLOCK,),
        in_specs=[
            block(tokens),
            block(tokens),
            block(STATE),
            full((tokens, LANES)),
            full((tokens, 2 * STATE)),
            block(1),
            block(width),
        ],
        out_shape=[
            jax.ShapeDtypeStruct((tokens, inner), f32),
            jax.ShapeDtypeStruct((tokens, inner), bf16),
            jax.ShapeDtypeStruct((tokens, width), f32),
            jax.ShapeDtypeStruct((tokens, LANES), f32),
        ],
        out_specs=[block(tokens), block(tokens), full((tokens, width)), full((tokens, LANES))],
        name="mix",
    )(yloc, gate, state_in, run, bc, gain, wout)


def gate_kernel(
    gm_ref, wout_ref, y_ref, gate_ref, gain_ref, coef_ref, run_ref, bc_ref,
    ggate_ref, dy_ref, term_ref, own_ref, ct,
):
    j = pl.program_id(0)
    tokens = y_ref.shape[0]
    chunks = tokens // CHUNK
    offsets = offsets_of(run_ref, chunks)

    @pl.when(j == 0)
    def _():
        for c in range(chunks):
            rows = slice(c * CHUNK, (c + 1) * CHUNK)
            ct[:, rows] = bc_ref[rows, STATE:].astype(f32).T.astype(bf16)

    own = jnp.zeros((STATE, BLOCK), f32)
    term = jnp.zeros((1, BLOCK), f32)
    for c in range(chunks):
        rows = slice(c * CHUNK, (c + 1) * CHUNK)
        ggw = mm(gm_ref[rows, :], wout_ref[...])
        y = y_ref[rows, :]
        gate = gate_ref[rows, :]
        sig = 1.0 / (1.0 + jnp.exp(-gate))
        act = gate * sig
        out = y * act
        term = term + jnp.sum(ggw * out, axis=0, keepdims=True)
        coef = jnp.concatenate([coef_ref[rows, :]] * (BLOCK // LANES), axis=1)
        gg = ggw * gain_ref[...] - coef * out
        dy = gg * act
        dy_ref[rows, :] = dy
        ggate_ref[0, rows, :] = (gg * y * (sig * (1.0 + gate * (1.0 - sig)))).astype(bf16)
        grow = rolled(jnp.exp(run_ref[rows, :] + offsets[c]), j)[:, :BLOCK_HEADS]
        own = own + mm_right(ct[:, rows], dy * widen(grow))
    own_ref[...] = own
    term_ref[...] = term


def gate_call(gm, wout, y, gate, gain, coef, run, bc):
    tokens, inner = y.shape
    width = wout.shape[0]
    full = lambda shape: pl.BlockSpec(shape, lambda j: (0,) * len(shape))
    block = lambda rows: pl.BlockSpec((rows, BLOCK), lambda j: (0, j))
    return pl.pallas_call(
        gate_kernel,
        grid=(inner // BLOCK,),
        in_specs=[
            full((tokens, width)),
            block(width),
            block(tokens),
            block(tokens),
            block(1),
            full((tokens, LANES)),
            full((tokens, LANES)),
            full((tokens, 2 * STATE)),
        ],
        out_shape=[
            jax.ShapeDtypeStruct((inner // BLOCK, tokens, BLOCK), bf16),
            jax.ShapeDtypeStruct((tokens, inner), f32),
            jax.ShapeDtypeStruct((1, inner), f32),
            jax.ShapeDtypeStruct((STATE, inner), f32),
        ],
        out_specs=[
            pl.BlockSpec((1, tokens, BLOCK), lambda j: (j, 0, 0)),
            block(tokens),
            block(1),
            block(STATE),
        ],
        scratch_shapes=[pltpu.VMEM((STATE, tokens), bf16)],
        name="gate_back",
    )(gm, wout, y, gate, gain, coef, run, bc)


def order_bits(part, bits):
    order = list(range(bits))
    if part == 1 and bits > 1:
        order[0], order[1] = 1, 0
    return order


def slot_of(owner, part, bits):
    slot = 0
    for bit in order_bits(part, bits):
        slot = slot * 2 + ((owner >> bit) & 1)
    return slot


class Reduction:
    def __init__(self, held, landing, out, part, bits, index, send_sems, recv_sems, cols):
        self.held, self.landing, self.out = held, landing, out
        self.part, self.bits, self.index = part, bits, index
        self.send_sems, self.recv_sems, self.cols = send_sems, recv_sems, cols

    def place(self, stage):
        base = 0
        size = 1 << self.bits
        for s, bit in enumerate(order_bits(self.part, self.bits)[: stage + 1]):
            mine = (self.index // (1 << bit)) % 2
            half = size >> (s + 1)
            keep, give = base + mine * half, base + (1 - mine) * half
            base = keep
        return keep, give, half, order_bits(self.part, self.bits)[stage]

    def copy(self, stage):
        _, give, half, bit = self.place(stage)
        mine = (self.index // (1 << bit)) % 2
        partner = self.index + (1 - 2 * mine) * (1 << bit)
        return pltpu.make_async_remote_copy(
            src_ref=self.held.at[pl.ds(give, half)],
            dst_ref=self.landing[stage],
            send_sem=self.send_sems.at[stage],
            recv_sem=self.recv_sems.at[stage],
            device_id={"seq": partner},
            device_id_type=pl.DeviceIdType.MESH,
        )

    def start(self, stage):
        self.copy(stage).start()

    def finish(self, stage):
        self.copy(stage).wait()
        keep, _, half, _ = self.place(stage)
        if stage == self.bits - 1:
            self.out[:, self.cols] = self.held[keep].astype(f32) + self.landing[stage][0].astype(f32)
        else:

            @pl.loop(0, half)
            def _(i):
                total = self.held[keep + i].astype(f32) + self.landing[stage][i].astype(f32)
                self.held[keep + i] = total.astype(bf16)

    def advance(self, stage):
        self.finish(stage)
        if stage + 1 < self.bits:
            self.start(stage + 1)


def exchange_sum(acc, landing, bit, index, send_sem, recv_sem):
    mine = (index // (1 << bit)) % 2
    partner = index + (1 - 2 * mine) * (1 << bit)
    copy = pltpu.make_async_remote_copy(
        src_ref=acc.at[bit],
        dst_ref=landing.at[bit],
        send_sem=send_sem.at[bit],
        recv_sem=recv_sem.at[bit],
        device_id={"seq": partner},
        device_id_type=pl.DeviceIdType.MESH,
    )
    copy.start()
    copy.wait()
    acc[bit + 1] = acc[bit] + landing[bit]


def back_kernel(
    bits,
    gmt_ref, normedt_ref, ggate_ref, run_ref, step_ref, slope_ref, bc_ref, sext_ref, skip_ref,
    decay_ref, cs_ref, wsmall_ref, gain_ref, tgate_ref,
    gw_ref, vext_ref, dy_ref, after_ref, in_ref, dstate_ref, cv_ref, runt_ref, stept_ref,
    wi_ref,
    hid_ref, cot_ref, scale_ref,
    gout_ref, ggw_ref, gvw_ref, gsmall_ref, ghid_ref, sums_ref, heads_ref,
    w_out, w_gate, w_values, w_small,
    land_out, land_gate, land_values, land_small,
    rs_send, rs_recv,
    gv, acc, acc_send, acc_land, acc_sems,
    edge_own, edge_tail, edge_land, edge_sems,
    dbc, dbc_land, dbc_sems, small, sedge_own, sedge_land, sedge_sems,
    vec, vec_land, vec_sems, norm_vec, norm_land, norm_sems, hvec, hvec_land, hvec_sems,
    scores, scorest, ct, dscores, end_w, ends, dcols, xdu, dyc, xdus, vwide, gext,
):
    step_id = pl.program_id(0)
    index = lax.axis_index("seq")
    core = lax.axis_index("head")
    size = 1 << bits
    tokens = dy_ref.shape[0]
    chunks = tokens // CHUNK
    nb = w_out.shape[0] * w_out.shape[3] // BLOCK
    half_nb = nb // 2
    width = normedt_ref.shape[0]
    rows_own = width // size
    part_cols = w_out.shape[3]
    t_out, t_gate, t_scan, t_values, t_grad, t_final = 0, nb, 2 * nb, 3 * nb, 4 * nb, 5 * nb
    after_id = lax.rem(index + 1, size)
    before_id = lax.rem(index + size - 1, size)

    def reduction(g, part):
        held, landing, out = (
            (w_out, land_out, gout_ref), (w_gate, land_gate, ggw_ref), (w_values, land_values, gvw_ref),
        )[g]
        land = [ref.at[part] for ref in landing]
        slot = 2 * g + part
        return Reduction(
            held.at[part], land, out, part, bits, index, rs_send.at[slot], rs_recv.at[slot],
            pl.ds(part * part_cols, part_cols),
        )

    rs = [[reduction(g, part) for part in range(2)] for g in range(3)]
    rs_small = Reduction(
        w_small, list(land_small), gsmall_ref, 1, bits, index, rs_send.at[6], rs_recv.at[6],
        pl.ds(0, w_small.shape[2]),
    )

    def when_after(step):
        return pl.when(step_id == step)

    def send_to(src, dst, send_sem, recv_sem, **where):
        return pltpu.make_async_remote_copy(
            src_ref=src, dst_ref=dst, send_sem=send_sem, recv_sem=recv_sem, device_id=where,
            device_id_type=pl.DeviceIdType.MESH,
        )

    @pl.when(step_id == 0)
    def _():
        barrier = pltpu.get_barrier_semaphore()
        for bit in range(bits):
            mine = (index // (1 << bit)) % 2
            pl.semaphore_signal(
                barrier, inc=1, device_id={"seq": index + (1 - 2 * mine) * (1 << bit)},
                device_id_type=pl.DeviceIdType.MESH,
            )
        for other in (after_id, before_id):
            pl.semaphore_signal(
                barrier, inc=1, device_id={"seq": other}, device_id_type=pl.DeviceIdType.MESH
            )
        pl.semaphore_signal(
            barrier, inc=1, device_id={"head": 1 - core}, device_id_type=pl.DeviceIdType.MESH
        )
        pl.semaphore_wait(barrier, bits + 3)

    def put_block(held, left, right, j):
        part = j // half_nb
        cols = pl.ds(pl.multiple_of((j % half_nb) * BLOCK, BLOCK), BLOCK)
        group = width // 4
        for q in range(4):
            piece = mm(left[q * group : (q + 1) * group, :], right).astype(bf16)
            for b in range(size // 4):
                owner = q * (size // 4) + b
                slots = [slot_of(owner, p, bits) for p in range(2)]
                slot = slots[0] + part * (slots[1] - slots[0])
                held[part, slot, :, cols] = piece[b * rows_own : (b + 1) * rows_own, :]

    @pl.when(step_id < t_gate)
    def _():
        put_block(w_out, gmt_ref, gw_ref[...], step_id)

    @pl.when((step_id >= t_gate) & (step_id < t_scan))
    def _():
        j = step_id - t_gate
        put_block(w_gate, normedt_ref, ggate_ref[j], j)

    @when_after(half_nb - 1)
    def _():
        rs[0][0].start(0)

    @when_after(t_gate - 1)
    def _():
        rs[0][1].start(0)

    @when_after(t_gate + half_nb - 1)
    def _():
        rs[1][0].start(0)

    @when_after(t_scan - 1)
    def _():
        rs[1][1].start(0)

    mask = causal()
    rows_i = lax.broadcasted_iota(jnp.int32, (CHUNK, CHUNK), 0)
    cols_i = lax.broadcasted_iota(jnp.int32, (CHUNK, CHUNK), 1)
    mask_t = rows_i <= cols_i

    @pl.when(step_id == t_scan)
    def _():
        dbc[...] = jnp.zeros_like(dbc)
        dscores[...] = jnp.zeros_like(dscores)
        dcols[...] = jnp.zeros_like(dcols)
        xdu[...] = jnp.zeros_like(xdu)
        dyc[...] = jnp.zeros_like(dyc)
        xdus[...] = jnp.zeros_like(xdus)
        ends[...] = jnp.zeros_like(ends)
        vec[...] = jnp.zeros_like(vec)
        for c in range(chunks):
            rows = slice(c * CHUNK, (c + 1) * CHUNK)
            b_rows = bc_ref[rows, :STATE]
            c_rows = bc_ref[rows, STATE:]
            scores[c] = mm(c_rows, b_rows, NT)
            scorest[c] = mm(b_rows, c_rows, NT)
            ct[:, rows] = c_rows.astype(f32).T.astype(bf16)
            run = run_ref[rows, :]
            end_w[rows, :] = jnp.exp(run[CHUNK - 1 :, :] - run)

    @pl.when((step_id >= t_scan) & (step_id < t_values))
    def _():
        j = step_id - t_scan
        offsets = offsets_of(run_ref, chunks)
        vwide[...] = vext_ref[...].astype(f32)
        conv = conv_rows(vwide, cv_ref[...], HALO - CONV + 1, tokens)
        sig_all = 1.0 / (1.0 + jnp.exp(-conv))
        act = (conv * sig_all).astype(bf16)
        slope = sig_all * (1.0 + conv * (1.0 - sig_all))
        run_cols = rolled(run_ref[...], j)
        step_cols = rolled(step_ref[...], j)
        end_cols = rolled(end_w[...], j)
        skip = widen(rolled(skip_ref[...], j)[:, :BLOCK_HEADS])
        channel = lax.broadcasted_iota(jnp.int32, (BLOCK, LANES), 0) // HEAD_DIM
        lane = lax.broadcasted_iota(jnp.int32, (BLOCK, LANES), 1)
        pick = (lane == BLOCK_HEADS * j + channel).astype(bf16)
        lane_row = lax.broadcasted_iota(jnp.int32, (CHUNK, LANES), 1)
        dstate = dstate_ref[...]
        dskip = jnp.zeros((1, BLOCK), f32)
        gext[tokens : tokens + 8, :] = jnp.zeros((8, BLOCK), f32)
        for c in reversed(range(chunks)):
            rows = slice(c * CHUNK, (c + 1) * CHUNK)
            cols = run_cols[rows, :BLOCK_HEADS]
            x = act[rows, :]
            wide_x = x.astype(f32)
            dy = dy_ref[rows, :]
            b_rows = bc_ref[rows, :STATE]
            c_rows = bc_ref[rows, STATE:]
            grow = widen(jnp.exp(cols))
            tail = widen(end_cols[rows, :BLOCK_HEADS])
            step_w = widen(step_cols[rows, :BLOCK_HEADS])
            last = grow[CHUNK - 1 :, :]
            base = rolled(jnp.exp(offsets[c]), j)[:, :BLOCK_HEADS]
            enter = widen(base) * in_ref[...]
            if c:
                enter = enter + after_ref[c - 1]
            du_state = tail * mm_right(b_rows, dstate)
            carried = grow * mm_right(c_rows, enter)
            weighted = wide_x * (tail * step_w)
            grown = dy * grow
            dbc[0, rows, :] += mm_both(weighted, dstate, NT)
            dbc[1, rows, :] += mm_both(grown, enter, NT)
            hold = last * jnp.sum(dstate * enter, axis=0, keepdims=True)
            ends[c : c + 1, :] += mm_exact(
                jnp.broadcast_to(hold, (8, BLOCK)), pick.astype(f32)
            )[:1, :]
            dstate = last * dstate + mm_right(ct[:, rows], grown)
            du_pairs = []
            col_sum = jnp.zeros((CHUNK, LANES), f32)
            for pair in range(BLOCK // LANES):
                lanes = slice(pair * LANES, (pair + 1) * LANES)
                low, high = stack_pair(dy[:, lanes])
                both = jnp.concatenate([low, high], axis=0)
                dmat = mm_left(both, x[:, lanes], NT)
                mats = []
                for k in range(2):
                    head = 2 * pair + k
                    col = cols[:, head : head + 1]
                    row = runt_ref[0, head : head + 1, rows]
                    keep = jnp.exp(jnp.where(mask, col - row, -1e30))
                    piece = dmat[k * CHUNK : (k + 1) * CHUNK, :] * keep
                    piece = piece * stept_ref[0, head : head + 1, rows]
                    dscores[c] += piece
                    full = piece * scores[c]
                    col_sum = jnp.where(
                        lane_row == BLOCK_HEADS * j + head,
                        jnp.sum(full, axis=1, keepdims=True),
                        col_sum,
                    )
                    dcols[j, head : head + 1, rows] = jnp.sum(full, axis=0, keepdims=True)
                    keep_t = jnp.exp(jnp.where(mask_t, row - col, -1e30))
                    mats.append(scorest[c] * keep_t)
                du_pairs.append(mm_both(jnp.concatenate(mats, axis=1), both))
            dyc[rows, :] += col_sum
            du = jnp.concatenate(du_pairs, axis=1) + du_state
            xdu[rows, :] += mm_left(wide_x * du, pick)
            dyc[rows, :] += mm_left(dy * carried, pick)
            xdus[rows, :] += mm_left(wide_x * du_state, pick)
            dskip = dskip + jnp.sum(dy * wide_x, axis=0, keepdims=True)
            gext[rows, :] = (step_w * du + skip * dy) * slope[rows, :]
        gconv = gext[0:tokens, :]
        for k in range(CONV):
            first = HALO - CONV + 1 + k
            vec[0, j, k : k + 1, :] = jnp.sum(
                vwide[first : first + tokens, :] * gconv, axis=0, keepdims=True
            )
        vec[0, j, CONV : CONV + 1, :] = jnp.sum(gconv, axis=0, keepdims=True)
        vec[0, j, CONV + 1 : CONV + 2, :] = tgate_ref[...]
        vec[0, j, CONV + 2 : CONV + 3, :] = dskip
        total = cv_ref[CONV - 1 : CONV, :] * gconv
        for k in range(CONV - 1):
            total = total + cv_ref[k : k + 1, :] * gext[CONV - 1 - k : CONV - 1 - k + tokens, :]
        gv[j] = total.astype(bf16)
        lacking = jnp.zeros((8, BLOCK), f32)
        edge_tail[j] = total[tokens - 8 :, :] + lacking
        edge_own[j] = gconv[0:8, :]
        send_to(
            edge_own.at[j], edge_land.at[j], edge_sems.at[0, j], edge_sems.at[1, j], seq=before_id
        ).start()

    @when_after(t_scan + half_nb)
    def _():
        rs[0][0].advance(0)
        rs[0][1].advance(0)

    @when_after(t_values - 1)
    def _():
        tri = mask.astype(f32)
        tri_t = mask_t.astype(f32)
        strict = (rows_i > cols_i).astype(f32)
        decay = jnp.exp(decay_ref[...])
        bias_sum = jnp.zeros((1, LANES), f32)
        decay_sum = jnp.zeros((1, LANES), f32)
        for c in range(chunks):
            rows = slice(c * CHUNK, (c + 1) * CHUNK)
            step = step_ref[rows, :]
            col_rows = [dcols[b, 0:BLOCK_HEADS, rows] for b in range(nb)]
            rest = LANES - BLOCK_HEADS * nb
            col_rows.append(jnp.zeros((rest, CHUNK), f32))
            dlog = dyc[rows, :] - jnp.concatenate(col_rows, axis=0).T
            drate = (
                mm_exact(tri_t, dlog)
                + mm_exact(strict, xdus[rows, :] * step)
                + ends[c : c + 1, :]
            )
            dstep = xdu[rows, :] - decay * drate
            draw = dstep * slope_ref[rows, :]
            small[rows, LANES:] = draw.astype(bf16)
            bias_sum = bias_sum + jnp.sum(draw, axis=0, keepdims=True)
            decay_sum = decay_sum - jnp.sum(drate * step, axis=0, keepdims=True) * decay
            b_rows = bc_ref[rows, :STATE]
            c_rows = bc_ref[rows, STATE:]
            high, low = parts(dscores[c])
            dbc[1, rows, :] += mm(high, b_rows) + mm(low, b_rows)
            dbc[0, rows, :] += mm(high, c_rows, TN) + mm(low, c_rows, TN)
        hvec[0] = jnp.zeros_like(hvec[0])
        hvec[0, 0:1, :] = bias_sum
        hvec[0, 1:2, :] = decay_sum
        send_to(
            dbc.at[1 - core], dbc_land, dbc_sems.at[0], dbc_sems.at[1], head=1 - core
        ).start()

    @pl.when((step_id >= t_values) & (step_id < t_grad))
    def _():
        j = step_id - t_values
        send_to(
            edge_own.at[j], edge_land.at[j], edge_sems.at[0, j], edge_sems.at[1, j], seq=before_id
        ).wait()
        cv = cv_ref[...]
        nxt = jnp.where(index == size - 1, 0.0, 1.0) * edge_land[j]
        row8 = lax.broadcasted_iota(jnp.int32, (8, BLOCK), 0)
        fix = edge_tail[j]
        for k in range(CONV - 1):
            ahead = CONV - 1 - k
            moved = pltpu.roll(nxt, 8 - ahead, 0)
            fix = fix + jnp.where(row8 >= 8 - ahead, cv[k : k + 1, :] * moved, 0.0)
        both_rows = jnp.concatenate([gv[j, tokens - 16 : tokens - 8, :].astype(f32), fix], axis=0)
        gv[j, tokens - 16 :, :] = both_rows.astype(bf16)
        put_block(w_values, normedt_ref, gv[j], j)

    @when_after(t_values + half_nb - 1)
    def _():
        rs[2][0].start(0)

    @when_after(t_values)
    def _():
        send_to(
            dbc.at[1 - core], dbc_land, dbc_sems.at[0], dbc_sems.at[1], head=1 - core
        ).wait()
        sext = sext_ref[core].astype(f32)
        taps = cs_ref[core]
        conv = conv_rows(sext, taps, HALO - CONV + 1, tokens)
        gs = (dbc[core] + dbc_land[...]) * silu_grad(conv)
        for k in range(CONV):
            first = HALO - CONV + 1 + k
            hvec[0, 2 + k : 3 + k, :] = jnp.sum(
                sext[first : first + tokens, :] * gs, axis=0, keepdims=True
            )
        hvec[0, 2 + CONV : 3 + CONV, :] = jnp.sum(gs, axis=0, keepdims=True)
        dbc[core] = gs
        sedge_own[...] = gs[0:8, :]
        send_to(
            sedge_own, sedge_land, sedge_sems.at[0], sedge_sems.at[1], seq=before_id
        ).start()

    @when_after(t_grad - 1)
    def _():
        rs[2][1].start(0)
        send_to(
            sedge_own, sedge_land, sedge_sems.at[0], sedge_sems.at[1], seq=before_id
        ).wait()
        taps = cs_ref[core]
        nxt = jnp.where(index == size - 1, 0.0, 1.0) * sedge_land[...]
        gs = jnp.concatenate([dbc[core], nxt], axis=0)
        total = taps[CONV - 1 : CONV, :] * gs[0:tokens, :]
        for k in range(CONV - 1):
            total = total + taps[k : k + 1, :] * gs[CONV - 1 - k : CONV - 1 - k + tokens, :]
        small[:, 0:LANES] = total.astype(bf16)
        group = width // 4
        for q in range(4):
            piece = mm(normedt_ref[q * group : (q + 1) * group, :], small[...]).astype(bf16)
            for b in range(size // 4):
                slot = slot_of(q * (size // 4) + b, 1, bits)
                w_small[slot] = piece[b * rows_own : (b + 1) * rows_own, :]
        rs_small.start(0)

    @pl.when((step_id >= t_grad) & (step_id < t_final))
    def _():
        j = step_id - t_grad
        part = mm(ggate_ref[j], wi_ref[0], NT) + mm(gv[j], wi_ref[1], NT)

        @pl.when(j == 0)
        def _():
            acc[...] = part + mm(small[...], wsmall_ref[...], NT)

        @pl.when(j > 0)
        def _():
            acc[...] += part

    @when_after(t_grad + half_nb)
    def _():
        rs[1][0].advance(0)
        rs[1][1].advance(0)

    @when_after(t_final - 1)
    def _():
        for c in range(chunks):
            rows = slice(c * CHUNK, (c + 1) * CHUNK)
            acc_send[c] = acc[rows, :].astype(bf16)
            send_to(
                acc_send.at[c], acc_land.at[c], acc_sems.at[0, c], acc_sems.at[1, c], head=1 - core
            ).start()

    @pl.when(step_id >= t_final)
    def _():
        c = step_id - t_final
        send_to(
            acc_send.at[c], acc_land.at[c], acc_sems.at[0, c], acc_sems.at[1, c], head=1 - core
        ).wait()
        total = acc[pl.ds(pl.multiple_of(c * CHUNK, CHUNK), CHUNK), :] + acc_land[c].astype(f32)
        scale = scale_ref[:, 0:1]
        hat = hid_ref[...].astype(f32) * scale
        term = jnp.sum(total * hat, axis=0, keepdims=True)

        @pl.when(c == 0)
        def _():
            norm_vec[0] = jnp.broadcast_to(term, norm_vec.shape[1:])

        @pl.when(c > 0)
        def _():
            norm_vec[0] += jnp.broadcast_to(term, norm_vec.shape[1:])

        ghat = total * gain_ref[...]
        mean = jnp.mean(ghat * hat, axis=1, keepdims=True)
        ghid_ref[...] = cot_ref[...].astype(f32) + scale * (ghat - hat * mean)

    @when_after(t_final + chunks - 1)
    def _():
        for bit in range(bits):
            exchange_sum(norm_vec, norm_land, bit, index, norm_sems.at[0], norm_sems.at[1])
            exchange_sum(vec, vec_land, bit, index, vec_sems.at[0], vec_sems.at[1])
            exchange_sum(hvec, hvec_land, bit, index, hvec_sems.at[0], hvec_sems.at[1])
        heads_ref[...] = hvec[bits]
        for b in range(nb):
            sums_ref[0:8, b * BLOCK : (b + 1) * BLOCK] = vec[bits, b]
        sums_ref[8:16, :] = norm_vec[bits]
        for stage in range(1, bits):
            for g in range(2):
                for part in range(2):
                    rs[g][part].advance(stage)
            for part in range(2):
                rs[2][part].advance(stage - 1)
            rs_small.advance(stage - 1)
        for part in range(2):
            rs[2][part].advance(bits - 1)
        rs_small.advance(bits - 1)


def back_call(
    gm_t, normed_t, ggate, run, step, slope, bc, sext, skip, decay, conv_shared, wsmall, gain,
    tgate, gated_w, vext, dy, after, state_in, dstate, conv_values, runt, stept, both, hidden,
    cotangent, scale,
):
    width, tokens = normed_t.shape
    inner = dy.shape[1]
    chunks = tokens // CHUNK
    nb = inner // BLOCK
    size = lax.axis_size("seq")
    bits = size.bit_length() - 1
    rows_own = width // size
    t_scan, t_values, t_grad, t_final = 2 * nb, 3 * nb, 4 * nb, 5 * nb

    def column(start):
        return lambda s: jnp.clip(s - start, 0, nb - 1)

    def full(shape):
        return pl.BlockSpec(shape, lambda s: (0,) * len(shape), pipeline_mode=pl.Buffered(1))

    def cols(rows, start):
        at = column(start)
        return pl.BlockSpec((rows, BLOCK), lambda s: (0, at(s)))

    def scan_or_values(s):
        return jnp.where(s < t_values, column(t_scan)(s), column(t_values)(s))

    row_block = lambda w: pl.BlockSpec((CHUNK, w), lambda s: (jnp.clip(s - t_final, 0, chunks - 1), 0))
    part_cols = inner // 2
    held = lambda: pltpu.VMEM((2, size, rows_own, part_cols), bf16)
    landing = lambda: tuple(
        pltpu.VMEM((2, size >> (s + 1), rows_own, part_cols), bf16) for s in range(bits)
    )
    sem = pltpu.SemaphoreType.DMA
    return pl.pallas_call(
        functools.partial(back_kernel, bits),
        grid=(5 * nb + chunks,),
        in_specs=[
            full((width, tokens)),
            full((width, tokens)),
            full((nb, tokens, BLOCK)),
            full((tokens, LANES)),
            full((tokens, LANES)),
            full((tokens, LANES)),
            full((tokens, 2 * STATE)),
            full((2, HALO + tokens, LANES)),
            full((1, LANES)),
            full((1, LANES)),
            full((2, CONV + 1, LANES)),
            full((width, 2 * LANES)),
            full((1, width)),
            cols(1, t_scan),
            cols(tokens, 0),
            cols(HALO + tokens, t_scan),
            cols(tokens, t_scan),
            pl.BlockSpec((chunks, STATE, BLOCK), lambda s: (0, 0, column(t_scan)(s))),
            cols(STATE, t_scan),
            cols(STATE, t_scan),
            pl.BlockSpec((CONV + 1, BLOCK), lambda s: (0, scan_or_values(s))),
            pl.BlockSpec((1, 8, tokens), lambda s: (column(t_scan)(s), 0, 0)),
            pl.BlockSpec((1, 8, tokens), lambda s: (column(t_scan)(s), 0, 0)),
            pl.BlockSpec((2, width, BLOCK), lambda s: (0, 0, column(t_grad)(s))),
            row_block(width),
            row_block(width),
            row_block(LANES),
        ],
        out_shape=[
            jax.ShapeDtypeStruct((rows_own, inner), f32),
            jax.ShapeDtypeStruct((rows_own, inner), f32),
            jax.ShapeDtypeStruct((rows_own, inner), f32),
            jax.ShapeDtypeStruct((rows_own, 2 * LANES), f32),
            jax.ShapeDtypeStruct((tokens, width), f32),
            jax.ShapeDtypeStruct((16, inner), f32),
            jax.ShapeDtypeStruct((8, LANES), f32),
        ],
        out_specs=[
            pl.BlockSpec((rows_own, inner), lambda s: (0, 0)),
            pl.BlockSpec((rows_own, inner), lambda s: (0, 0)),
            pl.BlockSpec((rows_own, inner), lambda s: (0, 0)),
            pl.BlockSpec((rows_own, 2 * LANES), lambda s: (0, 0)),
            row_block(width),
            pl.BlockSpec((16, inner), lambda s: (0, 0)),
            pl.BlockSpec((8, LANES), lambda s: (0, 0)),
        ],
        scratch_shapes=[
            held(), held(), held(),
            pltpu.VMEM((size, rows_own, 2 * LANES), bf16),
            landing(), landing(), landing(),
            tuple(pltpu.VMEM((size >> (s + 1), rows_own, 2 * LANES), bf16) for s in range(bits)),
            sem((7, bits)), sem((7, bits)),
            pltpu.VMEM((nb, tokens, BLOCK), bf16),
            pltpu.VMEM((tokens, width), f32),
            pltpu.VMEM((chunks, CHUNK, width), bf16),
            pltpu.VMEM((chunks, CHUNK, width), bf16),
            sem((2, chunks)),
            pltpu.VMEM((nb, 8, BLOCK), f32),
            pltpu.VMEM((nb, 8, BLOCK), f32),
            pltpu.VMEM((nb, 8, BLOCK), f32),
            sem((2, nb)),
            pltpu.VMEM((2, tokens, LANES), f32),
            pltpu.VMEM((tokens, LANES), f32),
            sem((2,)),
            pltpu.VMEM((tokens, 2 * LANES), bf16),
            pltpu.VMEM((8, LANES), f32),
            pltpu.VMEM((8, LANES), f32),
            sem((2,)),
            pltpu.VMEM((bits + 1, nb, 8, BLOCK), f32),
            pltpu.VMEM((bits, nb, 8, BLOCK), f32),
            sem((2, bits)),
            pltpu.VMEM((bits + 1, 8, width), f32),
            pltpu.VMEM((bits, 8, width), f32),
            sem((2, bits)),
            pltpu.VMEM((bits + 1, 8, LANES), f32),
            pltpu.VMEM((bits, 8, LANES), f32),
            sem((2, bits)),
            pltpu.VMEM((chunks, CHUNK, CHUNK), f32),
            pltpu.VMEM((chunks, CHUNK, CHUNK), f32),
            pltpu.VMEM((STATE, tokens), bf16),
            pltpu.VMEM((chunks, CHUNK, CHUNK), f32),
            pltpu.VMEM((tokens, LANES), f32),
            pltpu.VMEM((8, LANES), f32),
            pltpu.VMEM((nb, 8, tokens), f32),
            pltpu.VMEM((tokens, LANES), f32),
            pltpu.VMEM((tokens, LANES), f32),
            pltpu.VMEM((tokens, LANES), f32),
            pltpu.VMEM((HALO + tokens, BLOCK), f32),
            pltpu.VMEM((tokens + 8, BLOCK), f32),
        ],
        compiler_params=pltpu.CompilerParams(
            collective_id=3, has_side_effects=True, vmem_limit_bytes=66000000
        ),
        name="back",
    )(
        gm_t, normed_t, ggate, run, step, slope, bc, sext, skip, decay, conv_shared, wsmall, gain,
        tgate, gated_w, vext, dy, after, state_in, dstate, conv_values, runt, stept, both, hidden,
        cotangent, scale,
    )


def to_owners(states, kind):
    size = lax.axis_size("seq")
    pieces = states.astype(kind).reshape(size, states.shape[0] // size, states.shape[1])
    return lax.all_to_all(pieces, "seq", split_axis=0, concat_axis=0, tiled=True).astype(f32)


def from_owners(pieces, kind):
    back = lax.all_to_all(
        pieces.astype(kind), "seq", split_axis=0, concat_axis=0, tiled=True
    ).astype(f32)
    return back.reshape(-1, back.shape[2])


def carried_in(pieces, gains, reverse):
    size = pieces.shape[0]
    order = range(size - 1, -1, -1) if reverse else range(size)
    held = jnp.zeros_like(pieces[0])
    out = [None] * size
    for i in order:
        out[i] = held
        held = gains[i][None, :] * held + pieces[i]
    return jnp.stack(out)


def body(
    hidden, cotangent, norm_gain, proj_inner, proj_step, proj_shared, conv_values, conv_shared,
    step_bias, decay_log, skip_gain, gate_gain, proj_out,
):
    tokens = hidden.shape[0]
    inner = proj_inner.shape[2]
    heads = proj_step.shape[1]
    width = hidden.shape[1]
    size = lax.axis_size("seq")
    shared_here = conv_shared.shape[1] // lax.axis_size("head")
    shared_start = lax.axis_index("head") * shared_here
    halo = from_behind(hidden[-HALO:], 1)
    both = jnp.transpose(proj_inner, (1, 0, 2))
    lanes = lambda v: jnp.pad(v, (0, LANES - heads))[None, :]
    wstep = jnp.pad(proj_step, ((0, 0), (0, LANES - heads)))
    bias, decay, skip = lanes(step_bias), lanes(decay_log), lanes(skip_gain)
    (
        normed, norm_scale, gate_in, vext, yloc, after, step, slope, run, runt, stept, sext, bc,
    ) = front_call(
        hidden, halo, norm_gain[None, :], both, wstep, proj_shared, conv_values, conv_shared,
        bias, decay, skip,
    )
    total = jnp.sum(run[CHUNK - 1 :: CHUNK], axis=0)
    totals = lax.all_to_all(
        jnp.broadcast_to(total[None, None], (size, 1, LANES)), "seq", 0, 0, tiled=True
    )[:, 0, :heads]
    gains = jnp.repeat(jnp.exp(totals), HEAD_DIM, axis=1)
    state_in = from_owners(carried_in(to_owners(after[-1], f32), gains, False), f32)
    y, gated_w, partial_mix, squares = mix_call(
        yloc, gate_in, state_in, run, bc, gate_gain[None, :], proj_out
    )
    mixed_sum = partial_mix + swap(partial_mix)
    squares = squares[:, 0] + swap(squares[:, 0])
    inverse = lax.rsqrt(squares / INNER + norm_eps)[:, None]
    wide_hidden = hidden.astype(f32)
    wide_cot = cotangent.astype(f32)
    block_out = wide_hidden + mixed_sum * inverse
    grad_mixed = (wide_cot * inverse).astype(bf16)
    grad_inverse = jnp.sum(wide_cot * mixed_sum, axis=1, keepdims=True)
    coef = jnp.broadcast_to(grad_inverse * inverse**3 / INNER, (tokens, LANES))
    ggate, dy, term_gate, own_term = gate_call(
        grad_mixed, proj_out, y, gate_in, gate_gain[None, :], coef, run, bc
    )
    dstate = from_owners(carried_in(to_owners(own_term, bf16), gains, True), bf16)
    wshared_own = lax.dynamic_slice_in_dim(proj_shared, shared_start, shared_here, 1)
    (gout, ggw, gvw, gsmall, grad_hidden, sums, head_sums) = back_call(
        grad_mixed.T, normed.T, ggate, run, step, slope, bc, sext, skip, decay,
        conv_shared.reshape(CONV + 1, -1, LANES).transpose(1, 0, 2),
        jnp.concatenate([wshared_own, wstep], axis=1), norm_gain[None, :], term_gate, gated_w, vext,
        dy, after, state_in, dstate, conv_values, runt, stept, both, hidden, cotangent, norm_scale,
    )
    return (
        block_out,
        grad_hidden,
        sums[8],
        jnp.stack([ggw, gvw], axis=1),
        gsmall[:, shared_here : shared_here + heads],
        gsmall[:, :shared_here],
        sums[: CONV + 1],
        head_sums[2 : 3 + CONV],
        head_sums[0, :heads],
        head_sums[1, :heads],
        jnp.sum(sums[CONV + 2].reshape(heads, HEAD_DIM), axis=1),
        sums[CONV + 1],
        gout,
    )


def solution(mesh):
    return jax.shard_map(
        body,
        mesh=mesh,
        in_specs=(
            P("seq", None),
            P("seq", None),
            P(),
            P(None, None, "head"),
            P(None, "head"),
            P(),
            P(None, "head"),
            P(),
            P("head"),
            P("head"),
            P("head"),
            P("head"),
            P(None, "head"),
        ),
        out_specs=(
            P("seq", None),
            P("seq", None),
            P(),
            P("seq", None, "head"),
            P("seq", "head"),
            P("seq", "head"),
            P(None, "head"),
            P(None, "head"),
            P("head"),
            P("head"),
            P("head"),
            P("head"),
            P("seq", "head"),
        ),
        check_vma=False,
    )
```

```python
import functools

import jax
import jax.numpy as jnp
from jax import lax
from jax.experimental import pallas as pl
from jax.experimental.pallas import tpu as pltpu
from jax.sharding import PartitionSpec as P

HEAD_DIM = 64
STATE = 128
CONV = 4
INNER = 3072
CHUNK = 128
LANES = 128
BLOCK = 256
HALO = 16
BLOCK_HEADS = BLOCK // HEAD_DIM

norm_eps = 1e-05
highest = lax.Precision.HIGHEST
f32 = jnp.float32
bf16 = jnp.bfloat16
NN = (((1,), (0,)), ((), ()))
NT = (((1,), (1,)), ((), ()))
TN = (((0,), (0,)), ((), ()))


def flip(shard, bit):
    size = lax.axis_size("seq")
    return lax.ppermute(shard, "seq", [(i, i ^ (1 << bit)) for i in range(size)])


def swap(shard):
    return lax.ppermute(shard, "head", [(0, 1), (1, 0)])


def from_behind(shard, by):
    size = lax.axis_size("seq")
    pairs = [(i, i + by) for i in range(size) if 0 <= i + by < size]
    return lax.ppermute(shard, "seq", pairs)


def silu_grad(values):
    sigmoid = 1.0 / (1.0 + jnp.exp(-values))
    return sigmoid * (1.0 + values * (1.0 - sigmoid))


def silu(values):
    return values / (1.0 + jnp.exp(-values))


def mm(a, b, dims=NN):
    return lax.dot_general(a, b, dims, preferred_element_type=f32)


def parts(a):
    high = a.astype(bf16)
    return high, (a - high.astype(f32)).astype(bf16)


def mm_left(a, b, dims=NN):
    high, low = parts(a)
    return mm(high, b, dims) + mm(low, b, dims)


def mm_right(a, b, dims=NN):
    high, low = parts(b)
    return mm(a, high, dims) + mm(a, low, dims)


def mm_both(a, b, dims=NN):
    a_high, a_low = parts(a)
    b_high, b_low = parts(b)
    return mm(a_high, b_high, dims) + mm(a_low, b_high, dims) + mm(a_high, b_low, dims)


def mm_exact(a, b, dims=NN):
    return lax.dot_general(a, b, dims, precision=highest, preferred_element_type=f32)


def widen(cols):
    rows = cols.shape[0]
    lane = lax.broadcasted_iota(jnp.int32, (rows, LANES), 1)
    pieces = []
    for pair in range(BLOCK // LANES):
        first = jnp.broadcast_to(cols[:, 2 * pair : 2 * pair + 1], (rows, LANES))
        second = jnp.broadcast_to(cols[:, 2 * pair + 1 : 2 * pair + 2], (rows, LANES))
        pieces.append(jnp.where(lane < HEAD_DIM, first, second))
    return jnp.concatenate(pieces, axis=1)


def rolled(full, step):
    shift = lax.rem(LANES - BLOCK_HEADS * step, LANES)
    return pltpu.roll(full, shift, 1)


def causal():
    rows = lax.broadcasted_iota(jnp.int32, (CHUNK, CHUNK), 0)
    cols = lax.broadcasted_iota(jnp.int32, (CHUNK, CHUNK), 1)
    return rows >= cols


def conv_rows(ext, taps, first, rows):
    out = taps[CONV : CONV + 1, :]
    for k in range(CONV):
        out = out + taps[k : k + 1, :] * ext[first + k : first + k + rows, :]
    return out


def stack_pair(block):
    lane = lax.broadcasted_iota(jnp.int32, block.shape, 1)
    low = jnp.where(lane < HEAD_DIM, block, jnp.zeros_like(block))
    return low, block - low


class StateExchange:
    def __init__(self, index, size, reverse, own, landing, mixed, result, sems, gains):
        self.index, self.size, self.reverse = index, size, reverse
        self.own, self.landing, self.mixed, self.result = own, landing, mixed, result
        self.sems, self.gains = sems, gains

    def other(self, distance):
        return lax.rem(self.index + distance, self.size)

    def slot(self, source):
        return lax.rem(source - self.index - 1 + 2 * self.size, self.size)

    def send(self, j, value):
        share = value.shape[0] // self.size
        kind = self.own.dtype
        pieces = value.reshape(self.size, share, value.shape[1])
        self.own[j] = pieces.astype(kind)
        for d in range(1, self.size):
            pltpu.make_async_remote_copy(
                src_ref=self.own.at[j, self.other(d)],
                dst_ref=self.landing.at[j, self.size - d - 1],
                send_sem=self.sems.at[0, j],
                recv_sem=self.sems.at[1, j],
                device_id={"seq": self.other(d)},
                device_id_type=pl.DeviceIdType.MESH,
            ).start()

    def all_of(self, buffer, j, send, recv):
        return pltpu.make_async_remote_copy(
            src_ref=buffer.at[j, pl.ds(0, self.size - 1)],
            dst_ref=buffer.at[j, pl.ds(0, self.size - 1)],
            send_sem=self.sems.at[send, j],
            recv_sem=self.sems.at[recv, j],
            device_id={"seq": self.other(1)},
            device_id_type=pl.DeviceIdType.MESH,
        )

    def turn(self, j):
        self.all_of(self.landing, j, 0, 1).wait()
        kind = self.own.dtype
        self.landing[j, self.size - 1] = self.own[j, self.index]
        held = jnp.zeros(self.own.shape[2:], f32)
        order = range(self.size - 1, -1, -1) if self.reverse else range(self.size)
        for source in order:
            self.mixed[j, source] = held.astype(kind)
            gain = widen(rolled(self.gains[source : source + 1, :], j)[:, :BLOCK_HEADS])
            held = gain * held + self.landing[j, self.slot(source)].astype(f32)
        for d in range(1, self.size):
            pltpu.make_async_remote_copy(
                src_ref=self.mixed.at[j, self.other(d)],
                dst_ref=self.result.at[j, self.index],
                send_sem=self.sems.at[2, j],
                recv_sem=self.sems.at[3, j],
                device_id={"seq": self.other(d)},
                device_id_type=pl.DeviceIdType.MESH,
            ).start()

    def take(self, j):
        self.all_of(self.result, j, 2, 3).wait()
        self.result[j, self.index] = self.mixed[j, self.index]
        whole = self.result[j].astype(f32)
        return whole.reshape(whole.shape[0] * whole.shape[1], whole.shape[2])


def exchange_scratch(nb, size, kind):
    share = STATE // size
    return [pltpu.VMEM((nb, size, share, BLOCK), kind) for _ in range(4)] + [
        pltpu.SemaphoreType.DMA((4, nb))
    ]


def greet(index, core, size):
    barrier = pltpu.get_barrier_semaphore()
    for d in range(1, size):
        pl.semaphore_signal(
            barrier, inc=1, device_id={"seq": lax.rem(index + d, size)},
            device_id_type=pl.DeviceIdType.MESH,
        )
    pl.semaphore_signal(
        barrier, inc=1, device_id={"head": 1 - core}, device_id_type=pl.DeviceIdType.MESH
    )
    pl.semaphore_wait(barrier, size)


def send_to(src, dst, send_sem, recv_sem, **where):
    return pltpu.make_async_remote_copy(
        src_ref=src, dst_ref=dst, send_sem=send_sem, recv_sem=recv_sem, device_id=where,
        device_id_type=pl.DeviceIdType.MESH,
    )


def transposed(block):
    return block.astype(f32).T.astype(bf16)


def forward_kernel(
    size,
    hid_ref, gain_ref, wi_ref, wstep_ref, wshared_ref, cv_ref, cs_ref, bias_ref, decay_ref,
    skip_ref, ggain_ref, wout_ref, hrow_ref, crow_ref,
    normedt_ref, scale_ref, gate_ref, vext_ref, after_ref, y_ref, gw_ref, in_ref, step_ref,
    slope_ref, run_ref, runt_ref, stept_ref, sext_ref, bc_ref, gains_ref, out_ref, gmt_ref,
    coef_ref,
    nx, halo, halo_sems, scores, bt, end_w, vwide, act_all, gates, ys, states, acc, acc_send,
    acc_land, acc_sems, squares, sq_land, sq_sems, totals, totals_land, totals_sems,
    ex_own, ex_landing, ex_mixed, ex_result, ex_sems,
):
    step_id = pl.program_id(0)
    index = lax.axis_index("seq")
    core = lax.axis_index("head")
    tokens = hid_ref.shape[0]
    width = hid_ref.shape[1]
    chunks = tokens // CHUNK
    nb = act_all.shape[0]
    t_gate, t_mix, t_last = nb, 2 * nb, 3 * nb
    exchange = StateExchange(
        index, size, False, ex_own, ex_landing, ex_mixed, ex_result, ex_sems, gains_ref
    )

    def norm_rows(rows):
        wide = rows.astype(f32)
        scale = lax.rsqrt(jnp.mean(wide * wide, axis=1, keepdims=True) + norm_eps)
        return (wide * scale * gain_ref[...]).astype(bf16), scale

    def totals_copy(d):
        return send_to(
            totals, totals_land.at[size - d - 1], totals_sems.at[0], totals_sems.at[1],
            seq=lax.rem(index + d, size),
        )

    @pl.when(step_id == 0)
    def _():
        @pl.loop(0, chunks)
        def _(i):
            start = pl.multiple_of(i * CHUNK, CHUNK)
            for part in range(2):
                at = pl.multiple_of(start + part * 64, 64)
                rows, scale = norm_rows(hid_ref[pl.ds(at, 64), :])
                nx[pl.ds(pl.multiple_of(HALO + at, HALO), 64), :] = rows
                scale_ref[pl.ds(at, 64), :] = jnp.broadcast_to(scale, (64, LANES))

        greet(index, core, size)
        after_id = lax.rem(index + 1, size)
        halo_copy = send_to(
            hid_ref.at[pl.ds(tokens - HALO, HALO)], halo, halo_sems.at[0], halo_sems.at[1],
            seq=after_id,
        )
        halo_copy.start()
        for c in range(chunks):
            for b in range(width // LANES):
                normedt_ref[b * LANES : (b + 1) * LANES, c * CHUNK : (c + 1) * CHUNK] = transposed(
                    nx[HALO + c * CHUNK : HALO + (c + 1) * CHUNK, b * LANES : (b + 1) * LANES]
                )
        raw = mm(nx[HALO:, :], wstep_ref[...]) + bias_ref[...]
        small = jnp.exp(-jnp.abs(raw))
        step = jnp.maximum(raw, 0.0) + jnp.log1p(small)
        step_ref[...] = step
        slope_ref[...] = 1.0 / (1.0 + jnp.exp(-raw))
        rate = -step * jnp.exp(decay_ref[...])
        tri = causal().astype(f32)
        total = jnp.zeros((1, LANES), f32)
        for c in range(chunks):
            rows = slice(c * CHUNK, (c + 1) * CHUNK)
            run = mm_exact(tri, rate[rows, :])
            run_ref[rows, :] = run
            total = total + run[CHUNK - 1 :, :]
            run_t = run.T
            step_t = step[rows, :].T
            for b in range(nb):
                heads = slice(BLOCK_HEADS * b, BLOCK_HEADS * (b + 1))
                runt_ref[b, 0:BLOCK_HEADS, rows] = run_t[heads, :]
                stept_ref[b, 0:BLOCK_HEADS, rows] = step_t[heads, :]
                runt_ref[b, BLOCK_HEADS:, rows] = jnp.zeros((8 - BLOCK_HEADS, CHUNK), f32)
                stept_ref[b, BLOCK_HEADS:, rows] = jnp.zeros((8 - BLOCK_HEADS, CHUNK), f32)
            end_w[rows, :] = step[rows, :] * jnp.exp(run[CHUNK - 1 :, :] - run)
        totals[...] = jnp.broadcast_to(jnp.exp(total), totals.shape)
        for d in range(1, size):
            totals_copy(d).start()
        halo_copy.wait()
        keep = jnp.where(index == 0, 0.0, 1.0)
        nx[0:HALO, :] = (norm_rows(halo[...])[0].astype(f32) * keep).astype(bf16)
        shared = mm(nx[...], wshared_ref[...]).astype(bf16)
        sext_ref[0] = shared[:, :STATE]
        sext_ref[1] = shared[:, STATE:]
        conv = conv_rows(shared.astype(f32), cs_ref[...], HALO - CONV + 1, tokens)
        act = silu(conv).astype(bf16)
        bc_ref[...] = act
        for c in range(chunks):
            rows = slice(c * CHUNK, (c + 1) * CHUNK)
            b_rows = act[rows, :STATE]
            c_rows = act[rows, STATE:]
            scores[c] = mm(c_rows, b_rows, NT)
            bt[:, rows] = transposed(b_rows)

    @pl.when(step_id < t_gate)
    def _():
        j = step_id
        values = mm(nx[...], wi_ref[0]).astype(bf16)
        vext_ref[...] = values
        vwide[...] = values.astype(f32)
        conv = conv_rows(vwide, cv_ref[...], HALO - CONV + 1, tokens)
        act = silu(conv).astype(bf16)
        act_all[j] = act
        run_cols = rolled(run_ref[...], j)
        end_cols = rolled(end_w[...], j)
        state = jnp.zeros((STATE, BLOCK), f32)
        for c in range(chunks):
            rows = slice(c * CHUNK, (c + 1) * CHUNK)
            weighted = act[rows, :].astype(f32) * widen(end_cols[rows, :BLOCK_HEADS])
            last = widen(jnp.exp(run_cols[(c + 1) * CHUNK - 1 : (c + 1) * CHUNK, :BLOCK_HEADS]))
            state = last * state + mm_right(bt[:, rows], weighted)
            after_ref[c] = state
            states[j, c] = state
        exchange.send(j, state)

    @pl.when((step_id >= t_gate) & (step_id < t_mix))
    def _():
        j = step_id - t_gate
        gate = mm(nx[HALO:, :], wi_ref[0])
        gate_ref[...] = gate
        gates[j] = gate

        @pl.when(j == 0)
        def _():
            pltpu.make_async_remote_copy(
                src_ref=totals_land.at[pl.ds(0, size - 1)],
                dst_ref=totals_land.at[pl.ds(0, size - 1)],
                send_sem=totals_sems.at[0], recv_sem=totals_sems.at[1],
                device_id={"seq": lax.rem(index + 1, size)},
                device_id_type=pl.DeviceIdType.MESH,
            ).wait()
            totals_land[size - 1] = totals[...]
            for source in range(size):
                gains_ref[source : source + 1, :] = totals_land[exchange.slot(source), 0:1, :]

        run_cols = rolled(run_ref[...], j)
        mask = causal()
        skip = widen(rolled(skip_ref[...], j)[:, :BLOCK_HEADS])
        for c in range(chunks):
            rows = slice(c * CHUNK, (c + 1) * CHUNK)
            cols = run_cols[rows, :BLOCK_HEADS]
            x = act_all[j, rows, :]
            y_pairs = []
            for pair in range(BLOCK // LANES):
                mats = []
                for k in range(2):
                    head = 2 * pair + k
                    gap = cols[:, head : head + 1] - runt_ref[j, head : head + 1, rows]
                    decayed = jnp.exp(jnp.where(mask, gap, -1e30))
                    mats.append(scores[c] * decayed * stept_ref[j, head : head + 1, rows])
                low, high = stack_pair(x[:, pair * LANES : (pair + 1) * LANES])
                y_pairs.append(
                    mm_left(jnp.concatenate(mats, axis=1), jnp.concatenate([low, high], axis=0))
                )
            ys[j, rows, :] = jnp.concatenate(y_pairs, axis=1) + skip * x.astype(f32)
        exchange.turn(j)

    @pl.when((step_id >= t_mix) & (step_id < t_last))
    def _():
        j = step_id - t_mix
        entering = exchange.take(j)
        in_ref[...] = entering
        offsets = offsets_of(run_ref, chunks)
        gated = []
        for c in range(chunks):
            rows = slice(c * CHUNK, (c + 1) * CHUNK)
            grow = rolled(jnp.exp(run_ref[rows, :]), j)[:, :BLOCK_HEADS]
            base = rolled(jnp.exp(offsets[c]), j)[:, :BLOCK_HEADS]
            enter = widen(base) * entering
            if c:
                enter = enter + states[j, c - 1]
            y = ys[j, rows, :] + widen(grow) * mm_right(bc_ref[rows, STATE:], enter)
            y_ref[rows, :] = y
            out = y * silu(gates[j, rows, :])
            gw_ref[rows, :] = (out * ggain_ref[...]).astype(bf16)
            gated.append(
                jnp.broadcast_to(jnp.sum(out * out, axis=1, keepdims=True), (CHUNK, LANES))
            )
        part = mm(gw_ref[...], wout_ref[...], NT)
        block_squares = jnp.concatenate(gated, axis=0)

        @pl.when(j == 0)
        def _():
            acc[...] = part
            squares[...] = block_squares

        @pl.when(j > 0)
        def _():
            acc[...] += part
            squares[...] += block_squares

        @pl.when(j == nb - 1)
        def _():
            send_to(squares, sq_land, sq_sems.at[0], sq_sems.at[1], head=1 - core).start()
            for c in range(chunks):
                acc_send[c] = acc[c * CHUNK : (c + 1) * CHUNK, :].astype(bf16)
                send_to(
                    acc_send.at[c], acc_land.at[c], acc_sems.at[0, c], acc_sems.at[1, c],
                    head=1 - core,
                ).start()

    @pl.when(step_id >= t_last)
    def _():
        c = step_id - t_last

        @pl.when(c == 0)
        def _():
            send_to(squares, sq_land, sq_sems.at[0], sq_sems.at[1], head=1 - core).wait()

        send_to(
            acc_send.at[c], acc_land.at[c], acc_sems.at[0, c], acc_sems.at[1, c], head=1 - core
        ).wait()
        rows = pl.ds(pl.multiple_of(c * CHUNK, CHUNK), CHUNK)
        mixed = acc[rows, :] + acc_land[c].astype(f32)
        inverse = lax.rsqrt((squares[rows, 0:1] + sq_land[rows, 0:1]) / INNER + norm_eps)
        out_ref[...] = hrow_ref[...].astype(f32) + mixed * inverse
        cot = crow_ref[...].astype(f32)
        scaled = (cot * inverse).astype(bf16)
        for b in range(width // LANES):
            gmt_ref[b * LANES : (b + 1) * LANES, :] = transposed(
                scaled[:, b * LANES : (b + 1) * LANES]
            )
        grad_inverse = jnp.sum(cot * mixed, axis=1, keepdims=True)
        coef_ref[:, 0:LANES] = jnp.broadcast_to(
            grad_inverse * inverse * inverse * inverse / INNER, (CHUNK, LANES)
        )
        coef_ref[:, LANES:] = jnp.broadcast_to(inverse, (CHUNK, LANES))


def offsets_of(run_ref, chunks):
    rows = [jnp.zeros((1, LANES), f32)]
    for c in range(chunks):
        rows.append(rows[-1] + run_ref[(c + 1) * CHUNK - 1 : (c + 1) * CHUNK, :])
    return rows


def forward_call(
    hidden, cotangent, gain, both, wstep, wshared, conv_values, conv_shared, bias, decay, skip,
    gate_gain, wout,
):
    tokens, width = hidden.shape
    inner = both.shape[2]
    chunks = tokens // CHUNK
    nb = inner // BLOCK
    size = lax.axis_size("seq")
    t_gate, t_mix, t_last = nb, 2 * nb, 3 * nb

    def at(start):
        return lambda s: jnp.clip(s - start, 0, nb - 1)

    def full(shape):
        return pl.BlockSpec(shape, lambda s: (0,) * len(shape), pipeline_mode=pl.Buffered(1))

    def cols(rows, start):
        return pl.BlockSpec((rows, BLOCK), lambda s: (0, at(start)(s)))

    row_of = lambda s: jnp.clip(s - t_last, 0, chunks - 1)
    row_block = lambda w: pl.BlockSpec((CHUNK, w), lambda s: (row_of(s), 0))
    outs = [
        ((width, tokens), bf16, full((width, tokens))),
        ((tokens, LANES), f32, full((tokens, LANES))),
        ((tokens, inner), f32, cols(tokens, t_gate)),
        ((HALO + tokens, inner), bf16, cols(HALO + tokens, 0)),
        (
            (chunks, STATE, inner), f32,
            pl.BlockSpec((chunks, STATE, BLOCK), lambda s: (0, 0, at(0)(s))),
        ),
        ((tokens, inner), f32, cols(tokens, t_mix)),
        ((tokens, inner), bf16, cols(tokens, t_mix)),
        ((STATE, inner), f32, cols(STATE, t_mix)),
        ((tokens, LANES), f32, full((tokens, LANES))),
        ((tokens, LANES), f32, full((tokens, LANES))),
        ((tokens, LANES), f32, full((tokens, LANES))),
        ((nb, 8, tokens), f32, full((nb, 8, tokens))),
        ((nb, 8, tokens), f32, full((nb, 8, tokens))),
        ((2, HALO + tokens, STATE), bf16, full((2, HALO + tokens, STATE))),
        ((tokens, 2 * STATE), bf16, full((tokens, 2 * STATE))),
        ((size, LANES), f32, full((size, LANES))),
        ((tokens, width), f32, row_block(width)),
        ((width, tokens), bf16, pl.BlockSpec((width, CHUNK), lambda s: (0, row_of(s)))),
        ((tokens, 2 * LANES), f32, row_block(2 * LANES)),
    ]
    sem = pltpu.SemaphoreType.DMA
    return pl.pallas_call(
        functools.partial(forward_kernel, size),
        grid=(3 * nb + chunks,),
        in_specs=[
            full((tokens, width)),
            full((1, width)),
            pl.BlockSpec(
                (1, width, BLOCK),
                lambda s: (jnp.where(s < t_gate, 1, 0), 0, jnp.where(s < t_gate, at(0)(s), at(t_gate)(s))),
            ),
            full((width, LANES)),
            full((width, 2 * STATE)),
            cols(CONV + 1, 0),
            full((CONV + 1, 2 * STATE)),
            full((1, LANES)),
            full((1, LANES)),
            full((1, LANES)),
            cols(1, t_mix),
            cols(width, t_mix),
            row_block(width),
            row_block(width),
        ],
        out_shape=[jax.ShapeDtypeStruct(shape, kind) for shape, kind, _ in outs],
        out_specs=[spec for _, _, spec in outs],
        scratch_shapes=[
            pltpu.VMEM((HALO + tokens, width), bf16),
            pltpu.VMEM((HALO, width), bf16),
            sem((2,)),
            pltpu.VMEM((chunks, CHUNK, CHUNK), f32),
            pltpu.VMEM((STATE, tokens), bf16),
            pltpu.VMEM((tokens, LANES), f32),
            pltpu.VMEM((HALO + tokens, BLOCK), f32),
            pltpu.VMEM((nb, tokens, BLOCK), bf16),
            pltpu.VMEM((nb, tokens, BLOCK), f32),
            pltpu.VMEM((nb, tokens, BLOCK), f32),
            pltpu.VMEM((nb, chunks, STATE, BLOCK), f32),
            pltpu.VMEM((tokens, width), f32),
            pltpu.VMEM((chunks, CHUNK, width), bf16),
            pltpu.VMEM((chunks, CHUNK, width), bf16),
            sem((2, chunks)),
            pltpu.VMEM((tokens, LANES), f32),
            pltpu.VMEM((tokens, LANES), f32),
            sem((2,)),
            pltpu.VMEM((8, LANES), f32),
            pltpu.VMEM((size, 8, LANES), f32),
            sem((2,)),
        ] + exchange_scratch(nb, size, f32),
        compiler_params=pltpu.CompilerParams(
            collective_id=1, has_side_effects=True, vmem_limit_bytes=67043328
        ),
        name="forward",
    )(
        hidden, gain, both, wstep, wshared, conv_values, conv_shared, bias, decay, skip, gate_gain,
        wout, hidden, cotangent,
    )


def order_bits(part, bits):
    order = list(range(bits))
    if part == 1 and bits > 1:
        order[0], order[1] = 1, 0
    return order


def slot_of(owner, part, bits):
    slot = 0
    for bit in order_bits(part, bits):
        slot = slot * 2 + ((owner >> bit) & 1)
    return slot


class Reduction:
    def __init__(self, held, landing, out, part, bits, index, send_sems, recv_sems, cols):
        self.held, self.landing, self.out = held, landing, out
        self.part, self.bits, self.index = part, bits, index
        self.send_sems, self.recv_sems, self.cols = send_sems, recv_sems, cols

    def place(self, stage):
        base = 0
        size = 1 << self.bits
        for s, bit in enumerate(order_bits(self.part, self.bits)[: stage + 1]):
            mine = (self.index // (1 << bit)) % 2
            half = size >> (s + 1)
            keep, give = base + mine * half, base + (1 - mine) * half
            base = keep
        return keep, give, half, order_bits(self.part, self.bits)[stage]

    def copy(self, stage):
        _, give, half, bit = self.place(stage)
        mine = (self.index // (1 << bit)) % 2
        partner = self.index + (1 - 2 * mine) * (1 << bit)
        return pltpu.make_async_remote_copy(
            src_ref=self.held.at[pl.ds(give, half)],
            dst_ref=self.landing[stage],
            send_sem=self.send_sems.at[stage],
            recv_sem=self.recv_sems.at[stage],
            device_id={"seq": partner},
            device_id_type=pl.DeviceIdType.MESH,
        )

    def start(self, stage):
        self.copy(stage).start()

    def finish(self, stage):
        self.copy(stage).wait()
        keep, _, half, _ = self.place(stage)
        if stage == self.bits - 1:
            self.out[:, self.cols] = self.held[keep].astype(f32) + self.landing[stage][0].astype(f32)
        else:

            @pl.loop(0, half)
            def _(i):
                total = self.held[keep + i].astype(f32) + self.landing[stage][i].astype(f32)
                self.held[keep + i] = total.astype(bf16)

    def advance(self, stage):
        self.finish(stage)
        if stage + 1 < self.bits:
            self.start(stage + 1)


def sum_copy(acc, landing, bit, index, sems):
    mine = (index // (1 << bit)) % 2
    return pltpu.make_async_remote_copy(
        src_ref=acc.at[bit],
        dst_ref=landing.at[bit],
        send_sem=sems.at[0, bit],
        recv_sem=sems.at[1, bit],
        device_id={"seq": index + (1 - 2 * mine) * (1 << bit)},
        device_id_type=pl.DeviceIdType.MESH,
    )


def back_kernel(
    bits,
    gmt_ref, normedt_ref, coef_ref, gains_ref, run_ref, step_ref, slope_ref, bc_ref, sext_ref, skip_ref,
    decay_ref, cs_ref, wsmall_ref, gain_ref,
    wout_ref, y_ref, gate_ref, ggain_ref, gw_ref, vext_ref, after_ref, in_ref, cv_ref, runt_ref,
    stept_ref, wi_ref,
    hid_ref, cot_ref, scale_ref,
    gout_ref, ggw_ref, gvw_ref, gsmall_ref, ghid_ref, sums_ref, heads_ref,
    w_out, w_gate, w_values, w_small,
    land_out, land_gate, land_values, land_small,
    rs_send, rs_recv,
    gv, acc_send, acc_land, acc_sems,
    edge_own, edge_tail, edge_land, edge_sems,
    dbc, dbc_land, dbc_sems, small, sedge_own, sedge_land, sedge_sems,
    vec, vec_land, vec_sems,
    scores, scorest, ct, dscores, end_w, ends, dcols, xdu, dyc, xdus, vwide, gext,
    dys, ggates, term_gate, ex_own, ex_landing, ex_mixed, ex_result, ex_sems,
):
    step_id = pl.program_id(0)
    index = lax.axis_index("seq")
    core = lax.axis_index("head")
    size = 1 << bits
    tokens = y_ref.shape[0]
    chunks = tokens // CHUNK
    nb = w_out.shape[0] * w_out.shape[3] // BLOCK
    half_nb = nb // 2
    width = normedt_ref.shape[0]
    rows_own = width // size
    part_cols = w_out.shape[3]
    t_out, t_gate, t_scan, t_values, t_grad, t_final = (nb * i for i in range(1, 7))
    after_id = lax.rem(index + 1, size)
    before_id = lax.rem(index + size - 1, size)

    def reduction(g, part):
        held, landing, out = (
            (w_out, land_out, gout_ref), (w_gate, land_gate, ggw_ref), (w_values, land_values, gvw_ref),
        )[g]
        land = [ref.at[part] for ref in landing]
        slot = 2 * g + part
        return Reduction(
            held.at[part], land, out, part, bits, index, rs_send.at[slot], rs_recv.at[slot],
            pl.ds(part * part_cols, part_cols),
        )

    rs = [[reduction(g, part) for part in range(2)] for g in range(3)]
    rs_small = Reduction(
        w_small, list(land_small), gsmall_ref, 1, bits, index, rs_send.at[6], rs_recv.at[6],
        pl.ds(0, w_small.shape[2]),
    )

    def when_after(step):
        return pl.when(step_id == step)

    exchange = StateExchange(
        index, size, True, ex_own, ex_landing, ex_mixed, ex_result, ex_sems, gains_ref
    )

    @pl.when(step_id == 0)
    def _():
        greet(index, core, size)
        for c in range(chunks):
            rows = slice(c * CHUNK, (c + 1) * CHUNK)
            ct[:, rows] = transposed(bc_ref[rows, STATE:])
            for b in range(width // LANES):
                acc_send[c, :, b * LANES : (b + 1) * LANES] = transposed(
                    gmt_ref[b * LANES : (b + 1) * LANES, rows]
                )

    @pl.when(step_id < t_out)
    def _():
        j = step_id
        offsets = offsets_of(run_ref, chunks)
        own = jnp.zeros((STATE, BLOCK), f32)
        term = jnp.zeros((1, BLOCK), f32)
        for c in range(chunks):
            rows = slice(c * CHUNK, (c + 1) * CHUNK)
            ggw = mm(acc_send[c], wout_ref[...])
            y = y_ref[rows, :]
            gate = gate_ref[rows, :]
            sig = 1.0 / (1.0 + jnp.exp(-gate))
            act = gate * sig
            out = y * act
            term = term + jnp.sum(ggw * out, axis=0, keepdims=True)
            coef = jnp.concatenate([coef_ref[rows, 0:LANES]] * (BLOCK // LANES), axis=1)
            gg = ggw * ggain_ref[...] - coef * out
            dy = gg * act
            dys[j, rows, :] = dy
            ggates[j, rows, :] = (gg * y * (sig * (1.0 + gate * (1.0 - sig)))).astype(bf16)
            grow = rolled(jnp.exp(run_ref[rows, :] + offsets[c]), j)[:, :BLOCK_HEADS]
            own = own + mm_right(ct[:, rows], dy * widen(grow))
        term_gate[j, 0:1, :] = term
        exchange.send(j, own)

    def put_block(held, left, right, j):
        part = j // half_nb
        cols = pl.ds(pl.multiple_of((j % half_nb) * BLOCK, BLOCK), BLOCK)
        group = width // 4
        for q in range(4):
            piece = mm(left[q * group : (q + 1) * group, :], right).astype(bf16)
            for b in range(size // 4):
                owner = q * (size // 4) + b
                slots = [slot_of(owner, p, bits) for p in range(2)]
                slot = slots[0] + part * (slots[1] - slots[0])
                held[part, slot, :, cols] = piece[b * rows_own : (b + 1) * rows_own, :]

    @pl.when((step_id >= t_out) & (step_id < t_gate))
    def _():
        j = step_id - t_out
        put_block(w_out, gmt_ref, gw_ref[...], j)
        exchange.turn(j)

    @pl.when((step_id >= t_gate) & (step_id < t_scan))
    def _():
        j = step_id - t_gate
        put_block(w_gate, normedt_ref, ggates[j], j)

    @when_after(t_out + half_nb - 1)
    def _():
        rs[0][0].start(0)

    @when_after(t_gate - 1)
    def _():
        rs[0][1].start(0)

    @when_after(t_gate + half_nb - 1)
    def _():
        rs[1][0].start(0)

    @when_after(t_scan - 1)
    def _():
        rs[1][1].start(0)

    mask = causal()
    rows_i = lax.broadcasted_iota(jnp.int32, (CHUNK, CHUNK), 0)
    cols_i = lax.broadcasted_iota(jnp.int32, (CHUNK, CHUNK), 1)
    mask_t = rows_i <= cols_i

    @pl.when(step_id == t_scan)
    def _():
        dbc[...] = jnp.zeros_like(dbc)
        dscores[...] = jnp.zeros_like(dscores)
        dcols[...] = jnp.zeros_like(dcols)
        xdu[...] = jnp.zeros_like(xdu)
        dyc[...] = jnp.zeros_like(dyc)
        xdus[...] = jnp.zeros_like(xdus)
        ends[...] = jnp.zeros_like(ends)
        vec[...] = jnp.zeros_like(vec)
        for c in range(chunks):
            rows = slice(c * CHUNK, (c + 1) * CHUNK)
            b_rows = bc_ref[rows, :STATE]
            c_rows = bc_ref[rows, STATE:]
            scores[c] = mm(c_rows, b_rows, NT)
            scorest[c] = mm(b_rows, c_rows, NT)
            run = run_ref[rows, :]
            end_w[rows, :] = jnp.exp(run[CHUNK - 1 :, :] - run)

    @pl.when((step_id >= t_scan) & (step_id < t_values))
    def _():
        j = step_id - t_scan
        offsets = offsets_of(run_ref, chunks)
        vwide[...] = vext_ref[...].astype(f32)
        conv = conv_rows(vwide, cv_ref[...], HALO - CONV + 1, tokens)
        sig_all = 1.0 / (1.0 + jnp.exp(-conv))
        act = (conv * sig_all).astype(bf16)
        slope = sig_all * (1.0 + conv * (1.0 - sig_all))
        run_cols = rolled(run_ref[...], j)
        step_cols = rolled(step_ref[...], j)
        end_cols = rolled(end_w[...], j)
        skip = widen(rolled(skip_ref[...], j)[:, :BLOCK_HEADS])
        channel = lax.broadcasted_iota(jnp.int32, (BLOCK, LANES), 0) // HEAD_DIM
        lane = lax.broadcasted_iota(jnp.int32, (BLOCK, LANES), 1)
        pick = (lane == BLOCK_HEADS * j + channel).astype(bf16)
        lane_row = lax.broadcasted_iota(jnp.int32, (CHUNK, LANES), 1)
        dstate = exchange.take(j)
        dskip = jnp.zeros((1, BLOCK), f32)
        gext[tokens : tokens + 8, :] = jnp.zeros((8, BLOCK), f32)
        for c in reversed(range(chunks)):
            rows = slice(c * CHUNK, (c + 1) * CHUNK)
            cols = run_cols[rows, :BLOCK_HEADS]
            x = act[rows, :]
            wide_x = x.astype(f32)
            dy = dys[j, rows, :]
            b_rows = bc_ref[rows, :STATE]
            c_rows = bc_ref[rows, STATE:]
            grow = widen(jnp.exp(cols))
            tail = widen(end_cols[rows, :BLOCK_HEADS])
            step_w = widen(step_cols[rows, :BLOCK_HEADS])
            last = grow[CHUNK - 1 :, :]
            base = rolled(jnp.exp(offsets[c]), j)[:, :BLOCK_HEADS]
            enter = widen(base) * in_ref[...]
            if c:
                enter = enter + after_ref[c - 1]
            du_state = tail * mm_right(b_rows, dstate)
            carried = grow * mm_right(c_rows, enter)
            weighted = wide_x * (tail * step_w)
            grown = dy * grow
            dbc[0, rows, :] += mm_both(weighted, dstate, NT)
            dbc[1, rows, :] += mm_both(grown, enter, NT)
            hold = last * jnp.sum(dstate * enter, axis=0, keepdims=True)
            ends[c : c + 1, :] += mm_exact(
                jnp.broadcast_to(hold, (8, BLOCK)), pick.astype(f32)
            )[:1, :]
            dstate = last * dstate + mm_right(ct[:, rows], grown)
            du_pairs = []
            col_sum = jnp.zeros((CHUNK, LANES), f32)
            for pair in range(BLOCK // LANES):
                lanes = slice(pair * LANES, (pair + 1) * LANES)
                low, high = stack_pair(dy[:, lanes])
                both = jnp.concatenate([low, high], axis=0)
                dmat = mm_left(both, x[:, lanes], NT)
                mats = []
                for k in range(2):
                    head = 2 * pair + k
                    col = cols[:, head : head + 1]
                    row = runt_ref[0, head : head + 1, rows]
                    keep = jnp.exp(jnp.where(mask, col - row, -1e30))
                    piece = dmat[k * CHUNK : (k + 1) * CHUNK, :] * keep
                    piece = piece * stept_ref[0, head : head + 1, rows]
                    dscores[c] += piece
                    full = piece * scores[c]
                    col_sum = jnp.where(
                        lane_row == BLOCK_HEADS * j + head,
                        jnp.sum(full, axis=1, keepdims=True),
                        col_sum,
                    )
                    dcols[j, head : head + 1, rows] = jnp.sum(full, axis=0, keepdims=True)
                    keep_t = jnp.exp(jnp.where(mask_t, row - col, -1e30))
                    mats.append(scorest[c] * keep_t)
                du_pairs.append(mm_both(jnp.concatenate(mats, axis=1), both))
            dyc[rows, :] += col_sum
            du = jnp.concatenate(du_pairs, axis=1) + du_state
            xdu[rows, :] += mm_left(wide_x * du, pick)
            dyc[rows, :] += mm_left(dy * carried, pick)
            xdus[rows, :] += mm_left(wide_x * du_state, pick)
            dskip = dskip + jnp.sum(dy * wide_x, axis=0, keepdims=True)
            gext[rows, :] = (step_w * du + skip * dy) * slope[rows, :]
        gconv = gext[0:tokens, :]
        for k in range(CONV):
            first = HALO - CONV + 1 + k
            vec[0, j, k : k + 1, :] = jnp.sum(
                vwide[first : first + tokens, :] * gconv, axis=0, keepdims=True
            )
        vec[0, j, CONV : CONV + 1, :] = jnp.sum(gconv, axis=0, keepdims=True)
        vec[0, j, CONV + 1 : CONV + 2, :] = term_gate[j, 0:1, :]
        vec[0, j, CONV + 2 : CONV + 3, :] = dskip
        total = cv_ref[CONV - 1 : CONV, :] * gconv
        for k in range(CONV - 1):
            total = total + cv_ref[k : k + 1, :] * gext[CONV - 1 - k : CONV - 1 - k + tokens, :]
        gv[j] = total.astype(bf16)
        lacking = jnp.zeros((8, BLOCK), f32)
        edge_tail[j] = total[tokens - 8 :, :] + lacking
        edge_own[j] = gconv[0:8, :]
        send_to(
            edge_own.at[j], edge_land.at[j], edge_sems.at[0, j], edge_sems.at[1, j], seq=before_id
        ).start()

    @when_after(t_scan + half_nb)
    def _():
        rs[0][0].advance(0)
        rs[0][1].advance(0)

    @when_after(t_values - 1)
    def _():
        tri = mask.astype(f32)
        tri_t = mask_t.astype(f32)
        strict = (rows_i > cols_i).astype(f32)
        decay = jnp.exp(decay_ref[...])
        bias_sum = jnp.zeros((1, LANES), f32)
        decay_sum = jnp.zeros((1, LANES), f32)
        for c in range(chunks):
            rows = slice(c * CHUNK, (c + 1) * CHUNK)
            step = step_ref[rows, :]
            col_rows = [dcols[b, 0:BLOCK_HEADS, rows] for b in range(nb)]
            rest = LANES - BLOCK_HEADS * nb
            col_rows.append(jnp.zeros((rest, CHUNK), f32))
            dlog = dyc[rows, :] - jnp.concatenate(col_rows, axis=0).T
            drate = (
                mm_exact(tri_t, dlog)
                + mm_exact(strict, xdus[rows, :] * step)
                + ends[c : c + 1, :]
            )
            dstep = xdu[rows, :] - decay * drate
            draw = dstep * slope_ref[rows, :]
            small[rows, LANES:] = draw.astype(bf16)
            bias_sum = bias_sum + jnp.sum(draw, axis=0, keepdims=True)
            decay_sum = decay_sum - jnp.sum(drate * step, axis=0, keepdims=True) * decay
            b_rows = bc_ref[rows, :STATE]
            c_rows = bc_ref[rows, STATE:]
            high, low = parts(dscores[c])
            dbc[1, rows, :] += mm(high, b_rows) + mm(low, b_rows)
            dbc[0, rows, :] += mm(high, c_rows, TN) + mm(low, c_rows, TN)
        vec[0, nb, 0:1, 0:LANES] = bias_sum
        vec[0, nb, 1:2, 0:LANES] = decay_sum
        send_to(
            dbc.at[1 - core], dbc_land, dbc_sems.at[0], dbc_sems.at[1], head=1 - core
        ).start()

    @pl.when((step_id >= t_values) & (step_id < t_grad))
    def _():
        j = step_id - t_values
        send_to(
            edge_own.at[j], edge_land.at[j], edge_sems.at[0, j], edge_sems.at[1, j], seq=before_id
        ).wait()
        cv = cv_ref[...]
        nxt = jnp.where(index == size - 1, 0.0, 1.0) * edge_land[j]
        row8 = lax.broadcasted_iota(jnp.int32, (8, BLOCK), 0)
        fix = edge_tail[j]
        for k in range(CONV - 1):
            ahead = CONV - 1 - k
            moved = pltpu.roll(nxt, 8 - ahead, 0)
            fix = fix + jnp.where(row8 >= 8 - ahead, cv[k : k + 1, :] * moved, 0.0)
        both_rows = jnp.concatenate([gv[j, tokens - 16 : tokens - 8, :].astype(f32), fix], axis=0)
        gv[j, tokens - 16 :, :] = both_rows.astype(bf16)
        put_block(w_values, normedt_ref, gv[j], j)

    @when_after(t_values + half_nb - 1)
    def _():
        rs[2][0].start(0)

    @when_after(t_values)
    def _():
        send_to(
            dbc.at[1 - core], dbc_land, dbc_sems.at[0], dbc_sems.at[1], head=1 - core
        ).wait()
        sext = sext_ref[core].astype(f32)
        taps = cs_ref[core]
        conv = conv_rows(sext, taps, HALO - CONV + 1, tokens)
        gs = (dbc[core] + dbc_land[...]) * silu_grad(conv)
        for k in range(CONV):
            first = HALO - CONV + 1 + k
            vec[0, nb, 2 + k : 3 + k, 0:LANES] = jnp.sum(
                sext[first : first + tokens, :] * gs, axis=0, keepdims=True
            )
        vec[0, nb, 2 + CONV : 3 + CONV, 0:LANES] = jnp.sum(gs, axis=0, keepdims=True)
        dbc[core] = gs
        sedge_own[...] = gs[0:8, :]
        send_to(
            sedge_own, sedge_land, sedge_sems.at[0], sedge_sems.at[1], seq=before_id
        ).start()

    @when_after(t_grad - 1)
    def _():
        rs[2][1].start(0)
        send_to(
            sedge_own, sedge_land, sedge_sems.at[0], sedge_sems.at[1], seq=before_id
        ).wait()
        taps = cs_ref[core]
        nxt = jnp.where(index == size - 1, 0.0, 1.0) * sedge_land[...]
        gs = jnp.concatenate([dbc[core], nxt], axis=0)
        total = taps[CONV - 1 : CONV, :] * gs[0:tokens, :]
        for k in range(CONV - 1):
            total = total + taps[k : k + 1, :] * gs[CONV - 1 - k : CONV - 1 - k + tokens, :]
        small[:, 0:LANES] = total.astype(bf16)
        group = width // 4
        for q in range(4):
            piece = mm(normedt_ref[q * group : (q + 1) * group, :], small[...]).astype(bf16)
            for b in range(size // 4):
                slot = slot_of(q * (size // 4) + b, 1, bits)
                w_small[slot] = piece[b * rows_own : (b + 1) * rows_own, :]
        rs_small.start(0)

    @pl.when((step_id >= t_grad) & (step_id < t_final))
    def _():
        j = step_id - t_grad
        part = mm(ggates[j], wi_ref[0], NT) + mm(gv[j], wi_ref[1], NT)

        @pl.when(j == 0)
        def _():
            first = part + mm(small[...], wsmall_ref[...], NT)
            for b in range(width // BLOCK):
                dys[b] = first[:, b * BLOCK : (b + 1) * BLOCK]

        @pl.when(j > 0)
        def _():
            for b in range(width // BLOCK):
                dys[b] += part[:, b * BLOCK : (b + 1) * BLOCK]

    @when_after(t_grad + half_nb)
    def _():
        rs[1][0].advance(0)
        rs[1][1].advance(0)

    @when_after(t_final - 1)
    def _():
        for c in range(chunks):
            rows = slice(c * CHUNK, (c + 1) * CHUNK)
            for b in range(width // BLOCK):
                acc_send[c, :, b * BLOCK : (b + 1) * BLOCK] = dys[b, rows, :].astype(bf16)
            send_to(
                acc_send.at[c], acc_land.at[c], acc_sems.at[0, c], acc_sems.at[1, c], head=1 - core
            ).start()

    @pl.when(step_id >= t_final)
    def _():
        c = step_id - t_final
        send_to(
            acc_send.at[c], acc_land.at[c], acc_sems.at[0, c], acc_sems.at[1, c], head=1 - core
        ).wait()
        here = pl.ds(pl.multiple_of(c * CHUNK, CHUNK), CHUNK)
        own_total = jnp.concatenate([dys[b, here, :] for b in range(width // BLOCK)], axis=1)
        total = own_total + acc_land[c].astype(f32)
        scale = scale_ref[:, 0:1]
        hat = hid_ref[...].astype(f32) * scale
        term = jnp.sum(total * hat, axis=0, keepdims=True)

        for b in range(width // BLOCK):
            piece = term[:, b * BLOCK : (b + 1) * BLOCK]
            vec[0, b, 7:8, :] = vec[0, b, 7:8, :] + piece

        ghat = total * gain_ref[...]
        mean = jnp.mean(ghat * hat, axis=1, keepdims=True)
        ghid_ref[...] = cot_ref[...].astype(f32) + scale * (ghat - hat * mean)

    @when_after(t_final + chunks - 1)
    def _():
        def add(bit):
            sum_copy(vec, vec_land, bit, index, vec_sems).wait()
            vec[bit + 1] = vec[bit] + vec_land[bit]

        for stage in range(1, bits):
            sum_copy(vec, vec_land, stage - 1, index, vec_sems).start()
            for g in range(2):
                for part in range(2):
                    rs[g][part].advance(stage)
            for part in range(2):
                rs[2][part].advance(stage - 1)
            rs_small.advance(stage - 1)
            add(stage - 1)
        sum_copy(vec, vec_land, bits - 1, index, vec_sems).start()
        for part in range(2):
            rs[2][part].advance(bits - 1)
        rs_small.advance(bits - 1)
        add(bits - 1)
        heads_ref[...] = vec[bits, nb, :, 0:LANES]
        for b in range(nb):
            sums_ref[:, b * BLOCK : (b + 1) * BLOCK] = vec[bits, b]


def back_call(
    gm_t, normed_t, coef, gains, run, step, slope, bc, sext, skip, decay, conv_shared, wsmall, gain,
    wout, y, gate, gate_gain, gated_w, vext, after, state_in, conv_values, runt, stept, both,
    hidden, cotangent, scale,
):
    width, tokens = normed_t.shape
    inner = y.shape[1]
    chunks = tokens // CHUNK
    nb = inner // BLOCK
    size = lax.axis_size("seq")
    bits = size.bit_length() - 1
    rows_own = width // size
    t_out, t_gate, t_scan, t_values, t_grad, t_final = (nb * i for i in range(1, 7))

    def column(start):
        return lambda s: jnp.clip(s - start, 0, nb - 1)

    def full(shape):
        return pl.BlockSpec(shape, lambda s: (0,) * len(shape), pipeline_mode=pl.Buffered(1))

    def cols(rows, start):
        at = column(start)
        return pl.BlockSpec((rows, BLOCK), lambda s: (0, at(s)))

    def scan_or_values(s):
        return jnp.where(s < t_values, column(t_scan)(s), column(t_values)(s))

    row_block = lambda w: pl.BlockSpec((CHUNK, w), lambda s: (jnp.clip(s - t_final, 0, chunks - 1), 0))
    row_single = lambda w: pl.BlockSpec(
        (CHUNK, w),
        lambda s: (jnp.clip(s - t_final, 0, chunks - 1), 0),
        pipeline_mode=pl.Buffered(1),
    )
    part_cols = inner // 2
    held = lambda: pltpu.VMEM((2, size, rows_own, part_cols), bf16)
    landing = lambda: tuple(
        pltpu.VMEM((2, size >> (s + 1), rows_own, part_cols), bf16) for s in range(bits)
    )
    sem = pltpu.SemaphoreType.DMA
    return pl.pallas_call(
        functools.partial(back_kernel, bits),
        grid=(6 * nb + chunks,),
        in_specs=[
            full((width, tokens)),
            full((width, tokens)),
            full((tokens, LANES)),
            full((size, LANES)),
            full((tokens, LANES)),
            full((tokens, LANES)),
            full((tokens, LANES)),
            full((tokens, 2 * STATE)),
            full((2, HALO + tokens, LANES)),
            full((1, LANES)),
            full((1, LANES)),
            full((2, CONV + 1, LANES)),
            full((width, 2 * LANES)),
            full((1, width)),
            cols(width, 0),
            cols(tokens, 0),
            cols(tokens, 0),
            cols(1, 0),
            cols(tokens, t_out),
            pl.BlockSpec(
                (HALO + tokens, BLOCK), lambda s: (0, column(t_scan)(s)), pipeline_mode=pl.Buffered(1)
            ),
            pl.BlockSpec((chunks, STATE, BLOCK), lambda s: (0, 0, column(t_scan)(s))),
            cols(STATE, t_scan),
            pl.BlockSpec((CONV + 1, BLOCK), lambda s: (0, scan_or_values(s))),
            pl.BlockSpec((1, 8, tokens), lambda s: (column(t_scan)(s), 0, 0)),
            pl.BlockSpec((1, 8, tokens), lambda s: (column(t_scan)(s), 0, 0)),
            pl.BlockSpec(
                (2, width, BLOCK), lambda s: (0, 0, column(t_grad)(s)), pipeline_mode=pl.Buffered(1)
            ),
            row_single(width),
            row_single(width),
            row_block(LANES),
        ],
        out_shape=[
            jax.ShapeDtypeStruct((rows_own, inner), f32),
            jax.ShapeDtypeStruct((rows_own, inner), f32),
            jax.ShapeDtypeStruct((rows_own, inner), f32),
            jax.ShapeDtypeStruct((rows_own, 2 * LANES), f32),
            jax.ShapeDtypeStruct((tokens, width), f32),
            jax.ShapeDtypeStruct((8, inner), f32),
            jax.ShapeDtypeStruct((8, LANES), f32),
        ],
        out_specs=[
            full((rows_own, inner)),
            full((rows_own, inner)),
            full((rows_own, inner)),
            full((rows_own, 2 * LANES)),
            row_block(width),
            pl.BlockSpec((8, inner), lambda s: (0, 0)),
            pl.BlockSpec((8, LANES), lambda s: (0, 0)),
        ],
        scratch_shapes=[
            held(), held(), held(),
            pltpu.VMEM((size, rows_own, 2 * LANES), bf16),
            landing(), landing(), landing(),
            tuple(pltpu.VMEM((size >> (s + 1), rows_own, 2 * LANES), bf16) for s in range(bits)),
            sem((7, bits)), sem((7, bits)),
            pltpu.VMEM((nb, tokens, BLOCK), bf16),
            pltpu.VMEM((chunks, CHUNK, width), bf16),
            pltpu.VMEM((chunks, CHUNK, width), bf16),
            sem((2, chunks)),
            pltpu.VMEM((nb, 8, BLOCK), f32),
            pltpu.VMEM((nb, 8, BLOCK), f32),
            pltpu.VMEM((nb, 8, BLOCK), f32),
            sem((2, nb)),
            pltpu.VMEM((2, tokens, LANES), f32),
            pltpu.VMEM((tokens, LANES), f32),
            sem((2,)),
            pltpu.VMEM((tokens, 2 * LANES), bf16),
            pltpu.VMEM((8, LANES), f32),
            pltpu.VMEM((8, LANES), f32),
            sem((2,)),
            pltpu.VMEM((bits + 1, nb + 1, 8, BLOCK), f32),
            pltpu.VMEM((bits, nb + 1, 8, BLOCK), f32),
            sem((2, bits)),
            pltpu.VMEM((chunks, CHUNK, CHUNK), f32),
            pltpu.VMEM((chunks, CHUNK, CHUNK), f32),
            pltpu.VMEM((STATE, tokens), bf16),
            pltpu.VMEM((chunks, CHUNK, CHUNK), f32),
            pltpu.VMEM((tokens, LANES), f32),
            pltpu.VMEM((8, LANES), f32),
            pltpu.VMEM((nb, 8, tokens), f32),
            pltpu.VMEM((tokens, LANES), f32),
            pltpu.VMEM((tokens, LANES), f32),
            pltpu.VMEM((tokens, LANES), f32),
            pltpu.VMEM((HALO + tokens, BLOCK), f32),
            pltpu.VMEM((tokens + 8, BLOCK), f32),
            pltpu.VMEM((nb, tokens, BLOCK), f32),
            pltpu.VMEM((nb, tokens, BLOCK), bf16),
            pltpu.VMEM((nb, 8, BLOCK), f32),
        ] + exchange_scratch(nb, size, bf16),
        compiler_params=pltpu.CompilerParams(
            collective_id=3, has_side_effects=True, vmem_limit_bytes=67043328
        ),
        name="back",
    )(
        gm_t, normed_t, coef, gains, run, step, slope, bc, sext, skip, decay, conv_shared, wsmall,
        gain, wout, y, gate, gate_gain, gated_w, vext, after, state_in, conv_values, runt, stept,
        both, hidden, cotangent, scale,
    )


def body(
    hidden, cotangent, norm_gain, proj_inner, proj_step, proj_shared, conv_values, conv_shared,
    step_bias, decay_log, skip_gain, gate_gain, proj_out,
):
    tokens = hidden.shape[0]
    inner = proj_inner.shape[2]
    heads = proj_step.shape[1]
    width = hidden.shape[1]
    size = lax.axis_size("seq")
    shared_here = conv_shared.shape[1] // lax.axis_size("head")
    shared_start = lax.axis_index("head") * shared_here
    both = jnp.transpose(proj_inner, (1, 0, 2))
    lanes = lambda v: jnp.pad(v, (0, LANES - heads))[None, :]
    wstep = jnp.pad(proj_step, ((0, 0), (0, LANES - heads)))
    bias, decay, skip = lanes(step_bias), lanes(decay_log), lanes(skip_gain)
    wshared_own = lax.dynamic_slice_in_dim(proj_shared, shared_start, shared_here, 1)
    (
        normed_t, norm_scale, gate_in, vext, after, y, gated_w, state_in, step, slope, run, runt,
        stept, sext, bc, gains, block_out, gm_t, coef,
    ) = forward_call(
        hidden, cotangent, norm_gain[None, :], both, wstep, proj_shared, conv_values, conv_shared,
        bias, decay, skip, gate_gain[None, :], proj_out,
    )
    (gout, ggw, gvw, gsmall, grad_hidden, sums, head_sums) = back_call(
        gm_t, normed_t, coef, gains, run, step, slope, bc, sext, skip, decay,
        conv_shared.reshape(CONV + 1, -1, LANES).transpose(1, 0, 2),
        jnp.concatenate([wshared_own, wstep], axis=1), norm_gain[None, :], proj_out, y, gate_in,
        gate_gain[None, :], gated_w, vext, after, state_in, conv_values, runt, stept, both, hidden,
        cotangent, norm_scale,
    )
    return (
        block_out,
        grad_hidden,
        sums[7],
        jnp.stack([ggw, gvw], axis=1),
        gsmall[:, shared_here : shared_here + heads],
        gsmall[:, :shared_here],
        sums[: CONV + 1],
        head_sums[2 : 3 + CONV],
        head_sums[0, :heads],
        head_sums[1, :heads],
        jnp.sum(sums[CONV + 2].reshape(heads, HEAD_DIM), axis=1),
        sums[CONV + 1],
        gout,
    )


def solution(mesh):
    return jax.shard_map(
        body,
        mesh=mesh,
        in_specs=(
            P("seq", None),
            P("seq", None),
            P(),
            P(None, None, "head"),
            P(None, "head"),
            P(),
            P(None, "head"),
            P(),
            P("head"),
            P("head"),
            P("head"),
            P("head"),
            P(None, "head"),
        ),
        out_specs=(
            P("seq", None),
            P("seq", None),
            P(),
            P("seq", None, "head"),
            P("seq", "head"),
            P("seq", "head"),
            P(None, "head"),
            P(None, "head"),
            P("head"),
            P("head"),
            P("head"),
            P("head"),
            P("seq", "head"),
        ),
        check_vma=False,
    )
```

```python
import functools

import jax
import jax.numpy as jnp
from jax import lax
from jax.experimental import pallas as pl
from jax.experimental.pallas import tpu as pltpu
from jax.sharding import PartitionSpec as P

HEAD_DIM = 64
STATE = 128
CONV = 4
INNER = 3072
CHUNK = 128
LANES = 128
BLOCK = 256
HALO = 16
BLOCK_HEADS = BLOCK // HEAD_DIM

norm_eps = 1e-05
highest = lax.Precision.HIGHEST
f32 = jnp.float32
bf16 = jnp.bfloat16
NN = (((1,), (0,)), ((), ()))
NT = (((1,), (1,)), ((), ()))
TN = (((0,), (0,)), ((), ()))


def flip(shard, bit):
    size = lax.axis_size("seq")
    return lax.ppermute(shard, "seq", [(i, i ^ (1 << bit)) for i in range(size)])


def swap(shard):
    return lax.ppermute(shard, "head", [(0, 1), (1, 0)])


def from_behind(shard, by):
    size = lax.axis_size("seq")
    pairs = [(i, i + by) for i in range(size) if 0 <= i + by < size]
    return lax.ppermute(shard, "seq", pairs)


def silu_grad(values):
    sigmoid = 1.0 / (1.0 + jnp.exp(-values))
    return sigmoid * (1.0 + values * (1.0 - sigmoid))


def silu(values):
    return values / (1.0 + jnp.exp(-values))


def mm(a, b, dims=NN):
    return lax.dot_general(a, b, dims, preferred_element_type=f32)


def parts(a):
    high = a.astype(bf16)
    return high, (a - high.astype(f32)).astype(bf16)


def mm_left(a, b, dims=NN):
    high, low = parts(a)
    return mm(high, b, dims) + mm(low, b, dims)


def mm_right(a, b, dims=NN):
    high, low = parts(b)
    return mm(a, high, dims) + mm(a, low, dims)


def mm_both(a, b, dims=NN):
    a_high, a_low = parts(a)
    b_high, b_low = parts(b)
    return mm(a_high, b_high, dims) + mm(a_low, b_high, dims) + mm(a_high, b_low, dims)


def mm_exact(a, b, dims=NN):
    return lax.dot_general(a, b, dims, precision=highest, preferred_element_type=f32)


def widen(cols):
    rows = cols.shape[0]
    lane = lax.broadcasted_iota(jnp.int32, (rows, LANES), 1)
    pieces = []
    for pair in range(BLOCK // LANES):
        first = jnp.broadcast_to(cols[:, 2 * pair : 2 * pair + 1], (rows, LANES))
        second = jnp.broadcast_to(cols[:, 2 * pair + 1 : 2 * pair + 2], (rows, LANES))
        pieces.append(jnp.where(lane < HEAD_DIM, first, second))
    return jnp.concatenate(pieces, axis=1)


def rolled(full, step):
    shift = lax.rem(LANES - BLOCK_HEADS * step, LANES)
    return pltpu.roll(full, shift, 1)


def causal():
    rows = lax.broadcasted_iota(jnp.int32, (CHUNK, CHUNK), 0)
    cols = lax.broadcasted_iota(jnp.int32, (CHUNK, CHUNK), 1)
    return rows >= cols


def conv_rows(ext, taps, first, rows):
    out = taps[CONV : CONV + 1, :]
    for k in range(CONV):
        out = out + taps[k : k + 1, :] * ext[first + k : first + k + rows, :]
    return out


def stack_pair(block):
    lane = lax.broadcasted_iota(jnp.int32, block.shape, 1)
    low = jnp.where(lane < HEAD_DIM, block, jnp.zeros_like(block))
    return low, block - low


class StateExchange:
    def __init__(self, index, size, reverse, own, landing, mixed, result, sems, gains):
        self.index, self.size, self.reverse = index, size, reverse
        self.own, self.landing, self.mixed, self.result = own, landing, mixed, result
        self.sems, self.gains = sems, gains

    def other(self, distance):
        return lax.rem(self.index + distance, self.size)

    def slot(self, source):
        return lax.rem(source - self.index - 1 + 2 * self.size, self.size)

    def send(self, j, value):
        share = value.shape[0] // self.size
        kind = self.own.dtype
        pieces = value.reshape(self.size, share, value.shape[1])
        self.own[j] = pieces.astype(kind)
        for d in range(1, self.size):
            pltpu.make_async_remote_copy(
                src_ref=self.own.at[j, self.other(d)],
                dst_ref=self.landing.at[j, self.size - d - 1],
                send_sem=self.sems.at[0, j],
                recv_sem=self.sems.at[1, j],
                device_id={"seq": self.other(d)},
                device_id_type=pl.DeviceIdType.MESH,
            ).start()

    def all_of(self, buffer, j, send, recv):
        return pltpu.make_async_remote_copy(
            src_ref=buffer.at[j, pl.ds(0, self.size - 1)],
            dst_ref=buffer.at[j, pl.ds(0, self.size - 1)],
            send_sem=self.sems.at[send, j],
            recv_sem=self.sems.at[recv, j],
            device_id={"seq": self.other(1)},
            device_id_type=pl.DeviceIdType.MESH,
        )

    def turn(self, j):
        self.all_of(self.landing, j, 0, 1).wait()
        kind = self.own.dtype
        self.landing[j, self.size - 1] = self.own[j, self.index]
        held = jnp.zeros(self.own.shape[2:], f32)
        order = range(self.size - 1, -1, -1) if self.reverse else range(self.size)
        for source in order:
            self.mixed[j, source] = held.astype(kind)
            gain = widen(rolled(self.gains[source : source + 1, :], j)[:, :BLOCK_HEADS])
            held = gain * held + self.landing[j, self.slot(source)].astype(f32)
        for d in range(1, self.size):
            pltpu.make_async_remote_copy(
                src_ref=self.mixed.at[j, self.other(d)],
                dst_ref=self.result.at[j, self.index],
                send_sem=self.sems.at[2, j],
                recv_sem=self.sems.at[3, j],
                device_id={"seq": self.other(d)},
                device_id_type=pl.DeviceIdType.MESH,
            ).start()

    def take(self, j):
        self.all_of(self.result, j, 2, 3).wait()
        self.result[j, self.index] = self.mixed[j, self.index]
        whole = self.result[j].astype(f32)
        return whole.reshape(whole.shape[0] * whole.shape[1], whole.shape[2])


def exchange_scratch(nb, size, kind):
    share = STATE // size
    return [pltpu.VMEM((nb, size, share, BLOCK), kind) for _ in range(4)] + [
        pltpu.SemaphoreType.DMA((4, nb))
    ]


def greet(index, core, size):
    barrier = pltpu.get_barrier_semaphore()
    for d in range(1, size):
        pl.semaphore_signal(
            barrier, inc=1, device_id={"seq": lax.rem(index + d, size)},
            device_id_type=pl.DeviceIdType.MESH,
        )
    pl.semaphore_signal(
        barrier, inc=1, device_id={"head": 1 - core}, device_id_type=pl.DeviceIdType.MESH
    )
    pl.semaphore_wait(barrier, size)


def send_to(src, dst, send_sem, recv_sem, **where):
    return pltpu.make_async_remote_copy(
        src_ref=src, dst_ref=dst, send_sem=send_sem, recv_sem=recv_sem, device_id=where,
        device_id_type=pl.DeviceIdType.MESH,
    )


def transposed(block):
    return block.astype(f32).T.astype(bf16)


def forward_kernel(
    size,
    hid_ref, gain_ref, wi_ref, wstep_ref, wshared_ref, cv_ref, cs_ref, bias_ref, decay_ref,
    skip_ref, ggain_ref, wout_ref, hrow_ref, crow_ref,
    normedt_ref, scale_ref, gate_ref, vext_ref, after_ref, y_ref, gw_ref, in_ref, step_ref,
    slope_ref, run_ref, runt_ref, stept_ref, sext_ref, bc_ref, gains_ref, out_ref, gmt_ref,
    coef_ref, near_ref,
    nx, halo, halo_sems, scores, bt, end_w, vwide, gates, ys, states, acc, acc_send,
    acc_land, acc_sems, squares, sq_land, sq_sems, totals, totals_land, totals_sems,
    near_land, near_sems, ex_own, ex_landing, ex_mixed, ex_result, ex_sems,
):
    step_id = pl.program_id(0)
    index = lax.axis_index("seq")
    core = lax.axis_index("head")
    tokens = hid_ref.shape[0]
    width = hid_ref.shape[1]
    chunks = tokens // CHUNK
    nb = gates.shape[0]
    t_mix, t_last = nb, 2 * nb
    half_width = width // 2
    exchange = StateExchange(
        index, size, False, ex_own, ex_landing, ex_mixed, ex_result, ex_sems, gains_ref
    )

    def norm_rows(rows):
        wide = rows.astype(f32)
        scale = lax.rsqrt(jnp.mean(wide * wide, axis=1, keepdims=True) + norm_eps)
        return (wide * scale * gain_ref[...]).astype(bf16), scale

    def totals_copy(d):
        return send_to(
            totals, totals_land.at[size - d - 1], totals_sems.at[0], totals_sems.at[1],
            seq=lax.rem(index + d, size),
        )

    @pl.when(step_id == 0)
    def _():
        @pl.loop(0, chunks)
        def _(i):
            start = pl.multiple_of(i * CHUNK, CHUNK)
            for part in range(2):
                at = pl.multiple_of(start + part * 64, 64)
                rows, scale = norm_rows(hid_ref[pl.ds(at, 64), :])
                nx[pl.ds(pl.multiple_of(HALO + at, HALO), 64), :] = rows
                scale_ref[pl.ds(at, 64), :] = jnp.broadcast_to(scale, (64, LANES))

        greet(index, core, size)
        after_id = lax.rem(index + 1, size)
        halo_copy = send_to(
            hid_ref.at[pl.ds(tokens - HALO, HALO)], halo, halo_sems.at[0], halo_sems.at[1],
            seq=after_id,
        )
        halo_copy.start()
        for c in range(chunks):
            for b in range(width // LANES):
                normedt_ref[b * LANES : (b + 1) * LANES, c * CHUNK : (c + 1) * CHUNK] = transposed(
                    nx[HALO + c * CHUNK : HALO + (c + 1) * CHUNK, b * LANES : (b + 1) * LANES]
                )
        raw = mm(nx[HALO:, :], wstep_ref[...]) + bias_ref[...]
        small = jnp.exp(-jnp.abs(raw))
        step = jnp.maximum(raw, 0.0) + jnp.log1p(small)
        step_ref[...] = step
        slope_ref[...] = 1.0 / (1.0 + jnp.exp(-raw))
        rate = -step * jnp.exp(decay_ref[...])
        tri = causal().astype(f32)
        total = jnp.zeros((1, LANES), f32)
        for c in range(chunks):
            rows = slice(c * CHUNK, (c + 1) * CHUNK)
            run = mm_exact(tri, rate[rows, :])
            run_ref[rows, :] = run
            total = total + run[CHUNK - 1 :, :]
            run_t = run.T
            step_t = step[rows, :].T
            for b in range(nb):
                heads = slice(BLOCK_HEADS * b, BLOCK_HEADS * (b + 1))
                runt_ref[b, 0:BLOCK_HEADS, rows] = run_t[heads, :]
                stept_ref[b, 0:BLOCK_HEADS, rows] = step_t[heads, :]
                runt_ref[b, BLOCK_HEADS:, rows] = jnp.zeros((8 - BLOCK_HEADS, CHUNK), f32)
                stept_ref[b, BLOCK_HEADS:, rows] = jnp.zeros((8 - BLOCK_HEADS, CHUNK), f32)
            end_w[rows, :] = step[rows, :] * jnp.exp(run[CHUNK - 1 :, :] - run)
        totals[...] = jnp.broadcast_to(jnp.exp(total), totals.shape)
        for d in range(1, size):
            totals_copy(d).start()
        halo_copy.wait()
        keep = jnp.where(index == 0, 0.0, 1.0)
        nx[0:HALO, :] = (norm_rows(halo[...])[0].astype(f32) * keep).astype(bf16)
        shared = mm(nx[...], wshared_ref[...]).astype(bf16)
        sext_ref[0] = shared[:, :STATE]
        sext_ref[1] = shared[:, STATE:]
        conv = conv_rows(shared.astype(f32), cs_ref[...], HALO - CONV + 1, tokens)
        act = silu(conv).astype(bf16)
        bc_ref[...] = act
        for c in range(chunks):
            rows = slice(c * CHUNK, (c + 1) * CHUNK)
            b_rows = act[rows, :STATE]
            c_rows = act[rows, STATE:]
            scores[c] = mm(c_rows, b_rows, NT)
            bt[:, rows] = transposed(b_rows)

    @pl.when(step_id < t_mix)
    def _():
        j = step_id
        values = mm(nx[...], wi_ref[1]).astype(bf16)
        vext_ref[...] = values
        vwide[...] = values.astype(f32)
        conv = conv_rows(vwide, cv_ref[...], HALO - CONV + 1, tokens)
        act = silu(conv).astype(bf16)
        run_cols = rolled(run_ref[...], j)
        end_cols = rolled(end_w[...], j)
        state = jnp.zeros((STATE, BLOCK), f32)
        for c in range(chunks):
            rows = slice(c * CHUNK, (c + 1) * CHUNK)
            weighted = act[rows, :].astype(f32) * widen(end_cols[rows, :BLOCK_HEADS])
            last = widen(jnp.exp(run_cols[(c + 1) * CHUNK - 1 : (c + 1) * CHUNK, :BLOCK_HEADS]))
            state = last * state + mm_right(bt[:, rows], weighted)
            after_ref[c] = state
            states[j, c] = state
        exchange.send(j, state)
        gate = mm(nx[HALO:, :], wi_ref[0])
        gate_ref[...] = gate
        gates[j] = gate
        mask = causal()
        skip = widen(rolled(skip_ref[...], j)[:, :BLOCK_HEADS])
        for c in range(chunks):
            rows = slice(c * CHUNK, (c + 1) * CHUNK)
            cols = run_cols[rows, :BLOCK_HEADS]
            x = act[rows, :]
            y_pairs = []
            for pair in range(BLOCK // LANES):
                mats = []
                for k in range(2):
                    head = 2 * pair + k
                    gap = cols[:, head : head + 1] - runt_ref[j, head : head + 1, rows]
                    decayed = jnp.exp(jnp.where(mask, gap, -1e30))
                    mats.append(scores[c] * decayed * stept_ref[j, head : head + 1, rows])
                low, high = stack_pair(x[:, pair * LANES : (pair + 1) * LANES])
                y_pairs.append(
                    mm_left(jnp.concatenate(mats, axis=1), jnp.concatenate([low, high], axis=0))
                )
            ys[j, rows, :] = jnp.concatenate(y_pairs, axis=1) + skip * x.astype(f32)

    @pl.when(step_id == 1)
    def _():
        pltpu.make_async_remote_copy(
            src_ref=totals_land.at[pl.ds(0, size - 1)],
            dst_ref=totals_land.at[pl.ds(0, size - 1)],
            send_sem=totals_sems.at[0], recv_sem=totals_sems.at[1],
            device_id={"seq": lax.rem(index + 1, size)},
            device_id_type=pl.DeviceIdType.MESH,
        ).wait()
        totals_land[size - 1] = totals[...]
        for source in range(size):
            gains_ref[source : source + 1, :] = totals_land[exchange.slot(source), 0:1, :]

    @pl.when((step_id >= 2) & (step_id < nb + 2))
    def _():
        exchange.turn(step_id - 2)

    def neighbour_copy(bit):
        mine = (index // (1 << bit)) % 2
        return send_to(
            normedt_ref.at[pl.ds(pl.multiple_of(core * half_width, half_width), half_width)],
            near_land.at[bit], near_sems.at[0, bit], near_sems.at[1, bit],
            seq=index + (1 - 2 * mine) * (1 << bit),
        )

    @pl.when(step_id == nb + 1)
    def _():
        for bit in range(2):
            neighbour_copy(bit).start()

    @pl.when((step_id >= t_mix) & (step_id < t_last))
    def _():
        j = step_id - t_mix
        entering = exchange.take(j)
        in_ref[...] = entering
        offsets = offsets_of(run_ref, chunks)
        gated = []
        for c in range(chunks):
            rows = slice(c * CHUNK, (c + 1) * CHUNK)
            grow = rolled(jnp.exp(run_ref[rows, :]), j)[:, :BLOCK_HEADS]
            base = rolled(jnp.exp(offsets[c]), j)[:, :BLOCK_HEADS]
            enter = widen(base) * entering
            if c:
                enter = enter + states[j, c - 1]
            y = ys[j, rows, :] + widen(grow) * mm_right(bc_ref[rows, STATE:], enter)
            y_ref[rows, :] = y
            out = y * silu(gates[j, rows, :])
            gw_ref[rows, :] = (out * ggain_ref[...]).astype(bf16)
            gated.append(
                jnp.broadcast_to(jnp.sum(out * out, axis=1, keepdims=True), (CHUNK, LANES))
            )
        part = mm(gw_ref[...], wout_ref[...], NT)
        block_squares = jnp.concatenate(gated, axis=0)

        @pl.when(j == 0)
        def _():
            acc[...] = part
            squares[...] = block_squares

        @pl.when(j > 0)
        def _():
            acc[...] += part
            squares[...] += block_squares

        @pl.when(j == nb - 1)
        def _():
            send_to(squares, sq_land, sq_sems.at[0], sq_sems.at[1], head=1 - core).start()
            for c in range(chunks):
                acc_send[c] = acc[c * CHUNK : (c + 1) * CHUNK, :].astype(bf16)
                send_to(
                    acc_send.at[c], acc_land.at[c], acc_sems.at[0, c], acc_sems.at[1, c],
                    head=1 - core,
                ).start()

    @pl.when(step_id >= t_last)
    def _():
        c = step_id - t_last

        @pl.when(c == 0)
        def _():
            send_to(squares, sq_land, sq_sems.at[0], sq_sems.at[1], head=1 - core).wait()

        send_to(
            acc_send.at[c], acc_land.at[c], acc_sems.at[0, c], acc_sems.at[1, c], head=1 - core
        ).wait()
        rows = pl.ds(pl.multiple_of(c * CHUNK, CHUNK), CHUNK)
        mixed = acc[rows, :] + acc_land[c].astype(f32)
        inverse = lax.rsqrt((squares[rows, 0:1] + sq_land[rows, 0:1]) / INNER + norm_eps)
        out_ref[...] = hrow_ref[...].astype(f32) + mixed * inverse
        cot = crow_ref[...].astype(f32)
        scaled = (cot * inverse).astype(bf16)
        for b in range(width // LANES):
            gmt_ref[b * LANES : (b + 1) * LANES, :] = transposed(
                scaled[:, b * LANES : (b + 1) * LANES]
            )
        grad_inverse = jnp.sum(cot * mixed, axis=1, keepdims=True)
        coef_ref[...] = jnp.broadcast_to(
            grad_inverse * inverse * inverse * inverse / INNER, (CHUNK, LANES)
        )

        @pl.when(c == chunks - 1)
        def _():
            for bit in range(2):
                neighbour_copy(bit).wait()
                near_ref[bit] = near_land[bit]


def offsets_of(run_ref, chunks):
    rows = [jnp.zeros((1, LANES), f32)]
    for c in range(chunks):
        rows.append(rows[-1] + run_ref[(c + 1) * CHUNK - 1 : (c + 1) * CHUNK, :])
    return rows


def forward_call(
    hidden, cotangent, gain, both, wstep, wshared, conv_values, conv_shared, bias, decay, skip,
    gate_gain, wout,
):
    tokens, width = hidden.shape
    inner = both.shape[2]
    chunks = tokens // CHUNK
    nb = inner // BLOCK
    size = lax.axis_size("seq")
    t_mix, t_last = nb, 2 * nb

    def at(start):
        return lambda s: jnp.clip(s - start, 0, nb - 1)

    def full(shape):
        return pl.BlockSpec(shape, lambda s: (0,) * len(shape), pipeline_mode=pl.Buffered(1))

    def cols(rows, start):
        return pl.BlockSpec((rows, BLOCK), lambda s: (0, at(start)(s)))

    row_of = lambda s: jnp.clip(s - t_last, 0, chunks - 1)
    row_block = lambda w: pl.BlockSpec((CHUNK, w), lambda s: (row_of(s), 0))
    outs = [
        ((width, tokens), bf16, full((width, tokens))),
        ((tokens, LANES), f32, full((tokens, LANES))),
        ((tokens, inner), f32, cols(tokens, 0)),
        ((HALO + tokens, inner), bf16, cols(HALO + tokens, 0)),
        (
            (chunks, STATE, inner), f32,
            pl.BlockSpec((chunks, STATE, BLOCK), lambda s: (0, 0, at(0)(s))),
        ),
        ((tokens, inner), f32, cols(tokens, t_mix)),
        ((tokens, inner), bf16, cols(tokens, t_mix)),
        ((STATE, inner), f32, cols(STATE, t_mix)),
        ((tokens, LANES), f32, full((tokens, LANES))),
        ((tokens, LANES), f32, full((tokens, LANES))),
        ((tokens, LANES), f32, full((tokens, LANES))),
        ((nb, 8, tokens), f32, full((nb, 8, tokens))),
        ((nb, 8, tokens), f32, full((nb, 8, tokens))),
        ((2, HALO + tokens, STATE), bf16, full((2, HALO + tokens, STATE))),
        ((tokens, 2 * STATE), bf16, full((tokens, 2 * STATE))),
        ((size, LANES), f32, full((size, LANES))),
        ((tokens, width), f32, row_block(width)),
        ((width, tokens), bf16, pl.BlockSpec((width, CHUNK), lambda s: (0, row_of(s)))),
        ((tokens, LANES), f32, row_block(LANES)),
        ((2, width // 2, tokens), bf16, full((2, width // 2, tokens))),
    ]
    sem = pltpu.SemaphoreType.DMA
    return pl.pallas_call(
        functools.partial(forward_kernel, size),
        grid=(2 * nb + chunks,),
        in_specs=[
            full((tokens, width)),
            full((1, width)),
            pl.BlockSpec((2, width, BLOCK), lambda s: (0, 0, at(0)(s))),
            full((width, LANES)),
            full((width, 2 * STATE)),
            cols(CONV + 1, 0),
            full((CONV + 1, 2 * STATE)),
            full((1, LANES)),
            full((1, LANES)),
            full((1, LANES)),
            cols(1, t_mix),
            cols(width, t_mix),
            row_block(width),
            row_block(width),
        ],
        out_shape=[jax.ShapeDtypeStruct(shape, kind) for shape, kind, _ in outs],
        out_specs=[spec for _, _, spec in outs],
        scratch_shapes=[
            pltpu.VMEM((HALO + tokens, width), bf16),
            pltpu.VMEM((HALO, width), bf16),
            sem((2,)),
            pltpu.VMEM((chunks, CHUNK, CHUNK), f32),
            pltpu.VMEM((STATE, tokens), bf16),
            pltpu.VMEM((tokens, LANES), f32),
            pltpu.VMEM((HALO + tokens, BLOCK), f32),
            pltpu.VMEM((nb, tokens, BLOCK), f32),
            pltpu.VMEM((nb, tokens, BLOCK), f32),
            pltpu.VMEM((nb, chunks, STATE, BLOCK), f32),
            pltpu.VMEM((tokens, width), f32),
            pltpu.VMEM((chunks, CHUNK, width), bf16),
            pltpu.VMEM((chunks, CHUNK, width), bf16),
            sem((2, chunks)),
            pltpu.VMEM((tokens, LANES), f32),
            pltpu.VMEM((tokens, LANES), f32),
            sem((2,)),
            pltpu.VMEM((8, LANES), f32),
            pltpu.VMEM((size, 8, LANES), f32),
            sem((2,)),
            pltpu.VMEM((2, width // 2, tokens), bf16),
            sem((2, 2)),
        ] + exchange_scratch(nb, size, f32),
        compiler_params=pltpu.CompilerParams(
            collective_id=1, has_side_effects=True, vmem_limit_bytes=67043328
        ),
        name="forward",
    )(
        hidden, gain, both, wstep, wshared, conv_values, conv_shared, bias, decay, skip, gate_gain,
        wout, hidden, cotangent,
    )


def order_rows(part, bits):
    order = list(range(bits))
    if part == 1 and bits > 1:
        order[0], order[1] = 1, 0
    return order


def order_columns(part, bits):
    return [bit for bit in range(bits) if bit != part] + [part]


def slot_of(owner, order):
    slot = 0
    for bit in order:
        slot = slot * 2 + ((owner >> bit) & 1)
    return slot


class Reduction:
    def __init__(self, held, landing, order, index, sems, put, put_other=None):
        self.held, self.landing, self.order = held, landing, order
        self.index, self.sems, self.put, self.put_other = index, sems, put, put_other
        self.stages = len(order)

    def place(self, stage):
        base = 0
        size = 1 << self.stages
        for s, bit in enumerate(self.order[: stage + 1]):
            mine = (self.index // (1 << bit)) % 2
            half = size >> (s + 1)
            keep, give = base + mine * half, base + (1 - mine) * half
            base = keep
        return keep, give, half

    def copy(self, stage):
        _, give, half = self.place(stage)
        bit = self.order[stage]
        mine = (self.index // (1 << bit)) % 2
        return send_to(
            self.held.at[pl.ds(give, half)], self.landing[stage],
            self.sems.at[0, stage], self.sems.at[1, stage],
            seq=self.index + (1 - 2 * mine) * (1 << bit),
        )

    def start(self, stage):
        self.copy(stage).start()

    def advance(self, stage):
        self.copy(stage).wait()
        keep, _, half = self.place(stage)
        if stage < self.stages - 1:

            @pl.loop(0, half)
            def _(i):
                total = self.held[keep + i].astype(f32) + self.landing[stage][i].astype(f32)
                self.held[keep + i] = total.astype(bf16)

            self.start(stage + 1)
        elif self.put_other is None:
            self.put(self.held[keep].astype(f32) + self.landing[stage][0].astype(f32))
        else:
            self.put(self.held[keep].astype(f32))
            self.put_other(self.landing[stage][0].astype(f32))


def sum_copy(acc, landing, bit, index, sems):
    mine = (index // (1 << bit)) % 2
    return pltpu.make_async_remote_copy(
        src_ref=acc.at[bit],
        dst_ref=landing.at[bit],
        send_sem=sems.at[0, bit],
        recv_sem=sems.at[1, bit],
        device_id={"seq": index + (1 - 2 * mine) * (1 << bit)},
        device_id_type=pl.DeviceIdType.MESH,
    )


def back_kernel(
    bits,
    gmt_ref, normedt_ref, near_ref, gw_ref, coef_ref, gains_ref, run_ref, step_ref, slope_ref,
    bc_ref, sext_ref, skip_ref, decay_ref, cs_ref, wsmall_ref, gain_ref,
    wout_ref, y_ref, gate_ref, ggain_ref, vext_ref, after_ref, in_ref, cv_ref, runt_ref,
    stept_ref, wi_ref,
    hid_ref, cot_ref, scale_ref,
    gout_ref, ggw_ref, gvw_ref, gsmall_ref, ghid_ref, sums_ref, heads_ref,
    w_out, w_gate, w_values, w_small,
    land_out, land_gate, land_values, land_small,
    rs_sems, near, near_sems,
    own_cols, other_cols, land_cols, cols_sems,
    gv, acc_send, acc_land, acc_sems,
    edge_own, edge_tail, edge_land, edge_sems,
    dbc, dbc_land, dbc_sems, small, sedge_own, sedge_land, sedge_sems,
    vec, vec_land, vec_sems,
    scores, scorest, ct, dscores, end_w, ends, dcols, xdu, dyc, xdus, vwide, gext,
    dys, ggates, term_gate, ex_own, ex_landing, ex_mixed, ex_result, ex_sems,
):
    step_id = pl.program_id(0)
    index = lax.axis_index("seq")
    core = lax.axis_index("head")
    size = 1 << bits
    tokens = y_ref.shape[0]
    chunks = tokens // CHUNK
    nb = ggates.shape[0]
    half_nb = nb // 2
    width = normedt_ref.shape[0]
    half_width = width // 2
    rows_own = width // size
    t_scan, t_grad, t_final = nb, 2 * nb, 3 * nb
    after_id = lax.rem(index + 1, size)
    before_id = lax.rem(index + size - 1, size)
    bit_of = lambda bit: (index // (1 << bit)) % 2
    flip_of = lambda bit: index + (1 - 2 * bit_of(bit)) * (1 << bit)

    def out_reduction(part):
        cols = w_out.shape[3]

        def put(value):
            gout_ref[:, part * cols : (part + 1) * cols] = value

        return Reduction(
            w_out.at[part], [ref.at[part] for ref in land_out], order_rows(part, bits), index,
            rs_sems.at[part], put,
        )

    def columns_reduction(g, part):
        held, landing, out = ((w_gate, land_gate, ggw_ref), (w_values, land_values, gvw_ref))[g]

        def put_half(half):
            def put(value):
                for b in range(half_nb):
                    out[part * half_nb + b, half] = value[:, b * LANES : (b + 1) * LANES]

            return put

        return Reduction(
            held.at[part], [ref.at[part] for ref in landing], order_columns(part, bits), index,
            rs_sems.at[2 + 2 * g + part], put_half(bit_of(part)), put_half(1 - bit_of(part)),
        )

    def put_small(value):
        gsmall_ref[...] = value

    rs_out = [out_reduction(part) for part in range(2)]
    rs_gate = [columns_reduction(0, part) for part in range(2)]
    rs_values = [columns_reduction(1, part) for part in range(2)]
    rs_small = Reduction(
        w_small, list(land_small), order_rows(1, bits), index, rs_sems.at[6], put_small
    )

    def when_after(step):
        return pl.when(step_id == step)

    exchange = StateExchange(
        index, size, True, ex_own, ex_landing, ex_mixed, ex_result, ex_sems, gains_ref
    )

    def near_copies(bit):
        half = pl.ds(pl.multiple_of(core * half_width, half_width), half_width)
        return (
            pltpu.make_async_copy(near_ref.at[bit], near.at[bit, half], near_sems.at[0, bit]),
            send_to(
                near_ref.at[bit], near.at[bit, half], near_sems.at[1, bit], near_sems.at[2, bit],
                head=1 - core,
            ),
        )

    @pl.when(step_id == 0)
    def _():
        greet(index, core, size)
        for bit in range(2):
            for copy in near_copies(bit):
                copy.start()
        for c in range(chunks):
            rows = slice(c * CHUNK, (c + 1) * CHUNK)
            ct[:, rows] = transposed(bc_ref[rows, STATE:])
            for b in range(width // LANES):
                acc_send[c, :, b * LANES : (b + 1) * LANES] = transposed(
                    gmt_ref[b * LANES : (b + 1) * LANES, rows]
                )

    group = width // 4
    owners = size // 4

    def scatter(piece, q, order, store):
        for b in range(owners):
            store(slot_of(q * owners + b, order), piece[b * rows_own : (b + 1) * rows_own, :])

    def put_out(part):
        cols = w_out.shape[3]
        for q in range(4):
            left = gmt_ref[q * group : (q + 1) * group, :]
            piece = mm(left, gw_ref[:, part * cols : (part + 1) * cols]).astype(bf16)

            def store(slot, value):
                w_out[part, slot] = value

            scatter(piece, q, order_rows(part, bits), store)

    def columns_copy(g, part):
        return send_to(
            other_cols.at[g, part], land_cols.at[g, part], cols_sems.at[0, g, part],
            cols_sems.at[1, g, part], seq=flip_of(part),
        )

    def split_block(g, j, value):
        part = j // half_nb
        mine = jnp.where(part == 0, bit_of(0), bit_of(1))
        place = pl.ds(pl.multiple_of((j % half_nb) * LANES, LANES), LANES)
        first, second = value[:, :LANES], value[:, LANES:]
        own_cols[g, part, :, place] = jnp.where(mine == 0, first, second)
        other_cols[g, part, :, place] = jnp.where(mine == 0, second, first)

    def put_columns(g, part):
        columns_copy(g, part).wait()
        held = (w_gate, w_values)[g]
        for q in range(4):
            rows = slice(q * group, (q + 1) * group)
            piece = mm(normedt_ref[rows, :], own_cols[g, part]) + mm(
                near[part, rows, :], land_cols[g, part]
            )

            def store(slot, value):
                held[part, slot] = value

            scatter(piece.astype(bf16), q, order_columns(part, bits), store)
        (rs_gate, rs_values)[g][part].start(0)

    @pl.when(step_id < t_scan)
    def _():
        j = step_id
        offsets = offsets_of(run_ref, chunks)
        own = jnp.zeros((STATE, BLOCK), f32)
        term = jnp.zeros((1, BLOCK), f32)
        for c in range(chunks):
            rows = slice(c * CHUNK, (c + 1) * CHUNK)
            ggw = mm(acc_send[c], wout_ref[...])
            y = y_ref[rows, :]
            gate = gate_ref[rows, :]
            sig = 1.0 / (1.0 + jnp.exp(-gate))
            act = gate * sig
            out = y * act
            term = term + jnp.sum(ggw * out, axis=0, keepdims=True)
            coef = jnp.concatenate([coef_ref[rows, 0:LANES]] * (BLOCK // LANES), axis=1)
            gg = ggw * ggain_ref[...] - coef * out
            dy = gg * act
            dys[j, rows, :] = dy
            ggate = (gg * y * (sig * (1.0 + gate * (1.0 - sig)))).astype(bf16)
            ggates[j, rows, :] = ggate
            grow = rolled(jnp.exp(run_ref[rows, :] + offsets[c]), j)[:, :BLOCK_HEADS]
            own = own + mm_right(ct[:, rows], dy * widen(grow))
        term_gate[j, 0:1, :] = term
        exchange.send(j, own)
        split_block(0, j, ggates[j])

    for part in range(2):

        @when_after(part)
        def _(part=part):
            put_out(part)
            rs_out[part].start(0)

    @pl.when((step_id >= 2) & (step_id < nb + 2))
    def _():
        exchange.turn(step_id - 2)

    @when_after(half_nb - 1)
    def _():
        columns_copy(0, 0).start()

    @when_after(nb - 1)
    def _():
        columns_copy(0, 1).start()
        for bit in range(2):
            for copy in near_copies(bit):
                copy.wait()

    mask = causal()
    rows_i = lax.broadcasted_iota(jnp.int32, (CHUNK, CHUNK), 0)
    cols_i = lax.broadcasted_iota(jnp.int32, (CHUNK, CHUNK), 1)
    mask_t = rows_i <= cols_i

    @pl.when(step_id == t_scan)
    def _():
        dbc[...] = jnp.zeros_like(dbc)
        dscores[...] = jnp.zeros_like(dscores)
        dcols[...] = jnp.zeros_like(dcols)
        xdu[...] = jnp.zeros_like(xdu)
        dyc[...] = jnp.zeros_like(dyc)
        xdus[...] = jnp.zeros_like(xdus)
        ends[...] = jnp.zeros_like(ends)
        vec[...] = jnp.zeros_like(vec)
        for c in range(chunks):
            rows = slice(c * CHUNK, (c + 1) * CHUNK)
            b_rows = bc_ref[rows, :STATE]
            c_rows = bc_ref[rows, STATE:]
            scores[c] = mm(c_rows, b_rows, NT)
            scorest[c] = mm(b_rows, c_rows, NT)
            run = run_ref[rows, :]
            end_w[rows, :] = jnp.exp(run[CHUNK - 1 :, :] - run)

    @pl.when((step_id >= t_scan) & (step_id < t_grad))
    def _():
        j = step_id - t_scan
        offsets = offsets_of(run_ref, chunks)
        vwide[...] = vext_ref[...].astype(f32)
        conv = conv_rows(vwide, cv_ref[...], HALO - CONV + 1, tokens)
        sig_all = 1.0 / (1.0 + jnp.exp(-conv))
        act = (conv * sig_all).astype(bf16)
        slope = sig_all * (1.0 + conv * (1.0 - sig_all))
        run_cols = rolled(run_ref[...], j)
        step_cols = rolled(step_ref[...], j)
        end_cols = rolled(end_w[...], j)
        skip = widen(rolled(skip_ref[...], j)[:, :BLOCK_HEADS])
        channel = lax.broadcasted_iota(jnp.int32, (BLOCK, LANES), 0) // HEAD_DIM
        lane = lax.broadcasted_iota(jnp.int32, (BLOCK, LANES), 1)
        pick = (lane == BLOCK_HEADS * j + channel).astype(bf16)
        lane_row = lax.broadcasted_iota(jnp.int32, (CHUNK, LANES), 1)
        dstate = exchange.take(j)
        dskip = jnp.zeros((1, BLOCK), f32)
        gext[tokens : tokens + 8, :] = jnp.zeros((8, BLOCK), f32)
        for c in reversed(range(chunks)):
            rows = slice(c * CHUNK, (c + 1) * CHUNK)
            cols = run_cols[rows, :BLOCK_HEADS]
            x = act[rows, :]
            wide_x = x.astype(f32)
            dy = dys[j, rows, :]
            b_rows = bc_ref[rows, :STATE]
            c_rows = bc_ref[rows, STATE:]
            grow = widen(jnp.exp(cols))
            tail = widen(end_cols[rows, :BLOCK_HEADS])
            step_w = widen(step_cols[rows, :BLOCK_HEADS])
            last = grow[CHUNK - 1 :, :]
            base = rolled(jnp.exp(offsets[c]), j)[:, :BLOCK_HEADS]
            enter = widen(base) * in_ref[...]
            if c:
                enter = enter + after_ref[c - 1]
            du_state = tail * mm_right(b_rows, dstate)
            carried = grow * mm_right(c_rows, enter)
            weighted = wide_x * (tail * step_w)
            grown = dy * grow
            dbc[0, rows, :] += mm_both(weighted, dstate, NT)
            dbc[1, rows, :] += mm_both(grown, enter, NT)
            hold = last * jnp.sum(dstate * enter, axis=0, keepdims=True)
            ends[c : c + 1, :] += mm_exact(
                jnp.broadcast_to(hold, (8, BLOCK)), pick.astype(f32)
            )[:1, :]
            dstate = last * dstate + mm_right(ct[:, rows], grown)
            du_pairs = []
            col_sum = jnp.zeros((CHUNK, LANES), f32)
            for pair in range(BLOCK // LANES):
                lanes = slice(pair * LANES, (pair + 1) * LANES)
                low, high = stack_pair(dy[:, lanes])
                both = jnp.concatenate([low, high], axis=0)
                dmat = mm_left(both, x[:, lanes], NT)
                mats = []
                for k in range(2):
                    head = 2 * pair + k
                    col = cols[:, head : head + 1]
                    row = runt_ref[0, head : head + 1, rows]
                    keep = jnp.exp(jnp.where(mask, col - row, -1e30))
                    piece = dmat[k * CHUNK : (k + 1) * CHUNK, :] * keep
                    piece = piece * stept_ref[0, head : head + 1, rows]
                    dscores[c] += piece
                    full = piece * scores[c]
                    col_sum = jnp.where(
                        lane_row == BLOCK_HEADS * j + head,
                        jnp.sum(full, axis=1, keepdims=True),
                        col_sum,
                    )
                    dcols[j, head : head + 1, rows] = jnp.sum(full, axis=0, keepdims=True)
                    keep_t = jnp.exp(jnp.where(mask_t, row - col, -1e30))
                    mats.append(scorest[c] * keep_t)
                du_pairs.append(mm_both(jnp.concatenate(mats, axis=1), both))
            dyc[rows, :] += col_sum
            du = jnp.concatenate(du_pairs, axis=1) + du_state
            xdu[rows, :] += mm_left(wide_x * du, pick)
            dyc[rows, :] += mm_left(dy * carried, pick)
            xdus[rows, :] += mm_left(wide_x * du_state, pick)
            dskip = dskip + jnp.sum(dy * wide_x, axis=0, keepdims=True)
            gext[rows, :] = (step_w * du + skip * dy) * slope[rows, :]
        gconv = gext[0:tokens, :]
        for k in range(CONV):
            first = HALO - CONV + 1 + k
            vec[0, j, k : k + 1, :] = jnp.sum(
                vwide[first : first + tokens, :] * gconv, axis=0, keepdims=True
            )
        vec[0, j, CONV : CONV + 1, :] = jnp.sum(gconv, axis=0, keepdims=True)
        vec[0, j, CONV + 1 : CONV + 2, :] = term_gate[j, 0:1, :]
        vec[0, j, CONV + 2 : CONV + 3, :] = dskip
        total = cv_ref[CONV - 1 : CONV, :] * gconv
        for k in range(CONV - 1):
            total = total + cv_ref[k : k + 1, :] * gext[CONV - 1 - k : CONV - 1 - k + tokens, :]
        gv[j] = total.astype(bf16)
        edge_tail[j, 0:8, :] = total[tokens - 8 :, :]
        edge_tail[j, 8 : 8 + CONV + 1, :] = cv_ref[...]
        edge_own[j] = gconv[0:8, :]
        send_to(
            edge_own.at[j], edge_land.at[j], edge_sems.at[0, j], edge_sems.at[1, j], seq=before_id
        ).start()

    def finish_block(j):
        send_to(
            edge_own.at[j], edge_land.at[j], edge_sems.at[0, j], edge_sems.at[1, j], seq=before_id
        ).wait()
        nxt = jnp.where(index == size - 1, 0.0, 1.0) * edge_land[j]
        row8 = lax.broadcasted_iota(jnp.int32, (8, BLOCK), 0)
        fix = edge_tail[j, 0:8, :]
        for k in range(CONV - 1):
            ahead = CONV - 1 - k
            moved = pltpu.roll(nxt, 8 - ahead, 0)
            fix = fix + jnp.where(row8 >= 8 - ahead, edge_tail[j, 8 + k : 9 + k, :] * moved, 0.0)
        both_rows = jnp.concatenate([gv[j, tokens - 16 : tokens - 8, :].astype(f32), fix], axis=0)
        gv[j, tokens - 16 :, :] = both_rows.astype(bf16)
        split_block(1, j, gv[j])

    @pl.when((step_id > t_scan) & (step_id <= t_grad))
    def _():
        finish_block(step_id - t_scan - 1)

    @when_after(t_scan)
    def _():
        rs_out[0].advance(0)

    @when_after(t_scan + 1)
    def _():
        put_columns(0, 0)
        rs_out[1].advance(0)

    @when_after(t_scan + 2)
    def _():
        put_columns(0, 1)

    @when_after(t_scan + half_nb)
    def _():
        columns_copy(1, 0).start()
        rs_out[0].advance(1)
        rs_out[1].advance(1)

    @when_after(t_grad - 1)
    def _():
        rs_gate[0].advance(0)
        rs_gate[1].advance(0)
        rs_out[0].advance(2)
        rs_out[1].advance(2)

    @when_after(t_grad - 1)
    def _():
        tri = mask.astype(f32)
        tri_t = mask_t.astype(f32)
        strict = (rows_i > cols_i).astype(f32)
        decay = jnp.exp(decay_ref[...])
        bias_sum = jnp.zeros((1, LANES), f32)
        decay_sum = jnp.zeros((1, LANES), f32)
        for c in range(chunks):
            rows = slice(c * CHUNK, (c + 1) * CHUNK)
            step = step_ref[rows, :]
            col_rows = [dcols[b, 0:BLOCK_HEADS, rows] for b in range(nb)]
            rest = LANES - BLOCK_HEADS * nb
            col_rows.append(jnp.zeros((rest, CHUNK), f32))
            dlog = dyc[rows, :] - jnp.concatenate(col_rows, axis=0).T
            drate = (
                mm_exact(tri_t, dlog)
                + mm_exact(strict, xdus[rows, :] * step)
                + ends[c : c + 1, :]
            )
            dstep = xdu[rows, :] - decay * drate
            draw = dstep * slope_ref[rows, :]
            small[rows, LANES:] = draw.astype(bf16)
            bias_sum = bias_sum + jnp.sum(draw, axis=0, keepdims=True)
            decay_sum = decay_sum - jnp.sum(drate * step, axis=0, keepdims=True) * decay
            b_rows = bc_ref[rows, :STATE]
            c_rows = bc_ref[rows, STATE:]
            high, low = parts(dscores[c])
            dbc[1, rows, :] += mm(high, b_rows) + mm(low, b_rows)
            dbc[0, rows, :] += mm(high, c_rows, TN) + mm(low, c_rows, TN)
        vec[0, nb, 0:1, 0:LANES] = bias_sum
        vec[0, nb, 1:2, 0:LANES] = decay_sum
        send_to(
            dbc.at[1 - core], dbc_land, dbc_sems.at[0], dbc_sems.at[1], head=1 - core
        ).start()

    @when_after(t_grad)
    def _():
        columns_copy(1, 1).start()

    @when_after(t_grad)
    def _():
        send_to(
            dbc.at[1 - core], dbc_land, dbc_sems.at[0], dbc_sems.at[1], head=1 - core
        ).wait()
        sext = sext_ref[core].astype(f32)
        taps = cs_ref[core]
        conv = conv_rows(sext, taps, HALO - CONV + 1, tokens)
        gs = (dbc[core] + dbc_land[...]) * silu_grad(conv)
        for k in range(CONV):
            first = HALO - CONV + 1 + k
            vec[0, nb, 2 + k : 3 + k, 0:LANES] = jnp.sum(
                sext[first : first + tokens, :] * gs, axis=0, keepdims=True
            )
        vec[0, nb, 2 + CONV : 3 + CONV, 0:LANES] = jnp.sum(gs, axis=0, keepdims=True)
        dbc[core] = gs
        sedge_own[...] = gs[0:8, :]
        send_to(
            sedge_own, sedge_land, sedge_sems.at[0], sedge_sems.at[1], seq=before_id
        ).start()

    @when_after(t_grad + 1)
    def _():
        send_to(
            sedge_own, sedge_land, sedge_sems.at[0], sedge_sems.at[1], seq=before_id
        ).wait()
        taps = cs_ref[core]
        nxt = jnp.where(index == size - 1, 0.0, 1.0) * sedge_land[...]
        gs = jnp.concatenate([dbc[core], nxt], axis=0)
        total = taps[CONV - 1 : CONV, :] * gs[0:tokens, :]
        for k in range(CONV - 1):
            total = total + taps[k : k + 1, :] * gs[CONV - 1 - k : CONV - 1 - k + tokens, :]
        small[:, 0:LANES] = total.astype(bf16)
        for q in range(4):
            piece = mm(normedt_ref[q * group : (q + 1) * group, :], small[...]).astype(bf16)

            def store(slot, value):
                w_small[slot] = value

            scatter(piece, q, order_rows(1, bits), store)
        rs_small.start(0)

    @pl.when((step_id >= t_grad) & (step_id < t_final))
    def _():
        j = step_id - t_grad
        part = mm(ggates[j], wi_ref[0], NT) + mm(gv[j], wi_ref[1], NT)

        @pl.when(j == 0)
        def _():
            for b in range(width // BLOCK):
                dys[b] = part[:, b * BLOCK : (b + 1) * BLOCK]

        @pl.when(j > 0)
        def _():
            for b in range(width // BLOCK):
                dys[b] += part[:, b * BLOCK : (b + 1) * BLOCK]

    @when_after(t_grad + 2)
    def _():
        put_columns(1, 0)
        rs_gate[0].advance(1)
        rs_gate[1].advance(1)

    @when_after(t_grad + half_nb + 1)
    def _():
        put_columns(1, 1)
        rest = mm(small[...], wsmall_ref[...], NT)
        for b in range(width // BLOCK):
            dys[b] += rest[:, b * BLOCK : (b + 1) * BLOCK]

    @when_after(t_final - 1)
    def _():
        for c in range(chunks):
            rows = slice(c * CHUNK, (c + 1) * CHUNK)
            for b in range(width // BLOCK):
                acc_send[c, :, b * BLOCK : (b + 1) * BLOCK] = dys[b, rows, :].astype(bf16)
            send_to(
                acc_send.at[c], acc_land.at[c], acc_sems.at[0, c], acc_sems.at[1, c], head=1 - core
            ).start()

    @pl.when(step_id >= t_final)
    def _():
        c = step_id - t_final
        send_to(
            acc_send.at[c], acc_land.at[c], acc_sems.at[0, c], acc_sems.at[1, c], head=1 - core
        ).wait()
        here = pl.ds(pl.multiple_of(c * CHUNK, CHUNK), CHUNK)
        own_total = jnp.concatenate([dys[b, here, :] for b in range(width // BLOCK)], axis=1)
        total = own_total + acc_land[c].astype(f32)
        scale = scale_ref[:, 0:1]
        hat = hid_ref[...].astype(f32) * scale
        term = jnp.sum(total * hat, axis=0, keepdims=True)

        for b in range(width // BLOCK):
            piece = term[:, b * BLOCK : (b + 1) * BLOCK]
            vec[0, b, 7:8, :] = vec[0, b, 7:8, :] + piece

        ghat = total * gain_ref[...]
        mean = jnp.mean(ghat * hat, axis=1, keepdims=True)
        ghid_ref[...] = cot_ref[...].astype(f32) + scale * (ghat - hat * mean)

    @when_after(t_final + chunks - 1)
    def _():
        def add(bit):
            sum_copy(vec, vec_land, bit, index, vec_sems).wait()
            vec[bit + 1] = vec[bit] + vec_land[bit]

        for part in range(2):
            for stage in range(3, bits):
                rs_out[part].advance(stage)
        rs_small.advance(0)
        for stage in range(bits):
            sum_copy(vec, vec_land, stage, index, vec_sems).start()
            if stage + 2 < bits:
                for part in range(2):
                    rs_gate[part].advance(stage + 2)
            for part in range(2):
                rs_values[part].advance(stage)
            if stage + 1 < bits:
                rs_small.advance(stage + 1)
            add(stage)
        heads_ref[...] = vec[bits, nb, :, 0:LANES]
        for b in range(nb):
            sums_ref[:, b * BLOCK : (b + 1) * BLOCK] = vec[bits, b]


def back_call(
    gm_t, normed_t, near, gated_w, coef, gains, run, step, slope, bc, sext, skip, decay,
    conv_shared, wsmall, gain, wout, y, gate, gate_gain, vext, after, state_in, conv_values, runt, stept, both,
    hidden, cotangent, scale,
):
    width, tokens = normed_t.shape
    inner = y.shape[1]
    chunks = tokens // CHUNK
    nb = inner // BLOCK
    size = lax.axis_size("seq")
    bits = size.bit_length() - 1
    rows_own = width // size
    t_scan, t_grad, t_final = nb, 2 * nb, 3 * nb

    def column(start):
        return lambda s: jnp.clip(s - start, 0, nb - 1)

    def full(shape):
        return pl.BlockSpec(shape, lambda s: (0,) * len(shape), pipeline_mode=pl.Buffered(1))

    def cols(rows, start):
        at = column(start)
        return pl.BlockSpec((rows, BLOCK), lambda s: (0, at(s)))

    row_block = lambda w: pl.BlockSpec((CHUNK, w), lambda s: (jnp.clip(s - t_final, 0, chunks - 1), 0))
    row_single = lambda w: pl.BlockSpec(
        (CHUNK, w),
        lambda s: (jnp.clip(s - t_final, 0, chunks - 1), 0),
        pipeline_mode=pl.Buffered(1),
    )
    held = lambda cols: pltpu.VMEM((2, size, rows_own, cols), bf16)
    landing = lambda cols: tuple(
        pltpu.VMEM((2, size >> (s + 1), rows_own, cols), bf16) for s in range(bits)
    )
    columns = lambda: pltpu.VMEM((2, 2, tokens, inner // 4), bf16)
    sem = pltpu.SemaphoreType.DMA
    return pl.pallas_call(
        functools.partial(back_kernel, bits),
        grid=(3 * nb + chunks,),
        in_specs=[
            full((width, tokens)),
            full((width, tokens)),
            pl.BlockSpec(memory_space=pl.ANY),
            full((tokens, inner)),
            full((tokens, LANES)),
            full((size, LANES)),
            full((tokens, LANES)),
            full((tokens, LANES)),
            full((tokens, LANES)),
            full((tokens, 2 * STATE)),
            full((2, HALO + tokens, LANES)),
            full((1, LANES)),
            full((1, LANES)),
            full((2, CONV + 1, LANES)),
            full((width, 2 * LANES)),
            full((1, width)),
            cols(width, 0),
            cols(tokens, 0),
            cols(tokens, 0),
            cols(1, 0),
            pl.BlockSpec(
                (HALO + tokens, BLOCK), lambda s: (0, column(t_scan)(s)), pipeline_mode=pl.Buffered(1)
            ),
            pl.BlockSpec((chunks, STATE, BLOCK), lambda s: (0, 0, column(t_scan)(s))),
            cols(STATE, t_scan),
            cols(CONV + 1, t_scan),
            pl.BlockSpec((1, 8, tokens), lambda s: (column(t_scan)(s), 0, 0)),
            pl.BlockSpec((1, 8, tokens), lambda s: (column(t_scan)(s), 0, 0)),
            pl.BlockSpec(
                (2, width, BLOCK), lambda s: (0, 0, column(t_grad)(s)), pipeline_mode=pl.Buffered(1)
            ),
            row_single(width),
            row_single(width),
            row_block(LANES),
        ],
        out_shape=[
            jax.ShapeDtypeStruct((rows_own, inner), f32),
            jax.ShapeDtypeStruct((nb, 2, rows_own, LANES), f32),
            jax.ShapeDtypeStruct((nb, 2, rows_own, LANES), f32),
            jax.ShapeDtypeStruct((rows_own, 2 * LANES), f32),
            jax.ShapeDtypeStruct((tokens, width), f32),
            jax.ShapeDtypeStruct((8, inner), f32),
            jax.ShapeDtypeStruct((8, LANES), f32),
        ],
        out_specs=[
            full((rows_own, inner)),
            full((nb, 2, rows_own, LANES)),
            full((nb, 2, rows_own, LANES)),
            full((rows_own, 2 * LANES)),
            row_block(width),
            pl.BlockSpec((8, inner), lambda s: (0, 0)),
            pl.BlockSpec((8, LANES), lambda s: (0, 0)),
        ],
        scratch_shapes=[
            held(inner // 2), held(inner // 4), held(inner // 4),
            pltpu.VMEM((size, rows_own, 2 * LANES), bf16),
            landing(inner // 2), landing(inner // 4), landing(inner // 4),
            tuple(pltpu.VMEM((size >> (s + 1), rows_own, 2 * LANES), bf16) for s in range(bits)),
            sem((7, 2, bits)),
            pltpu.VMEM((2, width, tokens), bf16), sem((3, 2)),
            columns(), columns(), columns(), sem((2, 2, 2)),
            pltpu.VMEM((nb, tokens, BLOCK), bf16),
            pltpu.VMEM((chunks, CHUNK, width), bf16),
            pltpu.VMEM((chunks, CHUNK, width), bf16),
            sem((2, chunks)),
            pltpu.VMEM((nb, 8, BLOCK), f32),
            pltpu.VMEM((nb, 16, BLOCK), f32),
            pltpu.VMEM((nb, 8, BLOCK), f32),
            sem((2, nb)),
            pltpu.VMEM((2, tokens, LANES), f32),
            pltpu.VMEM((tokens, LANES), f32),
            sem((2,)),
            pltpu.VMEM((tokens, 2 * LANES), bf16),
            pltpu.VMEM((8, LANES), f32),
            pltpu.VMEM((8, LANES), f32),
            sem((2,)),
            pltpu.VMEM((bits + 1, nb + 1, 8, BLOCK), f32),
            pltpu.VMEM((bits, nb + 1, 8, BLOCK), f32),
            sem((2, bits)),
            pltpu.VMEM((chunks, CHUNK, CHUNK), f32),
            pltpu.VMEM((chunks, CHUNK, CHUNK), f32),
            pltpu.VMEM((STATE, tokens), bf16),
            pltpu.VMEM((chunks, CHUNK, CHUNK), f32),
            pltpu.VMEM((tokens, LANES), f32),
            pltpu.VMEM((8, LANES), f32),
            pltpu.VMEM((nb, 8, tokens), f32),
            pltpu.VMEM((tokens, LANES), f32),
            pltpu.VMEM((tokens, LANES), f32),
            pltpu.VMEM((tokens, LANES), f32),
            pltpu.VMEM((HALO + tokens, BLOCK), f32),
            pltpu.VMEM((tokens + 8, BLOCK), f32),
            pltpu.VMEM((nb, tokens, BLOCK), f32),
            pltpu.VMEM((nb, tokens, BLOCK), bf16),
            pltpu.VMEM((nb, 8, BLOCK), f32),
        ] + exchange_scratch(nb, size, bf16),
        compiler_params=pltpu.CompilerParams(
            collective_id=3, has_side_effects=True, vmem_limit_bytes=67043328
        ),
        name="back",
    )(
        gm_t, normed_t, near, gated_w, coef, gains, run, step, slope, bc, sext, skip, decay,
        conv_shared, wsmall, gain, wout, y, gate, gate_gain, vext, after, state_in, conv_values,
        runt, stept,
        both, hidden, cotangent, scale,
    )


def body(
    hidden, cotangent, norm_gain, proj_inner, proj_step, proj_shared, conv_values, conv_shared,
    step_bias, decay_log, skip_gain, gate_gain, proj_out,
):
    tokens = hidden.shape[0]
    inner = proj_inner.shape[2]
    heads = proj_step.shape[1]
    width = hidden.shape[1]
    size = lax.axis_size("seq")
    shared_here = conv_shared.shape[1] // lax.axis_size("head")
    shared_start = lax.axis_index("head") * shared_here
    both = jnp.transpose(proj_inner, (1, 0, 2))
    lanes = lambda v: jnp.pad(v, (0, LANES - heads))[None, :]
    wstep = jnp.pad(proj_step, ((0, 0), (0, LANES - heads)))
    bias, decay, skip = lanes(step_bias), lanes(decay_log), lanes(skip_gain)
    wshared_own = lax.dynamic_slice_in_dim(proj_shared, shared_start, shared_here, 1)
    (
        normed_t, norm_scale, gate_in, vext, after, y, gated_w, state_in, step, slope, run, runt,
        stept, sext, bc, gains, block_out, gm_t, coef, near,
    ) = forward_call(
        hidden, cotangent, norm_gain[None, :], both, wstep, proj_shared, conv_values, conv_shared,
        bias, decay, skip, gate_gain[None, :], proj_out,
    )
    (gout, ggw, gvw, gsmall, grad_hidden, sums, head_sums) = back_call(
        gm_t, normed_t, near, gated_w, coef, gains, run, step, slope, bc, sext, skip, decay,
        conv_shared.reshape(CONV + 1, -1, LANES).transpose(1, 0, 2),
        jnp.concatenate([wshared_own, wstep], axis=1), norm_gain[None, :], proj_out, y, gate_in,
        gate_gain[None, :], vext, after, state_in, conv_values, runt, stept, both, hidden,
        cotangent, norm_scale,
    )
    return (
        block_out,
        grad_hidden,
        sums[7],
        jnp.stack([ggw, gvw]).transpose(3, 0, 1, 2, 4).reshape(-1, 2, inner),
        gsmall[:, shared_here : shared_here + heads],
        gsmall[:, :shared_here],
        sums[: CONV + 1],
        head_sums[2 : 3 + CONV],
        head_sums[0, :heads],
        head_sums[1, :heads],
        jnp.sum(sums[CONV + 2].reshape(heads, HEAD_DIM), axis=1),
        sums[CONV + 1],
        gout,
    )


def solution(mesh):
    return jax.shard_map(
        body,
        mesh=mesh,
        in_specs=(
            P("seq", None),
            P("seq", None),
            P(),
            P(None, None, "head"),
            P(None, "head"),
            P(),
            P(None, "head"),
            P(),
            P("head"),
            P("head"),
            P("head"),
            P("head"),
            P(None, "head"),
        ),
        out_specs=(
            P("seq", None),
            P("seq", None),
            P(),
            P("seq", None, "head"),
            P("seq", "head"),
            P("seq", "head"),
            P(None, "head"),
            P(None, "head"),
            P("head"),
            P("head"),
            P("head"),
            P("head"),
            P("seq", "head"),
        ),
        check_vma=False,
    )
```

```python
import functools

import jax
import jax.numpy as jnp
from jax import lax
from jax.experimental import pallas as pl
from jax.experimental.pallas import tpu as pltpu
from jax.sharding import PartitionSpec as P

HEAD_DIM = 64
STATE = 128
CONV = 4
INNER = 3072
CHUNK = 128
LANES = 128
BLOCK = 256
HALO = 16
BLOCK_HEADS = BLOCK // HEAD_DIM

norm_eps = 1e-05
highest = lax.Precision.HIGHEST
f32 = jnp.float32
bf16 = jnp.bfloat16
NN = (((1,), (0,)), ((), ()))
NT = (((1,), (1,)), ((), ()))
TN = (((0,), (0,)), ((), ()))


def flip(shard, bit):
    size = lax.axis_size("seq")
    return lax.ppermute(shard, "seq", [(i, i ^ (1 << bit)) for i in range(size)])


def swap(shard):
    return lax.ppermute(shard, "head", [(0, 1), (1, 0)])


def from_behind(shard, by):
    size = lax.axis_size("seq")
    pairs = [(i, i + by) for i in range(size) if 0 <= i + by < size]
    return lax.ppermute(shard, "seq", pairs)


def silu_grad(values):
    sigmoid = 1.0 / (1.0 + jnp.exp(-values))
    return sigmoid * (1.0 + values * (1.0 - sigmoid))


def silu(values):
    return values / (1.0 + jnp.exp(-values))


def mm(a, b, dims=NN):
    return lax.dot_general(a, b, dims, preferred_element_type=f32)


def parts(a):
    high = a.astype(bf16)
    return high, (a - high.astype(f32)).astype(bf16)


def along(pieces, dims, side):
    return jnp.concatenate(pieces, axis=dims[0][side][0])


def mm_left(a, b, dims=NN):
    return mm(along(parts(a), dims, 0), along([b, b], dims, 1), dims)


def mm_right(a, b, dims=NN):
    return mm(along([a, a], dims, 0), along(parts(b), dims, 1), dims)


def mm_both(a, b, dims=NN):
    a_high, a_low = parts(a)
    b_high, b_low = parts(b)
    return mm(
        along([a_high, a_low, a_high], dims, 0), along([b_high, b_high, b_low], dims, 1), dims
    )


def mm_exact(a, b, dims=NN):
    return lax.dot_general(a, b, dims, precision=highest, preferred_element_type=f32)


def widen(cols):
    rows = cols.shape[0]
    lane = lax.broadcasted_iota(jnp.int32, (rows, LANES), 1)
    pieces = []
    for pair in range(BLOCK // LANES):
        first = jnp.broadcast_to(cols[:, 2 * pair : 2 * pair + 1], (rows, LANES))
        second = jnp.broadcast_to(cols[:, 2 * pair + 1 : 2 * pair + 2], (rows, LANES))
        pieces.append(jnp.where(lane < HEAD_DIM, first, second))
    return jnp.concatenate(pieces, axis=1)


def rolled(full, step):
    shift = lax.rem(LANES - BLOCK_HEADS * step, LANES)
    return pltpu.roll(full, shift, 1)


def causal():
    rows = lax.broadcasted_iota(jnp.int32, (CHUNK, CHUNK), 0)
    cols = lax.broadcasted_iota(jnp.int32, (CHUNK, CHUNK), 1)
    return rows >= cols


def conv_rows(ext, taps, first, rows):
    out = taps[CONV : CONV + 1, :]
    for k in range(CONV):
        out = out + taps[k : k + 1, :] * ext[first + k : first + k + rows, :]
    return out


def stack_pair(block):
    lane = lax.broadcasted_iota(jnp.int32, block.shape, 1)
    low = jnp.where(lane < HEAD_DIM, block, jnp.zeros_like(block))
    return low, block - low


class StateExchange:
    def __init__(self, index, size, reverse, own, landing, mixed, result, sems, gains):
        self.index, self.size, self.reverse = index, size, reverse
        self.own, self.landing, self.mixed, self.result = own, landing, mixed, result
        self.sems, self.gains = sems, gains

    def other(self, distance):
        return lax.rem(self.index + distance, self.size)

    def slot(self, source):
        return lax.rem(source - self.index - 1 + 2 * self.size, self.size)

    def send(self, j, value):
        share = value.shape[0] // self.size
        kind = self.own.dtype
        pieces = value.reshape(self.size, share, value.shape[1])
        self.own[j] = pieces.astype(kind)
        for d in range(1, self.size):
            pltpu.make_async_remote_copy(
                src_ref=self.own.at[j, self.other(d)],
                dst_ref=self.landing.at[j, self.size - d - 1],
                send_sem=self.sems.at[0, j],
                recv_sem=self.sems.at[1, j],
                device_id={"seq": self.other(d)},
                device_id_type=pl.DeviceIdType.MESH,
            ).start()

    def all_of(self, buffer, j, send, recv):
        return pltpu.make_async_remote_copy(
            src_ref=buffer.at[j, pl.ds(0, self.size - 1)],
            dst_ref=buffer.at[j, pl.ds(0, self.size - 1)],
            send_sem=self.sems.at[send, j],
            recv_sem=self.sems.at[recv, j],
            device_id={"seq": self.other(1)},
            device_id_type=pl.DeviceIdType.MESH,
        )

    def turn(self, j):
        self.all_of(self.landing, j, 0, 1).wait()
        kind = self.own.dtype
        self.landing[j, self.size - 1] = self.own[j, self.index]
        held = jnp.zeros(self.own.shape[2:], f32)
        order = range(self.size - 1, -1, -1) if self.reverse else range(self.size)
        for source in order:
            self.mixed[j, source] = held.astype(kind)
            gain = widen(rolled(self.gains[source : source + 1, :], j)[:, :BLOCK_HEADS])
            held = gain * held + self.landing[j, self.slot(source)].astype(f32)
        for d in range(1, self.size):
            pltpu.make_async_remote_copy(
                src_ref=self.mixed.at[j, self.other(d)],
                dst_ref=self.result.at[j, self.index],
                send_sem=self.sems.at[2, j],
                recv_sem=self.sems.at[3, j],
                device_id={"seq": self.other(d)},
                device_id_type=pl.DeviceIdType.MESH,
            ).start()

    def take(self, j):
        self.all_of(self.result, j, 2, 3).wait()
        self.result[j, self.index] = self.mixed[j, self.index]
        whole = self.result[j].astype(f32)
        return whole.reshape(whole.shape[0] * whole.shape[1], whole.shape[2])


def exchange_scratch(nb, size, kind):
    share = STATE // size
    return [pltpu.VMEM((nb, size, share, BLOCK), kind) for _ in range(4)] + [
        pltpu.SemaphoreType.DMA((4, nb))
    ]


def greet(index, core, size):
    barrier = pltpu.get_barrier_semaphore()
    for d in range(1, size):
        pl.semaphore_signal(
            barrier, inc=1, device_id={"seq": lax.rem(index + d, size)},
            device_id_type=pl.DeviceIdType.MESH,
        )
    pl.semaphore_signal(
        barrier, inc=1, device_id={"head": 1 - core}, device_id_type=pl.DeviceIdType.MESH
    )
    pl.semaphore_wait(barrier, size)


def send_to(src, dst, send_sem, recv_sem, **where):
    return pltpu.make_async_remote_copy(
        src_ref=src, dst_ref=dst, send_sem=send_sem, recv_sem=recv_sem, device_id=where,
        device_id_type=pl.DeviceIdType.MESH,
    )


def transposed(block):
    return block.astype(f32).T.astype(bf16)


def forward_kernel(
    size,
    hid_ref, gain_ref, wi_ref, wstep_ref, wshared_ref, cv_ref, cs_ref, bias_ref, decay_ref,
    skip_ref, ggain_ref, wout_ref, hrow_ref, crow_ref,
    normedt_ref, scale_ref, gate_ref, vext_ref, after_ref, y_ref, gw_ref, in_ref, step_ref,
    slope_ref, run_ref, runt_ref, stept_ref, sext_ref, bc_ref, gains_ref, out_ref, gmt_ref,
    coef_ref, near_ref,
    nx, halo, halo_sems, scores, bt, end_w, vwide, gates, ys, states, acc, acc_send,
    acc_land, acc_sems, squares, sq_land, sq_sems, totals, totals_land, totals_sems,
    near_land, near_sems, ex_own, ex_landing, ex_mixed, ex_result, ex_sems,
):
    step_id = pl.program_id(0)
    index = lax.axis_index("seq")
    core = lax.axis_index("head")
    tokens = hid_ref.shape[0]
    width = hid_ref.shape[1]
    chunks = tokens // CHUNK
    nb = gates.shape[0]
    t_mix, t_last = nb, 2 * nb
    half_width = width // 2
    exchange = StateExchange(
        index, size, False, ex_own, ex_landing, ex_mixed, ex_result, ex_sems, gains_ref
    )

    def norm_rows(rows):
        wide = rows.astype(f32)
        scale = lax.rsqrt(jnp.mean(wide * wide, axis=1, keepdims=True) + norm_eps)
        return (wide * scale * gain_ref[...]).astype(bf16), scale

    def totals_copy(d):
        return send_to(
            totals, totals_land.at[size - d - 1], totals_sems.at[0], totals_sems.at[1],
            seq=lax.rem(index + d, size),
        )

    @pl.when(step_id == 0)
    def _():
        @pl.loop(0, chunks)
        def _(i):
            start = pl.multiple_of(i * CHUNK, CHUNK)
            for part in range(2):
                at = pl.multiple_of(start + part * 64, 64)
                rows, scale = norm_rows(hid_ref[pl.ds(at, 64), :])
                nx[pl.ds(pl.multiple_of(HALO + at, HALO), 64), :] = rows
                scale_ref[pl.ds(at, 64), :] = jnp.broadcast_to(scale, (64, LANES))

        greet(index, core, size)
        after_id = lax.rem(index + 1, size)
        halo_copy = send_to(
            hid_ref.at[pl.ds(tokens - HALO, HALO)], halo, halo_sems.at[0], halo_sems.at[1],
            seq=after_id,
        )
        halo_copy.start()
        for c in range(chunks):
            for b in range(width // LANES):
                normedt_ref[b * LANES : (b + 1) * LANES, c * CHUNK : (c + 1) * CHUNK] = transposed(
                    nx[HALO + c * CHUNK : HALO + (c + 1) * CHUNK, b * LANES : (b + 1) * LANES]
                )
        raw = mm(nx[HALO:, :], wstep_ref[...]) + bias_ref[...]
        small = jnp.exp(-jnp.abs(raw))
        step = jnp.maximum(raw, 0.0) + jnp.log1p(small)
        step_ref[...] = step
        slope_ref[...] = 1.0 / (1.0 + jnp.exp(-raw))
        rate = -step * jnp.exp(decay_ref[...])
        tri = causal().astype(f32)
        total = jnp.zeros((1, LANES), f32)
        for c in range(chunks):
            rows = slice(c * CHUNK, (c + 1) * CHUNK)
            run = mm_exact(tri, rate[rows, :])
            run_ref[rows, :] = run
            total = total + run[CHUNK - 1 :, :]
            run_t = run.T
            step_t = step[rows, :].T
            for b in range(nb):
                heads = slice(BLOCK_HEADS * b, BLOCK_HEADS * (b + 1))
                runt_ref[b, 0:BLOCK_HEADS, rows] = run_t[heads, :]
                stept_ref[b, 0:BLOCK_HEADS, rows] = step_t[heads, :]
                runt_ref[b, BLOCK_HEADS:, rows] = jnp.zeros((8 - BLOCK_HEADS, CHUNK), f32)
                stept_ref[b, BLOCK_HEADS:, rows] = jnp.zeros((8 - BLOCK_HEADS, CHUNK), f32)
            end_w[rows, :] = step[rows, :] * jnp.exp(run[CHUNK - 1 :, :] - run)
        totals[...] = jnp.broadcast_to(jnp.exp(total), totals.shape)
        for d in range(1, size):
            totals_copy(d).start()
        halo_copy.wait()
        keep = jnp.where(index == 0, 0.0, 1.0)
        nx[0:HALO, :] = (norm_rows(halo[...])[0].astype(f32) * keep).astype(bf16)
        shared = mm(nx[...], wshared_ref[...]).astype(bf16)
        sext_ref[0] = shared[:, :STATE]
        sext_ref[1] = shared[:, STATE:]
        conv = conv_rows(shared.astype(f32), cs_ref[...], HALO - CONV + 1, tokens)
        act = silu(conv).astype(bf16)
        bc_ref[...] = act
        for c in range(chunks):
            rows = slice(c * CHUNK, (c + 1) * CHUNK)
            b_rows = act[rows, :STATE]
            c_rows = act[rows, STATE:]
            scores[c] = mm(c_rows, b_rows, NT)
            bt[:, rows] = transposed(b_rows)

    @pl.when(step_id < t_mix)
    def _():
        j = step_id
        values = mm(nx[...], wi_ref[1]).astype(bf16)
        vext_ref[...] = values
        vwide[...] = values.astype(f32)
        conv = conv_rows(vwide, cv_ref[...], HALO - CONV + 1, tokens)
        act = silu(conv).astype(bf16)
        run_cols = rolled(run_ref[...], j)
        end_cols = rolled(end_w[...], j)
        state = jnp.zeros((STATE, BLOCK), f32)
        for c in range(chunks):
            rows = slice(c * CHUNK, (c + 1) * CHUNK)
            weighted = act[rows, :].astype(f32) * widen(end_cols[rows, :BLOCK_HEADS])
            last = widen(jnp.exp(run_cols[(c + 1) * CHUNK - 1 : (c + 1) * CHUNK, :BLOCK_HEADS]))
            state = last * state + mm_right(bt[:, rows], weighted)
            after_ref[c] = state
            states[j, c] = state
        exchange.send(j, state)
        gate = mm(nx[HALO:, :], wi_ref[0])
        gate_ref[...] = gate
        gates[j] = gate
        mask = causal()
        skip = widen(rolled(skip_ref[...], j)[:, :BLOCK_HEADS])
        for c in range(chunks):
            rows = slice(c * CHUNK, (c + 1) * CHUNK)
            cols = run_cols[rows, :BLOCK_HEADS]
            x = act[rows, :]
            y_pairs = []
            for pair in range(BLOCK // LANES):
                mats = []
                for k in range(2):
                    head = 2 * pair + k
                    gap = cols[:, head : head + 1] - runt_ref[j, head : head + 1, rows]
                    decayed = jnp.exp(jnp.where(mask, gap, -1e30))
                    mats.append(scores[c] * decayed * stept_ref[j, head : head + 1, rows])
                low, high = stack_pair(x[:, pair * LANES : (pair + 1) * LANES])
                y_pairs.append(
                    mm_left(jnp.concatenate(mats, axis=1), jnp.concatenate([low, high], axis=0))
                )
            ys[j, rows, :] = jnp.concatenate(y_pairs, axis=1) + skip * x.astype(f32)

    @pl.when(step_id == 1)
    def _():
        pltpu.make_async_remote_copy(
            src_ref=totals_land.at[pl.ds(0, size - 1)],
            dst_ref=totals_land.at[pl.ds(0, size - 1)],
            send_sem=totals_sems.at[0], recv_sem=totals_sems.at[1],
            device_id={"seq": lax.rem(index + 1, size)},
            device_id_type=pl.DeviceIdType.MESH,
        ).wait()
        totals_land[size - 1] = totals[...]
        for source in range(size):
            gains_ref[source : source + 1, :] = totals_land[exchange.slot(source), 0:1, :]

    @pl.when((step_id >= 2) & (step_id < nb + 2))
    def _():
        exchange.turn(step_id - 2)

    def neighbour_copy(bit):
        mine = (index // (1 << bit)) % 2
        return send_to(
            normedt_ref.at[pl.ds(pl.multiple_of(core * half_width, half_width), half_width)],
            near_land.at[bit], near_sems.at[0, bit], near_sems.at[1, bit],
            seq=index + (1 - 2 * mine) * (1 << bit),
        )

    @pl.when(step_id == nb + 1)
    def _():
        for bit in range(2):
            neighbour_copy(bit).start()

    @pl.when((step_id >= t_mix) & (step_id < t_last))
    def _():
        j = step_id - t_mix
        entering = exchange.take(j)
        in_ref[...] = entering
        offsets = offsets_of(run_ref, chunks)
        gated = []
        for c in range(chunks):
            rows = slice(c * CHUNK, (c + 1) * CHUNK)
            grow = rolled(jnp.exp(run_ref[rows, :]), j)[:, :BLOCK_HEADS]
            base = rolled(jnp.exp(offsets[c]), j)[:, :BLOCK_HEADS]
            enter = widen(base) * entering
            if c:
                enter = enter + states[j, c - 1]
            y = ys[j, rows, :] + widen(grow) * mm_right(bc_ref[rows, STATE:], enter)
            y_ref[rows, :] = y
            out = y * silu(gates[j, rows, :])
            gw_ref[rows, :] = (out * ggain_ref[...]).astype(bf16)
            gated.append(
                jnp.broadcast_to(jnp.sum(out * out, axis=1, keepdims=True), (CHUNK, LANES))
            )
        part = mm(gw_ref[...], wout_ref[...], NT)
        block_squares = jnp.concatenate(gated, axis=0)

        @pl.when(j == 0)
        def _():
            acc[...] = part
            squares[...] = block_squares

        @pl.when(j > 0)
        def _():
            acc[...] += part
            squares[...] += block_squares

        @pl.when(j == nb - 1)
        def _():
            send_to(squares, sq_land, sq_sems.at[0], sq_sems.at[1], head=1 - core).start()
            for c in range(chunks):
                acc_send[c] = acc[c * CHUNK : (c + 1) * CHUNK, :].astype(bf16)
                send_to(
                    acc_send.at[c], acc_land.at[c], acc_sems.at[0, c], acc_sems.at[1, c],
                    head=1 - core,
                ).start()

    @pl.when(step_id >= t_last)
    def _():
        c = step_id - t_last

        @pl.when(c == 0)
        def _():
            send_to(squares, sq_land, sq_sems.at[0], sq_sems.at[1], head=1 - core).wait()

        send_to(
            acc_send.at[c], acc_land.at[c], acc_sems.at[0, c], acc_sems.at[1, c], head=1 - core
        ).wait()
        rows = pl.ds(pl.multiple_of(c * CHUNK, CHUNK), CHUNK)
        mixed = acc[rows, :] + acc_land[c].astype(f32)
        inverse = lax.rsqrt((squares[rows, 0:1] + sq_land[rows, 0:1]) / INNER + norm_eps)
        out_ref[...] = hrow_ref[...].astype(f32) + mixed * inverse
        cot = crow_ref[...].astype(f32)
        scaled = (cot * inverse).astype(bf16)
        for b in range(width // LANES):
            gmt_ref[b * LANES : (b + 1) * LANES, :] = transposed(
                scaled[:, b * LANES : (b + 1) * LANES]
            )
        grad_inverse = jnp.sum(cot * mixed, axis=1, keepdims=True)
        coef_ref[...] = jnp.broadcast_to(
            grad_inverse * inverse * inverse * inverse / INNER, (CHUNK, LANES)
        )

        @pl.when(c == chunks - 1)
        def _():
            for bit in range(2):
                neighbour_copy(bit).wait()
                near_ref[bit] = near_land[bit]


def offsets_of(run_ref, chunks):
    rows = [jnp.zeros((1, LANES), f32)]
    for c in range(chunks):
        rows.append(rows[-1] + run_ref[(c + 1) * CHUNK - 1 : (c + 1) * CHUNK, :])
    return rows


def forward_call(
    hidden, cotangent, gain, both, wstep, wshared, conv_values, conv_shared, bias, decay, skip,
    gate_gain, wout,
):
    tokens, width = hidden.shape
    inner = both.shape[2]
    chunks = tokens // CHUNK
    nb = inner // BLOCK
    size = lax.axis_size("seq")
    t_mix, t_last = nb, 2 * nb

    def at(start):
        return lambda s: jnp.clip(s - start, 0, nb - 1)

    def full(shape):
        return pl.BlockSpec(shape, lambda s: (0,) * len(shape), pipeline_mode=pl.Buffered(1))

    def cols(rows, start):
        return pl.BlockSpec((rows, BLOCK), lambda s: (0, at(start)(s)))

    row_of = lambda s: jnp.clip(s - t_last, 0, chunks - 1)
    row_block = lambda w: pl.BlockSpec((CHUNK, w), lambda s: (row_of(s), 0))
    outs = [
        ((width, tokens), bf16, full((width, tokens))),
        ((tokens, LANES), f32, full((tokens, LANES))),
        ((tokens, inner), f32, cols(tokens, 0)),
        ((HALO + tokens, inner), bf16, cols(HALO + tokens, 0)),
        (
            (chunks, STATE, inner), f32,
            pl.BlockSpec((chunks, STATE, BLOCK), lambda s: (0, 0, at(0)(s))),
        ),
        ((tokens, inner), f32, cols(tokens, t_mix)),
        ((tokens, inner), bf16, cols(tokens, t_mix)),
        ((STATE, inner), f32, cols(STATE, t_mix)),
        ((tokens, LANES), f32, full((tokens, LANES))),
        ((tokens, LANES), f32, full((tokens, LANES))),
        ((tokens, LANES), f32, full((tokens, LANES))),
        ((nb, 8, tokens), f32, full((nb, 8, tokens))),
        ((nb, 8, tokens), f32, full((nb, 8, tokens))),
        ((2, HALO + tokens, STATE), bf16, full((2, HALO + tokens, STATE))),
        ((tokens, 2 * STATE), bf16, full((tokens, 2 * STATE))),
        ((size, LANES), f32, full((size, LANES))),
        ((tokens, width), f32, row_block(width)),
        ((width, tokens), bf16, pl.BlockSpec((width, CHUNK), lambda s: (0, row_of(s)))),
        ((tokens, LANES), f32, row_block(LANES)),
        ((2, width // 2, tokens), bf16, full((2, width // 2, tokens))),
    ]
    sem = pltpu.SemaphoreType.DMA
    return pl.pallas_call(
        functools.partial(forward_kernel, size),
        grid=(2 * nb + chunks,),
        in_specs=[
            full((tokens, width)),
            full((1, width)),
            pl.BlockSpec((2, width, BLOCK), lambda s: (0, 0, at(0)(s))),
            full((width, LANES)),
            full((width, 2 * STATE)),
            cols(CONV + 1, 0),
            full((CONV + 1, 2 * STATE)),
            full((1, LANES)),
            full((1, LANES)),
            full((1, LANES)),
            cols(1, t_mix),
            cols(width, t_mix),
            row_block(width),
            row_block(width),
        ],
        out_shape=[jax.ShapeDtypeStruct(shape, kind) for shape, kind, _ in outs],
        out_specs=[spec for _, _, spec in outs],
        scratch_shapes=[
            pltpu.VMEM((HALO + tokens, width), bf16),
            pltpu.VMEM((HALO, width), bf16),
            sem((2,)),
            pltpu.VMEM((chunks, CHUNK, CHUNK), f32),
            pltpu.VMEM((STATE, tokens), bf16),
            pltpu.VMEM((tokens, LANES), f32),
            pltpu.VMEM((HALO + tokens, BLOCK), f32),
            pltpu.VMEM((nb, tokens, BLOCK), f32),
            pltpu.VMEM((nb, tokens, BLOCK), f32),
            pltpu.VMEM((nb, chunks, STATE, BLOCK), f32),
            pltpu.VMEM((tokens, width), f32),
            pltpu.VMEM((chunks, CHUNK, width), bf16),
            pltpu.VMEM((chunks, CHUNK, width), bf16),
            sem((2, chunks)),
            pltpu.VMEM((tokens, LANES), f32),
            pltpu.VMEM((tokens, LANES), f32),
            sem((2,)),
            pltpu.VMEM((8, LANES), f32),
            pltpu.VMEM((size, 8, LANES), f32),
            sem((2,)),
            pltpu.VMEM((2, width // 2, tokens), bf16),
            sem((2, 2)),
        ] + exchange_scratch(nb, size, f32),
        compiler_params=pltpu.CompilerParams(
            collective_id=1, has_side_effects=True, vmem_limit_bytes=67043328
        ),
        name="forward",
    )(
        hidden, gain, both, wstep, wshared, conv_values, conv_shared, bias, decay, skip, gate_gain,
        wout, hidden, cotangent,
    )


def order_rows(part, bits):
    order = list(range(bits))
    if part == 1:
        order[:3] = order[:3][::-1]
    if part == 2:
        order[:2] = order[:2][::-1]
    return order


def order_columns(part, bits):
    return [bit for bit in range(bits) if bit != part] + [part]


def slot_of(owner, order):
    slot = 0
    for bit in order:
        slot = slot * 2 + ((owner >> bit) & 1)
    return slot


class Reduction:
    def __init__(self, held, landing, order, index, sems, put, put_other=None):
        self.held, self.landing, self.order = held, landing, order
        self.index, self.sems, self.put, self.put_other = index, sems, put, put_other
        self.stages = len(order)

    def place(self, stage):
        base = 0
        size = 1 << self.stages
        for s, bit in enumerate(self.order[: stage + 1]):
            mine = (self.index // (1 << bit)) % 2
            half = size >> (s + 1)
            keep, give = base + mine * half, base + (1 - mine) * half
            base = keep
        return keep, give, half

    def copy(self, stage):
        _, give, half = self.place(stage)
        bit = self.order[stage]
        mine = (self.index // (1 << bit)) % 2
        return send_to(
            self.held.at[pl.ds(give, half)], self.landing[stage],
            self.sems.at[0, stage], self.sems.at[1, stage],
            seq=self.index + (1 - 2 * mine) * (1 << bit),
        )

    def start(self, stage):
        self.copy(stage).start()

    def start_piece(self, piece, pieces):
        _, give, half = self.place(0)
        count = half // pieces
        bit = self.order[0]
        mine = (self.index // (1 << bit)) % 2
        send_to(
            self.held.at[pl.ds(give + piece * count, count)],
            self.landing[0].at[pl.ds(piece * count, count)],
            self.sems.at[0, 0], self.sems.at[1, 0],
            seq=self.index + (1 - 2 * mine) * (1 << bit),
        ).start()

    def advance(self, stage):
        self.copy(stage).wait()
        keep, _, half = self.place(stage)
        if stage < self.stages - 1:

            @pl.loop(0, half)
            def _(i):
                total = self.held[keep + i].astype(f32) + self.landing[stage][i].astype(f32)
                self.held[keep + i] = total.astype(bf16)

            self.start(stage + 1)
        elif self.put_other is None:
            self.put(self.held[keep].astype(f32) + self.landing[stage][0].astype(f32))
        else:
            self.put(self.held[keep].astype(f32))
            self.put_other(self.landing[stage][0].astype(f32))


def sum_copy(acc, landing, bit, index, sems):
    mine = (index // (1 << bit)) % 2
    return pltpu.make_async_remote_copy(
        src_ref=acc.at[bit],
        dst_ref=landing.at[bit],
        send_sem=sems.at[0, bit],
        recv_sem=sems.at[1, bit],
        device_id={"seq": index + (1 - 2 * mine) * (1 << bit)},
        device_id_type=pl.DeviceIdType.MESH,
    )


def back_kernel(
    bits,
    gmt_ref, normedt_ref, near_ref, gw_ref, coef_ref, gains_ref, run_ref, step_ref, slope_ref,
    bc_ref, sext_ref, skip_ref, decay_ref, cs_ref, wsmall_ref, gain_ref,
    wout_ref, y_ref, gate_ref, ggain_ref, vext_ref, after_ref, in_ref, cv_ref, runt_ref,
    stept_ref, wi_ref,
    hid_ref, cot_ref, scale_ref,
    gout_ref, ggw_ref, gvw_ref, gsmall_ref, ghid_ref, sums_ref, heads_ref,
    w_out, w_gate, w_values, w_small,
    land_out, land_gate, land_values, land_small,
    rs_sems, near, near_sems,
    own_cols, other_cols, land_cols, cols_sems,
    gv, acc_send, acc_land, acc_sems,
    edge_own, edge_tail, edge_land, edge_sems,
    dbc, dbc_land, dbc_sems, small, sedge_own, sedge_land, sedge_sems,
    vec, vec_land, vec_sems,
    scores, scorest, ct, dscores, end_w, ends, dcols, xdu, dyc, xdus, vwide, gext,
    dys, ggates, term_gate, ex_own, ex_landing, ex_mixed, ex_result, ex_sems,
):
    step_id = pl.program_id(0)
    index = lax.axis_index("seq")
    core = lax.axis_index("head")
    size = 1 << bits
    tokens = y_ref.shape[0]
    chunks = tokens // CHUNK
    nb = ggates.shape[0]
    half_nb = nb // 2
    width = normedt_ref.shape[0]
    half_width = width // 2
    rows_own = width // size
    t_scan, t_grad, t_final = nb, 2 * nb, 3 * nb
    after_id = lax.rem(index + 1, size)
    before_id = lax.rem(index + size - 1, size)
    bit_of = lambda bit: (index // (1 << bit)) % 2
    flip_of = lambda bit: index + (1 - 2 * bit_of(bit)) * (1 << bit)

    def out_reduction(part):
        cols = w_out.shape[3]

        def put(value):
            gout_ref[:, part * cols : (part + 1) * cols] = value

        return Reduction(
            w_out.at[part], [ref.at[part] for ref in land_out], order_rows(part, bits), index,
            rs_sems.at[part], put,
        )

    def columns_reduction(g, part):
        held, landing, out = ((w_gate, land_gate, ggw_ref), (w_values, land_values, gvw_ref))[g]

        def put_half(half):
            def put(value):
                for b in range(half_nb):
                    out[part * half_nb + b, half] = value[:, b * LANES : (b + 1) * LANES]

            return put

        return Reduction(
            held.at[part], [ref.at[part] for ref in landing], order_columns(part, bits), index,
            rs_sems.at[2 + 2 * g + part], put_half(bit_of(part)), put_half(1 - bit_of(part)),
        )

    def put_small(value):
        gsmall_ref[...] = value

    rs_out = [out_reduction(part) for part in range(2)]
    rs_gate = [columns_reduction(0, part) for part in range(2)]
    rs_values = [columns_reduction(1, part) for part in range(2)]
    rs_small = Reduction(
        w_small, list(land_small), order_rows(2, bits), index, rs_sems.at[6], put_small
    )

    def when_after(step):
        return pl.when(step_id == step)

    exchange = StateExchange(
        index, size, True, ex_own, ex_landing, ex_mixed, ex_result, ex_sems, gains_ref
    )

    def near_copies(bit):
        half = pl.ds(pl.multiple_of(core * half_width, half_width), half_width)
        return (
            pltpu.make_async_copy(near_ref.at[bit], near.at[bit, half], near_sems.at[0, bit]),
            send_to(
                near_ref.at[bit], near.at[bit, half], near_sems.at[1, bit], near_sems.at[2, bit],
                head=1 - core,
            ),
        )

    @pl.when(step_id == 0)
    def _():
        greet(index, core, size)
        for bit in range(2):
            for copy in near_copies(bit):
                copy.start()
        for c in range(chunks):
            rows = slice(c * CHUNK, (c + 1) * CHUNK)
            ct[:, rows] = transposed(bc_ref[rows, STATE:])
            for b in range(width // LANES):
                acc_send[c, :, b * LANES : (b + 1) * LANES] = transposed(
                    gmt_ref[b * LANES : (b + 1) * LANES, rows]
                )

    group = width // 4
    owners = size // 4

    def scatter(piece, q, order, store):
        for b in range(owners):
            store(slot_of(q * owners + b, order), piece[b * rows_own : (b + 1) * rows_own, :])

    def put_out(part):
        cols = w_out.shape[3]
        for q in range(4):
            left = gmt_ref[q * group : (q + 1) * group, :]
            piece = mm(left, gw_ref[:, part * cols : (part + 1) * cols]).astype(bf16)

            def store(slot, value):
                w_out[part, slot] = value

            scatter(piece, q, order_rows(part, bits), store)

    def columns_copy(g, part):
        return send_to(
            other_cols.at[g, part], land_cols.at[g, part], cols_sems.at[0, g, part],
            cols_sems.at[1, g, part], seq=flip_of(part),
        )

    def split_block(g, j, value):
        part = j // half_nb
        mine = jnp.where(part == 0, bit_of(0), bit_of(1))
        place = pl.ds(pl.multiple_of((j % half_nb) * LANES, LANES), LANES)
        first, second = value[:, :LANES], value[:, LANES:]
        own_cols[g, part, :, place] = jnp.where(mine == 0, first, second)
        other_cols[g, part, :, place] = jnp.where(mine == 0, second, first)

    def put_columns(g, part):
        columns_copy(g, part).wait()
        held = (w_gate, w_values)[g]
        for q in range(4):
            rows = slice(q * group, (q + 1) * group)
            piece = mm(normedt_ref[rows, :], own_cols[g, part]) + mm(
                near[part, rows, :], land_cols[g, part]
            )

            def store(slot, value):
                held[part, slot] = value

            scatter(piece.astype(bf16), q, order_columns(part, bits), store)
        (rs_gate, rs_values)[g][part].start(0)

    @pl.when(step_id < t_scan)
    def _():
        j = step_id
        offsets = offsets_of(run_ref, chunks)
        own = jnp.zeros((STATE, BLOCK), f32)
        term = jnp.zeros((1, BLOCK), f32)
        for c in range(chunks):
            rows = slice(c * CHUNK, (c + 1) * CHUNK)
            ggw = mm(acc_send[c], wout_ref[...])
            y = y_ref[rows, :]
            gate = gate_ref[rows, :]
            sig = 1.0 / (1.0 + jnp.exp(-gate))
            act = gate * sig
            out = y * act
            term = term + jnp.sum(ggw * out, axis=0, keepdims=True)
            coef = jnp.concatenate([coef_ref[rows, 0:LANES]] * (BLOCK // LANES), axis=1)
            gg = ggw * ggain_ref[...] - coef * out
            dy = gg * act
            dys[j, rows, :] = dy
            ggate = (gg * y * (sig * (1.0 + gate * (1.0 - sig)))).astype(bf16)
            ggates[j, rows, :] = ggate
            grow = rolled(jnp.exp(run_ref[rows, :] + offsets[c]), j)[:, :BLOCK_HEADS]
            own = own + mm_right(ct[:, rows], dy * widen(grow))
        term_gate[j, 0:1, :] = term
        exchange.send(j, own)
        split_block(0, j, ggates[j])

    for part in range(2):

        @when_after(part)
        def _(part=part):
            put_out(part)

    pieces = size // 2

    @pl.when((step_id >= 1) & (step_id < nb))
    def _():
        for reduction in rs_out:
            reduction.start_piece(step_id - 1, pieces)

    rest = pieces - (nb - 1)

    @when_after(nb)
    def _():
        for piece in range(nb - 1, nb - 1 + (rest + 1) // 2):
            for reduction in rs_out:
                reduction.start_piece(piece, pieces)

    @when_after(nb + 1)
    def _():
        for piece in range(nb - 1 + (rest + 1) // 2, pieces):
            for reduction in rs_out:
                reduction.start_piece(piece, pieces)

    @pl.when((step_id >= 2) & (step_id < nb + 2))
    def _():
        exchange.turn(step_id - 2)

    @when_after(half_nb - 1)
    def _():
        columns_copy(0, 0).start()

    @when_after(nb - 1)
    def _():
        columns_copy(0, 1).start()
        for bit in range(2):
            for copy in near_copies(bit):
                copy.wait()
        put_columns(0, 0)

    mask = causal()
    rows_i = lax.broadcasted_iota(jnp.int32, (CHUNK, CHUNK), 0)
    cols_i = lax.broadcasted_iota(jnp.int32, (CHUNK, CHUNK), 1)
    mask_t = rows_i <= cols_i

    @pl.when(step_id == t_scan)
    def _():
        dbc[...] = jnp.zeros_like(dbc)
        dscores[...] = jnp.zeros_like(dscores)
        dcols[...] = jnp.zeros_like(dcols)
        xdu[...] = jnp.zeros_like(xdu)
        dyc[...] = jnp.zeros_like(dyc)
        xdus[...] = jnp.zeros_like(xdus)
        ends[...] = jnp.zeros_like(ends)
        vec[...] = jnp.zeros_like(vec)
        for c in range(chunks):
            rows = slice(c * CHUNK, (c + 1) * CHUNK)
            b_rows = bc_ref[rows, :STATE]
            c_rows = bc_ref[rows, STATE:]
            scores[c] = mm(c_rows, b_rows, NT)
            scorest[c] = mm(b_rows, c_rows, NT)
            run = run_ref[rows, :]
            end_w[rows, :] = jnp.exp(run[CHUNK - 1 :, :] - run)

    @pl.when((step_id >= t_scan) & (step_id < t_grad))
    def _():
        j = step_id - t_scan
        offsets = offsets_of(run_ref, chunks)
        vwide[...] = vext_ref[...].astype(f32)
        taps = [jnp.zeros((1, BLOCK), f32)] * (CONV + 1)
        run_cols = rolled(run_ref[...], j)
        step_cols = rolled(step_ref[...], j)
        end_cols = rolled(end_w[...], j)
        skip = widen(rolled(skip_ref[...], j)[:, :BLOCK_HEADS])
        channel = lax.broadcasted_iota(jnp.int32, (BLOCK, LANES), 0) // HEAD_DIM
        lane = lax.broadcasted_iota(jnp.int32, (BLOCK, LANES), 1)
        pick = (lane == BLOCK_HEADS * j + channel).astype(bf16)
        lane_row = lax.broadcasted_iota(jnp.int32, (CHUNK, LANES), 1)
        dstate = exchange.take(j)
        dskip = jnp.zeros((1, BLOCK), f32)
        gext[tokens : tokens + 8, :] = jnp.zeros((8, BLOCK), f32)
        for c in reversed(range(chunks)):
            rows = slice(c * CHUNK, (c + 1) * CHUNK)
            cols = run_cols[rows, :BLOCK_HEADS]
            conv = conv_rows(vwide, cv_ref[...], HALO - CONV + 1 + c * CHUNK, CHUNK)
            sig = 1.0 / (1.0 + jnp.exp(-conv))
            x = (conv * sig).astype(bf16)
            slope = sig * (1.0 + conv * (1.0 - sig))
            wide_x = x.astype(f32)
            dy = dys[j, rows, :]
            b_rows = bc_ref[rows, :STATE]
            c_rows = bc_ref[rows, STATE:]
            grow = widen(jnp.exp(cols))
            tail = widen(end_cols[rows, :BLOCK_HEADS])
            step_w = widen(step_cols[rows, :BLOCK_HEADS])
            last = grow[CHUNK - 1 :, :]
            base = rolled(jnp.exp(offsets[c]), j)[:, :BLOCK_HEADS]
            enter = widen(base) * in_ref[...]
            if c:
                enter = enter + after_ref[c - 1]
            du_state = tail * mm_right(b_rows, dstate)
            carried = grow * mm_right(c_rows, enter)
            weighted = wide_x * (tail * step_w)
            grown = dy * grow
            dbc[0, rows, :] += mm_both(weighted, dstate, NT)
            dbc[1, rows, :] += mm_both(grown, enter, NT)
            hold = last * jnp.sum(dstate * enter, axis=0, keepdims=True)
            dstate = last * dstate + mm_right(ct[:, rows], grown)
            du_pairs = []
            col_sum = jnp.zeros((CHUNK, LANES), f32)
            dscore = dscores[c]
            for pair in range(BLOCK // LANES):
                lanes = slice(pair * LANES, (pair + 1) * LANES)
                low, high = stack_pair(dy[:, lanes])
                both = jnp.concatenate([low, high], axis=0)
                dmat = mm_left(both, x[:, lanes], NT)
                mats = []
                for k in range(2):
                    head = 2 * pair + k
                    col = cols[:, head : head + 1]
                    row = runt_ref[0, head : head + 1, rows]
                    keep = jnp.exp(jnp.where(mask, col - row, -1e30))
                    piece = dmat[k * CHUNK : (k + 1) * CHUNK, :] * keep
                    piece = piece * stept_ref[0, head : head + 1, rows]
                    dscore = dscore + piece
                    full = piece * scores[c]
                    col_sum = jnp.where(
                        lane_row == BLOCK_HEADS * j + head,
                        jnp.sum(full, axis=1, keepdims=True),
                        col_sum,
                    )
                    dcols[j, head : head + 1, rows] = jnp.sum(full, axis=0, keepdims=True)
                    keep_t = jnp.exp(jnp.where(mask_t, row - col, -1e30))
                    mats.append(scorest[c] * keep_t)
                du_pairs.append(mm_both(jnp.concatenate(mats, axis=1), both))
            dscores[c] = dscore
            du = jnp.concatenate(du_pairs, axis=1) + du_state
            by_head = mm_left(
                jnp.concatenate(
                    [
                        wide_x * du,
                        dy * carried,
                        wide_x * du_state,
                        jnp.broadcast_to(hold, (HALO, BLOCK)),
                    ],
                    axis=0,
                ),
                pick,
            )
            xdu[rows, :] += by_head[0:CHUNK, :]
            dyc[rows, :] += by_head[CHUNK : 2 * CHUNK, :] + col_sum
            xdus[rows, :] += by_head[2 * CHUNK : 3 * CHUNK, :]
            ends[c : c + 1, :] += by_head[3 * CHUNK : 3 * CHUNK + 1, :]
            dskip = dskip + jnp.sum(dy * wide_x, axis=0, keepdims=True)
            gconv = (step_w * du + skip * dy) * slope
            gext[rows, :] = gconv
            taps[CONV] = taps[CONV] + jnp.sum(gconv, axis=0, keepdims=True)
            values = vwide[HALO + c * CHUNK : HALO + (c + 1) * CHUNK, :]
            total = cv_ref[CONV - 1 : CONV, :] * gconv
            taps[CONV - 1] = taps[CONV - 1] + jnp.sum(values * gconv, axis=0, keepdims=True)
            for k in range(CONV - 1):
                ahead = c * CHUNK + CONV - 1 - k
                moved = gext[ahead : ahead + CHUNK, :]
                total = total + cv_ref[k : k + 1, :] * moved
                taps[k] = taps[k] + jnp.sum(values * moved, axis=0, keepdims=True)
            gv[j, rows, :] = total.astype(bf16)
            if c == chunks - 1:
                edge_tail[j, 0:8, :] = total[CHUNK - 8 :, :]
        row8 = lax.broadcasted_iota(jnp.int32, (8, BLOCK), 0)
        ahead_rows = vwide[HALO - CONV + 1 : HALO - CONV + 9, :]
        for k in range(CONV):
            tap = taps[k]
            if k < CONV - 1:
                moved = pltpu.roll(gext[0:8, :], k, 0) if k else gext[0:8, :]
                inside = (row8 >= k) & (row8 < CONV - 1)
                tap = tap + jnp.sum(
                    jnp.where(inside, ahead_rows * moved, 0.0), axis=0, keepdims=True
                )
            vec[0, j, k : k + 1, :] = tap
        vec[0, j, CONV : CONV + 1, :] = taps[CONV]
        vec[0, j, CONV + 1 : CONV + 2, :] = term_gate[j, 0:1, :]
        vec[0, j, CONV + 2 : CONV + 3, :] = dskip
        edge_tail[j, 8 : 8 + CONV + 1, :] = cv_ref[...]
        edge_own[j] = gext[0:8, :]
        send_to(
            edge_own.at[j], edge_land.at[j], edge_sems.at[0, j], edge_sems.at[1, j], seq=before_id
        ).start()

    def finish_block(j):
        send_to(
            edge_own.at[j], edge_land.at[j], edge_sems.at[0, j], edge_sems.at[1, j], seq=before_id
        ).wait()
        nxt = jnp.where(index == size - 1, 0.0, 1.0) * edge_land[j]
        row8 = lax.broadcasted_iota(jnp.int32, (8, BLOCK), 0)
        fix = edge_tail[j, 0:8, :]
        for k in range(CONV - 1):
            ahead = CONV - 1 - k
            moved = pltpu.roll(nxt, 8 - ahead, 0)
            fix = fix + jnp.where(row8 >= 8 - ahead, edge_tail[j, 8 + k : 9 + k, :] * moved, 0.0)
        both_rows = jnp.concatenate([gv[j, tokens - 16 : tokens - 8, :].astype(f32), fix], axis=0)
        gv[j, tokens - 16 :, :] = both_rows.astype(bf16)
        split_block(1, j, gv[j])

    @pl.when((step_id > t_scan + 1) & (step_id < t_grad))
    def _():
        finish_block(step_id - t_scan - 2)

    @when_after(t_scan + 1)
    def _():
        put_columns(0, 1)

    @when_after(t_scan + 2)
    def _():
        rs_gate[0].advance(0)
        rs_out[0].advance(0)
        rs_out[1].advance(0)

    @when_after(t_scan + half_nb + 1)
    def _():
        columns_copy(1, 0).start()
        rs_gate[0].advance(1)
        rs_gate[1].advance(0)

    @when_after(t_grad - 1)
    def _():
        rs_out[0].advance(1)

    @when_after(t_grad - 1)
    def _():
        tri = mask.astype(f32)
        tri_t = mask_t.astype(f32)
        strict = (rows_i > cols_i).astype(f32)
        decay = jnp.exp(decay_ref[...])
        bias_sum = jnp.zeros((1, LANES), f32)
        decay_sum = jnp.zeros((1, LANES), f32)
        for c in range(chunks):
            rows = slice(c * CHUNK, (c + 1) * CHUNK)
            step = step_ref[rows, :]
            col_rows = [dcols[b, 0:BLOCK_HEADS, rows] for b in range(nb)]
            rest = LANES - BLOCK_HEADS * nb
            col_rows.append(jnp.zeros((rest, CHUNK), f32))
            dlog = dyc[rows, :] - jnp.concatenate(col_rows, axis=0).T
            drate = (
                mm_exact(tri_t, dlog)
                + mm_exact(strict, xdus[rows, :] * step)
                + ends[c : c + 1, :]
            )
            dstep = xdu[rows, :] - decay * drate
            draw = dstep * slope_ref[rows, :]
            small[rows, LANES:] = draw.astype(bf16)
            bias_sum = bias_sum + jnp.sum(draw, axis=0, keepdims=True)
            decay_sum = decay_sum - jnp.sum(drate * step, axis=0, keepdims=True) * decay
            b_rows = bc_ref[rows, :STATE]
            c_rows = bc_ref[rows, STATE:]
            high, low = parts(dscores[c])
            dbc[1, rows, :] += mm(high, b_rows) + mm(low, b_rows)
            dbc[0, rows, :] += mm(high, c_rows, TN) + mm(low, c_rows, TN)
        vec[0, nb, 0:1, 0:LANES] = bias_sum
        vec[0, nb, 1:2, 0:LANES] = decay_sum
        send_to(
            dbc.at[1 - core], dbc_land, dbc_sems.at[0], dbc_sems.at[1], head=1 - core
        ).start()

    @when_after(t_grad)
    def _():
        finish_block(nb - 2)
        finish_block(nb - 1)
        columns_copy(1, 1).start()
        put_columns(1, 0)
        rs_gate[0].advance(2)
        rs_gate[1].advance(1)
        rs_out[1].advance(1)

    @when_after(t_grad + 1)
    def _():
        rs_gate[0].advance(3)

    @when_after(t_grad)
    def _():
        send_to(
            dbc.at[1 - core], dbc_land, dbc_sems.at[0], dbc_sems.at[1], head=1 - core
        ).wait()
        sext = sext_ref[core].astype(f32)
        taps = cs_ref[core]
        conv = conv_rows(sext, taps, HALO - CONV + 1, tokens)
        gs = (dbc[core] + dbc_land[...]) * silu_grad(conv)
        for k in range(CONV):
            first = HALO - CONV + 1 + k
            vec[0, nb, 2 + k : 3 + k, 0:LANES] = jnp.sum(
                sext[first : first + tokens, :] * gs, axis=0, keepdims=True
            )
        vec[0, nb, 2 + CONV : 3 + CONV, 0:LANES] = jnp.sum(gs, axis=0, keepdims=True)
        dbc[core] = gs
        sedge_own[...] = gs[0:8, :]
        send_to(
            sedge_own, sedge_land, sedge_sems.at[0], sedge_sems.at[1], seq=before_id
        ).start()

    @when_after(t_grad + 1)
    def _():
        send_to(
            sedge_own, sedge_land, sedge_sems.at[0], sedge_sems.at[1], seq=before_id
        ).wait()
        taps = cs_ref[core]
        nxt = jnp.where(index == size - 1, 0.0, 1.0) * sedge_land[...]
        gs = jnp.concatenate([dbc[core], nxt], axis=0)
        total = taps[CONV - 1 : CONV, :] * gs[0:tokens, :]
        for k in range(CONV - 1):
            total = total + taps[k : k + 1, :] * gs[CONV - 1 - k : CONV - 1 - k + tokens, :]
        small[:, 0:LANES] = total.astype(bf16)
        for q in range(4):
            piece = mm(normedt_ref[q * group : (q + 1) * group, :], small[...]).astype(bf16)

            def store(slot, value):
                w_small[slot] = value

            scatter(piece, q, order_rows(2, bits), store)
        rs_small.start(0)

    @pl.when((step_id >= t_grad) & (step_id < t_final))
    def _():
        j = step_id - t_grad
        part = mm(ggates[j], wi_ref[0], NT) + mm(gv[j], wi_ref[1], NT)

        @pl.when(j == 0)
        def _():
            for b in range(width // BLOCK):
                dys[b] = part[:, b * BLOCK : (b + 1) * BLOCK]

        @pl.when(j > 0)
        def _():
            for b in range(width // BLOCK):
                dys[b] += part[:, b * BLOCK : (b + 1) * BLOCK]

    @when_after(t_grad + 2)
    def _():
        rs_out[0].advance(2)

    @when_after(t_grad + 3)
    def _():
        put_columns(1, 1)
        rs_out[1].advance(2)

    @when_after(t_grad + 4)
    def _():
        rs_gate[1].advance(2)
        rest = mm(small[...], wsmall_ref[...], NT)
        for b in range(width // BLOCK):
            dys[b] += rest[:, b * BLOCK : (b + 1) * BLOCK]

    @when_after(t_final - 1)
    def _():
        for c in range(chunks):
            rows = slice(c * CHUNK, (c + 1) * CHUNK)
            for b in range(width // BLOCK):
                acc_send[c, :, b * BLOCK : (b + 1) * BLOCK] = dys[b, rows, :].astype(bf16)
            send_to(
                acc_send.at[c], acc_land.at[c], acc_sems.at[0, c], acc_sems.at[1, c], head=1 - core
            ).start()

    @pl.when(step_id >= t_final)
    def _():
        c = step_id - t_final
        send_to(
            acc_send.at[c], acc_land.at[c], acc_sems.at[0, c], acc_sems.at[1, c], head=1 - core
        ).wait()
        here = pl.ds(pl.multiple_of(c * CHUNK, CHUNK), CHUNK)
        own_total = jnp.concatenate([dys[b, here, :] for b in range(width // BLOCK)], axis=1)
        total = own_total + acc_land[c].astype(f32)
        scale = scale_ref[:, 0:1]
        hat = hid_ref[...].astype(f32) * scale
        term = jnp.sum(total * hat, axis=0, keepdims=True)

        for b in range(width // BLOCK):
            piece = term[:, b * BLOCK : (b + 1) * BLOCK]
            vec[0, b, 7:8, :] = vec[0, b, 7:8, :] + piece

        ghat = total * gain_ref[...]
        mean = jnp.mean(ghat * hat, axis=1, keepdims=True)
        ghid_ref[...] = cot_ref[...].astype(f32) + scale * (ghat - hat * mean)

    @when_after(t_final)
    def _():
        rs_out[0].advance(3)

    @when_after(t_final + 1)
    def _():
        rs_values[0].advance(0)

    @when_after(t_final + chunks - 1)
    def _():
        rs_out[1].advance(3)

        def begin(bit):
            sum_copy(vec, vec_land, bit, index, vec_sems).start()

        def add(bit):
            sum_copy(vec, vec_land, bit, index, vec_sems).wait()
            vec[bit + 1] = vec[bit] + vec_land[bit]
            if bit + 1 < bits:
                begin(bit + 1)

        begin(0)
        rs_values[1].advance(0)
        add(0)
        rs_small.advance(0)
        rs_gate[1].advance(3)
        add(1)
        rs_values[0].advance(1)
        rs_small.advance(1)
        rs_values[1].advance(1)
        add(2)
        rs_values[0].advance(2)
        rs_small.advance(2)
        rs_values[0].advance(3)
        rs_values[1].advance(2)
        add(3)
        rs_values[1].advance(3)
        rs_small.advance(3)
        for stage in range(4, bits):
            for reduction in rs_out + rs_gate + rs_values + [rs_small]:
                reduction.advance(stage)
            add(stage)
        heads_ref[...] = vec[bits, nb, :, 0:LANES]
        for b in range(nb):
            sums_ref[:, b * BLOCK : (b + 1) * BLOCK] = vec[bits, b]


def back_call(
    gm_t, normed_t, near, gated_w, coef, gains, run, step, slope, bc, sext, skip, decay,
    conv_shared, wsmall, gain, wout, y, gate, gate_gain, vext, after, state_in, conv_values, runt, stept, both,
    hidden, cotangent, scale,
):
    width, tokens = normed_t.shape
    inner = y.shape[1]
    chunks = tokens // CHUNK
    nb = inner // BLOCK
    size = lax.axis_size("seq")
    bits = size.bit_length() - 1
    rows_own = width // size
    t_scan, t_grad, t_final = nb, 2 * nb, 3 * nb

    def column(start):
        return lambda s: jnp.clip(s - start, 0, nb - 1)

    def full(shape):
        return pl.BlockSpec(shape, lambda s: (0,) * len(shape), pipeline_mode=pl.Buffered(1))

    def cols(rows, start):
        at = column(start)
        return pl.BlockSpec((rows, BLOCK), lambda s: (0, at(s)))

    row_block = lambda w: pl.BlockSpec((CHUNK, w), lambda s: (jnp.clip(s - t_final, 0, chunks - 1), 0))
    row_single = lambda w: pl.BlockSpec(
        (CHUNK, w),
        lambda s: (jnp.clip(s - t_final, 0, chunks - 1), 0),
        pipeline_mode=pl.Buffered(1),
    )
    held = lambda cols: pltpu.VMEM((2, size, rows_own, cols), bf16)
    landing = lambda cols: tuple(
        pltpu.VMEM((2, size >> (s + 1), rows_own, cols), bf16) for s in range(bits)
    )
    columns = lambda: pltpu.VMEM((2, 2, tokens, inner // 4), bf16)
    sem = pltpu.SemaphoreType.DMA
    return pl.pallas_call(
        functools.partial(back_kernel, bits),
        grid=(3 * nb + chunks,),
        in_specs=[
            full((width, tokens)),
            full((width, tokens)),
            pl.BlockSpec(memory_space=pl.ANY),
            full((tokens, inner)),
            full((tokens, LANES)),
            full((size, LANES)),
            full((tokens, LANES)),
            full((tokens, LANES)),
            full((tokens, LANES)),
            full((tokens, 2 * STATE)),
            full((2, HALO + tokens, LANES)),
            full((1, LANES)),
            full((1, LANES)),
            full((2, CONV + 1, LANES)),
            full((width, 2 * LANES)),
            full((1, width)),
            cols(width, 0),
            cols(tokens, 0),
            cols(tokens, 0),
            cols(1, 0),
            pl.BlockSpec(
                (HALO + tokens, BLOCK), lambda s: (0, column(t_scan)(s)), pipeline_mode=pl.Buffered(1)
            ),
            pl.BlockSpec((chunks, STATE, BLOCK), lambda s: (0, 0, column(t_scan)(s))),
            cols(STATE, t_scan),
            cols(CONV + 1, t_scan),
            pl.BlockSpec((1, 8, tokens), lambda s: (column(t_scan)(s), 0, 0)),
            pl.BlockSpec((1, 8, tokens), lambda s: (column(t_scan)(s), 0, 0)),
            pl.BlockSpec(
                (2, width, BLOCK), lambda s: (0, 0, column(t_grad)(s)), pipeline_mode=pl.Buffered(1)
            ),
            row_single(width),
            row_single(width),
            row_block(LANES),
        ],
        out_shape=[
            jax.ShapeDtypeStruct((rows_own, inner), f32),
            jax.ShapeDtypeStruct((nb, 2, rows_own, LANES), f32),
            jax.ShapeDtypeStruct((nb, 2, rows_own, LANES), f32),
            jax.ShapeDtypeStruct((rows_own, 2 * LANES), f32),
            jax.ShapeDtypeStruct((tokens, width), f32),
            jax.ShapeDtypeStruct((8, inner), f32),
            jax.ShapeDtypeStruct((8, LANES), f32),
        ],
        out_specs=[
            full((rows_own, inner)),
            full((nb, 2, rows_own, LANES)),
            full((nb, 2, rows_own, LANES)),
            full((rows_own, 2 * LANES)),
            row_block(width),
            pl.BlockSpec((8, inner), lambda s: (0, 0)),
            pl.BlockSpec((8, LANES), lambda s: (0, 0)),
        ],
        scratch_shapes=[
            held(inner // 2), held(inner // 4), held(inner // 4),
            pltpu.VMEM((size, rows_own, 2 * LANES), bf16),
            landing(inner // 2), landing(inner // 4), landing(inner // 4),
            tuple(pltpu.VMEM((size >> (s + 1), rows_own, 2 * LANES), bf16) for s in range(bits)),
            sem((7, 2, bits)),
            pltpu.VMEM((2, width, tokens), bf16), sem((3, 2)),
            columns(), columns(), columns(), sem((2, 2, 2)),
            pltpu.VMEM((nb, tokens, BLOCK), bf16),
            pltpu.VMEM((chunks, CHUNK, width), bf16),
            pltpu.VMEM((chunks, CHUNK, width), bf16),
            sem((2, chunks)),
            pltpu.VMEM((nb, 8, BLOCK), f32),
            pltpu.VMEM((nb, 16, BLOCK), f32),
            pltpu.VMEM((nb, 8, BLOCK), f32),
            sem((2, nb)),
            pltpu.VMEM((2, tokens, LANES), f32),
            pltpu.VMEM((tokens, LANES), f32),
            sem((2,)),
            pltpu.VMEM((tokens, 2 * LANES), bf16),
            pltpu.VMEM((8, LANES), f32),
            pltpu.VMEM((8, LANES), f32),
            sem((2,)),
            pltpu.VMEM((bits + 1, nb + 1, 8, BLOCK), f32),
            pltpu.VMEM((bits, nb + 1, 8, BLOCK), f32),
            sem((2, bits)),
            pltpu.VMEM((chunks, CHUNK, CHUNK), f32),
            pltpu.VMEM((chunks, CHUNK, CHUNK), f32),
            pltpu.VMEM((STATE, tokens), bf16),
            pltpu.VMEM((chunks, CHUNK, CHUNK), f32),
            pltpu.VMEM((tokens, LANES), f32),
            pltpu.VMEM((8, LANES), f32),
            pltpu.VMEM((nb, 8, tokens), f32),
            pltpu.VMEM((tokens, LANES), f32),
            pltpu.VMEM((tokens, LANES), f32),
            pltpu.VMEM((tokens, LANES), f32),
            pltpu.VMEM((HALO + tokens, BLOCK), f32),
            pltpu.VMEM((tokens + 8, BLOCK), f32),
            pltpu.VMEM((nb, tokens, BLOCK), f32),
            pltpu.VMEM((nb, tokens, BLOCK), bf16),
            pltpu.VMEM((nb, 8, BLOCK), f32),
        ] + exchange_scratch(nb, size, bf16),
        compiler_params=pltpu.CompilerParams(
            collective_id=3, has_side_effects=True, vmem_limit_bytes=67043328
        ),
        name="back",
    )(
        gm_t, normed_t, near, gated_w, coef, gains, run, step, slope, bc, sext, skip, decay,
        conv_shared, wsmall, gain, wout, y, gate, gate_gain, vext, after, state_in, conv_values,
        runt, stept,
        both, hidden, cotangent, scale,
    )


def body(
    hidden, cotangent, norm_gain, proj_inner, proj_step, proj_shared, conv_values, conv_shared,
    step_bias, decay_log, skip_gain, gate_gain, proj_out,
):
    tokens = hidden.shape[0]
    inner = proj_inner.shape[2]
    heads = proj_step.shape[1]
    width = hidden.shape[1]
    size = lax.axis_size("seq")
    shared_here = conv_shared.shape[1] // lax.axis_size("head")
    shared_start = lax.axis_index("head") * shared_here
    both = jnp.transpose(proj_inner, (1, 0, 2))
    lanes = lambda v: jnp.pad(v, (0, LANES - heads))[None, :]
    wstep = jnp.pad(proj_step, ((0, 0), (0, LANES - heads)))
    bias, decay, skip = lanes(step_bias), lanes(decay_log), lanes(skip_gain)
    wshared_own = lax.dynamic_slice_in_dim(proj_shared, shared_start, shared_here, 1)
    (
        normed_t, norm_scale, gate_in, vext, after, y, gated_w, state_in, step, slope, run, runt,
        stept, sext, bc, gains, block_out, gm_t, coef, near,
    ) = forward_call(
        hidden, cotangent, norm_gain[None, :], both, wstep, proj_shared, conv_values, conv_shared,
        bias, decay, skip, gate_gain[None, :], proj_out,
    )
    (gout, ggw, gvw, gsmall, grad_hidden, sums, head_sums) = back_call(
        gm_t, normed_t, near, gated_w, coef, gains, run, step, slope, bc, sext, skip, decay,
        conv_shared.reshape(CONV + 1, -1, LANES).transpose(1, 0, 2),
        jnp.concatenate([wshared_own, wstep], axis=1), norm_gain[None, :], proj_out, y, gate_in,
        gate_gain[None, :], vext, after, state_in, conv_values, runt, stept, both, hidden,
        cotangent, norm_scale,
    )
    return (
        block_out,
        grad_hidden,
        sums[7],
        jnp.stack([ggw, gvw]).transpose(3, 0, 1, 2, 4).reshape(-1, 2, inner),
        gsmall[:, shared_here : shared_here + heads],
        gsmall[:, :shared_here],
        sums[: CONV + 1],
        head_sums[2 : 3 + CONV],
        head_sums[0, :heads],
        head_sums[1, :heads],
        jnp.sum(sums[CONV + 2].reshape(heads, HEAD_DIM), axis=1),
        sums[CONV + 1],
        gout,
    )


def solution(mesh):
    return jax.shard_map(
        body,
        mesh=mesh,
        in_specs=(
            P("seq", None),
            P("seq", None),
            P(),
            P(None, None, "head"),
            P(None, "head"),
            P(),
            P(None, "head"),
            P(),
            P("head"),
            P("head"),
            P("head"),
            P("head"),
            P(None, "head"),
        ),
        out_specs=(
            P("seq", None),
            P("seq", None),
            P(),
            P("seq", None, "head"),
            P("seq", "head"),
            P("seq", "head"),
            P(None, "head"),
            P(None, "head"),
            P("head"),
            P("head"),
            P("head"),
            P("head"),
            P("seq", "head"),
        ),
        check_vma=False,
    )
```

```python
import functools

import jax
import jax.numpy as jnp
from jax import lax
from jax.experimental import pallas as pl
from jax.experimental.pallas import tpu as pltpu
from jax.sharding import PartitionSpec as P

HEAD_DIM = 64
STATE = 128
CONV = 4
INNER = 3072
CHUNK = 128
LANES = 128
BLOCK = 256
HALO = 16
BLOCK_HEADS = BLOCK // HEAD_DIM

norm_eps = 1e-05
highest = lax.Precision.HIGHEST
f32 = jnp.float32
bf16 = jnp.bfloat16
NN = (((1,), (0,)), ((), ()))
NT = (((1,), (1,)), ((), ()))
TN = (((0,), (0,)), ((), ()))


def flip(shard, bit):
    size = lax.axis_size("seq")
    return lax.ppermute(shard, "seq", [(i, i ^ (1 << bit)) for i in range(size)])


def swap(shard):
    return lax.ppermute(shard, "head", [(0, 1), (1, 0)])


def from_behind(shard, by):
    size = lax.axis_size("seq")
    pairs = [(i, i + by) for i in range(size) if 0 <= i + by < size]
    return lax.ppermute(shard, "seq", pairs)


def silu_grad(values):
    sigmoid = 1.0 / (1.0 + jnp.exp(-values))
    return sigmoid * (1.0 + values * (1.0 - sigmoid))


def silu(values):
    return values / (1.0 + jnp.exp(-values))


def mm(a, b, dims=NN):
    return lax.dot_general(a, b, dims, preferred_element_type=f32)


def parts(a):
    high = a.astype(bf16)
    return high, (a - high.astype(f32)).astype(bf16)


def along(pieces, dims, side):
    return jnp.concatenate(pieces, axis=dims[0][side][0])


def mm_left(a, b, dims=NN):
    return mm(along(parts(a), dims, 0), along([b, b], dims, 1), dims)


def mm_right(a, b, dims=NN):
    return mm(along([a, a], dims, 0), along(parts(b), dims, 1), dims)


def mm_both(a, b, dims=NN):
    a_high, a_low = parts(a)
    b_high, b_low = parts(b)
    return mm(
        along([a_high, a_low, a_high], dims, 0), along([b_high, b_high, b_low], dims, 1), dims
    )


def mm_exact(a, b, dims=NN):
    return lax.dot_general(a, b, dims, precision=highest, preferred_element_type=f32)


def widen(cols):
    rows = cols.shape[0]
    lane = lax.broadcasted_iota(jnp.int32, (rows, LANES), 1)
    pieces = []
    for pair in range(BLOCK // LANES):
        first = jnp.broadcast_to(cols[:, 2 * pair : 2 * pair + 1], (rows, LANES))
        second = jnp.broadcast_to(cols[:, 2 * pair + 1 : 2 * pair + 2], (rows, LANES))
        pieces.append(jnp.where(lane < HEAD_DIM, first, second))
    return jnp.concatenate(pieces, axis=1)


def rolled(full, step):
    shift = lax.rem(LANES - BLOCK_HEADS * step, LANES)
    return pltpu.roll(full, shift, 1)


def causal():
    rows = lax.broadcasted_iota(jnp.int32, (CHUNK, CHUNK), 0)
    cols = lax.broadcasted_iota(jnp.int32, (CHUNK, CHUNK), 1)
    return rows >= cols


def conv_rows(ext, taps, first, rows):
    out = taps[CONV : CONV + 1, :]
    for k in range(CONV):
        out = out + taps[k : k + 1, :] * ext[first + k : first + k + rows, :]
    return out


def stack_pair(block):
    lane = lax.broadcasted_iota(jnp.int32, block.shape, 1)
    low = jnp.where(lane < HEAD_DIM, block, jnp.zeros_like(block))
    return low, block - low


class StateExchange:
    def __init__(self, index, size, reverse, own, landing, mixed, result, sems, gains):
        self.index, self.size, self.reverse = index, size, reverse
        self.own, self.landing, self.mixed, self.result = own, landing, mixed, result
        self.sems, self.gains = sems, gains

    def other(self, distance):
        return lax.rem(self.index + distance, self.size)

    def slot(self, source):
        return lax.rem(source - self.index - 1 + 2 * self.size, self.size)

    def send(self, j, value):
        share = value.shape[0] // self.size
        kind = self.own.dtype
        pieces = value.reshape(self.size, share, value.shape[1])
        self.own[j] = pieces.astype(kind)
        for d in range(1, self.size):
            pltpu.make_async_remote_copy(
                src_ref=self.own.at[j, self.other(d)],
                dst_ref=self.landing.at[j, self.size - d - 1],
                send_sem=self.sems.at[0, j],
                recv_sem=self.sems.at[1, j],
                device_id={"seq": self.other(d)},
                device_id_type=pl.DeviceIdType.MESH,
            ).start()

    def all_of(self, buffer, j, send, recv):
        return pltpu.make_async_remote_copy(
            src_ref=buffer.at[j, pl.ds(0, self.size - 1)],
            dst_ref=buffer.at[j, pl.ds(0, self.size - 1)],
            send_sem=self.sems.at[send, j],
            recv_sem=self.sems.at[recv, j],
            device_id={"seq": self.other(1)},
            device_id_type=pl.DeviceIdType.MESH,
        )

    def turn(self, j):
        self.all_of(self.landing, j, 0, 1).wait()
        kind = self.own.dtype
        self.landing[j, self.size - 1] = self.own[j, self.index]
        held = jnp.zeros(self.own.shape[2:], f32)
        order = range(self.size - 1, -1, -1) if self.reverse else range(self.size)
        for source in order:
            self.mixed[j, source] = held.astype(kind)
            gain = widen(rolled(self.gains[source : source + 1, :], j)[:, :BLOCK_HEADS])
            held = gain * held + self.landing[j, self.slot(source)].astype(f32)
        for d in range(1, self.size):
            pltpu.make_async_remote_copy(
                src_ref=self.mixed.at[j, self.other(d)],
                dst_ref=self.result.at[j, self.index],
                send_sem=self.sems.at[2, j],
                recv_sem=self.sems.at[3, j],
                device_id={"seq": self.other(d)},
                device_id_type=pl.DeviceIdType.MESH,
            ).start()

    def take(self, j):
        self.all_of(self.result, j, 2, 3).wait()
        self.result[j, self.index] = self.mixed[j, self.index]
        whole = self.result[j].astype(f32)
        return whole.reshape(whole.shape[0] * whole.shape[1], whole.shape[2])


def exchange_scratch(nb, size, kind):
    share = STATE // size
    return [pltpu.VMEM((nb, size, share, BLOCK), kind) for _ in range(4)] + [
        pltpu.SemaphoreType.DMA((4, nb))
    ]


def greet_all(index, core, size):
    barrier = pltpu.get_barrier_semaphore()
    for d in range(1, size):
        pl.semaphore_signal(
            barrier, inc=1, device_id={"seq": lax.rem(index + d, size)},
            device_id_type=pl.DeviceIdType.MESH,
        )
    pl.semaphore_signal(
        barrier, inc=1, device_id={"head": 1 - core}, device_id_type=pl.DeviceIdType.MESH
    )


def await_all(size):
    pl.semaphore_wait(pltpu.get_barrier_semaphore(), size)


def send_to(src, dst, send_sem, recv_sem, **where):
    return pltpu.make_async_remote_copy(
        src_ref=src, dst_ref=dst, send_sem=send_sem, recv_sem=recv_sem, device_id=where,
        device_id_type=pl.DeviceIdType.MESH,
    )


def transposed(block):
    return block.astype(f32).T.astype(bf16)


def forward_kernel(
    size,
    hid_ref, gain_ref, wi_ref, wstep_ref, wshared_ref, cv_ref, cs_ref, bias_ref, decay_ref,
    skip_ref, ggain_ref, wout_ref, hrow_ref, crow_ref,
    normedt_ref, scale_ref, gate_ref, vext_ref, after_ref, y_ref, gw_ref, in_ref, step_ref,
    slope_ref, run_ref, runt_ref, stept_ref, sext_ref, bc_ref, gains_ref, out_ref, gmt_ref,
    coef_ref, near_ref,
    nx, halo, halo_sems, scores, bt, end_w, vwide, gates, ys, states, acc, acc_send,
    acc_land, acc_sems, squares, sq_land, sq_sems, totals, totals_land, totals_sems,
    near_land, near_sems, ex_own, ex_landing, ex_mixed, ex_result, ex_sems,
):
    step_id = pl.program_id(0)
    index = lax.axis_index("seq")
    core = lax.axis_index("head")
    tokens = hid_ref.shape[0]
    width = hid_ref.shape[1]
    chunks = tokens // CHUNK
    nb = gates.shape[0]
    t_mix, t_last = nb, 2 * nb
    half_width = width // 2
    exchange = StateExchange(
        index, size, False, ex_own, ex_landing, ex_mixed, ex_result, ex_sems, gains_ref
    )

    def norm_rows(rows):
        wide = rows.astype(f32)
        scale = lax.rsqrt(jnp.mean(wide * wide, axis=1, keepdims=True) + norm_eps)
        return (wide * scale * gain_ref[...]).astype(bf16), scale

    def totals_copy(d):
        return send_to(
            totals, totals_land.at[size - d - 1], totals_sems.at[0], totals_sems.at[1],
            seq=lax.rem(index + d, size),
        )

    @pl.when(step_id == 0)
    def _():
        greet_all(index, core, size)

        @pl.loop(0, chunks)
        def _(i):
            start = pl.multiple_of(i * CHUNK, CHUNK)
            for part in range(2):
                at = pl.multiple_of(start + part * 64, 64)
                rows, scale = norm_rows(hid_ref[pl.ds(at, 64), :])
                nx[pl.ds(pl.multiple_of(HALO + at, HALO), 64), :] = rows
                scale_ref[pl.ds(at, 64), :] = jnp.broadcast_to(scale, (64, LANES))

        await_all(size)
        after_id = lax.rem(index + 1, size)
        halo_copy = send_to(
            hid_ref.at[pl.ds(tokens - HALO, HALO)], halo, halo_sems.at[0], halo_sems.at[1],
            seq=after_id,
        )
        halo_copy.start()
        for c in range(chunks):
            for b in range(width // LANES):
                normedt_ref[b * LANES : (b + 1) * LANES, c * CHUNK : (c + 1) * CHUNK] = transposed(
                    nx[HALO + c * CHUNK : HALO + (c + 1) * CHUNK, b * LANES : (b + 1) * LANES]
                )
        raw = mm(nx[HALO:, :], wstep_ref[...]) + bias_ref[...]
        small = jnp.exp(-jnp.abs(raw))
        step = jnp.maximum(raw, 0.0) + jnp.log1p(small)
        step_ref[...] = step
        slope_ref[...] = 1.0 / (1.0 + jnp.exp(-raw))
        rate = -step * jnp.exp(decay_ref[...])
        tri = causal().astype(f32)
        total = jnp.zeros((1, LANES), f32)
        for c in range(chunks):
            rows = slice(c * CHUNK, (c + 1) * CHUNK)
            run = mm_exact(tri, rate[rows, :])
            run_ref[rows, :] = run
            total = total + run[CHUNK - 1 :, :]
            run_t = run.T
            step_t = step[rows, :].T
            for b in range(nb):
                heads = slice(BLOCK_HEADS * b, BLOCK_HEADS * (b + 1))
                runt_ref[b, 0:BLOCK_HEADS, rows] = run_t[heads, :]
                stept_ref[b, 0:BLOCK_HEADS, rows] = step_t[heads, :]
                runt_ref[b, BLOCK_HEADS:, rows] = jnp.zeros((8 - BLOCK_HEADS, CHUNK), f32)
                stept_ref[b, BLOCK_HEADS:, rows] = jnp.zeros((8 - BLOCK_HEADS, CHUNK), f32)
            end_w[rows, :] = step[rows, :] * jnp.exp(run[CHUNK - 1 :, :] - run)
        totals[...] = jnp.broadcast_to(jnp.exp(total), totals.shape)
        for d in range(1, size):
            totals_copy(d).start()
        halo_copy.wait()
        keep = jnp.where(index == 0, 0.0, 1.0)
        nx[0:HALO, :] = (norm_rows(halo[...])[0].astype(f32) * keep).astype(bf16)
        shared = mm(nx[...], wshared_ref[...]).astype(bf16)
        sext_ref[0] = shared[:, :STATE]
        sext_ref[1] = shared[:, STATE:]
        conv = conv_rows(shared.astype(f32), cs_ref[...], HALO - CONV + 1, tokens)
        act = silu(conv).astype(bf16)
        bc_ref[...] = act
        for c in range(chunks):
            rows = slice(c * CHUNK, (c + 1) * CHUNK)
            b_rows = act[rows, :STATE]
            c_rows = act[rows, STATE:]
            scores[c] = mm(c_rows, b_rows, NT)
            bt[:, rows] = transposed(b_rows)

    @pl.when(step_id < t_mix)
    def _():
        j = step_id
        values = mm(nx[...], wi_ref[1]).astype(bf16)
        vext_ref[...] = values
        vwide[...] = values.astype(f32)
        conv = conv_rows(vwide, cv_ref[...], HALO - CONV + 1, tokens)
        act = silu(conv).astype(bf16)
        run_cols = rolled(run_ref[...], j)
        end_cols = rolled(end_w[...], j)
        state = jnp.zeros((STATE, BLOCK), f32)
        for c in range(chunks):
            rows = slice(c * CHUNK, (c + 1) * CHUNK)
            weighted = act[rows, :].astype(f32) * widen(end_cols[rows, :BLOCK_HEADS])
            last = widen(jnp.exp(run_cols[(c + 1) * CHUNK - 1 : (c + 1) * CHUNK, :BLOCK_HEADS]))
            state = last * state + mm_right(bt[:, rows], weighted)
            after_ref[c] = state
            states[j, c] = state
        exchange.send(j, state)
        gate = mm(nx[HALO:, :], wi_ref[0])
        gate_ref[...] = gate
        gates[j] = gate
        mask = causal()
        skip = widen(rolled(skip_ref[...], j)[:, :BLOCK_HEADS])
        for c in range(chunks):
            rows = slice(c * CHUNK, (c + 1) * CHUNK)
            cols = run_cols[rows, :BLOCK_HEADS]
            x = act[rows, :]
            y_pairs = []
            for pair in range(BLOCK // LANES):
                mats = []
                for k in range(2):
                    head = 2 * pair + k
                    gap = cols[:, head : head + 1] - runt_ref[j, head : head + 1, rows]
                    decayed = jnp.exp(jnp.where(mask, gap, -1e30))
                    mats.append(scores[c] * decayed * stept_ref[j, head : head + 1, rows])
                low, high = stack_pair(x[:, pair * LANES : (pair + 1) * LANES])
                y_pairs.append(
                    mm_left(jnp.concatenate(mats, axis=1), jnp.concatenate([low, high], axis=0))
                )
            ys[j, rows, :] = jnp.concatenate(y_pairs, axis=1) + skip * x.astype(f32)

    @pl.when(step_id == 1)
    def _():
        pltpu.make_async_remote_copy(
            src_ref=totals_land.at[pl.ds(0, size - 1)],
            dst_ref=totals_land.at[pl.ds(0, size - 1)],
            send_sem=totals_sems.at[0], recv_sem=totals_sems.at[1],
            device_id={"seq": lax.rem(index + 1, size)},
            device_id_type=pl.DeviceIdType.MESH,
        ).wait()
        totals_land[size - 1] = totals[...]
        for source in range(size):
            gains_ref[source : source + 1, :] = totals_land[exchange.slot(source), 0:1, :]

    @pl.when((step_id >= 2) & (step_id < nb + 2))
    def _():
        exchange.turn(step_id - 2)

    def neighbour_copy(bit, first, count):
        mine = (index // (1 << bit)) % 2
        source = pl.multiple_of(core * half_width + first, LANES)
        return send_to(
            normedt_ref.at[pl.ds(source, count)],
            near_land.at[bit, pl.ds(first, count)], near_sems.at[0, bit], near_sems.at[1, bit],
            seq=index + (1 - 2 * mine) * (1 << bit),
        )

    @pl.when((step_id >= 1) & (step_id <= half_width // LANES))
    def _():
        first = pl.multiple_of((step_id - 1) * LANES, LANES)
        for bit in range(2):
            neighbour_copy(bit, first, LANES).start()

    @pl.when((step_id >= t_mix) & (step_id < t_last))
    def _():
        j = step_id - t_mix
        entering = exchange.take(j)
        in_ref[...] = entering
        offsets = offsets_of(run_ref, chunks)
        gated = []
        for c in range(chunks):
            rows = slice(c * CHUNK, (c + 1) * CHUNK)
            grow = rolled(jnp.exp(run_ref[rows, :]), j)[:, :BLOCK_HEADS]
            base = rolled(jnp.exp(offsets[c]), j)[:, :BLOCK_HEADS]
            enter = widen(base) * entering
            if c:
                enter = enter + states[j, c - 1]
            y = ys[j, rows, :] + widen(grow) * mm_right(bc_ref[rows, STATE:], enter)
            y_ref[rows, :] = y
            out = y * silu(gates[j, rows, :])
            gw_ref[rows, :] = (out * ggain_ref[...]).astype(bf16)
            gated.append(
                jnp.broadcast_to(jnp.sum(out * out, axis=1, keepdims=True), (CHUNK, LANES))
            )
        part = mm(gw_ref[...], wout_ref[...], NT)
        block_squares = jnp.concatenate(gated, axis=0)

        @pl.when(j == 0)
        def _():
            acc[...] = part
            squares[...] = block_squares

        @pl.when(j > 0)
        def _():
            acc[...] += part
            squares[...] += block_squares

        @pl.when(j == nb - 1)
        def _():
            send_to(squares, sq_land, sq_sems.at[0], sq_sems.at[1], head=1 - core).start()
            for c in range(chunks):
                acc_send[c] = acc[c * CHUNK : (c + 1) * CHUNK, :].astype(bf16)
                send_to(
                    acc_send.at[c], acc_land.at[c], acc_sems.at[0, c], acc_sems.at[1, c],
                    head=1 - core,
                ).start()

    @pl.when(step_id >= t_last)
    def _():
        c = step_id - t_last

        @pl.when(c == 0)
        def _():
            send_to(squares, sq_land, sq_sems.at[0], sq_sems.at[1], head=1 - core).wait()

        send_to(
            acc_send.at[c], acc_land.at[c], acc_sems.at[0, c], acc_sems.at[1, c], head=1 - core
        ).wait()
        rows = pl.ds(pl.multiple_of(c * CHUNK, CHUNK), CHUNK)
        mixed = acc[rows, :] + acc_land[c].astype(f32)
        inverse = lax.rsqrt((squares[rows, 0:1] + sq_land[rows, 0:1]) / INNER + norm_eps)
        out_ref[...] = hrow_ref[...].astype(f32) + mixed * inverse
        cot = crow_ref[...].astype(f32)
        scaled = (cot * inverse).astype(bf16)
        for b in range(width // LANES):
            gmt_ref[b * LANES : (b + 1) * LANES, :] = transposed(
                scaled[:, b * LANES : (b + 1) * LANES]
            )
        grad_inverse = jnp.sum(cot * mixed, axis=1, keepdims=True)
        coef_ref[...] = jnp.broadcast_to(
            grad_inverse * inverse * inverse * inverse / INNER, (CHUNK, LANES)
        )

        @pl.when(c == chunks - 1)
        def _():
            for bit in range(2):
                neighbour_copy(bit, 0, half_width).wait()
                near_ref[bit] = near_land[bit]


def offsets_of(run_ref, chunks):
    rows = [jnp.zeros((1, LANES), f32)]
    for c in range(chunks):
        rows.append(rows[-1] + run_ref[(c + 1) * CHUNK - 1 : (c + 1) * CHUNK, :])
    return rows


def forward_call(
    hidden, cotangent, gain, both, wstep, wshared, conv_values, conv_shared, bias, decay, skip,
    gate_gain, wout,
):
    tokens, width = hidden.shape
    inner = both.shape[2]
    chunks = tokens // CHUNK
    nb = inner // BLOCK
    size = lax.axis_size("seq")
    t_mix, t_last = nb, 2 * nb

    def at(start):
        return lambda s: jnp.clip(s - start, 0, nb - 1)

    def full(shape):
        return pl.BlockSpec(shape, lambda s: (0,) * len(shape), pipeline_mode=pl.Buffered(1))

    def cols(rows, start):
        return pl.BlockSpec((rows, BLOCK), lambda s: (0, at(start)(s)))

    row_of = lambda s: jnp.clip(s - t_last, 0, chunks - 1)
    row_block = lambda w: pl.BlockSpec((CHUNK, w), lambda s: (row_of(s), 0))
    outs = [
        ((width, tokens), bf16, full((width, tokens))),
        ((tokens, LANES), f32, full((tokens, LANES))),
        ((tokens, inner), f32, cols(tokens, 0)),
        ((HALO + tokens, inner), bf16, cols(HALO + tokens, 0)),
        (
            (chunks, STATE, inner), f32,
            pl.BlockSpec((chunks, STATE, BLOCK), lambda s: (0, 0, at(0)(s))),
        ),
        ((tokens, inner), f32, cols(tokens, t_mix)),
        ((tokens, inner), bf16, cols(tokens, t_mix)),
        ((STATE, inner), f32, cols(STATE, t_mix)),
        ((tokens, LANES), f32, full((tokens, LANES))),
        ((tokens, LANES), f32, full((tokens, LANES))),
        ((tokens, LANES), f32, full((tokens, LANES))),
        ((nb, 8, tokens), f32, full((nb, 8, tokens))),
        ((nb, 8, tokens), f32, full((nb, 8, tokens))),
        ((2, HALO + tokens, STATE), bf16, full((2, HALO + tokens, STATE))),
        ((tokens, 2 * STATE), bf16, full((tokens, 2 * STATE))),
        ((size, LANES), f32, full((size, LANES))),
        ((tokens, width), f32, row_block(width)),
        ((width, tokens), bf16, pl.BlockSpec((width, CHUNK), lambda s: (0, row_of(s)))),
        ((tokens, LANES), f32, row_block(LANES)),
        ((2, width // 2, tokens), bf16, full((2, width // 2, tokens))),
    ]
    sem = pltpu.SemaphoreType.DMA
    return pl.pallas_call(
        functools.partial(forward_kernel, size),
        grid=(2 * nb + chunks,),
        in_specs=[
            full((tokens, width)),
            full((1, width)),
            pl.BlockSpec((2, width, BLOCK), lambda s: (0, 0, at(0)(s))),
            full((width, LANES)),
            full((width, 2 * STATE)),
            cols(CONV + 1, 0),
            full((CONV + 1, 2 * STATE)),
            full((1, LANES)),
            full((1, LANES)),
            full((1, LANES)),
            cols(1, t_mix),
            cols(width, t_mix),
            row_block(width),
            row_block(width),
        ],
        out_shape=[jax.ShapeDtypeStruct(shape, kind) for shape, kind, _ in outs],
        out_specs=[spec for _, _, spec in outs],
        scratch_shapes=[
            pltpu.VMEM((HALO + tokens, width), bf16),
            pltpu.VMEM((HALO, width), bf16),
            sem((2,)),
            pltpu.VMEM((chunks, CHUNK, CHUNK), f32),
            pltpu.VMEM((STATE, tokens), bf16),
            pltpu.VMEM((tokens, LANES), f32),
            pltpu.VMEM((HALO + tokens, BLOCK), f32),
            pltpu.VMEM((nb, tokens, BLOCK), f32),
            pltpu.VMEM((nb, tokens, BLOCK), f32),
            pltpu.VMEM((nb, chunks, STATE, BLOCK), f32),
            pltpu.VMEM((tokens, width), f32),
            pltpu.VMEM((chunks, CHUNK, width), bf16),
            pltpu.VMEM((chunks, CHUNK, width), bf16),
            sem((2, chunks)),
            pltpu.VMEM((tokens, LANES), f32),
            pltpu.VMEM((tokens, LANES), f32),
            sem((2,)),
            pltpu.VMEM((8, LANES), f32),
            pltpu.VMEM((size, 8, LANES), f32),
            sem((2,)),
            pltpu.VMEM((2, width // 2, tokens), bf16),
            sem((2, 2)),
        ] + exchange_scratch(nb, size, f32),
        compiler_params=pltpu.CompilerParams(
            collective_id=1, has_side_effects=True, vmem_limit_bytes=67043328
        ),
        name="forward",
    )(
        hidden, gain, both, wstep, wshared, conv_values, conv_shared, bias, decay, skip, gate_gain,
        wout, hidden, cotangent,
    )


def order_rows(part, bits):
    order = list(range(bits))
    if part == 1:
        order[:3] = order[:3][::-1]
    if part == 2:
        order[:2] = order[:2][::-1]
    return order


def order_columns(part, bits):
    return [bit for bit in range(bits) if bit != part] + [part]


def slot_of(owner, order):
    slot = 0
    for bit in order:
        slot = slot * 2 + ((owner >> bit) & 1)
    return slot


class Reduction:
    def __init__(self, held, landing, order, index, sems, put, put_other=None):
        self.held, self.landing, self.order = held, landing, order
        self.index, self.sems, self.put, self.put_other = index, sems, put, put_other
        self.stages = len(order)

    def place(self, stage):
        base = 0
        size = 1 << self.stages
        for s, bit in enumerate(self.order[: stage + 1]):
            mine = (self.index // (1 << bit)) % 2
            half = size >> (s + 1)
            keep, give = base + mine * half, base + (1 - mine) * half
            base = keep
        return keep, give, half

    def copy(self, stage):
        _, give, half = self.place(stage)
        bit = self.order[stage]
        mine = (self.index // (1 << bit)) % 2
        return send_to(
            self.held.at[pl.ds(give, half)], self.landing[stage],
            self.sems.at[0, stage], self.sems.at[1, stage],
            seq=self.index + (1 - 2 * mine) * (1 << bit),
        )

    def start(self, stage):
        self.copy(stage).start()

    def start_piece(self, piece, pieces):
        _, give, half = self.place(0)
        count = half // pieces
        bit = self.order[0]
        mine = (self.index // (1 << bit)) % 2
        send_to(
            self.held.at[pl.ds(give + piece * count, count)],
            self.landing[0].at[pl.ds(piece * count, count)],
            self.sems.at[0, 0], self.sems.at[1, 0],
            seq=self.index + (1 - 2 * mine) * (1 << bit),
        ).start()

    def advance(self, stage):
        self.copy(stage).wait()
        keep, _, half = self.place(stage)
        if stage < self.stages - 1:

            @pl.loop(0, half)
            def _(i):
                total = self.held[keep + i].astype(f32) + self.landing[stage][i].astype(f32)
                self.held[keep + i] = total.astype(bf16)

            self.start(stage + 1)
        elif self.put_other is None:
            self.put(self.held[keep].astype(f32) + self.landing[stage][0].astype(f32))
        else:
            self.put(self.held[keep].astype(f32))
            self.put_other(self.landing[stage][0].astype(f32))


def sum_copy(acc, landing, bit, index, sems):
    mine = (index // (1 << bit)) % 2
    return pltpu.make_async_remote_copy(
        src_ref=acc.at[bit],
        dst_ref=landing.at[bit],
        send_sem=sems.at[0, bit],
        recv_sem=sems.at[1, bit],
        device_id={"seq": index + (1 - 2 * mine) * (1 << bit)},
        device_id_type=pl.DeviceIdType.MESH,
    )


def back_kernel(
    bits,
    gmt_ref, normedt_ref, near_ref, gw_ref, coef_ref, gains_ref, run_ref, step_ref, slope_ref,
    bc_ref, sext_ref, skip_ref, decay_ref, cs_ref, wshared_ref, wstep_ref, gain_ref,
    wout_ref, y_ref, gate_ref, ggain_ref, vext_ref, after_ref, in_ref, cv_ref, runt_ref,
    stept_ref, wi_ref,
    hid_ref, cot_ref, scale_ref,
    gout_ref, ginner_ref, gsmall_ref, ghid_ref, sums_ref,
    w_out, w_gate, w_values, w_small,
    land_out, land_gate, land_values, land_small,
    rs_sems, near, near_sems,
    own_cols, other_cols, land_cols, cols_sems,
    gv, acc_send, acc_land, acc_sems,
    edge_own, edge_tail, edge_land, edge_sems,
    dbc, dbc_land, dbc_sems, small, sedge_own, sedge_land, sedge_sems,
    vec, vec_land, vec_sems,
    scores, scorest, ct, dscores, end_w, ends, dcols, xdu, dyc, xdus, vwide, gext,
    dys, ggates, term_gate, ex_own, ex_landing, ex_mixed, ex_result, ex_sems,
):
    step_id = pl.program_id(0)
    index = lax.axis_index("seq")
    core = lax.axis_index("head")
    size = 1 << bits
    tokens = y_ref.shape[0]
    chunks = tokens // CHUNK
    nb = ggates.shape[0]
    half_nb = nb // 2
    width = normedt_ref.shape[0]
    half_width = width // 2
    rows_own = width // size
    t_scan, t_grad, t_final = nb, 2 * nb, 3 * nb
    after_id = lax.rem(index + 1, size)
    before_id = lax.rem(index + size - 1, size)
    bit_of = lambda bit: (index // (1 << bit)) % 2
    flip_of = lambda bit: index + (1 - 2 * bit_of(bit)) * (1 << bit)

    def out_reduction(part):
        cols = w_out.shape[3]

        def put(value):
            gout_ref[:, part * cols : (part + 1) * cols] = value

        return Reduction(
            w_out.at[part], [ref.at[part] for ref in land_out], order_rows(part, bits), index,
            rs_sems.at[part], put,
        )

    def columns_reduction(g, part):
        held, landing = ((w_gate, land_gate), (w_values, land_values))[g]

        def put_half(half):
            def put(value):
                for b in range(half_nb):
                    lane = (part * half_nb + b) * BLOCK + half * LANES
                    place = pl.ds(pl.multiple_of(lane, LANES), LANES)
                    ginner_ref[g, :, place] = value[:, b * LANES : (b + 1) * LANES]

            return put

        return Reduction(
            held.at[part], [ref.at[part] for ref in landing], order_columns(part, bits), index,
            rs_sems.at[2 + 2 * g + part], put_half(bit_of(part)), put_half(1 - bit_of(part)),
        )

    def put_small(value):
        gsmall_ref[...] = value

    rs_out = [out_reduction(part) for part in range(2)]
    rs_gate = [columns_reduction(0, part) for part in range(2)]
    rs_values = [columns_reduction(1, part) for part in range(2)]
    rs_small = Reduction(
        w_small, list(land_small), order_rows(2, bits), index, rs_sems.at[6], put_small
    )

    def when_after(step):
        return pl.when(step_id == step)

    exchange = StateExchange(
        index, size, True, ex_own, ex_landing, ex_mixed, ex_result, ex_sems, gains_ref
    )

    def near_copies(bit):
        half = pl.ds(pl.multiple_of(core * half_width, half_width), half_width)
        return (
            pltpu.make_async_copy(near_ref.at[bit], near.at[bit, half], near_sems.at[0, bit]),
            send_to(
                near_ref.at[bit], near.at[bit, half], near_sems.at[1, bit], near_sems.at[2, bit],
                head=1 - core,
            ),
        )

    @pl.when(step_id == 0)
    def _():
        greet_all(index, core, size)
        for c in range(chunks):
            rows = slice(c * CHUNK, (c + 1) * CHUNK)
            ct[:, rows] = transposed(bc_ref[rows, STATE:])
            for b in range(width // LANES):
                acc_send[c, :, b * LANES : (b + 1) * LANES] = transposed(
                    gmt_ref[b * LANES : (b + 1) * LANES, rows]
                )
        await_all(size)
        for bit in range(2):
            for copy in near_copies(bit):
                copy.start()

    group = width // 4
    owners = size // 4

    def scatter(piece, q, order, store):
        for b in range(owners):
            store(slot_of(q * owners + b, order), piece[b * rows_own : (b + 1) * rows_own, :])

    def put_out(part):
        cols = w_out.shape[3]
        for q in range(4):
            left = gmt_ref[q * group : (q + 1) * group, :]
            piece = mm(left, gw_ref[:, part * cols : (part + 1) * cols]).astype(bf16)

            def store(slot, value):
                w_out[part, slot] = value

            scatter(piece, q, order_rows(part, bits), store)

    def columns_copy(g, part):
        return send_to(
            other_cols.at[g, part], land_cols.at[g, part], cols_sems.at[0, g, part],
            cols_sems.at[1, g, part], seq=flip_of(part),
        )

    def split_block(g, j, value):
        part = j // half_nb
        mine = jnp.where(part == 0, bit_of(0), bit_of(1))
        place = pl.ds(pl.multiple_of((j % half_nb) * LANES, LANES), LANES)
        first, second = value[:, :LANES], value[:, LANES:]
        own_cols[g, part, :, place] = jnp.where(mine == 0, first, second)
        other_cols[g, part, :, place] = jnp.where(mine == 0, second, first)

    def put_columns(g, part):
        columns_copy(g, part).wait()
        held = (w_gate, w_values)[g]
        for q in range(4):
            rows = slice(q * group, (q + 1) * group)
            piece = mm(
                jnp.concatenate([normedt_ref[rows, :], near[part, rows, :]], axis=1),
                jnp.concatenate([own_cols[g, part], land_cols[g, part]], axis=0),
            )

            def store(slot, value):
                held[part, slot] = value

            scatter(piece.astype(bf16), q, order_columns(part, bits), store)
        (rs_gate, rs_values)[g][part].start(0)

    @pl.when(step_id < t_scan)
    def _():
        j = step_id
        offsets = offsets_of(run_ref, chunks)
        own = jnp.zeros((STATE, BLOCK), f32)
        term = jnp.zeros((1, BLOCK), f32)
        for c in range(chunks):
            rows = slice(c * CHUNK, (c + 1) * CHUNK)
            ggw = mm(acc_send[c], wout_ref[...])
            y = y_ref[rows, :]
            gate = gate_ref[rows, :]
            sig = 1.0 / (1.0 + jnp.exp(-gate))
            act = gate * sig
            out = y * act
            term = term + jnp.sum(ggw * out, axis=0, keepdims=True)
            coef = jnp.concatenate([coef_ref[rows, 0:LANES]] * (BLOCK // LANES), axis=1)
            gg = ggw * ggain_ref[...] - coef * out
            dy = gg * act
            dys[j, rows, :] = dy
            ggate = (gg * y * (sig * (1.0 + gate * (1.0 - sig)))).astype(bf16)
            ggates[j, rows, :] = ggate
            grow = rolled(jnp.exp(run_ref[rows, :] + offsets[c]), j)[:, :BLOCK_HEADS]
            own = own + mm(ct[:, rows], (dy * widen(grow)).astype(bf16))
        term_gate[j, 0:1, :] = term
        exchange.send(j, own)
        split_block(0, j, ggates[j])

    for part in range(2):

        @when_after(part)
        def _(part=part):
            put_out(part)

    pieces = size // 2

    @pl.when((step_id >= 1) & (step_id < nb))
    def _():
        for reduction in rs_out:
            reduction.start_piece(step_id - 1, pieces)

    rest = pieces - (nb - 1)

    @when_after(nb)
    def _():
        for piece in range(nb - 1, nb - 1 + (rest + 1) // 2):
            for reduction in rs_out:
                reduction.start_piece(piece, pieces)

    @when_after(nb + 1)
    def _():
        for piece in range(nb - 1 + (rest + 1) // 2, pieces):
            for reduction in rs_out:
                reduction.start_piece(piece, pieces)

    @pl.when((step_id >= 2) & (step_id < nb + 2))
    def _():
        exchange.turn(step_id - 2)

    @when_after(half_nb - 1)
    def _():
        columns_copy(0, 0).start()

    @when_after(nb - 1)
    def _():
        columns_copy(0, 1).start()
        for bit in range(2):
            for copy in near_copies(bit):
                copy.wait()
        put_columns(0, 0)

    mask = causal()
    rows_i = lax.broadcasted_iota(jnp.int32, (CHUNK, CHUNK), 0)
    cols_i = lax.broadcasted_iota(jnp.int32, (CHUNK, CHUNK), 1)
    mask_t = rows_i <= cols_i

    @pl.when(step_id == t_scan)
    def _():
        dbc[...] = jnp.zeros_like(dbc)
        dscores[...] = jnp.zeros_like(dscores)
        dcols[...] = jnp.zeros_like(dcols)
        xdu[...] = jnp.zeros_like(xdu)
        dyc[...] = jnp.zeros_like(dyc)
        xdus[...] = jnp.zeros_like(xdus)
        ends[...] = jnp.zeros_like(ends)
        vec[...] = jnp.zeros_like(vec)
        for c in range(chunks):
            rows = slice(c * CHUNK, (c + 1) * CHUNK)
            b_rows = bc_ref[rows, :STATE]
            c_rows = bc_ref[rows, STATE:]
            scores[c] = mm(c_rows, b_rows, NT)
            scorest[c] = mm(b_rows, c_rows, NT)
            run = run_ref[rows, :]
            end_w[rows, :] = jnp.exp(run[CHUNK - 1 :, :] - run)

    @pl.when((step_id >= t_scan) & (step_id < t_grad))
    def _():
        j = step_id - t_scan
        offsets = offsets_of(run_ref, chunks)
        vwide[...] = vext_ref[...].astype(f32)
        taps = [jnp.zeros((1, BLOCK), f32)] * (CONV + 1)
        run_cols = rolled(run_ref[...], j)
        step_cols = rolled(step_ref[...], j)
        end_cols = rolled(end_w[...], j)
        skip = widen(rolled(skip_ref[...], j)[:, :BLOCK_HEADS])
        channel = lax.broadcasted_iota(jnp.int32, (BLOCK, LANES), 0) // HEAD_DIM
        lane = lax.broadcasted_iota(jnp.int32, (BLOCK, LANES), 1)
        pick = (lane == BLOCK_HEADS * j + channel).astype(bf16)
        lane_row = lax.broadcasted_iota(jnp.int32, (CHUNK, LANES), 1)
        dstate = exchange.take(j)
        dskip = jnp.zeros((1, BLOCK), f32)
        gext[tokens : tokens + 8, :] = jnp.zeros((8, BLOCK), f32)
        for c in reversed(range(chunks)):
            rows = slice(c * CHUNK, (c + 1) * CHUNK)
            cols = run_cols[rows, :BLOCK_HEADS]
            conv = conv_rows(vwide, cv_ref[...], HALO - CONV + 1 + c * CHUNK, CHUNK)
            sig = 1.0 / (1.0 + jnp.exp(-conv))
            x = (conv * sig).astype(bf16)
            slope = sig * (1.0 + conv * (1.0 - sig))
            wide_x = x.astype(f32)
            dy = dys[j, rows, :]
            b_rows = bc_ref[rows, :STATE]
            c_rows = bc_ref[rows, STATE:]
            grow = widen(jnp.exp(cols))
            tail = widen(end_cols[rows, :BLOCK_HEADS])
            step_w = widen(step_cols[rows, :BLOCK_HEADS])
            last = grow[CHUNK - 1 :, :]
            base = rolled(jnp.exp(offsets[c]), j)[:, :BLOCK_HEADS]
            enter = widen(base) * in_ref[...]
            if c:
                enter = enter + after_ref[c - 1]
            du_state = tail * mm(b_rows, dstate.astype(bf16))
            carried = grow * mm(c_rows, enter.astype(bf16))
            weighted = wide_x * (tail * step_w)
            grown = dy * grow
            dbc[0, rows, :] += mm_both(weighted, dstate, NT)
            dbc[1, rows, :] += mm_both(grown, enter, NT)
            hold = last * jnp.sum(dstate * enter, axis=0, keepdims=True)
            dstate = last * dstate + mm_right(ct[:, rows], grown)
            du_pairs = []
            col_sum = jnp.zeros((CHUNK, LANES), f32)
            dscore = dscores[c]
            for pair in range(BLOCK // LANES):
                lanes = slice(pair * LANES, (pair + 1) * LANES)
                low, high = stack_pair(dy[:, lanes])
                both = jnp.concatenate([low, high], axis=0)
                dmat = mm_left(both, x[:, lanes], NT)
                mats = []
                for k in range(2):
                    head = 2 * pair + k
                    col = cols[:, head : head + 1]
                    row = runt_ref[0, head : head + 1, rows]
                    keep = jnp.exp(jnp.where(mask, col - row, -1e30))
                    piece = dmat[k * CHUNK : (k + 1) * CHUNK, :] * keep
                    piece = piece * stept_ref[0, head : head + 1, rows]
                    dscore = dscore + piece
                    full = piece * scores[c]
                    col_sum = jnp.where(
                        lane_row == BLOCK_HEADS * j + head,
                        jnp.sum(full, axis=1, keepdims=True),
                        col_sum,
                    )
                    dcols[j, head : head + 1, rows] = jnp.sum(full, axis=0, keepdims=True)
                    keep_t = jnp.exp(jnp.where(mask_t, row - col, -1e30))
                    mats.append(scorest[c] * keep_t)
                du_pairs.append(
                    mm(jnp.concatenate(mats, axis=1).astype(bf16), both.astype(bf16))
                )
            dscores[c] = dscore
            du = jnp.concatenate(du_pairs, axis=1) + du_state
            by_head = mm(
                jnp.concatenate(
                    [
                        (wide_x * du).astype(bf16),
                        (dy * carried).astype(bf16),
                        (wide_x * du_state).astype(bf16),
                        *parts(jnp.broadcast_to(hold, (HALO, BLOCK))),
                    ],
                    axis=0,
                ),
                pick,
            )
            xdu[rows, :] += by_head[0:CHUNK, :]
            dyc[rows, :] += by_head[CHUNK : 2 * CHUNK, :] + col_sum
            xdus[rows, :] += by_head[2 * CHUNK : 3 * CHUNK, :]
            end = 3 * CHUNK
            ends[c : c + 1, :] += (
                by_head[end : end + 1, :] + by_head[end + HALO : end + HALO + 1, :]
            )
            dskip = dskip + jnp.sum(dy * wide_x, axis=0, keepdims=True)
            gconv = (step_w * du + skip * dy) * slope
            gext[rows, :] = gconv
            taps[CONV] = taps[CONV] + jnp.sum(gconv, axis=0, keepdims=True)
            values = vwide[HALO + c * CHUNK : HALO + (c + 1) * CHUNK, :]
            total = cv_ref[CONV - 1 : CONV, :] * gconv
            taps[CONV - 1] = taps[CONV - 1] + jnp.sum(values * gconv, axis=0, keepdims=True)
            for k in range(CONV - 1):
                ahead = c * CHUNK + CONV - 1 - k
                moved = gext[ahead : ahead + CHUNK, :]
                total = total + cv_ref[k : k + 1, :] * moved
                taps[k] = taps[k] + jnp.sum(values * moved, axis=0, keepdims=True)
            gv[j, rows, :] = total.astype(bf16)
            if c == chunks - 1:
                edge_tail[j, 0:8, :] = total[CHUNK - 8 :, :]
        row8 = lax.broadcasted_iota(jnp.int32, (8, BLOCK), 0)
        ahead_rows = vwide[HALO - CONV + 1 : HALO - CONV + 9, :]
        for k in range(CONV):
            tap = taps[k]
            if k < CONV - 1:
                moved = pltpu.roll(gext[0:8, :], k, 0) if k else gext[0:8, :]
                inside = (row8 >= k) & (row8 < CONV - 1)
                tap = tap + jnp.sum(
                    jnp.where(inside, ahead_rows * moved, 0.0), axis=0, keepdims=True
                )
            vec[0, j, k : k + 1, :] = tap
        vec[0, j, CONV : CONV + 1, :] = taps[CONV]
        vec[0, j, CONV + 1 : CONV + 2, :] = term_gate[j, 0:1, :]
        vec[0, j, CONV + 2 : CONV + 3, :] = dskip
        edge_tail[j, 8 : 8 + CONV + 1, :] = cv_ref[...]
        edge_own[j] = gext[0:8, :]
        send_to(
            edge_own.at[j], edge_land.at[j], edge_sems.at[0, j], edge_sems.at[1, j], seq=before_id
        ).start()

    def finish_block(j):
        send_to(
            edge_own.at[j], edge_land.at[j], edge_sems.at[0, j], edge_sems.at[1, j], seq=before_id
        ).wait()
        nxt = jnp.where(index == size - 1, 0.0, 1.0) * edge_land[j]
        row8 = lax.broadcasted_iota(jnp.int32, (8, BLOCK), 0)
        fix = edge_tail[j, 0:8, :]
        for k in range(CONV - 1):
            ahead = CONV - 1 - k
            moved = pltpu.roll(nxt, 8 - ahead, 0)
            fix = fix + jnp.where(row8 >= 8 - ahead, edge_tail[j, 8 + k : 9 + k, :] * moved, 0.0)
        both_rows = jnp.concatenate([gv[j, tokens - 16 : tokens - 8, :].astype(f32), fix], axis=0)
        gv[j, tokens - 16 :, :] = both_rows.astype(bf16)
        split_block(1, j, gv[j])

    @pl.when((step_id > t_scan + 1) & (step_id < t_grad))
    def _():
        finish_block(step_id - t_scan - 2)

    @when_after(t_scan + 1)
    def _():
        put_columns(0, 1)

    @when_after(t_scan + 2)
    def _():
        rs_gate[0].advance(0)
        rs_out[0].advance(0)
        rs_out[1].advance(0)

    @when_after(t_scan + half_nb + 1)
    def _():
        columns_copy(1, 0).start()
        rs_gate[0].advance(1)
        rs_gate[1].advance(0)

    @when_after(t_grad - 1)
    def _():
        rs_out[0].advance(1)

    @when_after(t_grad - 1)
    def _():
        tri = mask.astype(f32)
        tri_t = mask_t.astype(f32)
        strict = (rows_i > cols_i).astype(f32)
        decay = jnp.exp(decay_ref[...])
        bias_sum = jnp.zeros((1, LANES), f32)
        decay_sum = jnp.zeros((1, LANES), f32)
        for c in range(chunks):
            rows = slice(c * CHUNK, (c + 1) * CHUNK)
            step = step_ref[rows, :]
            col_rows = [dcols[b, 0:BLOCK_HEADS, rows] for b in range(nb)]
            rest = LANES - BLOCK_HEADS * nb
            col_rows.append(jnp.zeros((rest, CHUNK), f32))
            dlog = dyc[rows, :] - jnp.concatenate(col_rows, axis=0).T
            drate = (
                mm_exact(tri_t, dlog)
                + mm_exact(strict, xdus[rows, :] * step)
                + ends[c : c + 1, :]
            )
            dstep = xdu[rows, :] - decay * drate
            draw = dstep * slope_ref[rows, :]
            small[rows, LANES:] = draw.astype(bf16)
            bias_sum = bias_sum + jnp.sum(draw, axis=0, keepdims=True)
            decay_sum = decay_sum - jnp.sum(drate * step, axis=0, keepdims=True) * decay
            b_rows = bc_ref[rows, :STATE]
            c_rows = bc_ref[rows, STATE:]
            high, low = parts(dscores[c])
            dbc[1, rows, :] += mm(high, b_rows) + mm(low, b_rows)
            dbc[0, rows, :] += mm(high, c_rows, TN) + mm(low, c_rows, TN)
        vec[0, nb, 0:1, 0:LANES] = bias_sum
        vec[0, nb, 1:2, 0:LANES] = decay_sum
        send_to(
            dbc.at[1 - core], dbc_land, dbc_sems.at[0], dbc_sems.at[1], head=1 - core
        ).start()

    @when_after(t_grad)
    def _():
        finish_block(nb - 2)
        finish_block(nb - 1)
        columns_copy(1, 1).start()
        put_columns(1, 0)
        rs_gate[0].advance(2)
        rs_gate[1].advance(1)
        rs_out[1].advance(1)

    @when_after(t_grad + 1)
    def _():
        rs_gate[0].advance(3)

    @when_after(t_grad)
    def _():
        send_to(
            dbc.at[1 - core], dbc_land, dbc_sems.at[0], dbc_sems.at[1], head=1 - core
        ).wait()
        sext = sext_ref[core].astype(f32)
        taps = cs_ref[core]
        conv = conv_rows(sext, taps, HALO - CONV + 1, tokens)
        gs = (dbc[core] + dbc_land[...]) * silu_grad(conv)
        for k in range(CONV):
            first = HALO - CONV + 1 + k
            vec[0, nb, 2 + k : 3 + k, 0:LANES] = jnp.sum(
                sext[first : first + tokens, :] * gs, axis=0, keepdims=True
            )
        vec[0, nb, 2 + CONV : 3 + CONV, 0:LANES] = jnp.sum(gs, axis=0, keepdims=True)
        dbc[core] = gs
        sedge_own[...] = gs[0:8, :]
        send_to(
            sedge_own, sedge_land, sedge_sems.at[0], sedge_sems.at[1], seq=before_id
        ).start()

    @when_after(t_grad + 1)
    def _():
        send_to(
            sedge_own, sedge_land, sedge_sems.at[0], sedge_sems.at[1], seq=before_id
        ).wait()
        taps = cs_ref[core]
        nxt = jnp.where(index == size - 1, 0.0, 1.0) * sedge_land[...]
        gs = jnp.concatenate([dbc[core], nxt], axis=0)
        total = taps[CONV - 1 : CONV, :] * gs[0:tokens, :]
        for k in range(CONV - 1):
            total = total + taps[k : k + 1, :] * gs[CONV - 1 - k : CONV - 1 - k + tokens, :]
        small[:, 0:LANES] = total.astype(bf16)
        for q in range(4):
            piece = mm(normedt_ref[q * group : (q + 1) * group, :], small[...]).astype(bf16)

            def store(slot, value):
                w_small[slot] = value

            scatter(piece, q, order_rows(2, bits), store)
        rs_small.start(0)

    @pl.when((step_id >= t_grad) & (step_id < t_final))
    def _():
        j = step_id - t_grad
        part = mm(
            jnp.concatenate([ggates[j], gv[j]], axis=1),
            jnp.concatenate([wi_ref[0], wi_ref[1]], axis=1),
            NT,
        )

        @pl.when(j == 0)
        def _():
            for b in range(width // BLOCK):
                dys[b] = part[:, b * BLOCK : (b + 1) * BLOCK]

        @pl.when(j > 0)
        def _():
            for b in range(width // BLOCK):
                dys[b] += part[:, b * BLOCK : (b + 1) * BLOCK]

    @when_after(t_grad + 2)
    def _():
        rs_out[0].advance(2)

    @when_after(t_grad + 3)
    def _():
        put_columns(1, 1)
        rs_out[1].advance(2)

    @when_after(t_grad + 4)
    def _():
        rs_gate[1].advance(2)
        own = pl.ds(pl.multiple_of(core * LANES, LANES), LANES)
        rest = mm(
            small[...], jnp.concatenate([wshared_ref[:, own], wstep_ref[...]], axis=1), NT
        )
        for b in range(width // BLOCK):
            dys[b] += rest[:, b * BLOCK : (b + 1) * BLOCK]

    @when_after(t_final - 1)
    def _():
        for c in range(chunks):
            rows = slice(c * CHUNK, (c + 1) * CHUNK)
            for b in range(width // BLOCK):
                acc_send[c, :, b * BLOCK : (b + 1) * BLOCK] = dys[b, rows, :].astype(bf16)
            send_to(
                acc_send.at[c], acc_land.at[c], acc_sems.at[0, c], acc_sems.at[1, c], head=1 - core
            ).start()

    @pl.when(step_id >= t_final)
    def _():
        c = step_id - t_final
        send_to(
            acc_send.at[c], acc_land.at[c], acc_sems.at[0, c], acc_sems.at[1, c], head=1 - core
        ).wait()
        here = pl.ds(pl.multiple_of(c * CHUNK, CHUNK), CHUNK)
        own_total = jnp.concatenate([dys[b, here, :] for b in range(width // BLOCK)], axis=1)
        total = own_total + acc_land[c].astype(f32)
        scale = scale_ref[:, 0:1]
        hat = hid_ref[...].astype(f32) * scale
        term = jnp.sum(total * hat, axis=0, keepdims=True)

        for b in range(width // BLOCK):
            piece = term[:, b * BLOCK : (b + 1) * BLOCK]
            vec[0, b, 7:8, :] = vec[0, b, 7:8, :] + piece

        ghat = total * gain_ref[...]
        mean = jnp.mean(ghat * hat, axis=1, keepdims=True)
        ghid_ref[...] = cot_ref[...].astype(f32) + scale * (ghat - hat * mean)

    @when_after(t_final)
    def _():
        rs_out[0].advance(3)

    @when_after(t_final + 1)
    def _():
        rs_values[0].advance(0)

    @when_after(t_final + chunks - 1)
    def _():
        rs_out[1].advance(3)

        def begin(bit):
            sum_copy(vec, vec_land, bit, index, vec_sems).start()

        def add(bit):
            sum_copy(vec, vec_land, bit, index, vec_sems).wait()
            vec[bit + 1] = vec[bit] + vec_land[bit]
            if bit + 1 < bits:
                begin(bit + 1)

        begin(0)
        rs_values[1].advance(0)
        add(0)
        rs_small.advance(0)
        rs_gate[1].advance(3)
        add(1)
        rs_values[0].advance(1)
        rs_small.advance(1)
        rs_values[1].advance(1)
        add(2)
        rs_values[0].advance(2)
        rs_small.advance(2)
        rs_values[0].advance(3)
        rs_values[1].advance(2)
        add(3)
        rs_values[1].advance(3)
        rs_small.advance(3)
        for stage in range(4, bits):
            for reduction in rs_out + rs_gate + rs_values + [rs_small]:
                reduction.advance(stage)
            add(stage)
        sums_ref[8:16, 0:BLOCK] = vec[bits, nb]
        for b in range(nb):
            sums_ref[0:8, b * BLOCK : (b + 1) * BLOCK] = vec[bits, b]


def back_call(
    gm_t, normed_t, near, gated_w, coef, gains, run, step, slope, bc, sext, skip, decay,
    conv_shared, wshared, wstep, gain, wout, y, gate, gate_gain, vext, after, state_in, conv_values, runt, stept, both,
    hidden, cotangent, scale,
):
    width, tokens = normed_t.shape
    inner = y.shape[1]
    chunks = tokens // CHUNK
    nb = inner // BLOCK
    size = lax.axis_size("seq")
    bits = size.bit_length() - 1
    rows_own = width // size
    t_scan, t_grad, t_final = nb, 2 * nb, 3 * nb

    def column(start):
        return lambda s: jnp.clip(s - start, 0, nb - 1)

    def full(shape):
        return pl.BlockSpec(shape, lambda s: (0,) * len(shape), pipeline_mode=pl.Buffered(1))

    def cols(rows, start):
        at = column(start)
        return pl.BlockSpec((rows, BLOCK), lambda s: (0, at(s)))

    row_block = lambda w: pl.BlockSpec((CHUNK, w), lambda s: (jnp.clip(s - t_final, 0, chunks - 1), 0))
    row_single = lambda w: pl.BlockSpec(
        (CHUNK, w),
        lambda s: (jnp.clip(s - t_final, 0, chunks - 1), 0),
        pipeline_mode=pl.Buffered(1),
    )
    held = lambda cols: pltpu.VMEM((2, size, rows_own, cols), bf16)
    landing = lambda cols: tuple(
        pltpu.VMEM((2, size >> (s + 1), rows_own, cols), bf16) for s in range(bits)
    )
    columns = lambda: pltpu.VMEM((2, 2, tokens, inner // 4), bf16)
    sem = pltpu.SemaphoreType.DMA
    return pl.pallas_call(
        functools.partial(back_kernel, bits),
        grid=(3 * nb + chunks,),
        in_specs=[
            full((width, tokens)),
            full((width, tokens)),
            pl.BlockSpec(memory_space=pl.ANY),
            full((tokens, inner)),
            full((tokens, LANES)),
            full((size, LANES)),
            full((tokens, LANES)),
            full((tokens, LANES)),
            full((tokens, LANES)),
            full((tokens, 2 * STATE)),
            full((2, HALO + tokens, LANES)),
            full((1, LANES)),
            full((1, LANES)),
            full((2, CONV + 1, LANES)),
            full((width, 2 * LANES)),
            full((width, LANES)),
            full((1, width)),
            cols(width, 0),
            cols(tokens, 0),
            cols(tokens, 0),
            cols(1, 0),
            pl.BlockSpec(
                (HALO + tokens, BLOCK), lambda s: (0, column(t_scan)(s)), pipeline_mode=pl.Buffered(1)
            ),
            pl.BlockSpec((chunks, STATE, BLOCK), lambda s: (0, 0, column(t_scan)(s))),
            cols(STATE, t_scan),
            cols(CONV + 1, t_scan),
            pl.BlockSpec((1, 8, tokens), lambda s: (column(t_scan)(s), 0, 0)),
            pl.BlockSpec((1, 8, tokens), lambda s: (column(t_scan)(s), 0, 0)),
            pl.BlockSpec(
                (2, width, BLOCK), lambda s: (0, 0, column(t_grad)(s)), pipeline_mode=pl.Buffered(1)
            ),
            row_single(width),
            row_single(width),
            row_block(LANES),
        ],
        out_shape=[
            jax.ShapeDtypeStruct((rows_own, inner), f32),
            jax.ShapeDtypeStruct((2, rows_own, inner), f32),
            jax.ShapeDtypeStruct((rows_own, 2 * LANES), f32),
            jax.ShapeDtypeStruct((tokens, width), f32),
            jax.ShapeDtypeStruct((16, inner), f32),
        ],
        out_specs=[
            full((rows_own, inner)),
            full((2, rows_own, inner)),
            full((rows_own, 2 * LANES)),
            row_block(width),
            pl.BlockSpec((16, inner), lambda s: (0, 0)),
        ],
        scratch_shapes=[
            held(inner // 2), held(inner // 4), held(inner // 4),
            pltpu.VMEM((size, rows_own, 2 * LANES), bf16),
            landing(inner // 2), landing(inner // 4), landing(inner // 4),
            tuple(pltpu.VMEM((size >> (s + 1), rows_own, 2 * LANES), bf16) for s in range(bits)),
            sem((7, 2, bits)),
            pltpu.VMEM((2, width, tokens), bf16), sem((3, 2)),
            columns(), columns(), columns(), sem((2, 2, 2)),
            pltpu.VMEM((nb, tokens, BLOCK), bf16),
            pltpu.VMEM((chunks, CHUNK, width), bf16),
            pltpu.VMEM((chunks, CHUNK, width), bf16),
            sem((2, chunks)),
            pltpu.VMEM((nb, 8, BLOCK), f32),
            pltpu.VMEM((nb, 16, BLOCK), f32),
            pltpu.VMEM((nb, 8, BLOCK), f32),
            sem((2, nb)),
            pltpu.VMEM((2, tokens, LANES), f32),
            pltpu.VMEM((tokens, LANES), f32),
            sem((2,)),
            pltpu.VMEM((tokens, 2 * LANES), bf16),
            pltpu.VMEM((8, LANES), f32),
            pltpu.VMEM((8, LANES), f32),
            sem((2,)),
            pltpu.VMEM((bits + 1, nb + 1, 8, BLOCK), f32),
            pltpu.VMEM((bits, nb + 1, 8, BLOCK), f32),
            sem((2, bits)),
            pltpu.VMEM((chunks, CHUNK, CHUNK), f32),
            pltpu.VMEM((chunks, CHUNK, CHUNK), f32),
            pltpu.VMEM((STATE, tokens), bf16),
            pltpu.VMEM((chunks, CHUNK, CHUNK), f32),
            pltpu.VMEM((tokens, LANES), f32),
            pltpu.VMEM((8, LANES), f32),
            pltpu.VMEM((nb, 8, tokens), f32),
            pltpu.VMEM((tokens, LANES), f32),
            pltpu.VMEM((tokens, LANES), f32),
            pltpu.VMEM((tokens, LANES), f32),
            pltpu.VMEM((HALO + tokens, BLOCK), f32),
            pltpu.VMEM((tokens + 8, BLOCK), f32),
            pltpu.VMEM((nb, tokens, BLOCK), f32),
            pltpu.VMEM((nb, tokens, BLOCK), bf16),
            pltpu.VMEM((nb, 8, BLOCK), f32),
        ] + exchange_scratch(nb, size, bf16),
        compiler_params=pltpu.CompilerParams(
            collective_id=3, has_side_effects=True, vmem_limit_bytes=67043328
        ),
        name="back",
    )(
        gm_t, normed_t, near, gated_w, coef, gains, run, step, slope, bc, sext, skip, decay,
        conv_shared, wshared, wstep, gain, wout, y, gate, gate_gain, vext, after, state_in,
        conv_values,
        runt, stept,
        both, hidden, cotangent, scale,
    )


def body(
    hidden, cotangent, norm_gain, proj_inner, proj_step, proj_shared, conv_values, conv_shared,
    step_bias, decay_log, skip_gain, gate_gain, proj_out,
):
    tokens = hidden.shape[0]
    inner = proj_inner.shape[2]
    heads = proj_step.shape[1]
    width = hidden.shape[1]
    size = lax.axis_size("seq")
    shared_here = conv_shared.shape[1] // lax.axis_size("head")
    shared_start = lax.axis_index("head") * shared_here
    both = jnp.transpose(proj_inner, (1, 0, 2))
    rows = [jnp.pad(v, (0, width - v.shape[0])) for v in (step_bias, decay_log, skip_gain)]
    rows = jnp.stack(rows + [norm_gain])
    wstep = jnp.pad(proj_step, ((0, 0), (0, LANES - heads)))
    bias, decay, skip, gain = (rows[i : i + 1] for i in range(4))
    bias, decay, skip = bias[:, :LANES], decay[:, :LANES], skip[:, :LANES]
    (
        normed_t, norm_scale, gate_in, vext, after, y, gated_w, state_in, step, slope, run, runt,
        stept, sext, bc, gains, block_out, gm_t, coef, near,
    ) = forward_call(
        hidden, cotangent, norm_gain[None, :], both, wstep, proj_shared, conv_values, conv_shared,
        bias, decay, skip, gate_gain[None, :], proj_out,
    )
    (gout, ginner, gsmall, grad_hidden, sums) = back_call(
        gm_t, normed_t, near, gated_w, coef, gains, run, step, slope, bc, sext, skip, decay,
        conv_shared.reshape(CONV + 1, -1, LANES).transpose(1, 0, 2),
        proj_shared, wstep, norm_gain[None, :], proj_out, y, gate_in,
        gate_gain[None, :], vext, after, state_in, conv_values, runt, stept, both, hidden,
        cotangent, norm_scale,
    )
    return (
        block_out,
        grad_hidden,
        sums[7],
        ginner.transpose(1, 0, 2),
        gsmall[:, shared_here : shared_here + heads],
        gsmall[:, :shared_here],
        sums[: CONV + 1],
        sums[10 : 11 + CONV, :LANES],
        sums[8, :heads],
        sums[9, :heads],
        jnp.sum(sums[CONV + 2].reshape(heads, HEAD_DIM), axis=1),
        sums[CONV + 1],
        gout,
    )


def solution(mesh):
    return jax.shard_map(
        body,
        mesh=mesh,
        in_specs=(
            P("seq", None),
            P("seq", None),
            P(),
            P(None, None, "head"),
            P(None, "head"),
            P(),
            P(None, "head"),
            P(),
            P("head"),
            P("head"),
            P("head"),
            P("head"),
            P(None, "head"),
        ),
        out_specs=(
            P("seq", None),
            P("seq", None),
            P(),
            P("seq", None, "head"),
            P("seq", "head"),
            P("seq", "head"),
            P(None, "head"),
            P(None, "head"),
            P("head"),
            P("head"),
            P("head"),
            P("head"),
            P("seq", "head"),
        ),
        check_vma=False,
    )
```

```python
import functools

import jax
import jax.numpy as jnp
from jax import lax
from jax.experimental import pallas as pl
from jax.experimental.pallas import tpu as pltpu
from jax.sharding import PartitionSpec as P

HEAD_DIM = 64
STATE = 128
CONV = 4
INNER = 3072
CHUNK = 128
LANES = 128
BLOCK = 256
HALO = 16
BLOCK_HEADS = BLOCK // HEAD_DIM

norm_eps = 1e-05
highest = lax.Precision.HIGHEST
f32 = jnp.float32
bf16 = jnp.bfloat16
NN = (((1,), (0,)), ((), ()))
NT = (((1,), (1,)), ((), ()))
TN = (((0,), (0,)), ((), ()))


def flip(shard, bit):
    size = lax.axis_size("seq")
    return lax.ppermute(shard, "seq", [(i, i ^ (1 << bit)) for i in range(size)])


def swap(shard):
    return lax.ppermute(shard, "head", [(0, 1), (1, 0)])


def from_behind(shard, by):
    size = lax.axis_size("seq")
    pairs = [(i, i + by) for i in range(size) if 0 <= i + by < size]
    return lax.ppermute(shard, "seq", pairs)


def silu_grad(values):
    sigmoid = 1.0 / (1.0 + jnp.exp(-values))
    return sigmoid * (1.0 + values * (1.0 - sigmoid))


def silu(values):
    return values / (1.0 + jnp.exp(-values))


def mm(a, b, dims=NN):
    return lax.dot_general(a, b, dims, preferred_element_type=f32)


def parts(a):
    high = a.astype(bf16)
    return high, (a - high.astype(f32)).astype(bf16)


def along(pieces, dims, side):
    return jnp.concatenate(pieces, axis=dims[0][side][0])


def mm_left(a, b, dims=NN):
    return mm(along(parts(a), dims, 0), along([b, b], dims, 1), dims)


def mm_right(a, b, dims=NN):
    return mm(along([a, a], dims, 0), along(parts(b), dims, 1), dims)


def mm_both(a, b, dims=NN):
    a_high, a_low = parts(a)
    b_high, b_low = parts(b)
    return mm(
        along([a_high, a_low, a_high], dims, 0), along([b_high, b_high, b_low], dims, 1), dims
    )


def mm_exact(a, b, dims=NN):
    return lax.dot_general(a, b, dims, precision=highest, preferred_element_type=f32)


def widen(cols):
    rows = cols.shape[0]
    lane = lax.broadcasted_iota(jnp.int32, (rows, LANES), 1)
    pieces = []
    for pair in range(BLOCK // LANES):
        first = jnp.broadcast_to(cols[:, 2 * pair : 2 * pair + 1], (rows, LANES))
        second = jnp.broadcast_to(cols[:, 2 * pair + 1 : 2 * pair + 2], (rows, LANES))
        pieces.append(jnp.where(lane < HEAD_DIM, first, second))
    return jnp.concatenate(pieces, axis=1)


def rolled(full, step):
    shift = lax.rem(LANES - BLOCK_HEADS * step, LANES)
    return pltpu.roll(full, shift, 1)


def causal():
    rows = lax.broadcasted_iota(jnp.int32, (CHUNK, CHUNK), 0)
    cols = lax.broadcasted_iota(jnp.int32, (CHUNK, CHUNK), 1)
    return rows >= cols


def conv_rows(ext, taps, first, rows):
    out = taps[CONV : CONV + 1, :]
    for k in range(CONV):
        out = out + taps[k : k + 1, :] * ext[first + k : first + k + rows, :]
    return out


def stack_pair(block):
    lane = lax.broadcasted_iota(jnp.int32, block.shape, 1)
    low = jnp.where(lane < HEAD_DIM, block, jnp.zeros_like(block))
    return low, block - low


class StateExchange:
    def __init__(self, index, size, reverse, own, landing, mixed, result, sems, gains):
        self.index, self.size, self.reverse = index, size, reverse
        self.own, self.landing, self.mixed, self.result = own, landing, mixed, result
        self.sems, self.gains = sems, gains

    def other(self, distance):
        return lax.rem(self.index + distance, self.size)

    def slot(self, source):
        return lax.rem(source - self.index - 1 + 2 * self.size, self.size)

    def send(self, j, value):
        share = value.shape[0] // self.size
        kind = self.own.dtype
        pieces = value.reshape(self.size, share, value.shape[1])
        self.own[j] = pieces.astype(kind)
        for d in range(1, self.size):
            pltpu.make_async_remote_copy(
                src_ref=self.own.at[j, self.other(d)],
                dst_ref=self.landing.at[j, self.size - d - 1],
                send_sem=self.sems.at[0, j],
                recv_sem=self.sems.at[1, j],
                device_id={"seq": self.other(d)},
                device_id_type=pl.DeviceIdType.MESH,
            ).start()

    def all_of(self, buffer, j, send, recv):
        return pltpu.make_async_remote_copy(
            src_ref=buffer.at[j, pl.ds(0, self.size - 1)],
            dst_ref=buffer.at[j, pl.ds(0, self.size - 1)],
            send_sem=self.sems.at[send, j],
            recv_sem=self.sems.at[recv, j],
            device_id={"seq": self.other(1)},
            device_id_type=pl.DeviceIdType.MESH,
        )

    def turn(self, j):
        self.all_of(self.landing, j, 0, 1).wait()
        kind = self.own.dtype
        self.landing[j, self.size - 1] = self.own[j, self.index]
        held = jnp.zeros(self.own.shape[2:], f32)
        order = range(self.size - 1, -1, -1) if self.reverse else range(self.size)
        for source in order:
            self.mixed[j, source] = held.astype(kind)
            gain = widen(rolled(self.gains[source : source + 1, :], j)[:, :BLOCK_HEADS])
            held = gain * held + self.landing[j, self.slot(source)].astype(f32)
        for d in range(1, self.size):
            pltpu.make_async_remote_copy(
                src_ref=self.mixed.at[j, self.other(d)],
                dst_ref=self.result.at[j, self.index],
                send_sem=self.sems.at[2, j],
                recv_sem=self.sems.at[3, j],
                device_id={"seq": self.other(d)},
                device_id_type=pl.DeviceIdType.MESH,
            ).start()

    def take(self, j):
        self.all_of(self.result, j, 2, 3).wait()
        self.result[j, self.index] = self.mixed[j, self.index]
        whole = self.result[j].astype(f32)
        return whole.reshape(whole.shape[0] * whole.shape[1], whole.shape[2])


def exchange_scratch(nb, size, kind):
    share = STATE // size
    return [pltpu.VMEM((nb, size, share, BLOCK), kind) for _ in range(4)] + [
        pltpu.SemaphoreType.DMA((4, nb))
    ]


def greet_all(index, core, size):
    barrier = pltpu.get_barrier_semaphore()
    for d in range(1, size):
        pl.semaphore_signal(
            barrier, inc=1, device_id={"seq": lax.rem(index + d, size)},
            device_id_type=pl.DeviceIdType.MESH,
        )
    pl.semaphore_signal(
        barrier, inc=1, device_id={"head": 1 - core}, device_id_type=pl.DeviceIdType.MESH
    )


def await_all(size):
    pl.semaphore_wait(pltpu.get_barrier_semaphore(), size)


def send_to(src, dst, send_sem, recv_sem, **where):
    return pltpu.make_async_remote_copy(
        src_ref=src, dst_ref=dst, send_sem=send_sem, recv_sem=recv_sem, device_id=where,
        device_id_type=pl.DeviceIdType.MESH,
    )


def transposed(block):
    return block.astype(f32).T.astype(bf16)


def forward_kernel(
    size,
    hid_ref, gain_ref, wi_ref, wstep_ref, wshared_ref, cv_ref, cs_ref, bias_ref, decay_ref,
    skip_ref, ggain_ref, wout_ref, hrow_ref, crow_ref,
    normedt_ref, scale_ref, gate_ref, vext_ref, after_ref, y_ref, gw_ref, in_ref, step_ref,
    slope_ref, run_ref, runt_ref, stept_ref, sext_ref, bc_ref, gains_ref, out_ref, gmt_ref,
    coef_ref, near_ref, rows_ref,
    nx, halo, halo_sems, scores, bt, end_w, vwide, gates, ys, states, acc, acc_send,
    acc_land, acc_sems, squares, sq_land, sq_sems, totals, totals_land, totals_sems,
    near_land, near_sems, ex_own, ex_landing, ex_mixed, ex_result, ex_sems,
):
    step_id = pl.program_id(0)
    index = lax.axis_index("seq")
    core = lax.axis_index("head")
    tokens = hid_ref.shape[0]
    width = hid_ref.shape[1]
    chunks = tokens // CHUNK
    nb = gates.shape[0]
    t_mix, t_last = nb, 2 * nb
    half_width = width // 2
    exchange = StateExchange(
        index, size, False, ex_own, ex_landing, ex_mixed, ex_result, ex_sems, gains_ref
    )

    def norm_rows(rows):
        wide = rows.astype(f32)
        scale = lax.rsqrt(jnp.mean(wide * wide, axis=1, keepdims=True) + norm_eps)
        return (wide * scale * gain_ref[...][None, :]).astype(bf16), scale

    def totals_copy(d):
        return send_to(
            totals, totals_land.at[size - d - 1], totals_sems.at[0], totals_sems.at[1],
            seq=lax.rem(index + d, size),
        )

    @pl.when(step_id == 0)
    def _():
        greet_all(index, core, size)

        @pl.loop(0, chunks)
        def _(i):
            start = pl.multiple_of(i * CHUNK, CHUNK)
            for part in range(2):
                at = pl.multiple_of(start + part * 64, 64)
                rows, scale = norm_rows(hid_ref[pl.ds(at, 64), :])
                nx[pl.ds(pl.multiple_of(HALO + at, HALO), 64), :] = rows
                scale_ref[pl.ds(at, 64), :] = jnp.broadcast_to(scale, (64, LANES))

        await_all(size)
        after_id = lax.rem(index + 1, size)
        halo_copy = send_to(
            hid_ref.at[pl.ds(tokens - HALO, HALO)], halo, halo_sems.at[0], halo_sems.at[1],
            seq=after_id,
        )
        halo_copy.start()
        for c in range(chunks):
            for b in range(width // LANES):
                normedt_ref[b * LANES : (b + 1) * LANES, c * CHUNK : (c + 1) * CHUNK] = transposed(
                    nx[HALO + c * CHUNK : HALO + (c + 1) * CHUNK, b * LANES : (b + 1) * LANES]
                )
        rows_ref[...] = jnp.zeros_like(rows_ref)
        heads = bias_ref.shape[0]
        for i, ref in enumerate((bias_ref, decay_ref, skip_ref)):
            rows_ref[i, 0:heads] = ref[...]
        raw = mm(nx[HALO:, :], wstep_ref[...])
        raw = jnp.concatenate([raw, jnp.zeros((tokens, LANES - heads), f32)], axis=1)
        raw = raw + rows_ref[0:1, :]
        small = jnp.exp(-jnp.abs(raw))
        step = jnp.maximum(raw, 0.0) + jnp.log1p(small)
        step_ref[...] = step
        slope_ref[...] = 1.0 / (1.0 + jnp.exp(-raw))
        rate = -step * jnp.exp(rows_ref[1:2, :])
        tri = causal().astype(f32)
        total = jnp.zeros((1, LANES), f32)
        for c in range(chunks):
            rows = slice(c * CHUNK, (c + 1) * CHUNK)
            run = mm_exact(tri, rate[rows, :])
            run_ref[rows, :] = run
            total = total + run[CHUNK - 1 :, :]
            run_t = run.T
            step_t = step[rows, :].T
            for b in range(nb):
                heads = slice(BLOCK_HEADS * b, BLOCK_HEADS * (b + 1))
                runt_ref[b, 0:BLOCK_HEADS, rows] = run_t[heads, :]
                stept_ref[b, 0:BLOCK_HEADS, rows] = step_t[heads, :]
                runt_ref[b, BLOCK_HEADS:, rows] = jnp.zeros((8 - BLOCK_HEADS, CHUNK), f32)
                stept_ref[b, BLOCK_HEADS:, rows] = jnp.zeros((8 - BLOCK_HEADS, CHUNK), f32)
            end_w[rows, :] = step[rows, :] * jnp.exp(run[CHUNK - 1 :, :] - run)
        totals[...] = jnp.broadcast_to(jnp.exp(total), totals.shape)
        for d in range(1, size):
            totals_copy(d).start()
        halo_copy.wait()
        keep = jnp.where(index == 0, 0.0, 1.0)
        nx[0:HALO, :] = (norm_rows(halo[...])[0].astype(f32) * keep).astype(bf16)
        shared = mm(nx[...], wshared_ref[...]).astype(bf16)
        sext_ref[0] = shared[:, :STATE]
        sext_ref[1] = shared[:, STATE:]
        conv = conv_rows(shared.astype(f32), cs_ref[...], HALO - CONV + 1, tokens)
        act = silu(conv).astype(bf16)
        bc_ref[...] = act
        for c in range(chunks):
            rows = slice(c * CHUNK, (c + 1) * CHUNK)
            b_rows = act[rows, :STATE]
            c_rows = act[rows, STATE:]
            scores[c] = mm(c_rows, b_rows, NT)
            bt[:, rows] = transposed(b_rows)

    @pl.when(step_id < t_mix)
    def _():
        j = step_id
        values = mm(nx[...], wi_ref[1]).astype(bf16)
        vext_ref[...] = values
        vwide[...] = values.astype(f32)
        conv = conv_rows(vwide, cv_ref[...], HALO - CONV + 1, tokens)
        act = silu(conv).astype(bf16)
        run_cols = rolled(run_ref[...], j)
        end_cols = rolled(end_w[...], j)
        state = jnp.zeros((STATE, BLOCK), f32)
        for c in range(chunks):
            rows = slice(c * CHUNK, (c + 1) * CHUNK)
            weighted = act[rows, :].astype(f32) * widen(end_cols[rows, :BLOCK_HEADS])
            last = widen(jnp.exp(run_cols[(c + 1) * CHUNK - 1 : (c + 1) * CHUNK, :BLOCK_HEADS]))
            state = last * state + mm_right(bt[:, rows], weighted)
            after_ref[c] = state
            states[j, c] = state
        exchange.send(j, state)
        gate = mm(nx[HALO:, :], wi_ref[0])
        gate_ref[...] = gate
        gates[j] = gate
        mask = causal()
        skip = widen(rolled(rows_ref[2:3, :], j)[:, :BLOCK_HEADS])
        for c in range(chunks):
            rows = slice(c * CHUNK, (c + 1) * CHUNK)
            cols = run_cols[rows, :BLOCK_HEADS]
            x = act[rows, :]
            y_pairs = []
            for pair in range(BLOCK // LANES):
                mats = []
                for k in range(2):
                    head = 2 * pair + k
                    gap = cols[:, head : head + 1] - runt_ref[j, head : head + 1, rows]
                    decayed = jnp.exp(jnp.where(mask, gap, -1e30))
                    mats.append(scores[c] * decayed * stept_ref[j, head : head + 1, rows])
                low, high = stack_pair(x[:, pair * LANES : (pair + 1) * LANES])
                y_pairs.append(
                    mm_left(jnp.concatenate(mats, axis=1), jnp.concatenate([low, high], axis=0))
                )
            ys[j, rows, :] = jnp.concatenate(y_pairs, axis=1) + skip * x.astype(f32)

    @pl.when(step_id == 1)
    def _():
        pltpu.make_async_remote_copy(
            src_ref=totals_land.at[pl.ds(0, size - 1)],
            dst_ref=totals_land.at[pl.ds(0, size - 1)],
            send_sem=totals_sems.at[0], recv_sem=totals_sems.at[1],
            device_id={"seq": lax.rem(index + 1, size)},
            device_id_type=pl.DeviceIdType.MESH,
        ).wait()
        totals_land[size - 1] = totals[...]
        for source in range(size):
            gains_ref[source : source + 1, :] = totals_land[exchange.slot(source), 0:1, :]

    @pl.when((step_id >= 2) & (step_id < nb + 2))
    def _():
        exchange.turn(step_id - 2)

    def neighbour_copy(bit, first, count):
        mine = (index // (1 << bit)) % 2
        source = pl.multiple_of(core * half_width + first, LANES)
        return send_to(
            normedt_ref.at[pl.ds(source, count)],
            near_land.at[bit, pl.ds(first, count)], near_sems.at[0, bit], near_sems.at[1, bit],
            seq=index + (1 - 2 * mine) * (1 << bit),
        )

    @pl.when((step_id >= 1) & (step_id <= half_width // LANES))
    def _():
        first = pl.multiple_of((step_id - 1) * LANES, LANES)
        for bit in range(2):
            neighbour_copy(bit, first, LANES).start()

    @pl.when((step_id >= t_mix) & (step_id < t_last))
    def _():
        j = step_id - t_mix
        entering = exchange.take(j)
        in_ref[...] = entering
        offsets = offsets_of(run_ref, chunks)
        gated = []
        for c in range(chunks):
            rows = slice(c * CHUNK, (c + 1) * CHUNK)
            grow = rolled(jnp.exp(run_ref[rows, :]), j)[:, :BLOCK_HEADS]
            base = rolled(jnp.exp(offsets[c]), j)[:, :BLOCK_HEADS]
            enter = widen(base) * entering
            if c:
                enter = enter + states[j, c - 1]
            y = ys[j, rows, :] + widen(grow) * mm_right(bc_ref[rows, STATE:], enter)
            y_ref[rows, :] = y
            out = y * silu(gates[j, rows, :])
            gw_ref[rows, :] = (out * ggain_ref[...]).astype(bf16)
            gated.append(
                jnp.broadcast_to(jnp.sum(out * out, axis=1, keepdims=True), (CHUNK, LANES))
            )
        part = mm(gw_ref[...], wout_ref[...], NT)
        block_squares = jnp.concatenate(gated, axis=0)

        @pl.when(j == 0)
        def _():
            acc[...] = part
            squares[...] = block_squares

        @pl.when(j > 0)
        def _():
            acc[...] += part
            squares[...] += block_squares

        @pl.when(j == nb - 1)
        def _():
            send_to(squares, sq_land, sq_sems.at[0], sq_sems.at[1], head=1 - core).start()
            for c in range(chunks):
                acc_send[c] = acc[c * CHUNK : (c + 1) * CHUNK, :].astype(bf16)
                send_to(
                    acc_send.at[c], acc_land.at[c], acc_sems.at[0, c], acc_sems.at[1, c],
                    head=1 - core,
                ).start()

    @pl.when(step_id >= t_last)
    def _():
        c = step_id - t_last

        @pl.when(c == 0)
        def _():
            send_to(squares, sq_land, sq_sems.at[0], sq_sems.at[1], head=1 - core).wait()

        send_to(
            acc_send.at[c], acc_land.at[c], acc_sems.at[0, c], acc_sems.at[1, c], head=1 - core
        ).wait()
        rows = pl.ds(pl.multiple_of(c * CHUNK, CHUNK), CHUNK)
        mixed = acc[rows, :] + acc_land[c].astype(f32)
        inverse = lax.rsqrt((squares[rows, 0:1] + sq_land[rows, 0:1]) / INNER + norm_eps)
        out_ref[...] = hrow_ref[...].astype(f32) + mixed * inverse
        cot = crow_ref[...].astype(f32)
        scaled = (cot * inverse).astype(bf16)
        for b in range(width // LANES):
            gmt_ref[b * LANES : (b + 1) * LANES, :] = transposed(
                scaled[:, b * LANES : (b + 1) * LANES]
            )
        grad_inverse = jnp.sum(cot * mixed, axis=1, keepdims=True)
        coef_ref[...] = jnp.broadcast_to(
            grad_inverse * inverse * inverse * inverse / INNER, (CHUNK, LANES)
        )

        @pl.when(c == chunks - 1)
        def _():
            for bit in range(2):
                neighbour_copy(bit, 0, half_width).wait()
                near_ref[bit] = near_land[bit]


def offsets_of(run_ref, chunks):
    rows = [jnp.zeros((1, LANES), f32)]
    for c in range(chunks):
        rows.append(rows[-1] + run_ref[(c + 1) * CHUNK - 1 : (c + 1) * CHUNK, :])
    return rows


def forward_call(
    hidden, cotangent, gain, both, wstep, wshared, conv_values, conv_shared, bias, decay, skip,
    gate_gain, wout,
):
    tokens, width = hidden.shape
    inner = both.shape[2]
    chunks = tokens // CHUNK
    nb = inner // BLOCK
    size = lax.axis_size("seq")
    t_mix, t_last = nb, 2 * nb

    def at(start):
        return lambda s: jnp.clip(s - start, 0, nb - 1)

    def full(shape):
        return pl.BlockSpec(shape, lambda s: (0,) * len(shape), pipeline_mode=pl.Buffered(1))

    def cols(rows, start):
        return pl.BlockSpec((rows, BLOCK), lambda s: (0, at(start)(s)))

    row_of = lambda s: jnp.clip(s - t_last, 0, chunks - 1)
    row_block = lambda w: pl.BlockSpec((CHUNK, w), lambda s: (row_of(s), 0))
    outs = [
        ((width, tokens), bf16, full((width, tokens))),
        ((tokens, LANES), f32, full((tokens, LANES))),
        ((tokens, inner), f32, cols(tokens, 0)),
        ((HALO + tokens, inner), bf16, cols(HALO + tokens, 0)),
        (
            (chunks, STATE, inner), f32,
            pl.BlockSpec((chunks, STATE, BLOCK), lambda s: (0, 0, at(0)(s))),
        ),
        ((tokens, inner), f32, cols(tokens, t_mix)),
        ((tokens, inner), bf16, cols(tokens, t_mix)),
        ((STATE, inner), f32, cols(STATE, t_mix)),
        ((tokens, LANES), f32, full((tokens, LANES))),
        ((tokens, LANES), f32, full((tokens, LANES))),
        ((tokens, LANES), f32, full((tokens, LANES))),
        ((nb, 8, tokens), f32, full((nb, 8, tokens))),
        ((nb, 8, tokens), f32, full((nb, 8, tokens))),
        ((2, HALO + tokens, STATE), bf16, full((2, HALO + tokens, STATE))),
        ((tokens, 2 * STATE), bf16, full((tokens, 2 * STATE))),
        ((size, LANES), f32, full((size, LANES))),
        ((tokens, width), f32, row_block(width)),
        ((width, tokens), bf16, pl.BlockSpec((width, CHUNK), lambda s: (0, row_of(s)))),
        ((tokens, LANES), f32, row_block(LANES)),
        ((2, width // 2, tokens), bf16, full((2, width // 2, tokens))),
        ((8, LANES), f32, full((8, LANES))),
    ]
    sem = pltpu.SemaphoreType.DMA
    return pl.pallas_call(
        functools.partial(forward_kernel, size),
        grid=(2 * nb + chunks,),
        in_specs=[
            full((tokens, width)),
            full((width,)),
            pl.BlockSpec((2, width, BLOCK), lambda s: (0, 0, at(0)(s))),
            full(wstep.shape),
            full((width, 2 * STATE)),
            cols(CONV + 1, 0),
            full((CONV + 1, 2 * STATE)),
            full(bias.shape),
            full(decay.shape),
            full(skip.shape),
            cols(1, t_mix),
            cols(width, t_mix),
            row_block(width),
            row_block(width),
        ],
        out_shape=[jax.ShapeDtypeStruct(shape, kind) for shape, kind, _ in outs],
        out_specs=[spec for _, _, spec in outs],
        scratch_shapes=[
            pltpu.VMEM((HALO + tokens, width), bf16),
            pltpu.VMEM((HALO, width), bf16),
            sem((2,)),
            pltpu.VMEM((chunks, CHUNK, CHUNK), f32),
            pltpu.VMEM((STATE, tokens), bf16),
            pltpu.VMEM((tokens, LANES), f32),
            pltpu.VMEM((HALO + tokens, BLOCK), f32),
            pltpu.VMEM((nb, tokens, BLOCK), f32),
            pltpu.VMEM((nb, tokens, BLOCK), f32),
            pltpu.VMEM((nb, chunks, STATE, BLOCK), f32),
            pltpu.VMEM((tokens, width), f32),
            pltpu.VMEM((chunks, CHUNK, width), bf16),
            pltpu.VMEM((chunks, CHUNK, width), bf16),
            sem((2, chunks)),
            pltpu.VMEM((tokens, LANES), f32),
            pltpu.VMEM((tokens, LANES), f32),
            sem((2,)),
            pltpu.VMEM((8, LANES), f32),
            pltpu.VMEM((size, 8, LANES), f32),
            sem((2,)),
            pltpu.VMEM((2, width // 2, tokens), bf16),
            sem((2, 2)),
        ] + exchange_scratch(nb, size, f32),
        compiler_params=pltpu.CompilerParams(
            collective_id=1, has_side_effects=True, vmem_limit_bytes=67043328
        ),
        name="forward",
    )(
        hidden, gain, both, wstep, wshared, conv_values, conv_shared, bias, decay, skip, gate_gain,
        wout, hidden, cotangent,
    )


def order_rows(part, bits):
    order = list(range(bits))
    if part == 1:
        order[:3] = order[:3][::-1]
    if part == 2:
        order[:2] = order[:2][::-1]
    return order


def order_columns(part, bits):
    return [bit for bit in range(bits) if bit != part] + [part]


def slot_of(owner, order):
    slot = 0
    for bit in order:
        slot = slot * 2 + ((owner >> bit) & 1)
    return slot


class Reduction:
    def __init__(self, held, landing, order, index, sems, put, put_other=None):
        self.held, self.landing, self.order = held, landing, order
        self.index, self.sems, self.put, self.put_other = index, sems, put, put_other
        self.stages = len(order)

    def place(self, stage):
        base = 0
        size = 1 << self.stages
        for s, bit in enumerate(self.order[: stage + 1]):
            mine = (self.index // (1 << bit)) % 2
            half = size >> (s + 1)
            keep, give = base + mine * half, base + (1 - mine) * half
            base = keep
        return keep, give, half

    def copy(self, stage):
        _, give, half = self.place(stage)
        bit = self.order[stage]
        mine = (self.index // (1 << bit)) % 2
        return send_to(
            self.held.at[pl.ds(give, half)], self.landing[stage],
            self.sems.at[0, stage], self.sems.at[1, stage],
            seq=self.index + (1 - 2 * mine) * (1 << bit),
        )

    def start(self, stage):
        self.copy(stage).start()

    def start_piece(self, piece, pieces):
        _, give, half = self.place(0)
        count = half // pieces
        bit = self.order[0]
        mine = (self.index // (1 << bit)) % 2
        send_to(
            self.held.at[pl.ds(give + piece * count, count)],
            self.landing[0].at[pl.ds(piece * count, count)],
            self.sems.at[0, 0], self.sems.at[1, 0],
            seq=self.index + (1 - 2 * mine) * (1 << bit),
        ).start()

    def advance(self, stage):
        self.copy(stage).wait()
        keep, _, half = self.place(stage)
        if stage < self.stages - 1:

            @pl.loop(0, half)
            def _(i):
                total = self.held[keep + i].astype(f32) + self.landing[stage][i].astype(f32)
                self.held[keep + i] = total.astype(bf16)

            self.start(stage + 1)
        elif self.put_other is None:
            self.put(self.held[keep].astype(f32) + self.landing[stage][0].astype(f32))
        else:
            self.put(self.held[keep].astype(f32))
            self.put_other(self.landing[stage][0].astype(f32))


def sum_copy(acc, landing, bit, index, sems):
    mine = (index // (1 << bit)) % 2
    return pltpu.make_async_remote_copy(
        src_ref=acc.at[bit],
        dst_ref=landing.at[bit],
        send_sem=sems.at[0, bit],
        recv_sem=sems.at[1, bit],
        device_id={"seq": index + (1 - 2 * mine) * (1 << bit)},
        device_id_type=pl.DeviceIdType.MESH,
    )


def back_kernel(
    bits,
    gmt_ref, normedt_ref, near_ref, gw_ref, coef_ref, gains_ref, run_ref, step_ref, slope_ref,
    bc_ref, sext_ref, rows_ref, cs_ref, wshared_ref, wstep_ref, gain_ref,
    wout_ref, y_ref, gate_ref, ggain_ref, vext_ref, after_ref, in_ref, cv_ref, runt_ref,
    stept_ref, wi_ref,
    hid_ref, cot_ref, scale_ref,
    gout_ref, ginner_ref, gsmall_ref, ghid_ref, sums_ref,
    w_out, w_gate, w_values, w_small,
    land_out, land_gate, land_values, land_small,
    rs_sems, near, near_sems,
    own_cols, other_cols, land_cols, cols_sems,
    gv, acc_send, acc_land, acc_sems,
    edge_own, edge_tail, edge_land, edge_sems,
    dbc, dbc_land, dbc_sems, small, sedge_own, sedge_land, sedge_sems,
    vec, vec_land, vec_sems,
    scores, scorest, ct, dscores, end_w, ends, dcols, xdu, dyc, xdus, vwide, gext,
    dys, ggates, term_gate, ex_own, ex_landing, ex_mixed, ex_result, ex_sems,
):
    step_id = pl.program_id(0)
    index = lax.axis_index("seq")
    core = lax.axis_index("head")
    size = 1 << bits
    tokens = y_ref.shape[0]
    chunks = tokens // CHUNK
    nb = ggates.shape[0]
    half_nb = nb // 2
    width = normedt_ref.shape[0]
    half_width = width // 2
    rows_own = width // size
    t_scan, t_grad, t_final = nb, 2 * nb, 3 * nb
    after_id = lax.rem(index + 1, size)
    before_id = lax.rem(index + size - 1, size)
    bit_of = lambda bit: (index // (1 << bit)) % 2
    flip_of = lambda bit: index + (1 - 2 * bit_of(bit)) * (1 << bit)

    def out_reduction(part):
        cols = w_out.shape[3]

        def put(value):
            gout_ref[:, part * cols : (part + 1) * cols] = value

        return Reduction(
            w_out.at[part], [ref.at[part] for ref in land_out], order_rows(part, bits), index,
            rs_sems.at[part], put,
        )

    def columns_reduction(g, part):
        held, landing = ((w_gate, land_gate), (w_values, land_values))[g]

        def put_half(half):
            def put(value):
                for b in range(half_nb):
                    lane = (part * half_nb + b) * BLOCK + half * LANES
                    place = pl.ds(pl.multiple_of(lane, LANES), LANES)
                    ginner_ref[g, :, place] = value[:, b * LANES : (b + 1) * LANES]

            return put

        return Reduction(
            held.at[part], [ref.at[part] for ref in landing], order_columns(part, bits), index,
            rs_sems.at[2 + 2 * g + part], put_half(bit_of(part)), put_half(1 - bit_of(part)),
        )

    def put_small(value):
        gsmall_ref[...] = value

    rs_out = [out_reduction(part) for part in range(2)]
    rs_gate = [columns_reduction(0, part) for part in range(2)]
    rs_values = [columns_reduction(1, part) for part in range(2)]
    rs_small = Reduction(
        w_small, list(land_small), order_rows(2, bits), index, rs_sems.at[6], put_small
    )

    def when_after(step):
        return pl.when(step_id == step)

    exchange = StateExchange(
        index, size, True, ex_own, ex_landing, ex_mixed, ex_result, ex_sems, gains_ref
    )

    def near_copies(bit):
        half = pl.ds(pl.multiple_of(core * half_width, half_width), half_width)
        return (
            pltpu.make_async_copy(near_ref.at[bit], near.at[bit, half], near_sems.at[0, bit]),
            send_to(
                near_ref.at[bit], near.at[bit, half], near_sems.at[1, bit], near_sems.at[2, bit],
                head=1 - core,
            ),
        )

    @pl.when(step_id == 0)
    def _():
        greet_all(index, core, size)
        for c in range(chunks):
            rows = slice(c * CHUNK, (c + 1) * CHUNK)
            ct[:, rows] = transposed(bc_ref[rows, STATE:])
            for b in range(width // LANES):
                acc_send[c, :, b * LANES : (b + 1) * LANES] = transposed(
                    gmt_ref[b * LANES : (b + 1) * LANES, rows]
                )
        await_all(size)
        for bit in range(2):
            for copy in near_copies(bit):
                copy.start()

    group = width // 4
    owners = size // 4

    def scatter(piece, q, order, store):
        for b in range(owners):
            store(slot_of(q * owners + b, order), piece[b * rows_own : (b + 1) * rows_own, :])

    def put_out(part):
        cols = w_out.shape[3]
        for q in range(4):
            left = gmt_ref[q * group : (q + 1) * group, :]
            piece = mm(left, gw_ref[:, part * cols : (part + 1) * cols]).astype(bf16)

            def store(slot, value):
                w_out[part, slot] = value

            scatter(piece, q, order_rows(part, bits), store)

    def columns_copy(g, part):
        return send_to(
            other_cols.at[g, part], land_cols.at[g, part], cols_sems.at[0, g, part],
            cols_sems.at[1, g, part], seq=flip_of(part),
        )

    def split_block(g, j, value):
        part = j // half_nb
        mine = jnp.where(part == 0, bit_of(0), bit_of(1))
        place = pl.ds(pl.multiple_of((j % half_nb) * LANES, LANES), LANES)
        first, second = value[:, :LANES], value[:, LANES:]
        own_cols[g, part, :, place] = jnp.where(mine == 0, first, second)
        other_cols[g, part, :, place] = jnp.where(mine == 0, second, first)

    def put_columns(g, part):
        columns_copy(g, part).wait()
        held = (w_gate, w_values)[g]
        for q in range(4):
            rows = slice(q * group, (q + 1) * group)
            piece = mm(
                jnp.concatenate([normedt_ref[rows, :], near[part, rows, :]], axis=1),
                jnp.concatenate([own_cols[g, part], land_cols[g, part]], axis=0),
            )

            def store(slot, value):
                held[part, slot] = value

            scatter(piece.astype(bf16), q, order_columns(part, bits), store)
        (rs_gate, rs_values)[g][part].start(0)

    @pl.when(step_id < t_scan)
    def _():
        j = step_id
        offsets = offsets_of(run_ref, chunks)
        own = jnp.zeros((STATE, BLOCK), f32)
        term = jnp.zeros((1, BLOCK), f32)
        for c in range(chunks):
            rows = slice(c * CHUNK, (c + 1) * CHUNK)
            ggw = mm(acc_send[c], wout_ref[...])
            y = y_ref[rows, :]
            gate = gate_ref[rows, :]
            sig = 1.0 / (1.0 + jnp.exp(-gate))
            act = gate * sig
            out = y * act
            term = term + jnp.sum(ggw * out, axis=0, keepdims=True)
            coef = jnp.concatenate([coef_ref[rows, 0:LANES]] * (BLOCK // LANES), axis=1)
            gg = ggw * ggain_ref[...] - coef * out
            dy = gg * act
            dys[j, rows, :] = dy
            ggate = (gg * y * (sig * (1.0 + gate * (1.0 - sig)))).astype(bf16)
            ggates[j, rows, :] = ggate
            grow = rolled(jnp.exp(run_ref[rows, :] + offsets[c]), j)[:, :BLOCK_HEADS]
            own = own + mm(ct[:, rows], (dy * widen(grow)).astype(bf16))
        term_gate[j, 0:1, :] = term
        exchange.send(j, own)
        split_block(0, j, ggates[j])

    for part in range(2):

        @when_after(part)
        def _(part=part):
            put_out(part)

    pieces = size // 2

    @pl.when((step_id >= 1) & (step_id < nb))
    def _():
        for reduction in rs_out:
            reduction.start_piece(step_id - 1, pieces)

    rest = pieces - (nb - 1)

    @when_after(nb)
    def _():
        for piece in range(nb - 1, nb - 1 + (rest + 1) // 2):
            for reduction in rs_out:
                reduction.start_piece(piece, pieces)

    @when_after(nb + 1)
    def _():
        for piece in range(nb - 1 + (rest + 1) // 2, pieces):
            for reduction in rs_out:
                reduction.start_piece(piece, pieces)

    @pl.when((step_id >= 2) & (step_id < nb + 2))
    def _():
        exchange.turn(step_id - 2)

    @when_after(half_nb - 1)
    def _():
        columns_copy(0, 0).start()

    @when_after(nb - 1)
    def _():
        columns_copy(0, 1).start()
        for bit in range(2):
            for copy in near_copies(bit):
                copy.wait()
        put_columns(0, 0)

    mask = causal()
    rows_i = lax.broadcasted_iota(jnp.int32, (CHUNK, CHUNK), 0)
    cols_i = lax.broadcasted_iota(jnp.int32, (CHUNK, CHUNK), 1)
    mask_t = rows_i <= cols_i

    @pl.when(step_id == t_scan)
    def _():
        dbc[...] = jnp.zeros_like(dbc)
        dscores[...] = jnp.zeros_like(dscores)
        dcols[...] = jnp.zeros_like(dcols)
        xdu[...] = jnp.zeros_like(xdu)
        dyc[...] = jnp.zeros_like(dyc)
        xdus[...] = jnp.zeros_like(xdus)
        ends[...] = jnp.zeros_like(ends)
        vec[...] = jnp.zeros_like(vec)
        for c in range(chunks):
            rows = slice(c * CHUNK, (c + 1) * CHUNK)
            b_rows = bc_ref[rows, :STATE]
            c_rows = bc_ref[rows, STATE:]
            scores[c] = mm(c_rows, b_rows, NT)
            scorest[c] = mm(b_rows, c_rows, NT)
            run = run_ref[rows, :]
            end_w[rows, :] = jnp.exp(run[CHUNK - 1 :, :] - run)

    @pl.when((step_id >= t_scan) & (step_id < t_grad))
    def _():
        j = step_id - t_scan
        offsets = offsets_of(run_ref, chunks)
        vwide[...] = vext_ref[...].astype(f32)
        taps = [jnp.zeros((1, BLOCK), f32)] * (CONV + 1)
        run_cols = rolled(run_ref[...], j)
        step_cols = rolled(step_ref[...], j)
        end_cols = rolled(end_w[...], j)
        skip = widen(rolled(rows_ref[2:3, :], j)[:, :BLOCK_HEADS])
        channel = lax.broadcasted_iota(jnp.int32, (BLOCK, LANES), 0) // HEAD_DIM
        lane = lax.broadcasted_iota(jnp.int32, (BLOCK, LANES), 1)
        pick = (lane == BLOCK_HEADS * j + channel).astype(bf16)
        lane_row = lax.broadcasted_iota(jnp.int32, (CHUNK, LANES), 1)
        dstate = exchange.take(j)
        dskip = jnp.zeros((1, BLOCK), f32)
        gext[tokens : tokens + 8, :] = jnp.zeros((8, BLOCK), f32)
        for c in reversed(range(chunks)):
            rows = slice(c * CHUNK, (c + 1) * CHUNK)
            cols = run_cols[rows, :BLOCK_HEADS]
            conv = conv_rows(vwide, cv_ref[...], HALO - CONV + 1 + c * CHUNK, CHUNK)
            sig = 1.0 / (1.0 + jnp.exp(-conv))
            x = (conv * sig).astype(bf16)
            slope = sig * (1.0 + conv * (1.0 - sig))
            wide_x = x.astype(f32)
            dy = dys[j, rows, :]
            b_rows = bc_ref[rows, :STATE]
            c_rows = bc_ref[rows, STATE:]
            grow = widen(jnp.exp(cols))
            tail = widen(end_cols[rows, :BLOCK_HEADS])
            step_w = widen(step_cols[rows, :BLOCK_HEADS])
            last = grow[CHUNK - 1 :, :]
            base = rolled(jnp.exp(offsets[c]), j)[:, :BLOCK_HEADS]
            enter = widen(base) * in_ref[...]
            if c:
                enter = enter + after_ref[c - 1]
            du_state = tail * mm(b_rows, dstate.astype(bf16))
            carried = grow * mm(c_rows, enter.astype(bf16))
            weighted = wide_x * (tail * step_w)
            grown = dy * grow
            dbc[0, rows, :] += mm_both(weighted, dstate, NT)
            dbc[1, rows, :] += mm_both(grown, enter, NT)
            hold = last * jnp.sum(dstate * enter, axis=0, keepdims=True)
            dstate = last * dstate + mm_right(ct[:, rows], grown)
            du_pairs = []
            col_sum = jnp.zeros((CHUNK, LANES), f32)
            dscore = dscores[c]
            for pair in range(BLOCK // LANES):
                lanes = slice(pair * LANES, (pair + 1) * LANES)
                low, high = stack_pair(dy[:, lanes])
                both = jnp.concatenate([low, high], axis=0)
                dmat = mm_left(both, x[:, lanes], NT)
                mats = []
                for k in range(2):
                    head = 2 * pair + k
                    col = cols[:, head : head + 1]
                    row = runt_ref[0, head : head + 1, rows]
                    keep = jnp.exp(jnp.where(mask, col - row, -1e30))
                    piece = dmat[k * CHUNK : (k + 1) * CHUNK, :] * keep
                    piece = piece * stept_ref[0, head : head + 1, rows]
                    dscore = dscore + piece
                    full = piece * scores[c]
                    col_sum = jnp.where(
                        lane_row == BLOCK_HEADS * j + head,
                        jnp.sum(full, axis=1, keepdims=True),
                        col_sum,
                    )
                    dcols[j, head : head + 1, rows] = jnp.sum(full, axis=0, keepdims=True)
                    keep_t = jnp.exp(jnp.where(mask_t, row - col, -1e30))
                    mats.append(scorest[c] * keep_t)
                du_pairs.append(
                    mm(jnp.concatenate(mats, axis=1).astype(bf16), both.astype(bf16))
                )
            dscores[c] = dscore
            du = jnp.concatenate(du_pairs, axis=1) + du_state
            by_head = mm(
                jnp.concatenate(
                    [
                        (wide_x * du).astype(bf16),
                        (dy * carried).astype(bf16),
                        (wide_x * du_state).astype(bf16),
                        *parts(jnp.broadcast_to(hold, (HALO, BLOCK))),
                    ],
                    axis=0,
                ),
                pick,
            )
            xdu[rows, :] += by_head[0:CHUNK, :]
            dyc[rows, :] += by_head[CHUNK : 2 * CHUNK, :] + col_sum
            xdus[rows, :] += by_head[2 * CHUNK : 3 * CHUNK, :]
            end = 3 * CHUNK
            ends[c : c + 1, :] += (
                by_head[end : end + 1, :] + by_head[end + HALO : end + HALO + 1, :]
            )
            dskip = dskip + jnp.sum(dy * wide_x, axis=0, keepdims=True)
            gconv = (step_w * du + skip * dy) * slope
            gext[rows, :] = gconv
            taps[CONV] = taps[CONV] + jnp.sum(gconv, axis=0, keepdims=True)
            values = vwide[HALO + c * CHUNK : HALO + (c + 1) * CHUNK, :]
            total = cv_ref[CONV - 1 : CONV, :] * gconv
            taps[CONV - 1] = taps[CONV - 1] + jnp.sum(values * gconv, axis=0, keepdims=True)
            for k in range(CONV - 1):
                ahead = c * CHUNK + CONV - 1 - k
                moved = gext[ahead : ahead + CHUNK, :]
                total = total + cv_ref[k : k + 1, :] * moved
                taps[k] = taps[k] + jnp.sum(values * moved, axis=0, keepdims=True)
            gv[j, rows, :] = total.astype(bf16)
            if c == chunks - 1:
                edge_tail[j, 0:8, :] = total[CHUNK - 8 :, :]
        row8 = lax.broadcasted_iota(jnp.int32, (8, BLOCK), 0)
        ahead_rows = vwide[HALO - CONV + 1 : HALO - CONV + 9, :]
        for k in range(CONV):
            tap = taps[k]
            if k < CONV - 1:
                moved = pltpu.roll(gext[0:8, :], k, 0) if k else gext[0:8, :]
                inside = (row8 >= k) & (row8 < CONV - 1)
                tap = tap + jnp.sum(
                    jnp.where(inside, ahead_rows * moved, 0.0), axis=0, keepdims=True
                )
            vec[0, j, k : k + 1, :] = tap
        vec[0, j, CONV : CONV + 1, :] = taps[CONV]
        vec[0, j, CONV + 1 : CONV + 2, :] = term_gate[j, 0:1, :]
        by_head = mm(jnp.concatenate(parts(jnp.broadcast_to(dskip, (HALO, BLOCK))), axis=0), pick)
        vec[0, nb, 7:8, 0:LANES] += by_head[0:1, :] + by_head[HALO : HALO + 1, :]
        edge_tail[j, 8 : 8 + CONV + 1, :] = cv_ref[...]
        edge_own[j] = gext[0:8, :]
        send_to(
            edge_own.at[j], edge_land.at[j], edge_sems.at[0, j], edge_sems.at[1, j], seq=before_id
        ).start()

    def finish_block(j):
        send_to(
            edge_own.at[j], edge_land.at[j], edge_sems.at[0, j], edge_sems.at[1, j], seq=before_id
        ).wait()
        nxt = jnp.where(index == size - 1, 0.0, 1.0) * edge_land[j]
        row8 = lax.broadcasted_iota(jnp.int32, (8, BLOCK), 0)
        fix = edge_tail[j, 0:8, :]
        for k in range(CONV - 1):
            ahead = CONV - 1 - k
            moved = pltpu.roll(nxt, 8 - ahead, 0)
            fix = fix + jnp.where(row8 >= 8 - ahead, edge_tail[j, 8 + k : 9 + k, :] * moved, 0.0)
        both_rows = jnp.concatenate([gv[j, tokens - 16 : tokens - 8, :].astype(f32), fix], axis=0)
        gv[j, tokens - 16 :, :] = both_rows.astype(bf16)
        split_block(1, j, gv[j])

    @pl.when((step_id > t_scan + 1) & (step_id < t_grad))
    def _():
        finish_block(step_id - t_scan - 2)

    @when_after(t_scan + 1)
    def _():
        put_columns(0, 1)

    @when_after(t_scan + 2)
    def _():
        rs_gate[0].advance(0)
        rs_out[0].advance(0)
        rs_out[1].advance(0)

    @when_after(t_scan + half_nb + 1)
    def _():
        columns_copy(1, 0).start()
        rs_gate[0].advance(1)
        rs_gate[1].advance(0)

    @when_after(t_grad - 1)
    def _():
        rs_out[0].advance(1)

    @when_after(t_grad - 1)
    def _():
        tri = mask.astype(f32)
        tri_t = mask_t.astype(f32)
        strict = (rows_i > cols_i).astype(f32)
        decay = jnp.exp(rows_ref[1:2, :])
        bias_sum = jnp.zeros((1, LANES), f32)
        decay_sum = jnp.zeros((1, LANES), f32)
        for c in range(chunks):
            rows = slice(c * CHUNK, (c + 1) * CHUNK)
            step = step_ref[rows, :]
            col_rows = [dcols[b, 0:BLOCK_HEADS, rows] for b in range(nb)]
            rest = LANES - BLOCK_HEADS * nb
            col_rows.append(jnp.zeros((rest, CHUNK), f32))
            dlog = dyc[rows, :] - jnp.concatenate(col_rows, axis=0).T
            drate = (
                mm_exact(tri_t, dlog)
                + mm_exact(strict, xdus[rows, :] * step)
                + ends[c : c + 1, :]
            )
            dstep = xdu[rows, :] - decay * drate
            draw = dstep * slope_ref[rows, :]
            small[rows, LANES:] = draw.astype(bf16)
            bias_sum = bias_sum + jnp.sum(draw, axis=0, keepdims=True)
            decay_sum = decay_sum - jnp.sum(drate * step, axis=0, keepdims=True) * decay
            b_rows = bc_ref[rows, :STATE]
            c_rows = bc_ref[rows, STATE:]
            high, low = parts(dscores[c])
            dbc[1, rows, :] += mm(high, b_rows) + mm(low, b_rows)
            dbc[0, rows, :] += mm(high, c_rows, TN) + mm(low, c_rows, TN)
        vec[0, nb, 0:1, 0:LANES] = bias_sum
        vec[0, nb, 1:2, 0:LANES] = decay_sum
        send_to(
            dbc.at[1 - core], dbc_land, dbc_sems.at[0], dbc_sems.at[1], head=1 - core
        ).start()

    @when_after(t_grad)
    def _():
        finish_block(nb - 2)
        finish_block(nb - 1)
        columns_copy(1, 1).start()
        put_columns(1, 0)
        rs_gate[0].advance(2)
        rs_gate[1].advance(1)
        rs_out[1].advance(1)

    @when_after(t_grad + 1)
    def _():
        rs_gate[0].advance(3)

    @when_after(t_grad)
    def _():
        send_to(
            dbc.at[1 - core], dbc_land, dbc_sems.at[0], dbc_sems.at[1], head=1 - core
        ).wait()
        sext = sext_ref[core].astype(f32)
        taps = cs_ref[core]
        conv = conv_rows(sext, taps, HALO - CONV + 1, tokens)
        gs = (dbc[core] + dbc_land[...]) * silu_grad(conv)
        for k in range(CONV):
            first = HALO - CONV + 1 + k
            vec[0, nb, 2 + k : 3 + k, 0:LANES] = jnp.sum(
                sext[first : first + tokens, :] * gs, axis=0, keepdims=True
            )
        vec[0, nb, 2 + CONV : 3 + CONV, 0:LANES] = jnp.sum(gs, axis=0, keepdims=True)
        dbc[core] = gs
        sedge_own[...] = gs[0:8, :]
        send_to(
            sedge_own, sedge_land, sedge_sems.at[0], sedge_sems.at[1], seq=before_id
        ).start()

    @when_after(t_grad + 1)
    def _():
        send_to(
            sedge_own, sedge_land, sedge_sems.at[0], sedge_sems.at[1], seq=before_id
        ).wait()
        taps = cs_ref[core]
        nxt = jnp.where(index == size - 1, 0.0, 1.0) * sedge_land[...]
        gs = jnp.concatenate([dbc[core], nxt], axis=0)
        total = taps[CONV - 1 : CONV, :] * gs[0:tokens, :]
        for k in range(CONV - 1):
            total = total + taps[k : k + 1, :] * gs[CONV - 1 - k : CONV - 1 - k + tokens, :]
        small[:, 0:LANES] = total.astype(bf16)
        for q in range(4):
            piece = mm(normedt_ref[q * group : (q + 1) * group, :], small[...]).astype(bf16)

            def store(slot, value):
                w_small[slot] = value

            scatter(piece, q, order_rows(2, bits), store)
        rs_small.start(0)

    @pl.when((step_id >= t_grad) & (step_id < t_final))
    def _():
        j = step_id - t_grad
        part = mm(
            jnp.concatenate([ggates[j], gv[j]], axis=1),
            jnp.concatenate([wi_ref[0], wi_ref[1]], axis=1),
            NT,
        )

        @pl.when(j == 0)
        def _():
            for b in range(width // BLOCK):
                dys[b] = part[:, b * BLOCK : (b + 1) * BLOCK]

        @pl.when(j > 0)
        def _():
            for b in range(width // BLOCK):
                dys[b] += part[:, b * BLOCK : (b + 1) * BLOCK]

    @when_after(t_grad + 2)
    def _():
        rs_out[0].advance(2)

    @when_after(t_grad + 3)
    def _():
        put_columns(1, 1)
        rs_out[1].advance(2)

    @when_after(t_grad + 4)
    def _():
        rs_gate[1].advance(2)
        own = pl.ds(pl.multiple_of(core * LANES, LANES), LANES)
        heads = wstep_ref.shape[1]
        rest = mm(small[:, 0:LANES], wshared_ref[:, own], NT) + mm(
            small[:, LANES : LANES + heads], wstep_ref[...], NT
        )
        for b in range(width // BLOCK):
            dys[b] += rest[:, b * BLOCK : (b + 1) * BLOCK]

    @when_after(t_final - 1)
    def _():
        for c in range(chunks):
            rows = slice(c * CHUNK, (c + 1) * CHUNK)
            for b in range(width // BLOCK):
                acc_send[c, :, b * BLOCK : (b + 1) * BLOCK] = dys[b, rows, :].astype(bf16)
            send_to(
                acc_send.at[c], acc_land.at[c], acc_sems.at[0, c], acc_sems.at[1, c], head=1 - core
            ).start()

    @pl.when(step_id >= t_final)
    def _():
        c = step_id - t_final
        send_to(
            acc_send.at[c], acc_land.at[c], acc_sems.at[0, c], acc_sems.at[1, c], head=1 - core
        ).wait()
        here = pl.ds(pl.multiple_of(c * CHUNK, CHUNK), CHUNK)
        own_total = jnp.concatenate([dys[b, here, :] for b in range(width // BLOCK)], axis=1)
        total = own_total + acc_land[c].astype(f32)
        scale = scale_ref[:, 0:1]
        hat = hid_ref[...].astype(f32) * scale
        term = jnp.sum(total * hat, axis=0, keepdims=True)

        for b in range(width // BLOCK):
            piece = term[:, b * BLOCK : (b + 1) * BLOCK]
            vec[0, b, 7:8, :] = vec[0, b, 7:8, :] + piece

        ghat = total * gain_ref[...][None, :]
        mean = jnp.mean(ghat * hat, axis=1, keepdims=True)
        ghid_ref[...] = cot_ref[...].astype(f32) + scale * (ghat - hat * mean)

    @when_after(t_final)
    def _():
        rs_out[0].advance(3)

    @when_after(t_final + 1)
    def _():
        rs_values[0].advance(0)

    @when_after(t_final + chunks - 1)
    def _():
        rs_out[1].advance(3)

        def begin(bit):
            sum_copy(vec, vec_land, bit, index, vec_sems).start()

        def add(bit):
            sum_copy(vec, vec_land, bit, index, vec_sems).wait()
            vec[bit + 1] = vec[bit] + vec_land[bit]
            if bit + 1 < bits:
                begin(bit + 1)

        begin(0)
        rs_values[1].advance(0)
        add(0)
        rs_small.advance(0)
        rs_gate[1].advance(3)
        add(1)
        rs_values[0].advance(1)
        rs_small.advance(1)
        rs_values[1].advance(1)
        add(2)
        rs_values[0].advance(2)
        rs_small.advance(2)
        rs_values[0].advance(3)
        rs_values[1].advance(2)
        add(3)
        rs_values[1].advance(3)
        rs_small.advance(3)
        for stage in range(4, bits):
            for reduction in rs_out + rs_gate + rs_values + [rs_small]:
                reduction.advance(stage)
            add(stage)
        sums_ref[8:16, 0:BLOCK] = vec[bits, nb]
        for b in range(nb):
            sums_ref[0:8, b * BLOCK : (b + 1) * BLOCK] = vec[bits, b]


def back_call(
    gm_t, normed_t, near, gated_w, coef, gains, run, step, slope, bc, sext, rows,
    conv_shared, wshared, wstep, gain, wout, y, gate, gate_gain, vext, after, state_in, conv_values, runt, stept, both,
    hidden, cotangent, scale,
):
    width, tokens = normed_t.shape
    inner = y.shape[1]
    chunks = tokens // CHUNK
    nb = inner // BLOCK
    size = lax.axis_size("seq")
    bits = size.bit_length() - 1
    rows_own = width // size
    t_scan, t_grad, t_final = nb, 2 * nb, 3 * nb

    def column(start):
        return lambda s: jnp.clip(s - start, 0, nb - 1)

    def full(shape):
        return pl.BlockSpec(shape, lambda s: (0,) * len(shape), pipeline_mode=pl.Buffered(1))

    def cols(rows, start):
        at = column(start)
        return pl.BlockSpec((rows, BLOCK), lambda s: (0, at(s)))

    row_block = lambda w: pl.BlockSpec((CHUNK, w), lambda s: (jnp.clip(s - t_final, 0, chunks - 1), 0))
    row_single = lambda w: pl.BlockSpec(
        (CHUNK, w),
        lambda s: (jnp.clip(s - t_final, 0, chunks - 1), 0),
        pipeline_mode=pl.Buffered(1),
    )
    held = lambda cols: pltpu.VMEM((2, size, rows_own, cols), bf16)
    landing = lambda cols: tuple(
        pltpu.VMEM((2, size >> (s + 1), rows_own, cols), bf16) for s in range(bits)
    )
    columns = lambda: pltpu.VMEM((2, 2, tokens, inner // 4), bf16)
    sem = pltpu.SemaphoreType.DMA
    return pl.pallas_call(
        functools.partial(back_kernel, bits),
        grid=(3 * nb + chunks,),
        in_specs=[
            full((width, tokens)),
            full((width, tokens)),
            pl.BlockSpec(memory_space=pl.ANY),
            full((tokens, inner)),
            full((tokens, LANES)),
            full((size, LANES)),
            full((tokens, LANES)),
            full((tokens, LANES)),
            full((tokens, LANES)),
            full((tokens, 2 * STATE)),
            full((2, HALO + tokens, LANES)),
            full((8, LANES)),
            full((2, CONV + 1, LANES)),
            full((width, 2 * LANES)),
            full(wstep.shape),
            full((width,)),
            cols(width, 0),
            cols(tokens, 0),
            cols(tokens, 0),
            cols(1, 0),
            pl.BlockSpec(
                (HALO + tokens, BLOCK), lambda s: (0, column(t_scan)(s)), pipeline_mode=pl.Buffered(1)
            ),
            pl.BlockSpec((chunks, STATE, BLOCK), lambda s: (0, 0, column(t_scan)(s))),
            cols(STATE, t_scan),
            cols(CONV + 1, t_scan),
            pl.BlockSpec((1, 8, tokens), lambda s: (column(t_scan)(s), 0, 0)),
            pl.BlockSpec((1, 8, tokens), lambda s: (column(t_scan)(s), 0, 0)),
            pl.BlockSpec(
                (2, width, BLOCK), lambda s: (0, 0, column(t_grad)(s)), pipeline_mode=pl.Buffered(1)
            ),
            row_single(width),
            row_single(width),
            row_block(LANES),
        ],
        out_shape=[
            jax.ShapeDtypeStruct((rows_own, inner), f32),
            jax.ShapeDtypeStruct((2, rows_own, inner), f32),
            jax.ShapeDtypeStruct((rows_own, 2 * LANES), f32),
            jax.ShapeDtypeStruct((tokens, width), f32),
            jax.ShapeDtypeStruct((16, inner), f32),
        ],
        out_specs=[
            full((rows_own, inner)),
            full((2, rows_own, inner)),
            full((rows_own, 2 * LANES)),
            row_block(width),
            pl.BlockSpec((16, inner), lambda s: (0, 0)),
        ],
        scratch_shapes=[
            held(inner // 2), held(inner // 4), held(inner // 4),
            pltpu.VMEM((size, rows_own, 2 * LANES), bf16),
            landing(inner // 2), landing(inner // 4), landing(inner // 4),
            tuple(pltpu.VMEM((size >> (s + 1), rows_own, 2 * LANES), bf16) for s in range(bits)),
            sem((7, 2, bits)),
            pltpu.VMEM((2, width, tokens), bf16), sem((3, 2)),
            columns(), columns(), columns(), sem((2, 2, 2)),
            pltpu.VMEM((nb, tokens, BLOCK), bf16),
            pltpu.VMEM((chunks, CHUNK, width), bf16),
            pltpu.VMEM((chunks, CHUNK, width), bf16),
            sem((2, chunks)),
            pltpu.VMEM((nb, 8, BLOCK), f32),
            pltpu.VMEM((nb, 16, BLOCK), f32),
            pltpu.VMEM((nb, 8, BLOCK), f32),
            sem((2, nb)),
            pltpu.VMEM((2, tokens, LANES), f32),
            pltpu.VMEM((tokens, LANES), f32),
            sem((2,)),
            pltpu.VMEM((tokens, 2 * LANES), bf16),
            pltpu.VMEM((8, LANES), f32),
            pltpu.VMEM((8, LANES), f32),
            sem((2,)),
            pltpu.VMEM((bits + 1, nb + 1, 8, BLOCK), f32),
            pltpu.VMEM((bits, nb + 1, 8, BLOCK), f32),
            sem((2, bits)),
            pltpu.VMEM((chunks, CHUNK, CHUNK), f32),
            pltpu.VMEM((chunks, CHUNK, CHUNK), f32),
            pltpu.VMEM((STATE, tokens), bf16),
            pltpu.VMEM((chunks, CHUNK, CHUNK), f32),
            pltpu.VMEM((tokens, LANES), f32),
            pltpu.VMEM((8, LANES), f32),
            pltpu.VMEM((nb, 8, tokens), f32),
            pltpu.VMEM((tokens, LANES), f32),
            pltpu.VMEM((tokens, LANES), f32),
            pltpu.VMEM((tokens, LANES), f32),
            pltpu.VMEM((HALO + tokens, BLOCK), f32),
            pltpu.VMEM((tokens + 8, BLOCK), f32),
            pltpu.VMEM((nb, tokens, BLOCK), f32),
            pltpu.VMEM((nb, tokens, BLOCK), bf16),
            pltpu.VMEM((nb, 8, BLOCK), f32),
        ] + exchange_scratch(nb, size, bf16),
        compiler_params=pltpu.CompilerParams(
            collective_id=3, has_side_effects=True, vmem_limit_bytes=67043328
        ),
        name="back",
    )(
        gm_t, normed_t, near, gated_w, coef, gains, run, step, slope, bc, sext, rows,
        conv_shared, wshared, wstep, gain, wout, y, gate, gate_gain, vext, after, state_in,
        conv_values,
        runt, stept,
        both, hidden, cotangent, scale,
    )


def final_kernel(
    heads, out_ref, ghid_ref, gout_ref, ginner_ref, gsmall_ref, sums_ref,
    out_to, ghid_to, gout_to, inner_to, step_to, shared_to, norm_to, gate_to, taps_to, staps_to,
    bias_to, decay_to, skip_to,
):
    out_to[...] = out_ref[...]
    ghid_to[...] = ghid_ref[...]

    @pl.when(pl.program_id(0) == 0)
    def _():
        gout_to[...] = gout_ref[...]
        for g in range(2):
            inner_to[:, g, :] = ginner_ref[g]
        shared_to[...] = gsmall_ref[:, 0:LANES]
        step_to[...] = gsmall_ref[:, LANES : LANES + heads]
        taps_to[...] = sums_ref[0 : CONV + 1, :]
        gate_to[...] = sums_ref[CONV + 1, :]
        norm_to[...] = sums_ref[7, :]
        bias_to[...] = sums_ref[8, 0:heads]
        decay_to[...] = sums_ref[9, 0:heads]
        staps_to[...] = sums_ref[10 : 11 + CONV, 0:LANES]
        skip_to[...] = sums_ref[15, 0:heads]


def final_call(heads, block_out, grad_hidden, gout, ginner, gsmall, sums):
    tokens, width = block_out.shape
    rows_own, inner = gout.shape
    rows = 64
    shapes = [
        (tokens, width), (tokens, width), (rows_own, inner), (rows_own, 2, inner),
        (rows_own, heads), (rows_own, LANES), (width,), (inner,), (CONV + 1, inner),
        (CONV + 1, LANES), (heads,), (heads,), (heads,),
    ]

    def full(shape):
        return pl.BlockSpec(shape, lambda i: (0,) * len(shape), pipeline_mode=pl.Buffered(1))

    block = lambda: pl.BlockSpec((rows, width), lambda i: (i, 0))
    return pl.pallas_call(
        functools.partial(final_kernel, heads),
        grid=(tokens // rows,),
        in_specs=[block(), block()] + [full(a.shape) for a in (gout, ginner, gsmall, sums)],
        out_shape=[jax.ShapeDtypeStruct(shape, f32) for shape in shapes],
        out_specs=[block(), block()] + [full(shape) for shape in shapes[2:]],
        name="final",
    )(block_out, grad_hidden, gout, ginner, gsmall, sums)


def body(
    hidden, cotangent, norm_gain, proj_inner, proj_step, proj_shared, conv_values, conv_shared,
    step_bias, decay_log, skip_gain, gate_gain, proj_out,
):
    tokens = hidden.shape[0]
    inner = proj_inner.shape[2]
    heads = proj_step.shape[1]
    width = hidden.shape[1]
    size = lax.axis_size("seq")
    both = jnp.transpose(proj_inner, (1, 0, 2))
    (
        normed_t, norm_scale, gate_in, vext, after, y, gated_w, state_in, step, slope, run, runt,
        stept, sext, bc, gains, block_out, gm_t, coef, near,
        rows,
    ) = forward_call(
        hidden, cotangent, norm_gain, both, proj_step, proj_shared, conv_values, conv_shared,
        step_bias, decay_log, skip_gain, gate_gain[None, :], proj_out,
    )
    (gout, ginner, gsmall, grad_hidden, sums) = back_call(
        gm_t, normed_t, near, gated_w, coef, gains, run, step, slope, bc, sext, rows,
        conv_shared.reshape(CONV + 1, -1, LANES).transpose(1, 0, 2), proj_shared, proj_step,
        norm_gain, proj_out, y, gate_in, gate_gain[None, :], vext, after, state_in, conv_values,
        runt, stept, both, hidden, cotangent, norm_scale,
    )
    (
        block_out, grad_hidden, gout, ginner, gstep, gshared, gnorm, ggain, gtaps, gstaps, gbias,
        gdecay, gskip,
    ) = final_call(heads, block_out, grad_hidden, gout, ginner, gsmall, sums)
    return (
        block_out, grad_hidden, gnorm, ginner, gstep, gshared, gtaps, gstaps, gbias, gdecay, gskip,
        ggain, gout,
    )


def solution(mesh):
    return jax.shard_map(
        body,
        mesh=mesh,
        in_specs=(
            P("seq", None),
            P("seq", None),
            P(),
            P(None, None, "head"),
            P(None, "head"),
            P(),
            P(None, "head"),
            P(),
            P("head"),
            P("head"),
            P("head"),
            P("head"),
            P(None, "head"),
        ),
        out_specs=(
            P("seq", None),
            P("seq", None),
            P(),
            P("seq", None, "head"),
            P("seq", "head"),
            P("seq", "head"),
            P(None, "head"),
            P(None, "head"),
            P("head"),
            P("head"),
            P("head"),
            P("head"),
            P("seq", "head"),
        ),
        check_vma=False,
    )
```

```python
import functools

import jax
import jax.numpy as jnp
from jax import lax
from jax.experimental import pallas as pl
from jax.experimental.pallas import tpu as pltpu
from jax.sharding import PartitionSpec as P

HEAD_DIM = 64
STATE = 128
CONV = 4
INNER = 3072
CHUNK = 128
LANES = 128
BLOCK = 256
HALO = 16
BLOCK_HEADS = BLOCK // HEAD_DIM

norm_eps = 1e-05
highest = lax.Precision.HIGHEST
f32 = jnp.float32
bf16 = jnp.bfloat16
NN = (((1,), (0,)), ((), ()))
NT = (((1,), (1,)), ((), ()))
TN = (((0,), (0,)), ((), ()))


def flip(shard, bit):
    size = lax.axis_size("seq")
    return lax.ppermute(shard, "seq", [(i, i ^ (1 << bit)) for i in range(size)])


def swap(shard):
    return lax.ppermute(shard, "head", [(0, 1), (1, 0)])


def from_behind(shard, by):
    size = lax.axis_size("seq")
    pairs = [(i, i + by) for i in range(size) if 0 <= i + by < size]
    return lax.ppermute(shard, "seq", pairs)


def silu_grad(values):
    sigmoid = 1.0 / (1.0 + jnp.exp(-values))
    return sigmoid * (1.0 + values * (1.0 - sigmoid))


def silu(values):
    return values / (1.0 + jnp.exp(-values))


def mm(a, b, dims=NN):
    return lax.dot_general(a, b, dims, preferred_element_type=f32)


def parts(a):
    high = a.astype(bf16)
    return high, (a - high.astype(f32)).astype(bf16)


def along(pieces, dims, side):
    return jnp.concatenate(pieces, axis=dims[0][side][0])


def mm_left(a, b, dims=NN):
    return mm(along(parts(a), dims, 0), along([b, b], dims, 1), dims)


def mm_right(a, b, dims=NN):
    return mm(along([a, a], dims, 0), along(parts(b), dims, 1), dims)


def mm_both(a, b, dims=NN):
    a_high, a_low = parts(a)
    b_high, b_low = parts(b)
    return mm(
        along([a_high, a_low, a_high], dims, 0), along([b_high, b_high, b_low], dims, 1), dims
    )


def mm_exact(a, b, dims=NN):
    return lax.dot_general(a, b, dims, precision=highest, preferred_element_type=f32)


def widen(cols):
    rows = cols.shape[0]
    lane = lax.broadcasted_iota(jnp.int32, (rows, LANES), 1)
    pieces = []
    for pair in range(BLOCK // LANES):
        first = jnp.broadcast_to(cols[:, 2 * pair : 2 * pair + 1], (rows, LANES))
        second = jnp.broadcast_to(cols[:, 2 * pair + 1 : 2 * pair + 2], (rows, LANES))
        pieces.append(jnp.where(lane < HEAD_DIM, first, second))
    return jnp.concatenate(pieces, axis=1)


def rolled(full, step):
    shift = lax.rem(LANES - BLOCK_HEADS * step, LANES)
    return pltpu.roll(full, shift, 1)


def causal():
    rows = lax.broadcasted_iota(jnp.int32, (CHUNK, CHUNK), 0)
    cols = lax.broadcasted_iota(jnp.int32, (CHUNK, CHUNK), 1)
    return rows >= cols


def conv_rows(ext, taps, first, rows):
    out = taps[CONV : CONV + 1, :]
    for k in range(CONV):
        out = out + taps[k : k + 1, :] * ext[first + k : first + k + rows, :]
    return out


def stack_pair(block):
    lane = lax.broadcasted_iota(jnp.int32, block.shape, 1)
    low = jnp.where(lane < HEAD_DIM, block, jnp.zeros_like(block))
    return low, block - low


class StateExchange:
    def __init__(self, index, size, reverse, own, landing, mixed, result, sems, gains):
        self.index, self.size, self.reverse = index, size, reverse
        self.own, self.landing, self.mixed, self.result = own, landing, mixed, result
        self.sems, self.gains = sems, gains

    def other(self, distance):
        return lax.rem(self.index + distance, self.size)

    def slot(self, source):
        return lax.rem(source - self.index - 1 + 2 * self.size, self.size)

    def send(self, j, value):
        share = value.shape[0] // self.size
        kind = self.own.dtype
        pieces = value.reshape(self.size, share, value.shape[1])
        self.own[j] = pieces.astype(kind)
        for d in range(1, self.size):
            pltpu.make_async_remote_copy(
                src_ref=self.own.at[j, self.other(d)],
                dst_ref=self.landing.at[j, self.size - d - 1],
                send_sem=self.sems.at[0, j],
                recv_sem=self.sems.at[1, j],
                device_id={"seq": self.other(d)},
                device_id_type=pl.DeviceIdType.MESH,
            ).start()

    def all_of(self, buffer, j, send, recv):
        return pltpu.make_async_remote_copy(
            src_ref=buffer.at[j, pl.ds(0, self.size - 1)],
            dst_ref=buffer.at[j, pl.ds(0, self.size - 1)],
            send_sem=self.sems.at[send, j],
            recv_sem=self.sems.at[recv, j],
            device_id={"seq": self.other(1)},
            device_id_type=pl.DeviceIdType.MESH,
        )

    def turn(self, j):
        self.all_of(self.landing, j, 0, 1).wait()
        kind = self.own.dtype
        self.landing[j, self.size - 1] = self.own[j, self.index]
        held = jnp.zeros(self.own.shape[2:], f32)
        order = range(self.size - 1, -1, -1) if self.reverse else range(self.size)
        for source in order:
            self.mixed[j, source] = held.astype(kind)
            gain = widen(rolled(self.gains[source : source + 1, :], j)[:, :BLOCK_HEADS])
            held = gain * held + self.landing[j, self.slot(source)].astype(f32)
        for d in range(1, self.size):
            pltpu.make_async_remote_copy(
                src_ref=self.mixed.at[j, self.other(d)],
                dst_ref=self.result.at[j, self.index],
                send_sem=self.sems.at[2, j],
                recv_sem=self.sems.at[3, j],
                device_id={"seq": self.other(d)},
                device_id_type=pl.DeviceIdType.MESH,
            ).start()

    def take(self, j):
        self.all_of(self.result, j, 2, 3).wait()
        self.result[j, self.index] = self.mixed[j, self.index]
        whole = self.result[j].astype(f32)
        return whole.reshape(whole.shape[0] * whole.shape[1], whole.shape[2])


def exchange_scratch(nb, size, kind):
    share = STATE // size
    return [pltpu.VMEM((nb, size, share, BLOCK), kind) for _ in range(4)] + [
        pltpu.SemaphoreType.DMA((4, nb))
    ]


def greet_all(index, core, size):
    barrier = pltpu.get_barrier_semaphore()
    for d in range(1, size):
        pl.semaphore_signal(
            barrier, inc=1, device_id={"seq": lax.rem(index + d, size)},
            device_id_type=pl.DeviceIdType.MESH,
        )
    pl.semaphore_signal(
        barrier, inc=1, device_id={"head": 1 - core}, device_id_type=pl.DeviceIdType.MESH
    )


def await_all(size):
    pl.semaphore_wait(pltpu.get_barrier_semaphore(), size)


def send_to(src, dst, send_sem, recv_sem, **where):
    return pltpu.make_async_remote_copy(
        src_ref=src, dst_ref=dst, send_sem=send_sem, recv_sem=recv_sem, device_id=where,
        device_id_type=pl.DeviceIdType.MESH,
    )


def transposed(block):
    return block.astype(f32).T.astype(bf16)


def forward_kernel(
    size,
    hid_ref, gain_ref, wi_ref, wstep_ref, wshared_ref, cv_ref, cs_ref, bias_ref, decay_ref,
    skip_ref, ggain_ref, wout_ref, hrow_ref, crow_ref,
    normedt_ref, scale_ref, gate_ref, vext_ref, after_ref, y_ref, gw_ref, in_ref, step_ref,
    slope_ref, run_ref, runt_ref, stept_ref, sext_ref, bc_ref, gains_ref, out_ref, gmt_ref,
    coef_ref, near_ref, rows_ref,
    nx, halo, halo_sems, scores, bt, end_w, vwide, gates, ys, states, acc, acc_send,
    acc_land, acc_sems, squares, sq_land, sq_sems, totals, totals_land, totals_sems,
    near_land, near_sems, ex_own, ex_landing, ex_mixed, ex_result, ex_sems,
):
    step_id = pl.program_id(0)
    index = lax.axis_index("seq")
    core = lax.axis_index("head")
    tokens = hid_ref.shape[0]
    width = hid_ref.shape[1]
    chunks = tokens // CHUNK
    nb = gates.shape[0]
    t_mix, t_last = nb, 2 * nb
    half_width = width // 2
    exchange = StateExchange(
        index, size, False, ex_own, ex_landing, ex_mixed, ex_result, ex_sems, gains_ref
    )

    def norm_rows(rows):
        wide = rows.astype(f32)
        scale = lax.rsqrt(jnp.mean(wide * wide, axis=1, keepdims=True) + norm_eps)
        return (wide * scale * gain_ref[...][None, :]).astype(bf16), scale

    def totals_copy(d):
        return send_to(
            totals, totals_land.at[size - d - 1], totals_sems.at[0], totals_sems.at[1],
            seq=lax.rem(index + d, size),
        )

    @pl.when(step_id == 0)
    def _():
        greet_all(index, core, size)

        @pl.loop(0, chunks)
        def _(i):
            start = pl.multiple_of(i * CHUNK, CHUNK)
            for part in range(2):
                at = pl.multiple_of(start + part * 64, 64)
                rows, scale = norm_rows(hid_ref[pl.ds(at, 64), :])
                nx[pl.ds(pl.multiple_of(HALO + at, HALO), 64), :] = rows
                scale_ref[pl.ds(at, 64), :] = jnp.broadcast_to(scale, (64, LANES))

        await_all(size)
        after_id = lax.rem(index + 1, size)
        halo_copy = send_to(
            hid_ref.at[pl.ds(tokens - HALO, HALO)], halo, halo_sems.at[0], halo_sems.at[1],
            seq=after_id,
        )
        halo_copy.start()
        for c in range(chunks):
            for b in range(width // LANES):
                normedt_ref[b * LANES : (b + 1) * LANES, c * CHUNK : (c + 1) * CHUNK] = transposed(
                    nx[HALO + c * CHUNK : HALO + (c + 1) * CHUNK, b * LANES : (b + 1) * LANES]
                )
        rows_ref[...] = jnp.zeros_like(rows_ref)
        heads = bias_ref.shape[0]
        for i, ref in enumerate((bias_ref, decay_ref, skip_ref)):
            rows_ref[i, 0:heads] = ref[...]
        raw = mm(nx[HALO:, :], wstep_ref[...])
        raw = jnp.concatenate([raw, jnp.zeros((tokens, LANES - heads), f32)], axis=1)
        raw = raw + rows_ref[0:1, :]
        small = jnp.exp(-jnp.abs(raw))
        step = jnp.maximum(raw, 0.0) + jnp.log1p(small)
        step_ref[...] = step
        slope_ref[...] = 1.0 / (1.0 + jnp.exp(-raw))
        rate = -step * jnp.exp(rows_ref[1:2, :])
        tri = causal().astype(f32)
        total = jnp.zeros((1, LANES), f32)
        for c in range(chunks):
            rows = slice(c * CHUNK, (c + 1) * CHUNK)
            run = mm_exact(tri, rate[rows, :])
            run_ref[rows, :] = run
            total = total + run[CHUNK - 1 :, :]
            run_t = run.T
            step_t = step[rows, :].T
            for b in range(nb):
                heads = slice(BLOCK_HEADS * b, BLOCK_HEADS * (b + 1))
                runt_ref[b, 0:BLOCK_HEADS, rows] = run_t[heads, :]
                stept_ref[b, 0:BLOCK_HEADS, rows] = step_t[heads, :]
                runt_ref[b, BLOCK_HEADS:, rows] = jnp.zeros((8 - BLOCK_HEADS, CHUNK), f32)
                stept_ref[b, BLOCK_HEADS:, rows] = jnp.zeros((8 - BLOCK_HEADS, CHUNK), f32)
            end_w[rows, :] = step[rows, :] * jnp.exp(run[CHUNK - 1 :, :] - run)
        totals[...] = jnp.broadcast_to(jnp.exp(total), totals.shape)
        for d in range(1, size):
            totals_copy(d).start()
        halo_copy.wait()
        keep = jnp.where(index == 0, 0.0, 1.0)
        nx[0:HALO, :] = (norm_rows(halo[...])[0].astype(f32) * keep).astype(bf16)
        shared = mm(nx[...], wshared_ref[...]).astype(bf16)
        sext_ref[0] = shared[:, :STATE]
        sext_ref[1] = shared[:, STATE:]
        conv = conv_rows(shared.astype(f32), cs_ref[...], HALO - CONV + 1, tokens)
        act = silu(conv).astype(bf16)
        bc_ref[...] = act
        for c in range(chunks):
            rows = slice(c * CHUNK, (c + 1) * CHUNK)
            b_rows = act[rows, :STATE]
            c_rows = act[rows, STATE:]
            scores[c] = mm(c_rows, b_rows, NT)
            bt[:, rows] = transposed(b_rows)

    @pl.when(step_id < t_mix)
    def _():
        j = step_id
        values = mm(nx[...], wi_ref[1]).astype(bf16)
        vext_ref[...] = values
        vwide[...] = values.astype(f32)
        conv = conv_rows(vwide, cv_ref[...], HALO - CONV + 1, tokens)
        act = silu(conv).astype(bf16)
        run_cols = rolled(run_ref[...], j)
        end_cols = rolled(end_w[...], j)
        state = jnp.zeros((STATE, BLOCK), f32)
        for c in range(chunks):
            rows = slice(c * CHUNK, (c + 1) * CHUNK)
            weighted = act[rows, :].astype(f32) * widen(end_cols[rows, :BLOCK_HEADS])
            last = widen(jnp.exp(run_cols[(c + 1) * CHUNK - 1 : (c + 1) * CHUNK, :BLOCK_HEADS]))
            state = last * state + mm_right(bt[:, rows], weighted)
            after_ref[c] = state
            states[j, c] = state
        exchange.send(j, state)
        gate = mm(nx[HALO:, :], wi_ref[0])
        gate_ref[...] = gate
        gates[j] = gate
        mask = causal()
        skip = widen(rolled(rows_ref[2:3, :], j)[:, :BLOCK_HEADS])
        for c in range(chunks):
            rows = slice(c * CHUNK, (c + 1) * CHUNK)
            cols = run_cols[rows, :BLOCK_HEADS]
            x = act[rows, :]
            y_pairs = []
            for pair in range(BLOCK // LANES):
                mats = []
                for k in range(2):
                    head = 2 * pair + k
                    gap = cols[:, head : head + 1] - runt_ref[j, head : head + 1, rows]
                    decayed = jnp.exp(jnp.where(mask, gap, -1e30))
                    mats.append(scores[c] * decayed * stept_ref[j, head : head + 1, rows])
                low, high = stack_pair(x[:, pair * LANES : (pair + 1) * LANES])
                y_pairs.append(
                    mm_left(jnp.concatenate(mats, axis=1), jnp.concatenate([low, high], axis=0))
                )
            ys[j, rows, :] = jnp.concatenate(y_pairs, axis=1) + skip * x.astype(f32)

    @pl.when(step_id == 1)
    def _():
        pltpu.make_async_remote_copy(
            src_ref=totals_land.at[pl.ds(0, size - 1)],
            dst_ref=totals_land.at[pl.ds(0, size - 1)],
            send_sem=totals_sems.at[0], recv_sem=totals_sems.at[1],
            device_id={"seq": lax.rem(index + 1, size)},
            device_id_type=pl.DeviceIdType.MESH,
        ).wait()
        totals_land[size - 1] = totals[...]
        for source in range(size):
            gains_ref[source : source + 1, :] = totals_land[exchange.slot(source), 0:1, :]

    @pl.when((step_id >= 2) & (step_id < nb + 2))
    def _():
        exchange.turn(step_id - 2)

    def neighbour_copy(bit, first, count):
        mine = (index // (1 << bit)) % 2
        source = pl.multiple_of(core * half_width + first, LANES)
        return send_to(
            normedt_ref.at[pl.ds(source, count)],
            near_land.at[bit, pl.ds(first, count)], near_sems.at[0, bit], near_sems.at[1, bit],
            seq=index + (1 - 2 * mine) * (1 << bit),
        )

    @pl.when((step_id >= 1) & (step_id <= half_width // LANES))
    def _():
        first = pl.multiple_of((step_id - 1) * LANES, LANES)
        for bit in range(2):
            neighbour_copy(bit, first, LANES).start()

    @pl.when((step_id >= t_mix) & (step_id < t_last))
    def _():
        j = step_id - t_mix
        entering = exchange.take(j)
        in_ref[...] = entering
        offsets = offsets_of(run_ref, chunks)
        gated = []
        for c in range(chunks):
            rows = slice(c * CHUNK, (c + 1) * CHUNK)
            grow = rolled(jnp.exp(run_ref[rows, :]), j)[:, :BLOCK_HEADS]
            base = rolled(jnp.exp(offsets[c]), j)[:, :BLOCK_HEADS]
            enter = widen(base) * entering
            if c:
                enter = enter + states[j, c - 1]
            y = ys[j, rows, :] + widen(grow) * mm_right(bc_ref[rows, STATE:], enter)
            y_ref[rows, :] = y
            out = y * silu(gates[j, rows, :])
            gw_ref[rows, :] = (out * ggain_ref[...]).astype(bf16)
            gated.append(
                jnp.broadcast_to(jnp.sum(out * out, axis=1, keepdims=True), (CHUNK, LANES))
            )
        part = mm(gw_ref[...], wout_ref[...], NT)
        block_squares = jnp.concatenate(gated, axis=0)

        @pl.when(j == 0)
        def _():
            acc[...] = part
            squares[...] = block_squares

        @pl.when(j > 0)
        def _():
            acc[...] += part
            squares[...] += block_squares

        @pl.when(j == nb - 1)
        def _():
            send_to(squares, sq_land, sq_sems.at[0], sq_sems.at[1], head=1 - core).start()
            for c in range(chunks):
                acc_send[c] = acc[c * CHUNK : (c + 1) * CHUNK, :].astype(bf16)
                send_to(
                    acc_send.at[c], acc_land.at[c], acc_sems.at[0, c], acc_sems.at[1, c],
                    head=1 - core,
                ).start()

    @pl.when(step_id >= t_last)
    def _():
        c = step_id - t_last

        @pl.when(c == 0)
        def _():
            send_to(squares, sq_land, sq_sems.at[0], sq_sems.at[1], head=1 - core).wait()

        send_to(
            acc_send.at[c], acc_land.at[c], acc_sems.at[0, c], acc_sems.at[1, c], head=1 - core
        ).wait()
        rows = pl.ds(pl.multiple_of(c * CHUNK, CHUNK), CHUNK)
        mixed = acc[rows, :] + acc_land[c].astype(f32)
        inverse = lax.rsqrt((squares[rows, 0:1] + sq_land[rows, 0:1]) / INNER + norm_eps)
        out_ref[...] = hrow_ref[...].astype(f32) + mixed * inverse
        cot = crow_ref[...].astype(f32)
        scaled = (cot * inverse).astype(bf16)
        for b in range(width // LANES):
            gmt_ref[b * LANES : (b + 1) * LANES, :] = transposed(
                scaled[:, b * LANES : (b + 1) * LANES]
            )
        grad_inverse = jnp.sum(cot * mixed, axis=1, keepdims=True)
        coef_ref[...] = jnp.broadcast_to(
            grad_inverse * inverse * inverse * inverse / INNER, (CHUNK, LANES)
        )

        @pl.when(c == chunks - 1)
        def _():
            for bit in range(2):
                neighbour_copy(bit, 0, half_width).wait()
                near_ref[bit] = near_land[bit]


def offsets_of(run_ref, chunks):
    rows = [jnp.zeros((1, LANES), f32)]
    for c in range(chunks):
        rows.append(rows[-1] + run_ref[(c + 1) * CHUNK - 1 : (c + 1) * CHUNK, :])
    return rows


def forward_call(
    hidden, cotangent, gain, both, wstep, wshared, conv_values, conv_shared, bias, decay, skip,
    gate_gain, wout,
):
    tokens, width = hidden.shape
    inner = both.shape[2]
    chunks = tokens // CHUNK
    nb = inner // BLOCK
    size = lax.axis_size("seq")
    t_mix, t_last = nb, 2 * nb

    def at(start):
        return lambda s: jnp.clip(s - start, 0, nb - 1)

    def full(shape):
        return pl.BlockSpec(shape, lambda s: (0,) * len(shape), pipeline_mode=pl.Buffered(1))

    def cols(rows, start):
        return pl.BlockSpec((rows, BLOCK), lambda s: (0, at(start)(s)))

    row_of = lambda s: jnp.clip(s - t_last, 0, chunks - 1)
    row_block = lambda w: pl.BlockSpec((CHUNK, w), lambda s: (row_of(s), 0))
    outs = [
        ((width, tokens), bf16, full((width, tokens))),
        ((tokens, LANES), f32, full((tokens, LANES))),
        ((tokens, inner), f32, cols(tokens, 0)),
        ((HALO + tokens, inner), bf16, cols(HALO + tokens, 0)),
        (
            (chunks, STATE, inner), f32,
            pl.BlockSpec((chunks, STATE, BLOCK), lambda s: (0, 0, at(0)(s))),
        ),
        ((tokens, inner), f32, cols(tokens, t_mix)),
        ((tokens, inner), bf16, cols(tokens, t_mix)),
        ((STATE, inner), f32, cols(STATE, t_mix)),
        ((tokens, LANES), f32, full((tokens, LANES))),
        ((tokens, LANES), f32, full((tokens, LANES))),
        ((tokens, LANES), f32, full((tokens, LANES))),
        ((nb, 8, tokens), f32, full((nb, 8, tokens))),
        ((nb, 8, tokens), f32, full((nb, 8, tokens))),
        ((2, HALO + tokens, STATE), bf16, full((2, HALO + tokens, STATE))),
        ((tokens, 2 * STATE), bf16, full((tokens, 2 * STATE))),
        ((size, LANES), f32, full((size, LANES))),
        ((tokens, width), f32, row_block(width)),
        ((width, tokens), bf16, pl.BlockSpec((width, CHUNK), lambda s: (0, row_of(s)))),
        ((tokens, LANES), f32, row_block(LANES)),
        ((2, width // 2, tokens), bf16, full((2, width // 2, tokens))),
        ((8, LANES), f32, full((8, LANES))),
    ]
    sem = pltpu.SemaphoreType.DMA
    return pl.pallas_call(
        functools.partial(forward_kernel, size),
        grid=(2 * nb + chunks,),
        in_specs=[
            full((tokens, width)),
            full((width,)),
            pl.BlockSpec((2, width, BLOCK), lambda s: (0, 0, at(0)(s))),
            full(wstep.shape),
            full((width, 2 * STATE)),
            cols(CONV + 1, 0),
            full((CONV + 1, 2 * STATE)),
            full(bias.shape),
            full(decay.shape),
            full(skip.shape),
            cols(1, t_mix),
            cols(width, t_mix),
            row_block(width),
            row_block(width),
        ],
        out_shape=[jax.ShapeDtypeStruct(shape, kind) for shape, kind, _ in outs],
        out_specs=[spec for _, _, spec in outs],
        scratch_shapes=[
            pltpu.VMEM((HALO + tokens, width), bf16),
            pltpu.VMEM((HALO, width), bf16),
            sem((2,)),
            pltpu.VMEM((chunks, CHUNK, CHUNK), f32),
            pltpu.VMEM((STATE, tokens), bf16),
            pltpu.VMEM((tokens, LANES), f32),
            pltpu.VMEM((HALO + tokens, BLOCK), f32),
            pltpu.VMEM((nb, tokens, BLOCK), f32),
            pltpu.VMEM((nb, tokens, BLOCK), f32),
            pltpu.VMEM((nb, chunks, STATE, BLOCK), f32),
            pltpu.VMEM((tokens, width), f32),
            pltpu.VMEM((chunks, CHUNK, width), bf16),
            pltpu.VMEM((chunks, CHUNK, width), bf16),
            sem((2, chunks)),
            pltpu.VMEM((tokens, LANES), f32),
            pltpu.VMEM((tokens, LANES), f32),
            sem((2,)),
            pltpu.VMEM((8, LANES), f32),
            pltpu.VMEM((size, 8, LANES), f32),
            sem((2,)),
            pltpu.VMEM((2, width // 2, tokens), bf16),
            sem((2, 2)),
        ] + exchange_scratch(nb, size, f32),
        compiler_params=pltpu.CompilerParams(
            collective_id=1, has_side_effects=True, vmem_limit_bytes=67043328
        ),
        name="forward",
    )(
        hidden, gain, both, wstep, wshared, conv_values, conv_shared, bias, decay, skip, gate_gain,
        wout, hidden, cotangent,
    )


def order_rows(part, bits):
    order = list(range(bits))
    if part == 1:
        order[:3] = order[:3][::-1]
    if part == 2:
        order[:2] = order[:2][::-1]
    return order


def order_columns(part, bits):
    return [bit for bit in range(bits) if bit != part] + [part]


def slot_of(owner, order):
    slot = 0
    for bit in order:
        slot = slot * 2 + ((owner >> bit) & 1)
    return slot


class Reduction:
    def __init__(self, held, landing, order, index, sems, put, put_other=None):
        self.held, self.landing, self.order = held, landing, order
        self.index, self.sems, self.put, self.put_other = index, sems, put, put_other
        self.stages = len(order)

    def place(self, stage):
        base = 0
        size = 1 << self.stages
        for s, bit in enumerate(self.order[: stage + 1]):
            mine = (self.index // (1 << bit)) % 2
            half = size >> (s + 1)
            keep, give = base + mine * half, base + (1 - mine) * half
            base = keep
        return keep, give, half

    def copy(self, stage):
        _, give, half = self.place(stage)
        bit = self.order[stage]
        mine = (self.index // (1 << bit)) % 2
        return send_to(
            self.held.at[pl.ds(give, half)], self.landing[stage],
            self.sems.at[0, stage], self.sems.at[1, stage],
            seq=self.index + (1 - 2 * mine) * (1 << bit),
        )

    def start(self, stage):
        self.copy(stage).start()

    def start_piece(self, piece, pieces):
        _, give, half = self.place(0)
        count = half // pieces
        bit = self.order[0]
        mine = (self.index // (1 << bit)) % 2
        send_to(
            self.held.at[pl.ds(give + piece * count, count)],
            self.landing[0].at[pl.ds(piece * count, count)],
            self.sems.at[0, 0], self.sems.at[1, 0],
            seq=self.index + (1 - 2 * mine) * (1 << bit),
        ).start()

    def advance(self, stage):
        self.copy(stage).wait()
        keep, _, half = self.place(stage)
        if stage < self.stages - 1:

            @pl.loop(0, half)
            def _(i):
                total = self.held[keep + i].astype(f32) + self.landing[stage][i].astype(f32)
                self.held[keep + i] = total.astype(bf16)

            self.start(stage + 1)
        elif self.put_other is None:
            self.put(self.held[keep].astype(f32) + self.landing[stage][0].astype(f32))
        else:
            self.put(self.held[keep].astype(f32))
            self.put_other(self.landing[stage][0].astype(f32))


def sum_copy(acc, landing, bit, index, sems):
    mine = (index // (1 << bit)) % 2
    return pltpu.make_async_remote_copy(
        src_ref=acc.at[bit],
        dst_ref=landing.at[bit],
        send_sem=sems.at[0, bit],
        recv_sem=sems.at[1, bit],
        device_id={"seq": index + (1 - 2 * mine) * (1 << bit)},
        device_id_type=pl.DeviceIdType.MESH,
    )


def back_kernel(
    bits,
    gmt_ref, normedt_ref, near_ref, gw_ref, coef_ref, gains_ref, run_ref, step_ref, slope_ref,
    bc_ref, sext_ref, rows_ref, cs_ref, wshared_ref, wstep_ref, gain_ref,
    wout_ref, y_ref, gate_ref, ggain_ref, vext_ref, after_ref, in_ref, cv_ref, runt_ref,
    stept_ref, wi_ref,
    hid_ref, cot_ref, scale_ref,
    gout_ref, ginner_ref, gsmall_ref, ghid_ref, sums_ref,
    w_out, w_gate, w_values, w_small,
    land_out, land_gate, land_values, land_small,
    rs_sems, near, near_sems,
    own_cols, other_cols, land_cols, cols_sems,
    gv, acc_send, acc_land, acc_sems,
    edge_own, edge_tail, edge_land, edge_sems,
    dbc, dbc_land, dbc_sems, small, sedge_own, sedge_land, sedge_sems,
    vec, vec_land, vec_sems,
    scores, scorest, ct, dscores, end_w, ends, dcols, xdu, dyc, xdus, vwide, gext,
    dys, ggates, term_gate, ex_own, ex_landing, ex_mixed, ex_result, ex_sems,
):
    step_id = pl.program_id(0)
    index = lax.axis_index("seq")
    core = lax.axis_index("head")
    size = 1 << bits
    tokens = y_ref.shape[0]
    chunks = tokens // CHUNK
    nb = ggates.shape[0]
    half_nb = nb // 2
    width = normedt_ref.shape[0]
    half_width = width // 2
    rows_own = width // size
    t_scan, t_grad, t_final = nb, 2 * nb, 3 * nb
    after_id = lax.rem(index + 1, size)
    before_id = lax.rem(index + size - 1, size)
    bit_of = lambda bit: (index // (1 << bit)) % 2
    flip_of = lambda bit: index + (1 - 2 * bit_of(bit)) * (1 << bit)

    def out_reduction(part):
        cols = w_out.shape[3]

        def put(value):
            gout_ref[:, part * cols : (part + 1) * cols] = value

        return Reduction(
            w_out.at[part], [ref.at[part] for ref in land_out], order_rows(part, bits), index,
            rs_sems.at[part], put,
        )

    def columns_reduction(g, part):
        held, landing = ((w_gate, land_gate), (w_values, land_values))[g]

        def put_half(half):
            def put(value):
                for b in range(half_nb):
                    lane = (part * half_nb + b) * BLOCK + half * LANES
                    place = pl.ds(pl.multiple_of(lane, LANES), LANES)
                    ginner_ref[g, :, place] = value[:, b * LANES : (b + 1) * LANES]

            return put

        return Reduction(
            held.at[part], [ref.at[part] for ref in landing], order_columns(part, bits), index,
            rs_sems.at[2 + 2 * g + part], put_half(bit_of(part)), put_half(1 - bit_of(part)),
        )

    def put_small(value):
        gsmall_ref[...] = value

    rs_out = [out_reduction(part) for part in range(2)]
    rs_gate = [columns_reduction(0, part) for part in range(2)]
    rs_values = [columns_reduction(1, part) for part in range(2)]
    rs_small = Reduction(
        w_small, list(land_small), order_rows(2, bits), index, rs_sems.at[6], put_small
    )

    def when_after(step):
        return pl.when(step_id == step)

    exchange = StateExchange(
        index, size, True, ex_own, ex_landing, ex_mixed, ex_result, ex_sems, gains_ref
    )

    def near_copies(bit):
        half = pl.ds(pl.multiple_of(core * half_width, half_width), half_width)
        return (
            pltpu.make_async_copy(near_ref.at[bit], near.at[bit, half], near_sems.at[0, bit]),
            send_to(
                near_ref.at[bit], near.at[bit, half], near_sems.at[1, bit], near_sems.at[2, bit],
                head=1 - core,
            ),
        )

    @pl.when(step_id == 0)
    def _():
        greet_all(index, core, size)
        for c in range(chunks):
            rows = slice(c * CHUNK, (c + 1) * CHUNK)
            ct[:, rows] = transposed(bc_ref[rows, STATE:])
            for b in range(width // LANES):
                acc_send[c, :, b * LANES : (b + 1) * LANES] = transposed(
                    gmt_ref[b * LANES : (b + 1) * LANES, rows]
                )
        await_all(size)
        for bit in range(2):
            for copy in near_copies(bit):
                copy.start()

    group = width // 4
    owners = size // 4

    def scatter(piece, q, order, store):
        for b in range(owners):
            store(slot_of(q * owners + b, order), piece[b * rows_own : (b + 1) * rows_own, :])

    def put_out(part):
        cols = w_out.shape[3]
        for q in range(4):
            left = gmt_ref[q * group : (q + 1) * group, :]
            piece = mm(left, gw_ref[:, part * cols : (part + 1) * cols]).astype(bf16)

            def store(slot, value):
                w_out[part, slot] = value

            scatter(piece, q, order_rows(part, bits), store)

    def columns_copy(g, part):
        return send_to(
            other_cols.at[g, part], land_cols.at[g, part], cols_sems.at[0, g, part],
            cols_sems.at[1, g, part], seq=flip_of(part),
        )

    def split_block(g, j, value):
        part = j // half_nb
        mine = jnp.where(part == 0, bit_of(0), bit_of(1))
        place = j % half_nb
        first, second = value[:, :LANES], value[:, LANES:]
        own_cols[g, part, place] = jnp.where(mine == 0, first, second)
        other_cols[g, part, place] = jnp.where(mine == 0, second, first)
        partner = flip_of(0) + part * (flip_of(1) - flip_of(0))
        send_to(
            other_cols.at[g, part, place], land_cols.at[g, part, place],
            cols_sems.at[0, g, part], cols_sems.at[1, g, part], seq=partner,
        ).start()

    def put_columns(g, part):
        columns_copy(g, part).wait()
        side = lambda ref: jnp.concatenate([ref[g, part, b] for b in range(half_nb)], axis=1)
        right = jnp.concatenate([side(own_cols), side(land_cols)], axis=0)
        held = (w_gate, w_values)[g]
        for q in range(4):
            rows = slice(q * group, (q + 1) * group)
            piece = mm(
                jnp.concatenate([normedt_ref[rows, :], near[part, rows, :]], axis=1),
                right,
            )

            def store(slot, value):
                held[part, slot] = value

            scatter(piece.astype(bf16), q, order_columns(part, bits), store)
        (rs_gate, rs_values)[g][part].start(0)

    @pl.when(step_id < t_scan)
    def _():
        j = step_id
        offsets = offsets_of(run_ref, chunks)
        own = jnp.zeros((STATE, BLOCK), f32)
        term = jnp.zeros((1, BLOCK), f32)
        for c in range(chunks):
            rows = slice(c * CHUNK, (c + 1) * CHUNK)
            ggw = mm(acc_send[c], wout_ref[...])
            y = y_ref[rows, :]
            gate = gate_ref[rows, :]
            sig = 1.0 / (1.0 + jnp.exp(-gate))
            act = gate * sig
            out = y * act
            term = term + jnp.sum(ggw * out, axis=0, keepdims=True)
            coef = jnp.concatenate([coef_ref[rows, 0:LANES]] * (BLOCK // LANES), axis=1)
            gg = ggw * ggain_ref[...] - coef * out
            dy = gg * act
            dys[j, rows, :] = dy
            ggate = (gg * y * (sig * (1.0 + gate * (1.0 - sig)))).astype(bf16)
            ggates[j, rows, :] = ggate
            grow = rolled(jnp.exp(run_ref[rows, :] + offsets[c]), j)[:, :BLOCK_HEADS]
            own = own + mm(ct[:, rows], (dy * widen(grow)).astype(bf16))
        term_gate[j, 0:1, :] = term
        exchange.send(j, own)
        split_block(0, j, ggates[j])

    for part in range(2):

        @when_after(part)
        def _(part=part):
            put_out(part)

    pieces = size // 2

    @pl.when((step_id >= 1) & (step_id < nb))
    def _():
        for reduction in rs_out:
            reduction.start_piece(step_id - 1, pieces)

    rest = pieces - (nb - 1)

    @when_after(nb)
    def _():
        for piece in range(nb - 1, nb - 1 + (rest + 1) // 2):
            for reduction in rs_out:
                reduction.start_piece(piece, pieces)

    @when_after(nb + 1)
    def _():
        for piece in range(nb - 1 + (rest + 1) // 2, pieces):
            for reduction in rs_out:
                reduction.start_piece(piece, pieces)

    @pl.when((step_id >= 2) & (step_id < nb + 2))
    def _():
        exchange.turn(step_id - 2)

    @when_after(nb - 1)
    def _():
        for bit in range(2):
            for copy in near_copies(bit):
                copy.wait()
        put_columns(0, 0)

    mask = causal()
    rows_i = lax.broadcasted_iota(jnp.int32, (CHUNK, CHUNK), 0)
    cols_i = lax.broadcasted_iota(jnp.int32, (CHUNK, CHUNK), 1)
    mask_t = rows_i <= cols_i

    @pl.when(step_id == t_scan)
    def _():
        dbc[...] = jnp.zeros_like(dbc)
        dscores[...] = jnp.zeros_like(dscores)
        dcols[...] = jnp.zeros_like(dcols)
        xdu[...] = jnp.zeros_like(xdu)
        dyc[...] = jnp.zeros_like(dyc)
        xdus[...] = jnp.zeros_like(xdus)
        ends[...] = jnp.zeros_like(ends)
        vec[...] = jnp.zeros_like(vec)
        for c in range(chunks):
            rows = slice(c * CHUNK, (c + 1) * CHUNK)
            b_rows = bc_ref[rows, :STATE]
            c_rows = bc_ref[rows, STATE:]
            scores[c] = mm(c_rows, b_rows, NT)
            scorest[c] = mm(b_rows, c_rows, NT)
            run = run_ref[rows, :]
            end_w[rows, :] = jnp.exp(run[CHUNK - 1 :, :] - run)

    @pl.when((step_id >= t_scan) & (step_id < t_grad))
    def _():
        j = step_id - t_scan
        offsets = offsets_of(run_ref, chunks)
        vwide[...] = vext_ref[...].astype(f32)
        taps = [jnp.zeros((1, BLOCK), f32)] * (CONV + 1)
        run_cols = rolled(run_ref[...], j)
        step_cols = rolled(step_ref[...], j)
        end_cols = rolled(end_w[...], j)
        skip = widen(rolled(rows_ref[2:3, :], j)[:, :BLOCK_HEADS])
        channel = lax.broadcasted_iota(jnp.int32, (BLOCK, LANES), 0) // HEAD_DIM
        lane = lax.broadcasted_iota(jnp.int32, (BLOCK, LANES), 1)
        pick = (lane == BLOCK_HEADS * j + channel).astype(bf16)
        lane_row = lax.broadcasted_iota(jnp.int32, (CHUNK, LANES), 1)
        dstate = exchange.take(j)
        dskip = jnp.zeros((1, BLOCK), f32)
        gext[tokens : tokens + 8, :] = jnp.zeros((8, BLOCK), f32)
        for c in reversed(range(chunks)):
            rows = slice(c * CHUNK, (c + 1) * CHUNK)
            cols = run_cols[rows, :BLOCK_HEADS]
            conv = conv_rows(vwide, cv_ref[...], HALO - CONV + 1 + c * CHUNK, CHUNK)
            sig = 1.0 / (1.0 + jnp.exp(-conv))
            x = (conv * sig).astype(bf16)
            slope = sig * (1.0 + conv * (1.0 - sig))
            wide_x = x.astype(f32)
            dy = dys[j, rows, :]
            b_rows = bc_ref[rows, :STATE]
            c_rows = bc_ref[rows, STATE:]
            grow = widen(jnp.exp(cols))
            tail = widen(end_cols[rows, :BLOCK_HEADS])
            step_w = widen(step_cols[rows, :BLOCK_HEADS])
            last = grow[CHUNK - 1 :, :]
            base = rolled(jnp.exp(offsets[c]), j)[:, :BLOCK_HEADS]
            enter = widen(base) * in_ref[...]
            if c:
                enter = enter + after_ref[c - 1]
            du_state = tail * mm(b_rows, dstate.astype(bf16))
            carried = grow * mm(c_rows, enter.astype(bf16))
            weighted = wide_x * (tail * step_w)
            grown = dy * grow
            dbc[0, rows, :] += mm_both(weighted, dstate, NT)
            dbc[1, rows, :] += mm_both(grown, enter, NT)
            hold = last * jnp.sum(dstate * enter, axis=0, keepdims=True)
            dstate = last * dstate + mm_right(ct[:, rows], grown)
            du_pairs = []
            col_sum = jnp.zeros((CHUNK, LANES), f32)
            dscore = dscores[c]
            for pair in range(BLOCK // LANES):
                lanes = slice(pair * LANES, (pair + 1) * LANES)
                low, high = stack_pair(dy[:, lanes])
                both = jnp.concatenate([low, high], axis=0)
                dmat = mm_left(both, x[:, lanes], NT)
                mats = []
                for k in range(2):
                    head = 2 * pair + k
                    col = cols[:, head : head + 1]
                    row = runt_ref[0, head : head + 1, rows]
                    keep = jnp.exp(jnp.where(mask, col - row, -1e30))
                    piece = dmat[k * CHUNK : (k + 1) * CHUNK, :] * keep
                    piece = piece * stept_ref[0, head : head + 1, rows]
                    dscore = dscore + piece
                    full = piece * scores[c]
                    col_sum = jnp.where(
                        lane_row == BLOCK_HEADS * j + head,
                        jnp.sum(full, axis=1, keepdims=True),
                        col_sum,
                    )
                    dcols[j, head : head + 1, rows] = jnp.sum(full, axis=0, keepdims=True)
                    keep_t = jnp.exp(jnp.where(mask_t, row - col, -1e30))
                    mats.append(scorest[c] * keep_t)
                du_pairs.append(
                    mm(jnp.concatenate(mats, axis=1).astype(bf16), both.astype(bf16))
                )
            dscores[c] = dscore
            du = jnp.concatenate(du_pairs, axis=1) + du_state
            by_head = mm(
                jnp.concatenate(
                    [
                        (wide_x * du).astype(bf16),
                        (dy * carried).astype(bf16),
                        (wide_x * du_state).astype(bf16),
                        *parts(jnp.broadcast_to(hold, (HALO, BLOCK))),
                    ],
                    axis=0,
                ),
                pick,
            )
            xdu[rows, :] += by_head[0:CHUNK, :]
            dyc[rows, :] += by_head[CHUNK : 2 * CHUNK, :] + col_sum
            xdus[rows, :] += by_head[2 * CHUNK : 3 * CHUNK, :]
            end = 3 * CHUNK
            ends[c : c + 1, :] += (
                by_head[end : end + 1, :] + by_head[end + HALO : end + HALO + 1, :]
            )
            dskip = dskip + jnp.sum(dy * wide_x, axis=0, keepdims=True)
            gconv = (step_w * du + skip * dy) * slope
            gext[rows, :] = gconv
            taps[CONV] = taps[CONV] + jnp.sum(gconv, axis=0, keepdims=True)
            values = vwide[HALO + c * CHUNK : HALO + (c + 1) * CHUNK, :]
            total = cv_ref[CONV - 1 : CONV, :] * gconv
            taps[CONV - 1] = taps[CONV - 1] + jnp.sum(values * gconv, axis=0, keepdims=True)
            for k in range(CONV - 1):
                ahead = c * CHUNK + CONV - 1 - k
                moved = gext[ahead : ahead + CHUNK, :]
                total = total + cv_ref[k : k + 1, :] * moved
                taps[k] = taps[k] + jnp.sum(values * moved, axis=0, keepdims=True)
            gv[j, rows, :] = total.astype(bf16)
            if c == chunks - 1:
                edge_tail[j, 0:8, :] = total[CHUNK - 8 :, :]
        row8 = lax.broadcasted_iota(jnp.int32, (8, BLOCK), 0)
        ahead_rows = vwide[HALO - CONV + 1 : HALO - CONV + 9, :]
        for k in range(CONV):
            tap = taps[k]
            if k < CONV - 1:
                moved = pltpu.roll(gext[0:8, :], k, 0) if k else gext[0:8, :]
                inside = (row8 >= k) & (row8 < CONV - 1)
                tap = tap + jnp.sum(
                    jnp.where(inside, ahead_rows * moved, 0.0), axis=0, keepdims=True
                )
            vec[0, j, k : k + 1, :] = tap
        vec[0, j, CONV : CONV + 1, :] = taps[CONV]
        vec[0, j, CONV + 1 : CONV + 2, :] = term_gate[j, 0:1, :]
        by_head = mm(jnp.concatenate(parts(jnp.broadcast_to(dskip, (HALO, BLOCK))), axis=0), pick)
        vec[0, nb, 7:8, 0:LANES] += by_head[0:1, :] + by_head[HALO : HALO + 1, :]
        edge_tail[j, 8 : 8 + CONV + 1, :] = cv_ref[...]
        edge_own[j] = gext[0:8, :]
        send_to(
            edge_own.at[j], edge_land.at[j], edge_sems.at[0, j], edge_sems.at[1, j], seq=before_id
        ).start()

    def finish_block(j):
        send_to(
            edge_own.at[j], edge_land.at[j], edge_sems.at[0, j], edge_sems.at[1, j], seq=before_id
        ).wait()
        nxt = jnp.where(index == size - 1, 0.0, 1.0) * edge_land[j]
        row8 = lax.broadcasted_iota(jnp.int32, (8, BLOCK), 0)
        fix = edge_tail[j, 0:8, :]
        for k in range(CONV - 1):
            ahead = CONV - 1 - k
            moved = pltpu.roll(nxt, 8 - ahead, 0)
            fix = fix + jnp.where(row8 >= 8 - ahead, edge_tail[j, 8 + k : 9 + k, :] * moved, 0.0)
        both_rows = jnp.concatenate([gv[j, tokens - 16 : tokens - 8, :].astype(f32), fix], axis=0)
        gv[j, tokens - 16 :, :] = both_rows.astype(bf16)
        split_block(1, j, gv[j])

    @pl.when((step_id > t_scan + 1) & (step_id < t_grad))
    def _():
        finish_block(step_id - t_scan - 2)

    @when_after(t_scan + 1)
    def _():
        put_columns(0, 1)

    @when_after(t_scan + 2)
    def _():
        rs_gate[0].advance(0)
        rs_out[0].advance(0)
        rs_out[1].advance(0)

    @when_after(t_scan + half_nb + 1)
    def _():
        rs_gate[0].advance(1)
        rs_gate[1].advance(0)

    @when_after(t_grad - 1)
    def _():
        rs_out[0].advance(1)

    @when_after(t_grad - 1)
    def _():
        tri = mask.astype(f32)
        tri_t = mask_t.astype(f32)
        strict = (rows_i > cols_i).astype(f32)
        decay = jnp.exp(rows_ref[1:2, :])
        bias_sum = jnp.zeros((1, LANES), f32)
        decay_sum = jnp.zeros((1, LANES), f32)
        for c in range(chunks):
            rows = slice(c * CHUNK, (c + 1) * CHUNK)
            step = step_ref[rows, :]
            col_rows = [dcols[b, 0:BLOCK_HEADS, rows] for b in range(nb)]
            rest = LANES - BLOCK_HEADS * nb
            col_rows.append(jnp.zeros((rest, CHUNK), f32))
            dlog = dyc[rows, :] - jnp.concatenate(col_rows, axis=0).T
            drate = (
                mm_exact(tri_t, dlog)
                + mm_exact(strict, xdus[rows, :] * step)
                + ends[c : c + 1, :]
            )
            dstep = xdu[rows, :] - decay * drate
            draw = dstep * slope_ref[rows, :]
            small[rows, LANES:] = draw.astype(bf16)
            bias_sum = bias_sum + jnp.sum(draw, axis=0, keepdims=True)
            decay_sum = decay_sum - jnp.sum(drate * step, axis=0, keepdims=True) * decay
            b_rows = bc_ref[rows, :STATE]
            c_rows = bc_ref[rows, STATE:]
            high, low = parts(dscores[c])
            dbc[1, rows, :] += mm(high, b_rows) + mm(low, b_rows)
            dbc[0, rows, :] += mm(high, c_rows, TN) + mm(low, c_rows, TN)
        vec[0, nb, 0:1, 0:LANES] = bias_sum
        vec[0, nb, 1:2, 0:LANES] = decay_sum
        send_to(
            dbc.at[1 - core], dbc_land, dbc_sems.at[0], dbc_sems.at[1], head=1 - core
        ).start()

    @when_after(t_grad)
    def _():
        finish_block(nb - 2)
        finish_block(nb - 1)
        put_columns(1, 0)
        rs_gate[0].advance(2)
        rs_gate[1].advance(1)
        rs_out[1].advance(1)

    @when_after(t_grad + 1)
    def _():
        rs_gate[0].advance(3)

    @when_after(t_grad)
    def _():
        send_to(
            dbc.at[1 - core], dbc_land, dbc_sems.at[0], dbc_sems.at[1], head=1 - core
        ).wait()
        sext = sext_ref[core].astype(f32)
        taps = cs_ref[core]
        conv = conv_rows(sext, taps, HALO - CONV + 1, tokens)
        gs = (dbc[core] + dbc_land[...]) * silu_grad(conv)
        for k in range(CONV):
            first = HALO - CONV + 1 + k
            vec[0, nb, 2 + k : 3 + k, 0:LANES] = jnp.sum(
                sext[first : first + tokens, :] * gs, axis=0, keepdims=True
            )
        vec[0, nb, 2 + CONV : 3 + CONV, 0:LANES] = jnp.sum(gs, axis=0, keepdims=True)
        dbc[core] = gs
        sedge_own[...] = gs[0:8, :]
        send_to(
            sedge_own, sedge_land, sedge_sems.at[0], sedge_sems.at[1], seq=before_id
        ).start()

    @when_after(t_grad + 1)
    def _():
        send_to(
            sedge_own, sedge_land, sedge_sems.at[0], sedge_sems.at[1], seq=before_id
        ).wait()
        taps = cs_ref[core]
        nxt = jnp.where(index == size - 1, 0.0, 1.0) * sedge_land[...]
        gs = jnp.concatenate([dbc[core], nxt], axis=0)
        total = taps[CONV - 1 : CONV, :] * gs[0:tokens, :]
        for k in range(CONV - 1):
            total = total + taps[k : k + 1, :] * gs[CONV - 1 - k : CONV - 1 - k + tokens, :]
        small[:, 0:LANES] = total.astype(bf16)
        for q in range(4):
            piece = mm(normedt_ref[q * group : (q + 1) * group, :], small[...]).astype(bf16)

            def store(slot, value):
                w_small[slot] = value

            scatter(piece, q, order_rows(2, bits), store)
        rs_small.start(0)

    @pl.when((step_id >= t_grad) & (step_id < t_final))
    def _():
        j = step_id - t_grad
        part = mm(
            jnp.concatenate([ggates[j], gv[j]], axis=1),
            jnp.concatenate([wi_ref[0], wi_ref[1]], axis=1),
            NT,
        )

        @pl.when(j == 0)
        def _():
            for b in range(width // BLOCK):
                dys[b] = part[:, b * BLOCK : (b + 1) * BLOCK]

        @pl.when(j > 0)
        def _():
            for b in range(width // BLOCK):
                dys[b] += part[:, b * BLOCK : (b + 1) * BLOCK]

    @when_after(t_grad + 2)
    def _():
        rs_out[0].advance(2)

    @when_after(t_grad + 3)
    def _():
        put_columns(1, 1)
        rs_out[1].advance(2)

    @when_after(t_grad + 4)
    def _():
        rs_gate[1].advance(2)
        own = pl.ds(pl.multiple_of(core * LANES, LANES), LANES)
        heads = wstep_ref.shape[1]
        rest = mm(small[:, 0:LANES], wshared_ref[:, own], NT) + mm(
            small[:, LANES : LANES + heads], wstep_ref[...], NT
        )
        for b in range(width // BLOCK):
            dys[b] += rest[:, b * BLOCK : (b + 1) * BLOCK]

    @when_after(t_final - 1)
    def _():
        for c in range(chunks):
            rows = slice(c * CHUNK, (c + 1) * CHUNK)
            for b in range(width // BLOCK):
                acc_send[c, :, b * BLOCK : (b + 1) * BLOCK] = dys[b, rows, :].astype(bf16)
            send_to(
                acc_send.at[c], acc_land.at[c], acc_sems.at[0, c], acc_sems.at[1, c], head=1 - core
            ).start()

    @pl.when(step_id >= t_final)
    def _():
        c = step_id - t_final
        send_to(
            acc_send.at[c], acc_land.at[c], acc_sems.at[0, c], acc_sems.at[1, c], head=1 - core
        ).wait()
        here = pl.ds(pl.multiple_of(c * CHUNK, CHUNK), CHUNK)
        own_total = jnp.concatenate([dys[b, here, :] for b in range(width // BLOCK)], axis=1)
        total = own_total + acc_land[c].astype(f32)
        scale = scale_ref[:, 0:1]
        hat = hid_ref[...].astype(f32) * scale
        term = jnp.sum(total * hat, axis=0, keepdims=True)

        for b in range(width // BLOCK):
            piece = term[:, b * BLOCK : (b + 1) * BLOCK]
            vec[0, b, 7:8, :] = vec[0, b, 7:8, :] + piece

        ghat = total * gain_ref[...][None, :]
        mean = jnp.mean(ghat * hat, axis=1, keepdims=True)
        ghid_ref[...] = cot_ref[...].astype(f32) + scale * (ghat - hat * mean)

    @when_after(t_final)
    def _():
        rs_out[0].advance(3)

    @when_after(t_final - 1)
    def _():
        rs_values[0].advance(0)

    @when_after(t_final + 2)
    def _():
        rs_values[0].advance(1)

    @when_after(t_final + chunks - 1)
    def _():
        rs_out[1].advance(3)

        def begin(bit):
            sum_copy(vec, vec_land, bit, index, vec_sems).start()

        def add(bit):
            sum_copy(vec, vec_land, bit, index, vec_sems).wait()
            vec[bit + 1] = vec[bit] + vec_land[bit]
            if bit + 1 < bits:
                begin(bit + 1)

        begin(0)
        rs_values[1].advance(0)
        add(0)
        rs_small.advance(0)
        rs_gate[1].advance(3)
        add(1)
        rs_small.advance(1)
        rs_values[1].advance(1)
        add(2)
        rs_values[0].advance(2)
        rs_small.advance(2)
        rs_values[0].advance(3)
        rs_values[1].advance(2)
        add(3)
        rs_values[1].advance(3)
        rs_small.advance(3)
        for stage in range(4, bits):
            for reduction in rs_out + rs_gate + rs_values + [rs_small]:
                reduction.advance(stage)
            add(stage)
        sums_ref[8:16, 0:BLOCK] = vec[bits, nb]
        for b in range(nb):
            sums_ref[0:8, b * BLOCK : (b + 1) * BLOCK] = vec[bits, b]


def back_call(
    gm_t, normed_t, near, gated_w, coef, gains, run, step, slope, bc, sext, rows,
    conv_shared, wshared, wstep, gain, wout, y, gate, gate_gain, vext, after, state_in, conv_values, runt, stept, both,
    hidden, cotangent, scale,
):
    width, tokens = normed_t.shape
    inner = y.shape[1]
    chunks = tokens // CHUNK
    nb = inner // BLOCK
    size = lax.axis_size("seq")
    bits = size.bit_length() - 1
    rows_own = width // size
    t_scan, t_grad, t_final = nb, 2 * nb, 3 * nb

    def column(start):
        return lambda s: jnp.clip(s - start, 0, nb - 1)

    def full(shape):
        return pl.BlockSpec(shape, lambda s: (0,) * len(shape), pipeline_mode=pl.Buffered(1))

    def cols(rows, start):
        at = column(start)
        return pl.BlockSpec((rows, BLOCK), lambda s: (0, at(s)))

    row_block = lambda w: pl.BlockSpec((CHUNK, w), lambda s: (jnp.clip(s - t_final, 0, chunks - 1), 0))
    row_single = lambda w: pl.BlockSpec(
        (CHUNK, w),
        lambda s: (jnp.clip(s - t_final, 0, chunks - 1), 0),
        pipeline_mode=pl.Buffered(1),
    )
    held = lambda cols: pltpu.VMEM((2, size, rows_own, cols), bf16)
    landing = lambda cols: tuple(
        pltpu.VMEM((2, size >> (s + 1), rows_own, cols), bf16) for s in range(bits)
    )
    columns = lambda: pltpu.VMEM((2, 2, nb // 2, tokens, LANES), bf16)
    sem = pltpu.SemaphoreType.DMA
    return pl.pallas_call(
        functools.partial(back_kernel, bits),
        grid=(3 * nb + chunks,),
        in_specs=[
            full((width, tokens)),
            full((width, tokens)),
            pl.BlockSpec(memory_space=pl.ANY),
            full((tokens, inner)),
            full((tokens, LANES)),
            full((size, LANES)),
            full((tokens, LANES)),
            full((tokens, LANES)),
            full((tokens, LANES)),
            full((tokens, 2 * STATE)),
            full((2, HALO + tokens, LANES)),
            full((8, LANES)),
            full((2, CONV + 1, LANES)),
            full((width, 2 * LANES)),
            full(wstep.shape),
            full((width,)),
            cols(width, 0),
            cols(tokens, 0),
            cols(tokens, 0),
            cols(1, 0),
            pl.BlockSpec(
                (HALO + tokens, BLOCK), lambda s: (0, column(t_scan)(s)), pipeline_mode=pl.Buffered(1)
            ),
            pl.BlockSpec((chunks, STATE, BLOCK), lambda s: (0, 0, column(t_scan)(s))),
            cols(STATE, t_scan),
            cols(CONV + 1, t_scan),
            pl.BlockSpec((1, 8, tokens), lambda s: (column(t_scan)(s), 0, 0)),
            pl.BlockSpec((1, 8, tokens), lambda s: (column(t_scan)(s), 0, 0)),
            pl.BlockSpec(
                (2, width, BLOCK), lambda s: (0, 0, column(t_grad)(s)), pipeline_mode=pl.Buffered(1)
            ),
            row_single(width),
            row_single(width),
            row_block(LANES),
        ],
        out_shape=[
            jax.ShapeDtypeStruct((rows_own, inner), f32),
            jax.ShapeDtypeStruct((2, rows_own, inner), f32),
            jax.ShapeDtypeStruct((rows_own, 2 * LANES), f32),
            jax.ShapeDtypeStruct((tokens, width), f32),
            jax.ShapeDtypeStruct((16, inner), f32),
        ],
        out_specs=[
            full((rows_own, inner)),
            full((2, rows_own, inner)),
            full((rows_own, 2 * LANES)),
            row_block(width),
            pl.BlockSpec((16, inner), lambda s: (0, 0)),
        ],
        scratch_shapes=[
            held(inner // 2), held(inner // 4), held(inner // 4),
            pltpu.VMEM((size, rows_own, 2 * LANES), bf16),
            landing(inner // 2), landing(inner // 4), landing(inner // 4),
            tuple(pltpu.VMEM((size >> (s + 1), rows_own, 2 * LANES), bf16) for s in range(bits)),
            sem((7, 2, bits)),
            pltpu.VMEM((2, width, tokens), bf16), sem((3, 2)),
            columns(), columns(), columns(), sem((2, 2, 2)),
            pltpu.VMEM((nb, tokens, BLOCK), bf16),
            pltpu.VMEM((chunks, CHUNK, width), bf16),
            pltpu.VMEM((chunks, CHUNK, width), bf16),
            sem((2, chunks)),
            pltpu.VMEM((nb, 8, BLOCK), f32),
            pltpu.VMEM((nb, 16, BLOCK), f32),
            pltpu.VMEM((nb, 8, BLOCK), f32),
            sem((2, nb)),
            pltpu.VMEM((2, tokens, LANES), f32),
            pltpu.VMEM((tokens, LANES), f32),
            sem((2,)),
            pltpu.VMEM((tokens, 2 * LANES), bf16),
            pltpu.VMEM((8, LANES), f32),
            pltpu.VMEM((8, LANES), f32),
            sem((2,)),
            pltpu.VMEM((bits + 1, nb + 1, 8, BLOCK), f32),
            pltpu.VMEM((bits, nb + 1, 8, BLOCK), f32),
            sem((2, bits)),
            pltpu.VMEM((chunks, CHUNK, CHUNK), f32),
            pltpu.VMEM((chunks, CHUNK, CHUNK), f32),
            pltpu.VMEM((STATE, tokens), bf16),
            pltpu.VMEM((chunks, CHUNK, CHUNK), f32),
            pltpu.VMEM((tokens, LANES), f32),
            pltpu.VMEM((8, LANES), f32),
            pltpu.VMEM((nb, 8, tokens), f32),
            pltpu.VMEM((tokens, LANES), f32),
            pltpu.VMEM((tokens, LANES), f32),
            pltpu.VMEM((tokens, LANES), f32),
            pltpu.VMEM((HALO + tokens, BLOCK), f32),
            pltpu.VMEM((tokens + 8, BLOCK), f32),
            pltpu.VMEM((nb, tokens, BLOCK), f32),
            pltpu.VMEM((nb, tokens, BLOCK), bf16),
            pltpu.VMEM((nb, 8, BLOCK), f32),
        ] + exchange_scratch(nb, size, bf16),
        compiler_params=pltpu.CompilerParams(
            collective_id=3, has_side_effects=True, vmem_limit_bytes=67043328
        ),
        name="back",
    )(
        gm_t, normed_t, near, gated_w, coef, gains, run, step, slope, bc, sext, rows,
        conv_shared, wshared, wstep, gain, wout, y, gate, gate_gain, vext, after, state_in,
        conv_values,
        runt, stept,
        both, hidden, cotangent, scale,
    )


def final_kernel(
    heads, out_ref, ghid_ref, gout_ref, ginner_ref, gsmall_ref, sums_ref,
    out_to, ghid_to, gout_to, inner_to, step_to, shared_to, norm_to, gate_to, taps_to, staps_to,
    bias_to, decay_to, skip_to,
):
    out_to[...] = out_ref[...]
    ghid_to[...] = ghid_ref[...]

    @pl.when(pl.program_id(0) == 0)
    def _():
        gout_to[...] = gout_ref[...]
        for g in range(2):
            inner_to[:, g, :] = ginner_ref[g]
        shared_to[...] = gsmall_ref[:, 0:LANES]
        step_to[...] = gsmall_ref[:, LANES : LANES + heads]
        taps_to[...] = sums_ref[0 : CONV + 1, :]
        gate_to[...] = sums_ref[CONV + 1, :]
        norm_to[...] = sums_ref[7, :]
        bias_to[...] = sums_ref[8, 0:heads]
        decay_to[...] = sums_ref[9, 0:heads]
        staps_to[...] = sums_ref[10 : 11 + CONV, 0:LANES]
        skip_to[...] = sums_ref[15, 0:heads]


def final_call(heads, block_out, grad_hidden, gout, ginner, gsmall, sums):
    tokens, width = block_out.shape
    rows_own, inner = gout.shape
    rows = 64
    shapes = [
        (tokens, width), (tokens, width), (rows_own, inner), (rows_own, 2, inner),
        (rows_own, heads), (rows_own, LANES), (width,), (inner,), (CONV + 1, inner),
        (CONV + 1, LANES), (heads,), (heads,), (heads,),
    ]

    def full(shape):
        return pl.BlockSpec(shape, lambda i: (0,) * len(shape), pipeline_mode=pl.Buffered(1))

    block = lambda: pl.BlockSpec((rows, width), lambda i: (i, 0))
    return pl.pallas_call(
        functools.partial(final_kernel, heads),
        grid=(tokens // rows,),
        in_specs=[block(), block()] + [full(a.shape) for a in (gout, ginner, gsmall, sums)],
        out_shape=[jax.ShapeDtypeStruct(shape, f32) for shape in shapes],
        out_specs=[block(), block()] + [full(shape) for shape in shapes[2:]],
        name="final",
    )(block_out, grad_hidden, gout, ginner, gsmall, sums)


def body(
    hidden, cotangent, norm_gain, proj_inner, proj_step, proj_shared, conv_values, conv_shared,
    step_bias, decay_log, skip_gain, gate_gain, proj_out,
):
    tokens = hidden.shape[0]
    inner = proj_inner.shape[2]
    heads = proj_step.shape[1]
    width = hidden.shape[1]
    size = lax.axis_size("seq")
    both = jnp.transpose(proj_inner, (1, 0, 2))
    (
        normed_t, norm_scale, gate_in, vext, after, y, gated_w, state_in, step, slope, run, runt,
        stept, sext, bc, gains, block_out, gm_t, coef, near,
        rows,
    ) = forward_call(
        hidden, cotangent, norm_gain, both, proj_step, proj_shared, conv_values, conv_shared,
        step_bias, decay_log, skip_gain, gate_gain[None, :], proj_out,
    )
    (gout, ginner, gsmall, grad_hidden, sums) = back_call(
        gm_t, normed_t, near, gated_w, coef, gains, run, step, slope, bc, sext, rows,
        conv_shared.reshape(CONV + 1, -1, LANES).transpose(1, 0, 2), proj_shared, proj_step,
        norm_gain, proj_out, y, gate_in, gate_gain[None, :], vext, after, state_in, conv_values,
        runt, stept, both, hidden, cotangent, norm_scale,
    )
    (
        block_out, grad_hidden, gout, ginner, gstep, gshared, gnorm, ggain, gtaps, gstaps, gbias,
        gdecay, gskip,
    ) = final_call(heads, block_out, grad_hidden, gout, ginner, gsmall, sums)
    return (
        block_out, grad_hidden, gnorm, ginner, gstep, gshared, gtaps, gstaps, gbias, gdecay, gskip,
        ggain, gout,
    )


def solution(mesh):
    return jax.shard_map(
        body,
        mesh=mesh,
        in_specs=(
            P("seq", None),
            P("seq", None),
            P(),
            P(None, None, "head"),
            P(None, "head"),
            P(),
            P(None, "head"),
            P(),
            P("head"),
            P("head"),
            P("head"),
            P("head"),
            P(None, "head"),
        ),
        out_specs=(
            P("seq", None),
            P("seq", None),
            P(),
            P("seq", None, "head"),
            P("seq", "head"),
            P("seq", "head"),
            P(None, "head"),
            P(None, "head"),
            P("head"),
            P("head"),
            P("head"),
            P("head"),
            P("seq", "head"),
        ),
        check_vma=False,
    )
```

```python
import functools

import jax
import jax.numpy as jnp
from jax import lax
from jax.experimental import pallas as pl
from jax.experimental.pallas import tpu as pltpu
from jax.sharding import PartitionSpec as P

HEAD_DIM = 64
STATE = 128
CONV = 4
INNER = 3072
CHUNK = 128
LANES = 128
BLOCK = 256
HALO = 16
BLOCK_HEADS = BLOCK // HEAD_DIM

norm_eps = 1e-05
highest = lax.Precision.HIGHEST
f32 = jnp.float32
bf16 = jnp.bfloat16
NN = (((1,), (0,)), ((), ()))
NT = (((1,), (1,)), ((), ()))
TN = (((0,), (0,)), ((), ()))


def flip(shard, bit):
    size = lax.axis_size("seq")
    return lax.ppermute(shard, "seq", [(i, i ^ (1 << bit)) for i in range(size)])


def swap(shard):
    return lax.ppermute(shard, "head", [(0, 1), (1, 0)])


def from_behind(shard, by):
    size = lax.axis_size("seq")
    pairs = [(i, i + by) for i in range(size) if 0 <= i + by < size]
    return lax.ppermute(shard, "seq", pairs)


def silu_grad(values):
    sigmoid = 1.0 / (1.0 + jnp.exp(-values))
    return sigmoid * (1.0 + values * (1.0 - sigmoid))


def silu(values):
    return values / (1.0 + jnp.exp(-values))


def mm(a, b, dims=NN):
    return lax.dot_general(a, b, dims, preferred_element_type=f32)


def parts(a):
    high = a.astype(bf16)
    return high, (a - high.astype(f32)).astype(bf16)


def along(pieces, dims, side):
    return jnp.concatenate(pieces, axis=dims[0][side][0])


def mm_left(a, b, dims=NN):
    return mm(along(parts(a), dims, 0), along([b, b], dims, 1), dims)


def mm_right(a, b, dims=NN):
    return mm(along([a, a], dims, 0), along(parts(b), dims, 1), dims)


def mm_both(a, b, dims=NN):
    a_high, a_low = parts(a)
    b_high, b_low = parts(b)
    return mm(
        along([a_high, a_low, a_high], dims, 0), along([b_high, b_high, b_low], dims, 1), dims
    )


def mm_exact(a, b, dims=NN):
    return lax.dot_general(a, b, dims, precision=highest, preferred_element_type=f32)


def widen(cols):
    rows = cols.shape[0]
    lane = lax.broadcasted_iota(jnp.int32, (rows, LANES), 1)
    pieces = []
    for pair in range(BLOCK // LANES):
        first = jnp.broadcast_to(cols[:, 2 * pair : 2 * pair + 1], (rows, LANES))
        second = jnp.broadcast_to(cols[:, 2 * pair + 1 : 2 * pair + 2], (rows, LANES))
        pieces.append(jnp.where(lane < HEAD_DIM, first, second))
    return jnp.concatenate(pieces, axis=1)


def rolled(full, step):
    shift = lax.rem(LANES - BLOCK_HEADS * step, LANES)
    return pltpu.roll(full, shift, 1)


def causal():
    rows = lax.broadcasted_iota(jnp.int32, (CHUNK, CHUNK), 0)
    cols = lax.broadcasted_iota(jnp.int32, (CHUNK, CHUNK), 1)
    return rows >= cols


def conv_rows(ext, taps, first, rows):
    out = taps[CONV : CONV + 1, :]
    for k in range(CONV):
        out = out + taps[k : k + 1, :] * ext[first + k : first + k + rows, :]
    return out


def stack_pair(block):
    lane = lax.broadcasted_iota(jnp.int32, block.shape, 1)
    low = jnp.where(lane < HEAD_DIM, block, jnp.zeros_like(block))
    return low, block - low


class StateExchange:
    def __init__(self, index, size, reverse, own, landing, mixed, result, sems, gains):
        self.index, self.size, self.reverse = index, size, reverse
        self.own, self.landing, self.mixed, self.result = own, landing, mixed, result
        self.sems, self.gains = sems, gains

    def other(self, distance):
        return lax.rem(self.index + distance, self.size)

    def slot(self, source):
        return lax.rem(source - self.index - 1 + 2 * self.size, self.size)

    def send(self, j, value):
        share = value.shape[0] // self.size
        kind = self.own.dtype
        pieces = value.reshape(self.size, share, value.shape[1])
        self.own[j] = pieces.astype(kind)
        for d in range(1, self.size):
            pltpu.make_async_remote_copy(
                src_ref=self.own.at[j, self.other(d)],
                dst_ref=self.landing.at[j, self.size - d - 1],
                send_sem=self.sems.at[0, j],
                recv_sem=self.sems.at[1, j],
                device_id={"seq": self.other(d)},
                device_id_type=pl.DeviceIdType.MESH,
            ).start()

    def all_of(self, buffer, j, send, recv):
        return pltpu.make_async_remote_copy(
            src_ref=buffer.at[j, pl.ds(0, self.size - 1)],
            dst_ref=buffer.at[j, pl.ds(0, self.size - 1)],
            send_sem=self.sems.at[send, j],
            recv_sem=self.sems.at[recv, j],
            device_id={"seq": self.other(1)},
            device_id_type=pl.DeviceIdType.MESH,
        )

    def turn(self, j):
        self.all_of(self.landing, j, 0, 1).wait()
        kind = self.own.dtype
        self.landing[j, self.size - 1] = self.own[j, self.index]
        held = jnp.zeros(self.own.shape[2:], f32)
        order = range(self.size - 1, -1, -1) if self.reverse else range(self.size)
        for source in order:
            self.mixed[j, source] = held.astype(kind)
            gain = widen(rolled(self.gains[source : source + 1, :], j)[:, :BLOCK_HEADS])
            held = gain * held + self.landing[j, self.slot(source)].astype(f32)
        for d in range(1, self.size):
            pltpu.make_async_remote_copy(
                src_ref=self.mixed.at[j, self.other(d)],
                dst_ref=self.result.at[j, self.index],
                send_sem=self.sems.at[2, j],
                recv_sem=self.sems.at[3, j],
                device_id={"seq": self.other(d)},
                device_id_type=pl.DeviceIdType.MESH,
            ).start()

    def take(self, j):
        self.all_of(self.result, j, 2, 3).wait()
        self.result[j, self.index] = self.mixed[j, self.index]
        whole = self.result[j].astype(f32)
        return whole.reshape(whole.shape[0] * whole.shape[1], whole.shape[2])


def exchange_scratch(nb, size, kind):
    share = STATE // size
    return [pltpu.VMEM((nb, size, share, BLOCK), kind) for _ in range(4)] + [
        pltpu.SemaphoreType.DMA((4, nb))
    ]


def greet_all(index, core, size):
    barrier = pltpu.get_barrier_semaphore()
    for d in range(1, size):
        pl.semaphore_signal(
            barrier, inc=1, device_id={"seq": lax.rem(index + d, size)},
            device_id_type=pl.DeviceIdType.MESH,
        )
    pl.semaphore_signal(
        barrier, inc=1, device_id={"head": 1 - core}, device_id_type=pl.DeviceIdType.MESH
    )


def await_all(size):
    pl.semaphore_wait(pltpu.get_barrier_semaphore(), size)


def send_to(src, dst, send_sem, recv_sem, **where):
    return pltpu.make_async_remote_copy(
        src_ref=src, dst_ref=dst, send_sem=send_sem, recv_sem=recv_sem, device_id=where,
        device_id_type=pl.DeviceIdType.MESH,
    )


def transposed(block):
    return block.astype(f32).T.astype(bf16)


def forward_kernel(
    size,
    hid_ref, gain_ref, wi_ref, wstep_ref, wshared_ref, cv_ref, cs_ref, bias_ref, decay_ref,
    skip_ref, ggain_ref, wout_ref, hrow_ref, crow_ref,
    normedt_ref, scale_ref, gate_ref, vext_ref, after_ref, y_ref, gw_ref, in_ref, step_ref,
    slope_ref, run_ref, runt_ref, stept_ref, sext_ref, bc_ref, gains_ref, out_ref, gmt_ref,
    coef_ref, near_ref, rows_ref,
    nx, halo, halo_sems, scores, bt, end_w, vwide, gates, ys, states, acc, acc_send,
    acc_land, acc_sems, squares, sq_land, sq_sems, totals, totals_land, totals_sems,
    near_land, near_sems, ex_own, ex_landing, ex_mixed, ex_result, ex_sems,
):
    step_id = pl.program_id(0)
    index = lax.axis_index("seq")
    core = lax.axis_index("head")
    tokens = hid_ref.shape[0]
    width = hid_ref.shape[1]
    chunks = tokens // CHUNK
    nb = gates.shape[0]
    t_mix, t_last = nb, 2 * nb
    half_width = width // 2
    exchange = StateExchange(
        index, size, False, ex_own, ex_landing, ex_mixed, ex_result, ex_sems, gains_ref
    )

    def norm_rows(rows):
        wide = rows.astype(f32)
        scale = lax.rsqrt(jnp.mean(wide * wide, axis=1, keepdims=True) + norm_eps)
        return (wide * scale * gain_ref[...][None, :]).astype(bf16), scale

    def totals_copy(d):
        return send_to(
            totals, totals_land.at[size - d - 1], totals_sems.at[0], totals_sems.at[1],
            seq=lax.rem(index + d, size),
        )

    @pl.when(step_id == 0)
    def _():
        greet_all(index, core, size)

        @pl.loop(0, chunks)
        def _(i):
            start = pl.multiple_of(i * CHUNK, CHUNK)
            for part in range(2):
                at = pl.multiple_of(start + part * 64, 64)
                rows, scale = norm_rows(hid_ref[pl.ds(at, 64), :])
                nx[pl.ds(pl.multiple_of(HALO + at, HALO), 64), :] = rows
                scale_ref[pl.ds(at, 64), :] = jnp.broadcast_to(scale, (64, LANES))

        await_all(size)
        after_id = lax.rem(index + 1, size)
        halo_copy = send_to(
            hid_ref.at[pl.ds(tokens - HALO, HALO)], halo, halo_sems.at[0], halo_sems.at[1],
            seq=after_id,
        )
        halo_copy.start()
        for c in range(chunks):
            for b in range(width // LANES):
                normedt_ref[b * LANES : (b + 1) * LANES, c * CHUNK : (c + 1) * CHUNK] = transposed(
                    nx[HALO + c * CHUNK : HALO + (c + 1) * CHUNK, b * LANES : (b + 1) * LANES]
                )
        rows_ref[...] = jnp.zeros_like(rows_ref)
        heads = bias_ref.shape[0]
        for i, ref in enumerate((bias_ref, decay_ref, skip_ref)):
            rows_ref[i, 0:heads] = ref[...]
        raw = mm(nx[HALO:, :], wstep_ref[...])
        raw = jnp.concatenate([raw, jnp.zeros((tokens, LANES - heads), f32)], axis=1)
        raw = raw + rows_ref[0:1, :]
        small = jnp.exp(-jnp.abs(raw))
        step = jnp.maximum(raw, 0.0) + jnp.log1p(small)
        step_ref[...] = step
        slope_ref[...] = 1.0 / (1.0 + jnp.exp(-raw))
        rate = -step * jnp.exp(rows_ref[1:2, :])
        tri = causal().astype(f32)
        total = jnp.zeros((1, LANES), f32)
        for c in range(chunks):
            rows = slice(c * CHUNK, (c + 1) * CHUNK)
            run = mm_exact(tri, rate[rows, :])
            run_ref[rows, :] = run
            total = total + run[CHUNK - 1 :, :]
            run_t = run.T
            step_t = step[rows, :].T
            for b in range(nb):
                heads = slice(BLOCK_HEADS * b, BLOCK_HEADS * (b + 1))
                runt_ref[b, 0:BLOCK_HEADS, rows] = run_t[heads, :]
                stept_ref[b, 0:BLOCK_HEADS, rows] = step_t[heads, :]
                runt_ref[b, BLOCK_HEADS:, rows] = jnp.zeros((8 - BLOCK_HEADS, CHUNK), f32)
                stept_ref[b, BLOCK_HEADS:, rows] = jnp.zeros((8 - BLOCK_HEADS, CHUNK), f32)
            end_w[rows, :] = step[rows, :] * jnp.exp(run[CHUNK - 1 :, :] - run)
        totals[...] = jnp.broadcast_to(jnp.exp(total), totals.shape)
        for d in range(1, size):
            totals_copy(d).start()
        halo_copy.wait()
        keep = jnp.where(index == 0, 0.0, 1.0)
        nx[0:HALO, :] = (norm_rows(halo[...])[0].astype(f32) * keep).astype(bf16)
        shared = mm(nx[...], wshared_ref[...]).astype(bf16)
        sext_ref[0] = shared[:, :STATE]
        sext_ref[1] = shared[:, STATE:]
        conv = conv_rows(shared.astype(f32), cs_ref[...], HALO - CONV + 1, tokens)
        act = silu(conv).astype(bf16)
        bc_ref[...] = act
        for c in range(chunks):
            rows = slice(c * CHUNK, (c + 1) * CHUNK)
            b_rows = act[rows, :STATE]
            c_rows = act[rows, STATE:]
            scores[c] = mm(c_rows, b_rows, NT)
            bt[:, rows] = transposed(b_rows)

    @pl.when(step_id < t_mix)
    def _():
        j = step_id
        values = mm(nx[...], wi_ref[1]).astype(bf16)
        vext_ref[...] = values
        vwide[...] = values.astype(f32)
        conv = conv_rows(vwide, cv_ref[...], HALO - CONV + 1, tokens)
        act = silu(conv).astype(bf16)
        run_cols = rolled(run_ref[...], j)
        end_cols = rolled(end_w[...], j)
        state = jnp.zeros((STATE, BLOCK), f32)
        for c in range(chunks):
            rows = slice(c * CHUNK, (c + 1) * CHUNK)
            weighted = act[rows, :].astype(f32) * widen(end_cols[rows, :BLOCK_HEADS])
            last = widen(jnp.exp(run_cols[(c + 1) * CHUNK - 1 : (c + 1) * CHUNK, :BLOCK_HEADS]))
            state = last * state + mm_right(bt[:, rows], weighted)
            after_ref[c] = state
            states[j, c] = state
        exchange.send(j, state)
        gate = mm(nx[HALO:, :], wi_ref[0])
        gate_ref[...] = gate
        gates[j] = gate
        mask = causal()
        skip = widen(rolled(rows_ref[2:3, :], j)[:, :BLOCK_HEADS])
        for c in range(chunks):
            rows = slice(c * CHUNK, (c + 1) * CHUNK)
            cols = run_cols[rows, :BLOCK_HEADS]
            x = act[rows, :]
            y_pairs = []
            for pair in range(BLOCK // LANES):
                mats = []
                for k in range(2):
                    head = 2 * pair + k
                    gap = cols[:, head : head + 1] - runt_ref[j, head : head + 1, rows]
                    decayed = jnp.exp(jnp.where(mask, gap, -1e30))
                    mats.append(scores[c] * decayed * stept_ref[j, head : head + 1, rows])
                low, high = stack_pair(x[:, pair * LANES : (pair + 1) * LANES])
                y_pairs.append(
                    mm_left(jnp.concatenate(mats, axis=1), jnp.concatenate([low, high], axis=0))
                )
            ys[j, rows, :] = jnp.concatenate(y_pairs, axis=1) + skip * x.astype(f32)

    @pl.when(step_id == 1)
    def _():
        pltpu.make_async_remote_copy(
            src_ref=totals_land.at[pl.ds(0, size - 1)],
            dst_ref=totals_land.at[pl.ds(0, size - 1)],
            send_sem=totals_sems.at[0], recv_sem=totals_sems.at[1],
            device_id={"seq": lax.rem(index + 1, size)},
            device_id_type=pl.DeviceIdType.MESH,
        ).wait()
        totals_land[size - 1] = totals[...]
        for source in range(size):
            gains_ref[source : source + 1, :] = totals_land[exchange.slot(source), 0:1, :]

    @pl.when((step_id >= 2) & (step_id < nb + 2))
    def _():
        exchange.turn(step_id - 2)

    def neighbour_copy(bit, first, count):
        mine = (index // (1 << bit)) % 2
        source = pl.multiple_of(core * half_width + first, LANES)
        return send_to(
            normedt_ref.at[pl.ds(source, count)],
            near_land.at[bit, pl.ds(first, count)], near_sems.at[0, bit], near_sems.at[1, bit],
            seq=index + (1 - 2 * mine) * (1 << bit),
        )

    @pl.when((step_id >= 1) & (step_id <= half_width // LANES))
    def _():
        first = pl.multiple_of((step_id - 1) * LANES, LANES)
        for bit in range(2):
            neighbour_copy(bit, first, LANES).start()

    @pl.when((step_id >= t_mix) & (step_id < t_last))
    def _():
        j = step_id - t_mix
        entering = exchange.take(j)
        in_ref[...] = entering
        offsets = offsets_of(run_ref, chunks)
        gated = []
        for c in range(chunks):
            rows = slice(c * CHUNK, (c + 1) * CHUNK)
            grow = rolled(jnp.exp(run_ref[rows, :]), j)[:, :BLOCK_HEADS]
            base = rolled(jnp.exp(offsets[c]), j)[:, :BLOCK_HEADS]
            enter = widen(base) * entering
            if c:
                enter = enter + states[j, c - 1]
            y = ys[j, rows, :] + widen(grow) * mm_right(bc_ref[rows, STATE:], enter)
            y_ref[rows, :] = y
            out = y * silu(gates[j, rows, :])
            gw_ref[rows, :] = (out * ggain_ref[...]).astype(bf16)
            gated.append(
                jnp.broadcast_to(jnp.sum(out * out, axis=1, keepdims=True), (CHUNK, LANES))
            )
        part = mm(gw_ref[...], wout_ref[...], NT)
        block_squares = jnp.concatenate(gated, axis=0)

        @pl.when(j == 0)
        def _():
            acc[...] = part
            squares[...] = block_squares

        @pl.when(j > 0)
        def _():
            acc[...] += part
            squares[...] += block_squares

        @pl.when(j == nb - 1)
        def _():
            send_to(squares, sq_land, sq_sems.at[0], sq_sems.at[1], head=1 - core).start()
            for c in range(chunks):
                acc_send[c] = acc[c * CHUNK : (c + 1) * CHUNK, :].astype(bf16)
                send_to(
                    acc_send.at[c], acc_land.at[c], acc_sems.at[0, c], acc_sems.at[1, c],
                    head=1 - core,
                ).start()

    @pl.when(step_id >= t_last)
    def _():
        c = step_id - t_last

        @pl.when(c == 0)
        def _():
            send_to(squares, sq_land, sq_sems.at[0], sq_sems.at[1], head=1 - core).wait()

        send_to(
            acc_send.at[c], acc_land.at[c], acc_sems.at[0, c], acc_sems.at[1, c], head=1 - core
        ).wait()
        rows = pl.ds(pl.multiple_of(c * CHUNK, CHUNK), CHUNK)
        mixed = acc[rows, :] + acc_land[c].astype(f32)
        inverse = lax.rsqrt((squares[rows, 0:1] + sq_land[rows, 0:1]) / INNER + norm_eps)
        out_ref[...] = hrow_ref[...].astype(f32) + mixed * inverse
        cot = crow_ref[...].astype(f32)
        scaled = (cot * inverse).astype(bf16)
        for b in range(width // LANES):
            gmt_ref[b * LANES : (b + 1) * LANES, :] = transposed(
                scaled[:, b * LANES : (b + 1) * LANES]
            )
        grad_inverse = jnp.sum(cot * mixed, axis=1, keepdims=True)
        coef_ref[...] = jnp.broadcast_to(
            grad_inverse * inverse * inverse * inverse / INNER, (CHUNK, LANES)
        )

        @pl.when(c == chunks - 1)
        def _():
            for bit in range(2):
                neighbour_copy(bit, 0, half_width).wait()
                near_ref[bit] = near_land[bit]


def offsets_of(run_ref, chunks):
    rows = [jnp.zeros((1, LANES), f32)]
    for c in range(chunks):
        rows.append(rows[-1] + run_ref[(c + 1) * CHUNK - 1 : (c + 1) * CHUNK, :])
    return rows


def forward_call(
    hidden, cotangent, gain, both, wstep, wshared, conv_values, conv_shared, bias, decay, skip,
    gate_gain, wout,
):
    tokens, width = hidden.shape
    inner = both.shape[2]
    chunks = tokens // CHUNK
    nb = inner // BLOCK
    size = lax.axis_size("seq")
    t_mix, t_last = nb, 2 * nb

    def at(start):
        return lambda s: jnp.clip(s - start, 0, nb - 1)

    def full(shape):
        return pl.BlockSpec(shape, lambda s: (0,) * len(shape), pipeline_mode=pl.Buffered(1))

    def cols(rows, start):
        return pl.BlockSpec((rows, BLOCK), lambda s: (0, at(start)(s)))

    row_of = lambda s: jnp.clip(s - t_last, 0, chunks - 1)
    row_block = lambda w: pl.BlockSpec((CHUNK, w), lambda s: (row_of(s), 0))
    outs = [
        ((width, tokens), bf16, full((width, tokens))),
        ((tokens, LANES), f32, full((tokens, LANES))),
        ((tokens, inner), f32, cols(tokens, 0)),
        ((HALO + tokens, inner), bf16, cols(HALO + tokens, 0)),
        (
            (chunks, STATE, inner), f32,
            pl.BlockSpec((chunks, STATE, BLOCK), lambda s: (0, 0, at(0)(s))),
        ),
        ((tokens, inner), f32, cols(tokens, t_mix)),
        ((tokens, inner), bf16, cols(tokens, t_mix)),
        ((STATE, inner), f32, cols(STATE, t_mix)),
        ((tokens, LANES), f32, full((tokens, LANES))),
        ((tokens, LANES), f32, full((tokens, LANES))),
        ((tokens, LANES), f32, full((tokens, LANES))),
        ((nb, 8, tokens), f32, full((nb, 8, tokens))),
        ((nb, 8, tokens), f32, full((nb, 8, tokens))),
        ((2, HALO + tokens, STATE), bf16, full((2, HALO + tokens, STATE))),
        ((tokens, 2 * STATE), bf16, full((tokens, 2 * STATE))),
        ((size, LANES), f32, full((size, LANES))),
        ((tokens, width), f32, row_block(width)),
        ((width, tokens), bf16, pl.BlockSpec((width, CHUNK), lambda s: (0, row_of(s)))),
        ((tokens, LANES), f32, row_block(LANES)),
        ((2, width // 2, tokens), bf16, full((2, width // 2, tokens))),
        ((8, LANES), f32, full((8, LANES))),
    ]
    sem = pltpu.SemaphoreType.DMA
    return pl.pallas_call(
        functools.partial(forward_kernel, size),
        grid=(2 * nb + chunks,),
        in_specs=[
            full((tokens, width)),
            full((width,)),
            pl.BlockSpec((2, width, BLOCK), lambda s: (0, 0, at(0)(s))),
            full(wstep.shape),
            full((width, 2 * STATE)),
            cols(CONV + 1, 0),
            full((CONV + 1, 2 * STATE)),
            full(bias.shape),
            full(decay.shape),
            full(skip.shape),
            cols(1, t_mix),
            cols(width, t_mix),
            row_block(width),
            row_block(width),
        ],
        out_shape=[jax.ShapeDtypeStruct(shape, kind) for shape, kind, _ in outs],
        out_specs=[spec for _, _, spec in outs],
        scratch_shapes=[
            pltpu.VMEM((HALO + tokens, width), bf16),
            pltpu.VMEM((HALO, width), bf16),
            sem((2,)),
            pltpu.VMEM((chunks, CHUNK, CHUNK), f32),
            pltpu.VMEM((STATE, tokens), bf16),
            pltpu.VMEM((tokens, LANES), f32),
            pltpu.VMEM((HALO + tokens, BLOCK), f32),
            pltpu.VMEM((nb, tokens, BLOCK), f32),
            pltpu.VMEM((nb, tokens, BLOCK), f32),
            pltpu.VMEM((nb, chunks, STATE, BLOCK), f32),
            pltpu.VMEM((tokens, width), f32),
            pltpu.VMEM((chunks, CHUNK, width), bf16),
            pltpu.VMEM((chunks, CHUNK, width), bf16),
            sem((2, chunks)),
            pltpu.VMEM((tokens, LANES), f32),
            pltpu.VMEM((tokens, LANES), f32),
            sem((2,)),
            pltpu.VMEM((8, LANES), f32),
            pltpu.VMEM((size, 8, LANES), f32),
            sem((2,)),
            pltpu.VMEM((2, width // 2, tokens), bf16),
            sem((2, 2)),
        ] + exchange_scratch(nb, size, f32),
        compiler_params=pltpu.CompilerParams(
            collective_id=1, has_side_effects=True, vmem_limit_bytes=67043328
        ),
        name="forward",
    )(
        hidden, gain, both, wstep, wshared, conv_values, conv_shared, bias, decay, skip, gate_gain,
        wout, hidden, cotangent,
    )


def order_rows(part, bits):
    order = list(range(bits))
    if part == 1:
        order[:3] = order[:3][::-1]
    if part == 2:
        order[:2] = order[:2][::-1]
    return order


def order_columns(part, bits):
    return [bit for bit in range(bits) if bit != part] + [part]


def slot_of(owner, order):
    slot = 0
    for bit in order:
        slot = slot * 2 + ((owner >> bit) & 1)
    return slot


class Reduction:
    def __init__(self, held, landing, order, index, sems, put, put_other=None):
        self.held, self.landing, self.order = held, landing, order
        self.index, self.sems, self.put, self.put_other = index, sems, put, put_other
        self.stages = len(order)

    def place(self, stage):
        base = 0
        size = 1 << self.stages
        for s, bit in enumerate(self.order[: stage + 1]):
            mine = (self.index // (1 << bit)) % 2
            half = size >> (s + 1)
            keep, give = base + mine * half, base + (1 - mine) * half
            base = keep
        return keep, give, half

    def copy(self, stage):
        _, give, half = self.place(stage)
        bit = self.order[stage]
        mine = (self.index // (1 << bit)) % 2
        return send_to(
            self.held.at[pl.ds(give, half)], self.landing[stage],
            self.sems.at[0, stage], self.sems.at[1, stage],
            seq=self.index + (1 - 2 * mine) * (1 << bit),
        )

    def start(self, stage):
        self.copy(stage).start()

    def start_piece(self, piece, pieces):
        _, give, half = self.place(0)
        count = half // pieces
        bit = self.order[0]
        mine = (self.index // (1 << bit)) % 2
        send_to(
            self.held.at[pl.ds(give + piece * count, count)],
            self.landing[0].at[pl.ds(piece * count, count)],
            self.sems.at[0, 0], self.sems.at[1, 0],
            seq=self.index + (1 - 2 * mine) * (1 << bit),
        ).start()

    def advance(self, stage):
        self.copy(stage).wait()
        keep, _, half = self.place(stage)
        if stage < self.stages - 1:

            @pl.loop(0, half)
            def _(i):
                total = self.held[keep + i].astype(f32) + self.landing[stage][i].astype(f32)
                self.held[keep + i] = total.astype(bf16)

            self.start(stage + 1)
        elif self.put_other is None:
            self.put(self.held[keep].astype(f32) + self.landing[stage][0].astype(f32))
        else:
            self.put(self.held[keep].astype(f32))
            self.put_other(self.landing[stage][0].astype(f32))


def sum_copy(acc, landing, bit, index, sems):
    mine = (index // (1 << bit)) % 2
    return pltpu.make_async_remote_copy(
        src_ref=acc.at[bit],
        dst_ref=landing.at[bit],
        send_sem=sems.at[0, bit],
        recv_sem=sems.at[1, bit],
        device_id={"seq": index + (1 - 2 * mine) * (1 << bit)},
        device_id_type=pl.DeviceIdType.MESH,
    )


def back_kernel(
    bits,
    gmt_ref, normedt_ref, near_ref, gw_ref, coef_ref, gains_ref, run_ref, step_ref, slope_ref,
    bc_ref, sext_ref, rows_ref, cs_ref, wshared_ref, wstep_ref, gain_ref,
    wout_ref, y_ref, gate_ref, ggain_ref, vext_ref, after_ref, in_ref, cv_ref, runt_ref,
    stept_ref, wi_ref,
    hid_ref, cot_ref, scale_ref,
    gout_ref, ginner_ref, gsmall_ref, ghid_ref, sums_ref,
    w_out, w_gate, w_values, w_small,
    land_out, land_gate, land_values, land_small,
    rs_sems, near, near_sems,
    own_cols, other_cols, land_cols, cols_sems,
    gv, acc_send, acc_land, acc_sems,
    edge_own, edge_tail, edge_land, edge_sems,
    dbc, dbc_land, dbc_sems, small, sedge_own, sedge_land, sedge_sems,
    vec, vec_land, vec_sems,
    scores, scorest, ct, dscores, end_w, ends, dcols, xdu, dyc, xdus, vwide, gext,
    dys, ggates, term_gate, ex_own, ex_landing, ex_mixed, ex_result, ex_sems,
):
    step_id = pl.program_id(0)
    index = lax.axis_index("seq")
    core = lax.axis_index("head")
    size = 1 << bits
    tokens = y_ref.shape[0]
    chunks = tokens // CHUNK
    nb = ggates.shape[0]
    half_nb = nb // 2
    width = normedt_ref.shape[0]
    half_width = width // 2
    rows_own = width // size
    t_scan, t_grad, t_final = nb, 2 * nb, 3 * nb
    after_id = lax.rem(index + 1, size)
    before_id = lax.rem(index + size - 1, size)
    bit_of = lambda bit: (index // (1 << bit)) % 2
    flip_of = lambda bit: index + (1 - 2 * bit_of(bit)) * (1 << bit)

    def out_reduction(part):
        cols = w_out.shape[3]

        def put(value):
            gout_ref[:, part * cols : (part + 1) * cols] = value

        return Reduction(
            w_out.at[part], [ref.at[part] for ref in land_out], order_rows(part, bits), index,
            rs_sems.at[part], put,
        )

    def columns_reduction(g, part):
        held, landing = ((w_gate, land_gate), (w_values, land_values))[g]

        def put_half(half):
            def put(value):
                for b in range(half_nb):
                    lane = (part * half_nb + b) * BLOCK + half * LANES
                    place = pl.ds(pl.multiple_of(lane, LANES), LANES)
                    ginner_ref[g, :, place] = value[:, b * LANES : (b + 1) * LANES]

            return put

        return Reduction(
            held.at[part], [ref.at[part] for ref in landing], order_columns(part, bits), index,
            rs_sems.at[2 + 2 * g + part], put_half(bit_of(part)), put_half(1 - bit_of(part)),
        )

    def put_small(value):
        gsmall_ref[...] = value

    rs_out = [out_reduction(part) for part in range(2)]
    rs_gate = [columns_reduction(0, part) for part in range(2)]
    rs_values = [columns_reduction(1, part) for part in range(2)]
    rs_small = Reduction(
        w_small, list(land_small), order_rows(2, bits), index, rs_sems.at[6], put_small
    )

    def when_after(step):
        return pl.when(step_id == step)

    exchange = StateExchange(
        index, size, True, ex_own, ex_landing, ex_mixed, ex_result, ex_sems, gains_ref
    )

    def near_copies(bit):
        half = pl.ds(pl.multiple_of(core * half_width, half_width), half_width)
        return (
            pltpu.make_async_copy(near_ref.at[bit], near.at[bit, half], near_sems.at[0, bit]),
            send_to(
                near_ref.at[bit], near.at[bit, half], near_sems.at[1, bit], near_sems.at[2, bit],
                head=1 - core,
            ),
        )

    @pl.when(step_id == 0)
    def _():
        greet_all(index, core, size)
        for c in range(chunks):
            rows = slice(c * CHUNK, (c + 1) * CHUNK)
            ct[:, rows] = transposed(bc_ref[rows, STATE:])
            for b in range(width // LANES):
                acc_send[c, :, b * LANES : (b + 1) * LANES] = transposed(
                    gmt_ref[b * LANES : (b + 1) * LANES, rows]
                )
        await_all(size)
        for bit in range(2):
            for copy in near_copies(bit):
                copy.start()

    group = width // 4
    owners = size // 4

    def scatter(piece, q, order, store):
        for b in range(owners):
            store(slot_of(q * owners + b, order), piece[b * rows_own : (b + 1) * rows_own, :])

    def put_out(part):
        cols = w_out.shape[3]
        for q in range(4):
            left = gmt_ref[q * group : (q + 1) * group, :]
            piece = mm(left, gw_ref[:, part * cols : (part + 1) * cols]).astype(bf16)

            def store(slot, value):
                w_out[part, slot] = value

            scatter(piece, q, order_rows(part, bits), store)

    def columns_copy(g, part):
        return send_to(
            other_cols.at[g, part], land_cols.at[g, part], cols_sems.at[0, g, part],
            cols_sems.at[1, g, part], seq=flip_of(part),
        )

    def split_block(g, j, value):
        part = j // half_nb
        mine = jnp.where(part == 0, bit_of(0), bit_of(1))
        place = j % half_nb
        first, second = value[:, :LANES], value[:, LANES:]
        own_cols[g, part, place] = jnp.where(mine == 0, first, second)
        other_cols[g, part, place] = jnp.where(mine == 0, second, first)
        partner = flip_of(0) + part * (flip_of(1) - flip_of(0))
        send_to(
            other_cols.at[g, part, place], land_cols.at[g, part, place],
            cols_sems.at[0, g, part], cols_sems.at[1, g, part], seq=partner,
        ).start()

    def put_columns(g, part):
        columns_copy(g, part).wait()
        side = lambda ref: jnp.concatenate([ref[g, part, b] for b in range(half_nb)], axis=1)
        right = jnp.concatenate([side(own_cols), side(land_cols)], axis=0)
        held = (w_gate, w_values)[g]
        for q in range(4):
            rows = slice(q * group, (q + 1) * group)
            piece = mm(
                jnp.concatenate([normedt_ref[rows, :], near[part, rows, :]], axis=1),
                right,
            )

            def store(slot, value):
                held[part, slot] = value

            scatter(piece.astype(bf16), q, order_columns(part, bits), store)
        (rs_gate, rs_values)[g][part].start(0)

    @pl.when(step_id < t_scan)
    def _():
        j = step_id
        offsets = offsets_of(run_ref, chunks)
        own = jnp.zeros((STATE, BLOCK), f32)
        term = jnp.zeros((1, BLOCK), f32)
        for c in range(chunks):
            rows = slice(c * CHUNK, (c + 1) * CHUNK)
            ggw = mm(acc_send[c], wout_ref[...])
            y = y_ref[rows, :]
            gate = gate_ref[rows, :]
            sig = 1.0 / (1.0 + jnp.exp(-gate))
            act = gate * sig
            out = y * act
            term = term + jnp.sum(ggw * out, axis=0, keepdims=True)
            coef = jnp.concatenate([coef_ref[rows, 0:LANES]] * (BLOCK // LANES), axis=1)
            gg = ggw * ggain_ref[...] - coef * out
            dy = gg * act
            dys[j, rows, :] = dy
            ggate = (gg * y * (sig * (1.0 + gate * (1.0 - sig)))).astype(bf16)
            ggates[j, rows, :] = ggate
            grow = rolled(jnp.exp(run_ref[rows, :] + offsets[c]), j)[:, :BLOCK_HEADS]
            own = own + mm(ct[:, rows], (dy * widen(grow)).astype(bf16))
        term_gate[j, 0:1, :] = term
        exchange.send(j, own)
        split_block(0, j, ggates[j])

    for part in range(2):

        @when_after(part)
        def _(part=part):
            put_out(part)

    pieces = size // 2

    @pl.when((step_id >= 1) & (step_id < nb))
    def _():
        for reduction in rs_out:
            reduction.start_piece(step_id - 1, pieces)

    rest = pieces - (nb - 1)

    @when_after(nb)
    def _():
        for piece in range(nb - 1, nb - 1 + (rest + 1) // 2):
            for reduction in rs_out:
                reduction.start_piece(piece, pieces)

    @when_after(nb + 1)
    def _():
        for piece in range(nb - 1 + (rest + 1) // 2, pieces):
            for reduction in rs_out:
                reduction.start_piece(piece, pieces)

    @pl.when((step_id >= 2) & (step_id < nb + 2))
    def _():
        exchange.turn(step_id - 2)

    @when_after(nb - 1)
    def _():
        for bit in range(2):
            for copy in near_copies(bit):
                copy.wait()
        put_columns(0, 0)

    mask = causal()
    rows_i = lax.broadcasted_iota(jnp.int32, (CHUNK, CHUNK), 0)
    cols_i = lax.broadcasted_iota(jnp.int32, (CHUNK, CHUNK), 1)
    mask_t = rows_i <= cols_i

    @pl.when(step_id == t_scan)
    def _():
        dbc[...] = jnp.zeros_like(dbc)
        dscores[...] = jnp.zeros_like(dscores)
        dcols[...] = jnp.zeros_like(dcols)
        xdu[...] = jnp.zeros_like(xdu)
        dyc[...] = jnp.zeros_like(dyc)
        xdus[...] = jnp.zeros_like(xdus)
        ends[...] = jnp.zeros_like(ends)
        vec[...] = jnp.zeros_like(vec)
        for c in range(chunks):
            rows = slice(c * CHUNK, (c + 1) * CHUNK)
            b_rows = bc_ref[rows, :STATE]
            c_rows = bc_ref[rows, STATE:]
            scores[c] = mm(c_rows, b_rows, NT)
            scorest[c] = mm(b_rows, c_rows, NT)
            run = run_ref[rows, :]
            end_w[rows, :] = jnp.exp(run[CHUNK - 1 :, :] - run)

    @pl.when((step_id >= t_scan) & (step_id < t_grad))
    def _():
        j = step_id - t_scan
        offsets = offsets_of(run_ref, chunks)
        vwide[...] = vext_ref[...].astype(f32)
        taps = [jnp.zeros((1, BLOCK), f32)] * (CONV + 1)
        run_cols = rolled(run_ref[...], j)
        step_cols = rolled(step_ref[...], j)
        end_cols = rolled(end_w[...], j)
        skip = widen(rolled(rows_ref[2:3, :], j)[:, :BLOCK_HEADS])
        channel = lax.broadcasted_iota(jnp.int32, (BLOCK, LANES), 0) // HEAD_DIM
        lane = lax.broadcasted_iota(jnp.int32, (BLOCK, LANES), 1)
        pick = (lane == BLOCK_HEADS * j + channel).astype(bf16)
        lane_row = lax.broadcasted_iota(jnp.int32, (CHUNK, LANES), 1)
        dstate = exchange.take(j)
        dskip = jnp.zeros((1, BLOCK), f32)
        gext[tokens : tokens + 8, :] = jnp.zeros((8, BLOCK), f32)
        for c in reversed(range(chunks)):
            rows = slice(c * CHUNK, (c + 1) * CHUNK)
            cols = run_cols[rows, :BLOCK_HEADS]
            conv = conv_rows(vwide, cv_ref[...], HALO - CONV + 1 + c * CHUNK, CHUNK)
            sig = 1.0 / (1.0 + jnp.exp(-conv))
            x = (conv * sig).astype(bf16)
            slope = sig * (1.0 + conv * (1.0 - sig))
            wide_x = x.astype(f32)
            dy = dys[j, rows, :]
            b_rows = bc_ref[rows, :STATE]
            c_rows = bc_ref[rows, STATE:]
            grow = widen(jnp.exp(cols))
            tail = widen(end_cols[rows, :BLOCK_HEADS])
            step_w = widen(step_cols[rows, :BLOCK_HEADS])
            last = grow[CHUNK - 1 :, :]
            base = rolled(jnp.exp(offsets[c]), j)[:, :BLOCK_HEADS]
            enter = widen(base) * in_ref[...]
            if c:
                enter = enter + after_ref[c - 1]
            du_state = tail * mm(b_rows, dstate.astype(bf16))
            carried = grow * mm(c_rows, enter.astype(bf16))
            weighted = wide_x * (tail * step_w)
            grown = dy * grow
            dbc[0, rows, :] += mm_both(weighted, dstate, NT)
            dbc[1, rows, :] += mm_both(grown, enter, NT)
            hold = last * jnp.sum(dstate * enter, axis=0, keepdims=True)
            dstate = last * dstate + mm_right(ct[:, rows], grown)
            du_pairs = []
            col_sum = jnp.zeros((CHUNK, LANES), f32)
            dscore = dscores[c]
            for pair in range(BLOCK // LANES):
                lanes = slice(pair * LANES, (pair + 1) * LANES)
                low, high = stack_pair(dy[:, lanes])
                both = jnp.concatenate([low, high], axis=0)
                dmat = mm_left(both, x[:, lanes], NT)
                mats = []
                for k in range(2):
                    head = 2 * pair + k
                    col = cols[:, head : head + 1]
                    row = runt_ref[0, head : head + 1, rows]
                    keep = jnp.exp(jnp.where(mask, col - row, -1e30))
                    piece = dmat[k * CHUNK : (k + 1) * CHUNK, :] * keep
                    piece = piece * stept_ref[0, head : head + 1, rows]
                    dscore = dscore + piece
                    full = piece * scores[c]
                    col_sum = jnp.where(
                        lane_row == BLOCK_HEADS * j + head,
                        jnp.sum(full, axis=1, keepdims=True),
                        col_sum,
                    )
                    dcols[j, head : head + 1, rows] = jnp.sum(full, axis=0, keepdims=True)
                    keep_t = jnp.exp(jnp.where(mask_t, row - col, -1e30))
                    mats.append(scorest[c] * keep_t)
                du_pairs.append(
                    mm(jnp.concatenate(mats, axis=1).astype(bf16), both.astype(bf16))
                )
            dscores[c] = dscore
            du = jnp.concatenate(du_pairs, axis=1) + du_state
            by_head = mm(
                jnp.concatenate(
                    [
                        (wide_x * du).astype(bf16),
                        (dy * carried).astype(bf16),
                        (wide_x * du_state).astype(bf16),
                        *parts(jnp.broadcast_to(hold, (HALO, BLOCK))),
                    ],
                    axis=0,
                ),
                pick,
            )
            xdu[rows, :] += by_head[0:CHUNK, :]
            dyc[rows, :] += by_head[CHUNK : 2 * CHUNK, :] + col_sum
            xdus[rows, :] += by_head[2 * CHUNK : 3 * CHUNK, :]
            end = 3 * CHUNK
            ends[c : c + 1, :] += (
                by_head[end : end + 1, :] + by_head[end + HALO : end + HALO + 1, :]
            )
            dskip = dskip + jnp.sum(dy * wide_x, axis=0, keepdims=True)
            gconv = (step_w * du + skip * dy) * slope
            gext[rows, :] = gconv
            taps[CONV] = taps[CONV] + jnp.sum(gconv, axis=0, keepdims=True)
            values = vwide[HALO + c * CHUNK : HALO + (c + 1) * CHUNK, :]
            total = cv_ref[CONV - 1 : CONV, :] * gconv
            taps[CONV - 1] = taps[CONV - 1] + jnp.sum(values * gconv, axis=0, keepdims=True)
            for k in range(CONV - 1):
                ahead = c * CHUNK + CONV - 1 - k
                moved = gext[ahead : ahead + CHUNK, :]
                total = total + cv_ref[k : k + 1, :] * moved
                taps[k] = taps[k] + jnp.sum(values * moved, axis=0, keepdims=True)
            gv[j, rows, :] = total.astype(bf16)
            if c == chunks - 1:
                edge_tail[j, 0:8, :] = total[CHUNK - 8 :, :]
        row8 = lax.broadcasted_iota(jnp.int32, (8, BLOCK), 0)
        ahead_rows = vwide[HALO - CONV + 1 : HALO - CONV + 9, :]
        for k in range(CONV):
            tap = taps[k]
            if k < CONV - 1:
                moved = pltpu.roll(gext[0:8, :], k, 0) if k else gext[0:8, :]
                inside = (row8 >= k) & (row8 < CONV - 1)
                tap = tap + jnp.sum(
                    jnp.where(inside, ahead_rows * moved, 0.0), axis=0, keepdims=True
                )
            vec[0, j, k : k + 1, :] = tap
        vec[0, j, CONV : CONV + 1, :] = taps[CONV]
        vec[0, j, CONV + 1 : CONV + 2, :] = term_gate[j, 0:1, :]
        by_head = mm(jnp.concatenate(parts(jnp.broadcast_to(dskip, (HALO, BLOCK))), axis=0), pick)
        vec[0, nb, 7:8, 0:LANES] += by_head[0:1, :] + by_head[HALO : HALO + 1, :]
        edge_tail[j, 8 : 8 + CONV + 1, :] = cv_ref[...]
        edge_own[j] = gext[0:8, :]
        send_to(
            edge_own.at[j], edge_land.at[j], edge_sems.at[0, j], edge_sems.at[1, j], seq=before_id
        ).start()

    def finish_block(j):
        send_to(
            edge_own.at[j], edge_land.at[j], edge_sems.at[0, j], edge_sems.at[1, j], seq=before_id
        ).wait()
        nxt = jnp.where(index == size - 1, 0.0, 1.0) * edge_land[j]
        row8 = lax.broadcasted_iota(jnp.int32, (8, BLOCK), 0)
        fix = edge_tail[j, 0:8, :]
        for k in range(CONV - 1):
            ahead = CONV - 1 - k
            moved = pltpu.roll(nxt, 8 - ahead, 0)
            fix = fix + jnp.where(row8 >= 8 - ahead, edge_tail[j, 8 + k : 9 + k, :] * moved, 0.0)
        both_rows = jnp.concatenate([gv[j, tokens - 16 : tokens - 8, :].astype(f32), fix], axis=0)
        gv[j, tokens - 16 :, :] = both_rows.astype(bf16)
        split_block(1, j, gv[j])

    @pl.when((step_id > t_scan + 1) & (step_id < t_grad))
    def _():
        finish_block(step_id - t_scan - 2)

    @when_after(t_scan + 1)
    def _():
        put_columns(0, 1)

    @when_after(t_scan + 2)
    def _():
        rs_gate[0].advance(0)
        rs_out[0].advance(0)
        rs_out[1].advance(0)

    @when_after(t_scan + half_nb + 1)
    def _():
        rs_gate[0].advance(1)
        rs_gate[1].advance(0)

    @when_after(t_grad - 1)
    def _():
        rs_out[0].advance(1)

    @when_after(t_grad - 1)
    def _():
        tri = mask.astype(f32)
        tri_t = mask_t.astype(f32)
        strict = (rows_i > cols_i).astype(f32)
        decay = jnp.exp(rows_ref[1:2, :])
        bias_sum = jnp.zeros((1, LANES), f32)
        decay_sum = jnp.zeros((1, LANES), f32)
        for c in range(chunks):
            rows = slice(c * CHUNK, (c + 1) * CHUNK)
            step = step_ref[rows, :]
            col_rows = [dcols[b, 0:BLOCK_HEADS, rows] for b in range(nb)]
            rest = LANES - BLOCK_HEADS * nb
            col_rows.append(jnp.zeros((rest, CHUNK), f32))
            dlog = dyc[rows, :] - jnp.concatenate(col_rows, axis=0).T
            drate = (
                mm_exact(tri_t, dlog)
                + mm_exact(strict, xdus[rows, :] * step)
                + ends[c : c + 1, :]
            )
            dstep = xdu[rows, :] - decay * drate
            draw = dstep * slope_ref[rows, :]
            small[rows, LANES:] = draw.astype(bf16)
            bias_sum = bias_sum + jnp.sum(draw, axis=0, keepdims=True)
            decay_sum = decay_sum - jnp.sum(drate * step, axis=0, keepdims=True) * decay
            b_rows = bc_ref[rows, :STATE]
            c_rows = bc_ref[rows, STATE:]
            high, low = parts(dscores[c])
            dbc[1, rows, :] += mm(high, b_rows) + mm(low, b_rows)
            dbc[0, rows, :] += mm(high, c_rows, TN) + mm(low, c_rows, TN)
        vec[0, nb, 0:1, 0:LANES] = bias_sum
        vec[0, nb, 1:2, 0:LANES] = decay_sum
        send_to(
            dbc.at[1 - core], dbc_land, dbc_sems.at[0], dbc_sems.at[1], head=1 - core
        ).start()

    @when_after(t_grad)
    def _():
        finish_block(nb - 2)
        finish_block(nb - 1)
        put_columns(1, 0)
        rs_gate[0].advance(2)
        rs_gate[1].advance(1)
        rs_out[1].advance(1)

    @when_after(t_grad + 1)
    def _():
        rs_gate[0].advance(3)

    @when_after(t_grad)
    def _():
        send_to(
            dbc.at[1 - core], dbc_land, dbc_sems.at[0], dbc_sems.at[1], head=1 - core
        ).wait()
        sext = sext_ref[core].astype(f32)
        taps = cs_ref[core]
        conv = conv_rows(sext, taps, HALO - CONV + 1, tokens)
        gs = (dbc[core] + dbc_land[...]) * silu_grad(conv)
        for k in range(CONV):
            first = HALO - CONV + 1 + k
            vec[0, nb, 2 + k : 3 + k, 0:LANES] = jnp.sum(
                sext[first : first + tokens, :] * gs, axis=0, keepdims=True
            )
        vec[0, nb, 2 + CONV : 3 + CONV, 0:LANES] = jnp.sum(gs, axis=0, keepdims=True)
        dbc[core] = gs
        sedge_own[...] = gs[0:8, :]
        send_to(
            sedge_own, sedge_land, sedge_sems.at[0], sedge_sems.at[1], seq=before_id
        ).start()

    @when_after(t_grad + 1)
    def _():
        send_to(
            sedge_own, sedge_land, sedge_sems.at[0], sedge_sems.at[1], seq=before_id
        ).wait()
        taps = cs_ref[core]
        nxt = jnp.where(index == size - 1, 0.0, 1.0) * sedge_land[...]
        gs = jnp.concatenate([dbc[core], nxt], axis=0)
        total = taps[CONV - 1 : CONV, :] * gs[0:tokens, :]
        for k in range(CONV - 1):
            total = total + taps[k : k + 1, :] * gs[CONV - 1 - k : CONV - 1 - k + tokens, :]
        small[:, 0:LANES] = total.astype(bf16)
        for q in range(4):
            piece = mm(normedt_ref[q * group : (q + 1) * group, :], small[...]).astype(bf16)

            def store(slot, value):
                w_small[slot] = value

            scatter(piece, q, order_rows(2, bits), store)
        rs_small.start(0)

    @pl.when((step_id >= t_grad) & (step_id < t_final))
    def _():
        j = step_id - t_grad
        part = mm(
            jnp.concatenate([ggates[j], gv[j]], axis=1),
            jnp.concatenate([wi_ref[0], wi_ref[1]], axis=1),
            NT,
        )

        @pl.when(j == 0)
        def _():
            for b in range(width // BLOCK):
                dys[b] = part[:, b * BLOCK : (b + 1) * BLOCK]

        @pl.when(j > 0)
        def _():
            for b in range(width // BLOCK):
                dys[b] += part[:, b * BLOCK : (b + 1) * BLOCK]

    @when_after(t_grad + 2)
    def _():
        rs_out[0].advance(2)

    @when_after(t_grad + 2)
    def _():
        put_columns(1, 1)

    @when_after(t_grad + 3)
    def _():
        rs_out[1].advance(2)

    @when_after(t_grad + 4)
    def _():
        rs_gate[1].advance(2)
        own = pl.ds(pl.multiple_of(core * LANES, LANES), LANES)
        heads = wstep_ref.shape[1]
        rest = mm(small[:, 0:LANES], wshared_ref[:, own], NT) + mm(
            small[:, LANES : LANES + heads], wstep_ref[...], NT
        )
        for b in range(width // BLOCK):
            dys[b] += rest[:, b * BLOCK : (b + 1) * BLOCK]

    @when_after(t_final - 1)
    def _():
        for c in range(chunks):
            rows = slice(c * CHUNK, (c + 1) * CHUNK)
            for b in range(width // BLOCK):
                acc_send[c, :, b * BLOCK : (b + 1) * BLOCK] = dys[b, rows, :].astype(bf16)
            send_to(
                acc_send.at[c], acc_land.at[c], acc_sems.at[0, c], acc_sems.at[1, c], head=1 - core
            ).start()

    @pl.when(step_id >= t_final)
    def _():
        c = step_id - t_final
        send_to(
            acc_send.at[c], acc_land.at[c], acc_sems.at[0, c], acc_sems.at[1, c], head=1 - core
        ).wait()
        here = pl.ds(pl.multiple_of(c * CHUNK, CHUNK), CHUNK)
        own_total = jnp.concatenate([dys[b, here, :] for b in range(width // BLOCK)], axis=1)
        total = own_total + acc_land[c].astype(f32)
        scale = scale_ref[:, 0:1]
        hat = hid_ref[...].astype(f32) * scale
        term = jnp.sum(total * hat, axis=0, keepdims=True)

        for b in range(width // BLOCK):
            piece = term[:, b * BLOCK : (b + 1) * BLOCK]
            vec[0, b, 7:8, :] = vec[0, b, 7:8, :] + piece

        ghat = total * gain_ref[...][None, :]
        mean = jnp.mean(ghat * hat, axis=1, keepdims=True)
        ghid_ref[...] = cot_ref[...].astype(f32) + scale * (ghat - hat * mean)

    @when_after(t_final)
    def _():
        rs_out[0].advance(3)

    @when_after(t_final - 1)
    def _():
        rs_values[0].advance(0)

    @when_after(t_final + 1)
    def _():
        rs_values[0].advance(1)

    @when_after(t_final + 2)
    def _():
        rs_values[1].advance(0)

    @when_after(t_final + chunks - 1)
    def _():
        rs_out[1].advance(3)

        def begin(bit):
            sum_copy(vec, vec_land, bit, index, vec_sems).start()

        def add(bit):
            sum_copy(vec, vec_land, bit, index, vec_sems).wait()
            vec[bit + 1] = vec[bit] + vec_land[bit]
            if bit + 1 < bits:
                begin(bit + 1)

        begin(0)
        add(0)
        rs_small.advance(0)
        rs_gate[1].advance(3)
        add(1)
        rs_small.advance(1)
        rs_values[1].advance(1)
        add(2)
        rs_values[0].advance(2)
        rs_small.advance(2)
        rs_values[0].advance(3)
        rs_values[1].advance(2)
        add(3)
        rs_values[1].advance(3)
        rs_small.advance(3)
        for stage in range(4, bits):
            for reduction in rs_out + rs_gate + rs_values + [rs_small]:
                reduction.advance(stage)
            add(stage)
        sums_ref[8:16, 0:BLOCK] = vec[bits, nb]
        for b in range(nb):
            sums_ref[0:8, b * BLOCK : (b + 1) * BLOCK] = vec[bits, b]


def back_call(
    gm_t, normed_t, near, gated_w, coef, gains, run, step, slope, bc, sext, rows,
    conv_shared, wshared, wstep, gain, wout, y, gate, gate_gain, vext, after, state_in, conv_values, runt, stept, both,
    hidden, cotangent, scale,
):
    width, tokens = normed_t.shape
    inner = y.shape[1]
    chunks = tokens // CHUNK
    nb = inner // BLOCK
    size = lax.axis_size("seq")
    bits = size.bit_length() - 1
    rows_own = width // size
    t_scan, t_grad, t_final = nb, 2 * nb, 3 * nb

    def column(start):
        return lambda s: jnp.clip(s - start, 0, nb - 1)

    def full(shape):
        return pl.BlockSpec(shape, lambda s: (0,) * len(shape), pipeline_mode=pl.Buffered(1))

    def cols(rows, start):
        at = column(start)
        return pl.BlockSpec((rows, BLOCK), lambda s: (0, at(s)))

    row_block = lambda w: pl.BlockSpec((CHUNK, w), lambda s: (jnp.clip(s - t_final, 0, chunks - 1), 0))
    row_single = lambda w: pl.BlockSpec(
        (CHUNK, w),
        lambda s: (jnp.clip(s - t_final, 0, chunks - 1), 0),
        pipeline_mode=pl.Buffered(1),
    )
    held = lambda cols: pltpu.VMEM((2, size, rows_own, cols), bf16)
    landing = lambda cols: tuple(
        pltpu.VMEM((2, size >> (s + 1), rows_own, cols), bf16) for s in range(bits)
    )
    columns = lambda: pltpu.VMEM((2, 2, nb // 2, tokens, LANES), bf16)
    sem = pltpu.SemaphoreType.DMA
    return pl.pallas_call(
        functools.partial(back_kernel, bits),
        grid=(3 * nb + chunks,),
        in_specs=[
            full((width, tokens)),
            full((width, tokens)),
            pl.BlockSpec(memory_space=pl.ANY),
            full((tokens, inner)),
            full((tokens, LANES)),
            full((size, LANES)),
            full((tokens, LANES)),
            full((tokens, LANES)),
            full((tokens, LANES)),
            full((tokens, 2 * STATE)),
            full((2, HALO + tokens, LANES)),
            full((8, LANES)),
            full((2, CONV + 1, LANES)),
            full((width, 2 * LANES)),
            full(wstep.shape),
            full((width,)),
            cols(width, 0),
            cols(tokens, 0),
            cols(tokens, 0),
            cols(1, 0),
            pl.BlockSpec(
                (HALO + tokens, BLOCK), lambda s: (0, column(t_scan)(s)), pipeline_mode=pl.Buffered(1)
            ),
            pl.BlockSpec((chunks, STATE, BLOCK), lambda s: (0, 0, column(t_scan)(s))),
            cols(STATE, t_scan),
            cols(CONV + 1, t_scan),
            pl.BlockSpec((1, 8, tokens), lambda s: (column(t_scan)(s), 0, 0)),
            pl.BlockSpec((1, 8, tokens), lambda s: (column(t_scan)(s), 0, 0)),
            pl.BlockSpec(
                (2, width, BLOCK), lambda s: (0, 0, column(t_grad)(s)), pipeline_mode=pl.Buffered(1)
            ),
            row_single(width),
            row_single(width),
            row_block(LANES),
        ],
        out_shape=[
            jax.ShapeDtypeStruct((rows_own, inner), f32),
            jax.ShapeDtypeStruct((2, rows_own, inner), f32),
            jax.ShapeDtypeStruct((rows_own, 2 * LANES), f32),
            jax.ShapeDtypeStruct((tokens, width), f32),
            jax.ShapeDtypeStruct((16, inner), f32),
        ],
        out_specs=[
            full((rows_own, inner)),
            full((2, rows_own, inner)),
            full((rows_own, 2 * LANES)),
            row_block(width),
            pl.BlockSpec((16, inner), lambda s: (0, 0)),
        ],
        scratch_shapes=[
            held(inner // 2), held(inner // 4), held(inner // 4),
            pltpu.VMEM((size, rows_own, 2 * LANES), bf16),
            landing(inner // 2), landing(inner // 4), landing(inner // 4),
            tuple(pltpu.VMEM((size >> (s + 1), rows_own, 2 * LANES), bf16) for s in range(bits)),
            sem((7, 2, bits)),
            pltpu.VMEM((2, width, tokens), bf16), sem((3, 2)),
            columns(), columns(), columns(), sem((2, 2, 2)),
            pltpu.VMEM((nb, tokens, BLOCK), bf16),
            pltpu.VMEM((chunks, CHUNK, width), bf16),
            pltpu.VMEM((chunks, CHUNK, width), bf16),
            sem((2, chunks)),
            pltpu.VMEM((nb, 8, BLOCK), f32),
            pltpu.VMEM((nb, 16, BLOCK), f32),
            pltpu.VMEM((nb, 8, BLOCK), f32),
            sem((2, nb)),
            pltpu.VMEM((2, tokens, LANES), f32),
            pltpu.VMEM((tokens, LANES), f32),
            sem((2,)),
            pltpu.VMEM((tokens, 2 * LANES), bf16),
            pltpu.VMEM((8, LANES), f32),
            pltpu.VMEM((8, LANES), f32),
            sem((2,)),
            pltpu.VMEM((bits + 1, nb + 1, 8, BLOCK), f32),
            pltpu.VMEM((bits, nb + 1, 8, BLOCK), f32),
            sem((2, bits)),
            pltpu.VMEM((chunks, CHUNK, CHUNK), f32),
            pltpu.VMEM((chunks, CHUNK, CHUNK), f32),
            pltpu.VMEM((STATE, tokens), bf16),
            pltpu.VMEM((chunks, CHUNK, CHUNK), f32),
            pltpu.VMEM((tokens, LANES), f32),
            pltpu.VMEM((8, LANES), f32),
            pltpu.VMEM((nb, 8, tokens), f32),
            pltpu.VMEM((tokens, LANES), f32),
            pltpu.VMEM((tokens, LANES), f32),
            pltpu.VMEM((tokens, LANES), f32),
            pltpu.VMEM((HALO + tokens, BLOCK), f32),
            pltpu.VMEM((tokens + 8, BLOCK), f32),
            pltpu.VMEM((nb, tokens, BLOCK), f32),
            pltpu.VMEM((nb, tokens, BLOCK), bf16),
            pltpu.VMEM((nb, 8, BLOCK), f32),
        ] + exchange_scratch(nb, size, bf16),
        compiler_params=pltpu.CompilerParams(
            collective_id=3, has_side_effects=True, vmem_limit_bytes=67043328
        ),
        name="back",
    )(
        gm_t, normed_t, near, gated_w, coef, gains, run, step, slope, bc, sext, rows,
        conv_shared, wshared, wstep, gain, wout, y, gate, gate_gain, vext, after, state_in,
        conv_values,
        runt, stept,
        both, hidden, cotangent, scale,
    )


def final_kernel(
    heads, out_ref, ghid_ref, gout_ref, ginner_ref, gsmall_ref, sums_ref,
    out_to, ghid_to, gout_to, inner_to, step_to, shared_to, norm_to, gate_to, taps_to, staps_to,
    bias_to, decay_to, skip_to,
):
    out_to[...] = out_ref[...]
    ghid_to[...] = ghid_ref[...]

    @pl.when(pl.program_id(0) == 0)
    def _():
        gout_to[...] = gout_ref[...]
        for g in range(2):
            inner_to[:, g, :] = ginner_ref[g]
        shared_to[...] = gsmall_ref[:, 0:LANES]
        step_to[...] = gsmall_ref[:, LANES : LANES + heads]
        taps_to[...] = sums_ref[0 : CONV + 1, :]
        gate_to[...] = sums_ref[CONV + 1, :]
        norm_to[...] = sums_ref[7, :]
        bias_to[...] = sums_ref[8, 0:heads]
        decay_to[...] = sums_ref[9, 0:heads]
        staps_to[...] = sums_ref[10 : 11 + CONV, 0:LANES]
        skip_to[...] = sums_ref[15, 0:heads]


def final_call(heads, block_out, grad_hidden, gout, ginner, gsmall, sums):
    tokens, width = block_out.shape
    rows_own, inner = gout.shape
    rows = 256
    shapes = [
        (tokens, width), (tokens, width), (rows_own, inner), (rows_own, 2, inner),
        (rows_own, heads), (rows_own, LANES), (width,), (inner,), (CONV + 1, inner),
        (CONV + 1, LANES), (heads,), (heads,), (heads,),
    ]

    def full(shape):
        return pl.BlockSpec(shape, lambda i: (0,) * len(shape), pipeline_mode=pl.Buffered(1))

    block = lambda: pl.BlockSpec((rows, width), lambda i: (i, 0))
    return pl.pallas_call(
        functools.partial(final_kernel, heads),
        grid=(tokens // rows,),
        in_specs=[block(), block()] + [full(a.shape) for a in (gout, ginner, gsmall, sums)],
        out_shape=[jax.ShapeDtypeStruct(shape, f32) for shape in shapes],
        out_specs=[block(), block()] + [full(shape) for shape in shapes[2:]],
        name="final",
    )(block_out, grad_hidden, gout, ginner, gsmall, sums)


def body(
    hidden, cotangent, norm_gain, proj_inner, proj_step, proj_shared, conv_values, conv_shared,
    step_bias, decay_log, skip_gain, gate_gain, proj_out,
):
    tokens = hidden.shape[0]
    inner = proj_inner.shape[2]
    heads = proj_step.shape[1]
    width = hidden.shape[1]
    size = lax.axis_size("seq")
    both = jnp.transpose(proj_inner, (1, 0, 2))
    (
        normed_t, norm_scale, gate_in, vext, after, y, gated_w, state_in, step, slope, run, runt,
        stept, sext, bc, gains, block_out, gm_t, coef, near,
        rows,
    ) = forward_call(
        hidden, cotangent, norm_gain, both, proj_step, proj_shared, conv_values, conv_shared,
        step_bias, decay_log, skip_gain, gate_gain[None, :], proj_out,
    )
    (gout, ginner, gsmall, grad_hidden, sums) = back_call(
        gm_t, normed_t, near, gated_w, coef, gains, run, step, slope, bc, sext, rows,
        conv_shared.reshape(CONV + 1, -1, LANES).transpose(1, 0, 2), proj_shared, proj_step,
        norm_gain, proj_out, y, gate_in, gate_gain[None, :], vext, after, state_in, conv_values,
        runt, stept, both, hidden, cotangent, norm_scale,
    )
    (
        block_out, grad_hidden, gout, ginner, gstep, gshared, gnorm, ggain, gtaps, gstaps, gbias,
        gdecay, gskip,
    ) = final_call(heads, block_out, grad_hidden, gout, ginner, gsmall, sums)
    return (
        block_out, grad_hidden, gnorm, ginner, gstep, gshared, gtaps, gstaps, gbias, gdecay, gskip,
        ggain, gout,
    )


def solution(mesh):
    return jax.shard_map(
        body,
        mesh=mesh,
        in_specs=(
            P("seq", None),
            P("seq", None),
            P(),
            P(None, None, "head"),
            P(None, "head"),
            P(),
            P(None, "head"),
            P(),
            P("head"),
            P("head"),
            P("head"),
            P("head"),
            P(None, "head"),
        ),
        out_specs=(
            P("seq", None),
            P("seq", None),
            P(),
            P("seq", None, "head"),
            P("seq", "head"),
            P("seq", "head"),
            P(None, "head"),
            P(None, "head"),
            P("head"),
            P("head"),
            P("head"),
            P("head"),
            P("seq", "head"),
        ),
        check_vma=False,
    )
```
